32 devices in a mesh: dp: 4 (over y, core), row: 2 (over x), col: 4 (over z).
Axes of the slice: x: 2, y: 2, z: 4, core: 2. Of those that a mesh axis runs over, the one named last changes fastest.
Arguments:
- block_input: bfloat16 [1536, 4096], P('row', ('dp', 'col')), may hold values from -6 to 6
- position_ids: int32 [4096], P(('dp', 'row')), may hold values from 0 to 2558, as said below
- attention_gain: float32 [1536], P('row'), may hold values from 0.5 to 1.5
- query_weight: bfloat16 [1536, 1536], P('row', 'col'), may hold values from -0.15625 to 0.15625
- query_bias: float32 [1536], P('col'), may hold values from -3 to 3
- key_value_weight: bfloat16 [1536, 512], P('row'), may hold values from -0.15625 to 0.15625
- key_value_bias: float32 [512], replicated, may hold values from -3 to 3
- output_weight: bfloat16 [1536, 1536], P('row', 'col'), may hold values from -0.5 to 0.5
- feedforward_gain: float32 [1536], P('row'), may hold values from 0.5 to 1.5
- gate_weight: bfloat16 [1536, 8960], P('row', 'col'), may hold values from -0.15625 to 0.15625
- upper_weight: bfloat16 [1536, 8960], P('row', 'col'), may hold values from -0.15625 to 0.15625
- down_weight: bfloat16 [1536, 8960], P('row', 'col'), may hold values from -0.0625 to 0.0625
- out_cotangent: bfloat16 [1536, 4096], P('row', ('dp', 'col')), may hold values from -6 to 6
Outputs:
- block_output: float32 [1536, 4096], P('row', ('dp', 'col'))
- input_grad: float32 [1536, 4096], P('row', ('dp', 'col'))
- attention_gain_grad: float32 [1536], P('row')
- query_weight_grad: float32 [1536, 1536], P(('row', 'dp'), 'col')
- query_bias_grad: float32 [1536], P(('col', 'dp'))
- keyval_weight_grad: float32 [1536, 512], P('row')
- key_value_bias_gradient: float32 [512], replicated
- output_weight_grad: float32 [1536, 1536], P(('row', 'dp'), 'col')
- feedforward_gain_grad: float32 [1536], P('row')
- gate_weight_grad: float32 [1536, 8960], P(('row', 'dp'), 'col')
- upper_weight_grad: float32 [1536, 8960], P(('row', 'dp'), 'col')
- down_weight_grad: float32 [1536, 8960], P(('row', 'dp'), 'col')
The draws below stay inside these ranges and needn't reach their ends.
Inputs may be any that keep to these rules, and one draw needn't show every extreme that they name: `position_ids`: within each sequence of 512 consecutive tokens the ids rise by 1 to 3 from one token to the next. The first sequence starts at 0; the last sequence's ids run from 1025 to 2558 in steps of 3.
All inputs are finite; a program needn't handle non-finite values.
Results may differ from the reference program's by a relative error of at most 0.035.
Values may be sent and summed in bfloat16 or wider, within the bound.
A program may use at most 320 MiB of HBM per device.

```python
import jax
import jax.numpy as jnp
from jax import lax

MODEL_WIDTH = 1536
QUERY_HEADS = 12
KEYVALUE_HEADS = 2
HEAD_SIZE = 128
FF = 8960
SEQUENCE_TOKENS = 512
TOKENS = 4096
N_COL = 4


def draw_position_ids(key, part):
    seq_count = TOKENS // SEQUENCE_TOKENS
    increments = jax.random.randint(key, (seq_count, SEQUENCE_TOKENS), 1, 4)
    starts = jax.random.randint(jax.random.fold_in(key, 7), (seq_count, 1), 0, 1024)
    increments = increments.at[0, 0].set(1)
    increments = increments.at[seq_count - 1].set(3)
    starts = starts.at[0, 0].set(0)
    starts = starts.at[seq_count - 1, 0].set(1023)
    return (starts + jnp.cumsum(increments, axis=1) - 1).reshape(TOKENS).astype(jnp.int32)


def level_of(stream_key, extent, split, low, largest):
    gain, own = 1.0, jax.random.fold_in(stream_key, 6)
    for dim, blocks in split:
        steps = jnp.exp(jax.random.uniform(jax.random.fold_in(own, dim), (blocks,), jnp.float32, low / len(split), largest / len(split)))
        gain = gain * jnp.repeat(steps, extent[dim] // blocks).reshape([-1 if axis == dim else 1 for axis in range(len(extent))])
    return gain


def scatter_about(rng, extent, scale, reach, shards=(), kind=jnp.bfloat16):
    result = scale * jax.random.normal(rng, extent, jnp.float32)
    if shards:
        result = result * level_of(rng, extent, shards, -0.22, 0.18)
    return jnp.clip(result, -reach, reach).astype(kind)


def setup_inputs(seed: int = 0) -> dict:
    splits = jax.random.split(jax.random.key(seed), 14)
    return {
        "block_input": scatter_about(splits[0], (MODEL_WIDTH, TOKENS), 1.0, 6.0, ((0, 2), (1, 16))),
        "position_ids": draw_position_ids(jax.random.fold_in(splits[13], 71), 0),
        "attention_gain": jnp.clip(1.0 + 0.1 * jax.random.normal(splits[2], (MODEL_WIDTH,), jnp.float32), 0.5, 1.5),
        "query_weight": scatter_about(splits[3], (MODEL_WIDTH, QUERY_HEADS * HEAD_SIZE), MODEL_WIDTH ** -0.5, 0.15625, ((0, 2), (1, 4))),
        "query_bias": scatter_about(splits[4], (QUERY_HEADS * HEAD_SIZE,), 0.5, 3.0, ((0, 4),), jnp.float32),
        "key_value_weight": scatter_about(splits[5], (MODEL_WIDTH, 2 * KEYVALUE_HEADS * HEAD_SIZE), MODEL_WIDTH ** -0.5, 0.15625, ((0, 2),)),
        "key_value_bias": scatter_about(splits[6], (2 * KEYVALUE_HEADS * HEAD_SIZE,), 0.5, 3.0, (), jnp.float32),
        "output_weight": scatter_about(splits[7], (MODEL_WIDTH, QUERY_HEADS * HEAD_SIZE), HEAD_SIZE ** -0.5, 0.5, ((0, 2), (1, 4))),
        "feedforward_gain": jnp.clip(1.0 + 0.1 * jax.random.normal(splits[8], (MODEL_WIDTH,), jnp.float32), 0.5, 1.5),
        "gate_weight": scatter_about(splits[9], (MODEL_WIDTH, FF), MODEL_WIDTH ** -0.5, 0.15625, ((0, 2), (1, 4))),
        "upper_weight": scatter_about(splits[10], (MODEL_WIDTH, FF), MODEL_WIDTH ** -0.5, 0.15625, ((0, 2), (1, 4))),
        "down_weight": scatter_about(splits[11], (MODEL_WIDTH, FF), FF ** -0.5, 0.0625, ((0, 2), (1, 4))),
        "out_cotangent": scatter_about(splits[12], (MODEL_WIDTH, TOKENS), 1.0, 6.0, ((0, 2), (1, 16))),
    }


EPS = 1e-06
THETA = 1000000.0
NEG = -1e+30

def rounded(values):
    return lax.optimization_barrier(values.astype(jnp.bfloat16)).astype(jnp.float32)

def rope_tables(position_ids):
    half_dim = HEAD_SIZE // 2
    frequencies = THETA ** (-(jnp.arange(half_dim, dtype=jnp.float32) * 2.0 / HEAD_SIZE))
    angles = position_ids.astype(jnp.float32)[:, None] * frequencies[None, :]
    cosine_values = jnp.cos(angles)
    sine_lookup = jnp.sin(angles)
    return (jnp.concatenate([cosine_values, cosine_values], -1), jnp.concatenate([sine_lookup, sine_lookup], -1))

def apply_rotation(values, cosine_values, sine_lookup):
    half_dim = HEAD_SIZE // 2
    turned = jnp.concatenate([-values[..., half_dim:], values[..., :half_dim]], -1)
    return values * cosine_values[:, None, :] + turned * sine_lookup[:, None, :]

def unrotate(gradient, cosine_values, sine_lookup):
    half_dim = HEAD_SIZE // 2
    scaled = gradient * sine_lookup[:, None, :]
    turned = jnp.concatenate([scaled[..., half_dim:], -scaled[..., :half_dim]], -1)
    return gradient * cosine_values[:, None, :] + turned

def causal_scores(query_rot, key_expand):
    scores = jnp.einsum('ihd,jhd->hij', query_rot, key_expand) * HEAD_SIZE ** (-0.5)
    length = query_rot.shape[0]
    allowed = jnp.arange(length)[:, None] >= jnp.arange(length)[None, :]
    return jnp.where(allowed[None], scores, NEG)

def reference(block_input, position_ids, attention_gain, query_weight, query_bias, key_value_weight, key_value_bias, output_weight, feedforward_gain, gate_weight, upper_weight, down_weight, out_cotangent):
    single_float_type = jnp.float32
    brain_float_type = jnp.bfloat16
    query_group_width = QUERY_HEADS // KEYVALUE_HEADS
    per_block = QUERY_HEADS // N_COL
    key_value_width = KEYVALUE_HEADS * HEAD_SIZE
    scale = HEAD_SIZE ** (-0.5)
    inputs_rows = block_input.T
    cotangent_rows = out_cotangent.T
    out_proj = output_weight.T
    down_proj = down_weight.T
    holder_list = jnp.arange(N_COL) * per_block // query_group_width
    holder_lookup = (holder_list[:, None] == jnp.arange(KEYVALUE_HEADS)[None, :]).astype(single_float_type)
    key_block_list = jnp.einsum('lwn,qw->lqn', key_value_weight[:, :key_value_width].astype(single_float_type).reshape(MODEL_WIDTH, KEYVALUE_HEADS, HEAD_SIZE), holder_lookup)
    value_block_list = jnp.einsum('lwn,qw->lqn', key_value_weight[:, key_value_width:].astype(single_float_type).reshape(MODEL_WIDTH, KEYVALUE_HEADS, HEAD_SIZE), holder_lookup)
    num_seqs = inputs_rows.shape[0] // SEQUENCE_TOKENS

    def one_sequence(totals, sequence_items):
        tokens, cotangent, positions = sequence_items
        cosine_values, sine_lookup = rope_tables(positions)
        x_float = tokens.astype(single_float_type)
        rinv_one = lax.rsqrt(lax.optimization_barrier(jnp.mean(x_float * x_float, -1, keepdims=True)) + EPS)
        normed_one = (x_float * rinv_one * attention_gain).astype(brain_float_type)
        query_lin = jnp.dot(normed_one, query_weight, preferred_element_type=single_float_type) + query_bias
        key_value_linear = jnp.dot(normed_one, key_value_weight, preferred_element_type=single_float_type) + key_value_bias
        query_rot = apply_rotation(query_lin.reshape(SEQUENCE_TOKENS, QUERY_HEADS, HEAD_SIZE), cosine_values, sine_lookup).astype(brain_float_type).astype(single_float_type)
        rotated_keys = apply_rotation(key_value_linear[:, :key_value_width].reshape(SEQUENCE_TOKENS, KEYVALUE_HEADS, HEAD_SIZE), cosine_values, sine_lookup).astype(brain_float_type)
        value_second_part = key_value_linear[:, key_value_width:].reshape(SEQUENCE_TOKENS, KEYVALUE_HEADS, HEAD_SIZE).astype(brain_float_type)
        key_expand = jnp.repeat(rotated_keys, query_group_width, axis=1).astype(single_float_type)
        value_expand = jnp.repeat(value_second_part, query_group_width, axis=1).astype(single_float_type)
        scores = causal_scores(query_rot, key_expand)
        row_max = lax.optimization_barrier(jnp.max(scores, -1, keepdims=True))
        log_total = row_max + jnp.log(lax.optimization_barrier(jnp.sum(jnp.exp(scores - row_max), -1, keepdims=True)))
        softmax_probs = jnp.exp(scores - log_total)
        probs_half = rounded(softmax_probs)
        attended = jnp.einsum('hij,jhd->ihd', probs_half, value_expand).astype(brain_float_type)
        attended_flat = attended.reshape(SEQUENCE_TOKENS, QUERY_HEADS * HEAD_SIZE)
        hidden_res = x_float + jnp.dot(attended_flat, out_proj, preferred_element_type=single_float_type)
        rinv_two = lax.rsqrt(lax.optimization_barrier(jnp.mean(hidden_res * hidden_res, -1, keepdims=True)) + EPS)
        normed_two = (hidden_res * rinv_two * feedforward_gain).astype(brain_float_type)
        gate_lin = jnp.dot(normed_two, gate_weight, preferred_element_type=single_float_type)
        upper_lin = jnp.dot(normed_two, upper_weight, preferred_element_type=single_float_type)
        sigmoid_gate = jax.nn.sigmoid(gate_lin)
        activated = (gate_lin * sigmoid_gate * upper_lin).astype(brain_float_type)
        output = hidden_res + jnp.dot(activated, down_proj, preferred_element_type=single_float_type)
        act_grad = jnp.dot(cotangent, down_weight, preferred_element_type=single_float_type)
        gate_half = (act_grad * upper_lin * sigmoid_gate * (1.0 + gate_lin * (1.0 - sigmoid_gate))).astype(brain_float_type)
        upper_half = (act_grad * gate_lin * sigmoid_gate).astype(brain_float_type)
        normed_two_grad = jnp.dot(gate_half, gate_weight.T, preferred_element_type=single_float_type) + jnp.dot(upper_half, upper_weight.T, preferred_element_type=single_float_type)
        scaled_two = normed_two_grad * feedforward_gain
        hidden_grad = cotangent.astype(single_float_type) + rinv_two * scaled_two - hidden_res * rinv_two ** 3 * lax.optimization_barrier(jnp.sum(scaled_two * hidden_res, -1, keepdims=True)) / MODEL_WIDTH
        hidden_half = hidden_grad.astype(brain_float_type)
        att_grad = rounded(jnp.dot(hidden_half, output_weight, preferred_element_type=single_float_type)).reshape(SEQUENCE_TOKENS, QUERY_HEADS, HEAD_SIZE)
        prob_grad = jnp.einsum('ihd,jhd->hij', att_grad, value_expand)
        row_delta = lax.optimization_barrier(jnp.sum(att_grad * attended.astype(single_float_type), -1)).T
        score_half = rounded(softmax_probs * (prob_grad - row_delta[:, :, None]))
        query_grad = jnp.einsum('hij,jhd->ihd', score_half, key_expand) * scale
        key_heads = jnp.einsum('hij,ihd->jhd', score_half, query_rot) * scale
        value_heads = jnp.einsum('hij,ihd->jhd', probs_half, att_grad)
        key_part = rounded(unrotate(key_heads.reshape(SEQUENCE_TOKENS, N_COL, per_block, HEAD_SIZE).sum(2), cosine_values, sine_lookup))
        value_part = rounded(value_heads.reshape(SEQUENCE_TOKENS, N_COL, per_block, HEAD_SIZE).sum(2))
        query_half = unrotate(query_grad, cosine_values, sine_lookup).astype(brain_float_type).reshape(SEQUENCE_TOKENS, QUERY_HEADS * HEAD_SIZE)
        normed_one_grad = jnp.dot(query_half, query_weight.T, preferred_element_type=single_float_type)
        normed_one_grad = normed_one_grad + jnp.einsum('tce,dce->td', key_part, key_block_list) + jnp.einsum('tce,dce->td', value_part, value_block_list)
        scaled_one = normed_one_grad * attention_gain
        input_grad = hidden_grad + rinv_one * scaled_one - x_float * rinv_one ** 3 * lax.optimization_barrier(jnp.sum(scaled_one * x_float, -1, keepdims=True)) / MODEL_WIDTH
        normed_float = normed_one.astype(single_float_type)
        key_weight_grad = jnp.einsum('dce,ch->dhe', jnp.einsum('td,tce->dce', normed_float, key_part), holder_lookup).reshape(MODEL_WIDTH, key_value_width)
        value_weight_grad = jnp.einsum('dce,ch->dhe', jnp.einsum('td,tce->dce', normed_float, value_part), holder_lookup).reshape(MODEL_WIDTH, key_value_width)
        key_bias_grad = jnp.einsum('tce,ch->he', key_part, holder_lookup).reshape(key_value_width)
        value_bias_grad = jnp.einsum('tce,ch->he', value_part, holder_lookup).reshape(key_value_width)
        updates = (lax.optimization_barrier(jnp.sum(normed_one_grad * x_float * rinv_one, 0)), jnp.dot(normed_one.T, query_half, preferred_element_type=single_float_type), lax.optimization_barrier(jnp.sum(query_half.astype(single_float_type), 0)), jnp.concatenate([key_weight_grad, value_weight_grad], 1), jnp.concatenate([key_bias_grad, value_bias_grad], 0), jnp.dot(hidden_half.T, attended_flat, preferred_element_type=single_float_type), lax.optimization_barrier(jnp.sum(normed_two_grad * hidden_res * rinv_two, 0)), jnp.dot(normed_two.T, gate_half, preferred_element_type=single_float_type), jnp.dot(normed_two.T, upper_half, preferred_element_type=single_float_type), jnp.dot(cotangent.T, activated, preferred_element_type=single_float_type))
        new_totals = tuple((older + newer for older, newer in zip(totals, updates)))
        return (new_totals, (output, input_grad))
    initial = (jnp.zeros((MODEL_WIDTH,), single_float_type), jnp.zeros((MODEL_WIDTH, QUERY_HEADS * HEAD_SIZE), single_float_type), jnp.zeros((QUERY_HEADS * HEAD_SIZE,), single_float_type), jnp.zeros((MODEL_WIDTH, 2 * key_value_width), single_float_type), jnp.zeros((2 * key_value_width,), single_float_type), jnp.zeros((MODEL_WIDTH, QUERY_HEADS * HEAD_SIZE), single_float_type), jnp.zeros((MODEL_WIDTH,), single_float_type), jnp.zeros((MODEL_WIDTH, FF), single_float_type), jnp.zeros((MODEL_WIDTH, FF), single_float_type), jnp.zeros((MODEL_WIDTH, FF), single_float_type))
    sequence_items = (inputs_rows.reshape(num_seqs, SEQUENCE_TOKENS, MODEL_WIDTH), cotangent_rows.reshape(num_seqs, SEQUENCE_TOKENS, MODEL_WIDTH), position_ids.reshape(num_seqs, SEQUENCE_TOKENS))
    totals, stacked = lax.scan(one_sequence, initial, sequence_items)
    block_output = stacked[0].reshape(num_seqs * SEQUENCE_TOKENS, MODEL_WIDTH).T
    input_grad = stacked[1].reshape(num_seqs * SEQUENCE_TOKENS, MODEL_WIDTH).T
    return (block_output, input_grad, totals[0], totals[1], totals[2], totals[3], totals[4], totals[5], totals[6], totals[7], totals[8], totals[9])
```

```python
import jax
import jax.numpy as jnp
from jax import lax
from jax.experimental import pallas as pl
from jax.experimental.pallas import tpu as pltpu
from jax.sharding import PartitionSpec as P

MODEL_WIDTH = 1536
KEYVALUE_HEADS = 2
HEAD_SIZE = 128


EPS = 1e-06
THETA = 1000000.0
NEG = -1e30


def rope_tables(position_ids):
    half_dim = HEAD_SIZE // 2
    frequencies = THETA ** (-(jnp.arange(half_dim, dtype=jnp.float32) * 2.0 / HEAD_SIZE))
    angles = position_ids.astype(jnp.float32)[:, None] * frequencies[None, :]
    cosine_values = jnp.cos(angles)
    sine_lookup = jnp.sin(angles)
    return (
        jnp.concatenate([cosine_values, cosine_values], -1),
        jnp.concatenate([sine_lookup, sine_lookup], -1),
    )


def apply_rotation(values, cosine_values, sine_lookup):
    half_dim = HEAD_SIZE // 2
    turned = jnp.concatenate([-values[..., half_dim:], values[..., :half_dim]], -1)
    return values * cosine_values[:, None, :] + turned * sine_lookup[:, None, :]


def unrotate(gradient, cosine_values, sine_lookup):
    half_dim = HEAD_SIZE // 2
    scaled = gradient * sine_lookup[:, None, :]
    turned = jnp.concatenate([scaled[..., half_dim:], -scaled[..., :half_dim]], -1)
    return gradient * cosine_values[:, None, :] + turned


def row_total(partial_value):
    return lax.psum(partial_value, "row")


def norm_forward(x_float, gain):
    squares = jnp.sum(x_float * x_float, -1)
    rinv = lax.rsqrt(row_total(squares) / MODEL_WIDTH + EPS)[:, None]
    return ((x_float * rinv * gain).astype(jnp.bfloat16), rinv)


def norm_backward(normed_grad, x_float, rinv, gain):
    scaled = normed_grad * gain
    inner = row_total(jnp.sum(scaled * x_float, -1))[:, None]
    input_part = rinv * scaled - x_float * rinv**3 * inner / MODEL_WIDTH
    gain_part = jnp.sum(normed_grad * x_float * rinv, 0)
    return (input_part, gain_part)


def column_gather(values):
    return lax.all_gather(values, "col", axis=0, tiled=True)


def column_sum(partial_value):
    return lax.psum_scatter(
        partial_value.astype(jnp.bfloat16), "col", scatter_dimension=0, tiled=True
    ).astype(jnp.float32)


def row_product(gathered, weight):
    return (
        lax.psum_scatter(
            jnp.dot(gathered, weight, preferred_element_type=jnp.float32).astype(jnp.bfloat16),
            "row",
            scatter_dimension=0,
            tiled=True,
        ).astype(jnp.float32),
        gathered,
    )


def row_project(local_part, weight):
    return lax.dot_general(
        lax.all_gather(local_part, "row", axis=0, tiled=True),
        weight,
        (((1,), (1,)), ((), ())),
        preferred_element_type=jnp.float32,
    )


def row_fold(local_part, partner, weight):
    pair_dims = (((0,), (0,)), ((), ()))

    def accumulate(block_rows):
        grad_sum = lax.dot_general(
            partner, block_rows, pair_dims, preferred_element_type=jnp.float32
        )
        if weight is None:
            return (grad_sum,)
        back_proj = lax.dot_general(
            block_rows, weight, (((1,), (1,)), ((), ())), preferred_element_type=jnp.float32
        )
        column_totals = jnp.sum(block_rows, 0, dtype=jnp.float32)
        return (grad_sum, back_proj, column_totals)

    return accumulate(lax.all_gather(local_part, "row", axis=0, tiled=True))


def causal_scores(query_rot, rotated_keys):
    scores = jnp.einsum(
        "ihd,jd->hij", query_rot, rotated_keys, preferred_element_type=jnp.float32
    ) * HEAD_SIZE ** (-0.5)
    length = query_rot.shape[0]
    allowed = jnp.arange(length)[:, None] >= jnp.arange(length)[None, :]
    return jnp.where(allowed[None], scores, NEG)


def attend(query_rot, rotated_keys, value_second_part):
    scores = causal_scores(query_rot, rotated_keys)
    row_max = jnp.max(scores, -1, keepdims=True)
    log_total = row_max + jnp.log(jnp.sum(jnp.exp(scores - row_max), -1, keepdims=True))
    probs_half = jnp.exp(scores - log_total).astype(jnp.bfloat16)
    attended = jnp.einsum(
        "hij,jd->ihd", probs_half, value_second_part, preferred_element_type=jnp.float32
    ).astype(jnp.bfloat16)
    return (attended, log_total)


def attend_back(query_rot, rotated_keys, value_second_part, attended, att_grad, log_total):
    scale = HEAD_SIZE ** (-0.5)
    softmax_probs = jnp.exp(causal_scores(query_rot, rotated_keys) - log_total)
    probs_half = softmax_probs.astype(jnp.bfloat16)
    prob_grad = jnp.einsum(
        "ihd,jd->hij", att_grad, value_second_part, preferred_element_type=jnp.float32
    )
    row_delta = jnp.einsum("ihd,ihd->hi", att_grad, attended, preferred_element_type=jnp.float32)
    score_half = (softmax_probs * (prob_grad - row_delta[:, :, None])).astype(jnp.bfloat16)
    query_grad = (
        jnp.einsum("hij,jd->ihd", score_half, rotated_keys, preferred_element_type=jnp.float32)
        * scale
    )
    key_grad = (
        jnp.einsum("hij,ihd->jd", score_half, query_rot, preferred_element_type=jnp.float32) * scale
    )
    value_grad = jnp.einsum("hij,ihd->jd", probs_half, att_grad, preferred_element_type=jnp.float32)
    return (query_grad, key_grad, value_grad)


def general_device(
    block_input,
    position_ids,
    attention_gain,
    query_weight,
    query_bias,
    key_value_weight,
    key_value_bias,
    output_weight,
    feedforward_gain,
    gate_weight,
    upper_weight,
    down_weight,
    out_cotangent,
):
    single_float_type = jnp.float32
    brain_float_type = jnp.bfloat16
    column_number = lax.axis_size("col")
    seq_len = position_ids.shape[0]
    heads_here = query_weight.shape[1] // HEAD_SIZE
    query_cols = query_weight.shape[1]
    hidden_cols = gate_weight.shape[1]
    key_value_head = lax.axis_index("col") // (column_number // KEYVALUE_HEADS)
    key_start = key_value_head * HEAD_SIZE
    value_offset = KEYVALUE_HEADS * HEAD_SIZE + key_value_head * HEAD_SIZE
    keyval_local = jnp.concatenate(
        [
            lax.dynamic_slice_in_dim(key_value_weight, key_start, HEAD_SIZE, 1),
            lax.dynamic_slice_in_dim(key_value_weight, value_offset, HEAD_SIZE, 1),
        ],
        1,
    )
    bias_local = jnp.concatenate(
        [
            lax.dynamic_slice_in_dim(key_value_bias, key_start, HEAD_SIZE, 0),
            lax.dynamic_slice_in_dim(key_value_bias, value_offset, HEAD_SIZE, 0),
        ],
        0,
    )
    proj_weight = jnp.concatenate([query_weight, keyval_local], 1)
    proj_bias = jnp.concatenate([query_bias, bias_local], 0)
    pair_weight = jnp.concatenate([gate_weight, upper_weight], 1)
    cosine_values, sine_lookup = rope_tables(position_ids)
    x_float = block_input.T.astype(single_float_type)
    cot_local = out_cotangent.T
    normed_one, rinv_one = norm_forward(x_float, attention_gain)
    normed_one_all = column_gather(normed_one)
    proj_out = row_product(normed_one_all, proj_weight)[0] + proj_bias
    query_rot = apply_rotation(
        proj_out[:, :query_cols].reshape(seq_len, heads_here, HEAD_SIZE), cosine_values, sine_lookup
    ).astype(brain_float_type)
    rotated_keys = apply_rotation(
        proj_out[:, query_cols : query_cols + HEAD_SIZE][:, None, :], cosine_values, sine_lookup
    )[:, 0].astype(brain_float_type)
    value_second_part = proj_out[:, query_cols + HEAD_SIZE :].astype(brain_float_type)
    attended, log_total = attend(query_rot, rotated_keys, value_second_part)
    attended_flat = attended.reshape(seq_len, query_cols)
    hidden_res = x_float + column_sum(row_project(attended_flat, output_weight))
    normed_two, rinv_two = norm_forward(hidden_res, feedforward_gain)
    normed_two_all = column_gather(normed_two)
    gate_upper, normed_two_seq = row_product(normed_two_all, pair_weight)
    gate_lin = gate_upper[:, :hidden_cols]
    upper_lin = gate_upper[:, hidden_cols:]
    sigmoid_gate = jax.nn.sigmoid(gate_lin)
    activated = (gate_lin * sigmoid_gate * upper_lin).astype(brain_float_type)
    block_output = hidden_res + column_sum(row_project(activated, down_weight))
    cotangent_all = column_gather(cot_local)
    act_grad = row_product(cotangent_all, down_weight)[0]
    down_grad = row_fold(activated, cotangent_all, None)[0]
    gate_grad = act_grad * upper_lin * sigmoid_gate * (1.0 + gate_lin * (1.0 - sigmoid_gate))
    upper_grad = act_grad * gate_lin * sigmoid_gate
    pair_grad_half = jnp.concatenate([gate_grad, upper_grad], 1).astype(brain_float_type)
    folded_two = row_fold(pair_grad_half, normed_two_all, pair_weight)
    pair_weight_grad = folded_two[0]
    spread_two = folded_two[1]
    normed_two_grad = column_sum(spread_two)
    hidden_part, ffn_gain_part = norm_backward(
        normed_two_grad, hidden_res, rinv_two, feedforward_gain
    )
    hidden_grad = cot_local.astype(single_float_type) + hidden_part
    hidden_half = hidden_grad.astype(brain_float_type)
    hidden_all = column_gather(hidden_half)
    att_grad = (
        row_product(hidden_all, output_weight)[0]
        .astype(brain_float_type)
        .reshape(seq_len, heads_here, HEAD_SIZE)
    )
    output_grad = row_fold(attended_flat, hidden_all, None)[0]
    query_grad, key_grad, value_grad = attend_back(
        query_rot, rotated_keys, value_second_part, attended, att_grad, log_total
    )
    query_half = (
        unrotate(query_grad, cosine_values, sine_lookup)
        .astype(brain_float_type)
        .reshape(seq_len, query_cols)
    )
    key_half = unrotate(key_grad[:, None, :], cosine_values, sine_lookup)[:, 0].astype(
        brain_float_type
    )
    value_grad_half = value_grad.astype(brain_float_type)
    proj_grad_half = jnp.concatenate([query_half, key_half, value_grad_half], 1)
    folded_one = row_fold(proj_grad_half, normed_one_all, proj_weight)
    projection_weight_gradient = folded_one[0]
    normed_one_grad = column_sum(folded_one[1])
    proj_bias_grad = folded_one[2]
    input_part, attn_gain_part = norm_backward(normed_one_grad, x_float, rinv_one, attention_gain)
    input_grad = hidden_grad + input_part
    key_value_gradient = jnp.zeros(
        (projection_weight_gradient.shape[0], 2 * KEYVALUE_HEADS * HEAD_SIZE), single_float_type
    )
    key_value_gradient = lax.dynamic_update_slice_in_dim(
        key_value_gradient,
        projection_weight_gradient[:, query_cols : query_cols + HEAD_SIZE],
        key_start,
        1,
    )
    key_value_gradient = lax.dynamic_update_slice_in_dim(
        key_value_gradient, projection_weight_gradient[:, query_cols + HEAD_SIZE :], value_offset, 1
    )
    key_value_bias_gradient = jnp.zeros((2 * KEYVALUE_HEADS * HEAD_SIZE,), single_float_type)
    key_value_bias_gradient = lax.dynamic_update_slice_in_dim(
        key_value_bias_gradient, proj_bias_grad[query_cols : query_cols + HEAD_SIZE], key_start, 0
    )
    key_value_bias_gradient = lax.dynamic_update_slice_in_dim(
        key_value_bias_gradient, proj_bias_grad[query_cols + HEAD_SIZE :], value_offset, 0
    )
    shared = (
        lax.psum(key_value_gradient.astype(jnp.bfloat16), ("dp", "col")).astype(jnp.float32),
        lax.psum(key_value_bias_gradient.astype(jnp.bfloat16), ("dp", "col")).astype(jnp.float32),
        lax.psum(attn_gain_part.astype(jnp.bfloat16), ("dp", "col")).astype(jnp.float32),
        lax.psum(ffn_gain_part.astype(jnp.bfloat16), ("dp", "col")).astype(jnp.float32),
    )
    summed = (
        lax.psum_scatter(
            projection_weight_gradient[:, :query_cols].astype(jnp.bfloat16),
            "dp",
            scatter_dimension=0,
            tiled=True,
        ).astype(jnp.float32),
        lax.psum_scatter(
            proj_bias_grad[:query_cols].astype(jnp.bfloat16), "dp", scatter_dimension=0, tiled=True
        ).astype(jnp.float32),
        lax.psum_scatter(
            output_grad.astype(jnp.bfloat16), "dp", scatter_dimension=0, tiled=True
        ).astype(jnp.float32),
        lax.psum_scatter(
            pair_weight_grad[:, :hidden_cols].astype(jnp.bfloat16),
            "dp",
            scatter_dimension=0,
            tiled=True,
        ).astype(jnp.float32),
        lax.psum_scatter(
            pair_weight_grad[:, hidden_cols:].astype(jnp.bfloat16),
            "dp",
            scatter_dimension=0,
            tiled=True,
        ).astype(jnp.float32),
        lax.psum_scatter(
            down_grad.astype(jnp.bfloat16), "dp", scatter_dimension=0, tiled=True
        ).astype(jnp.float32),
    )
    return (
        block_output.T,
        input_grad.T,
        shared[2],
        summed[0],
        summed[1],
        shared[0],
        shared[1],
        summed[2],
        shared[3],
        summed[3],
        summed[4],
        summed[5],
    )


MESH_ID = pl.DeviceIdType.MESH
F32 = jnp.float32
BF16 = jnp.bfloat16
LINE = 4
BLOCK = 128
LOCAL = LINE * BLOCK
HALF = MODEL_WIDTH // 2
VMEM_SPEC = pl.BlockSpec(memory_space=pltpu.VMEM)
ANY_SPEC = pl.BlockSpec(memory_space=pl.ANY)
PAIR_ROWS = (((0,), (0,)), ((), ()))
PAIR_COLS = (((1,), (1,)), ((), ()))
SCALE = HEAD_SIZE ** (-0.5)


def line_barrier(me):
    barrier = pltpu.get_barrier_semaphore()

    @pl.when(me > 0)
    def _():
        pl.semaphore_signal(barrier, 1, device_id={"col": me - 1}, device_id_type=MESH_ID)

    @pl.when(me < LINE - 1)
    def _():
        pl.semaphore_signal(barrier, 1, device_id={"col": me + 1}, device_id_type=MESH_ID)

    @pl.when((me > 0) & (me < LINE - 1))
    def _():
        pl.semaphore_wait(barrier, 2)

    @pl.when((me == 0) | (me == LINE - 1))
    def _():
        pl.semaphore_wait(barrier, 1)


def block_rows(index):
    return pl.ds(pl.multiple_of(index * BLOCK, BLOCK), BLOCK)


def gather_line(me, all_ref, sends, recv, each):
    def copy(j, to, sem):
        rows = all_ref.at[block_rows(j)]
        return pltpu.make_async_remote_copy(
            rows, rows, sem, recv.at[j], device_id={"col": to}, device_id_type=MESH_ID
        )

    def arrived(j):
        rows = all_ref.at[block_rows(j)]
        pltpu.make_async_copy(rows, rows, recv.at[j]).wait()

    for s in range(LINE):
        left, right = me - s, me + s

        @pl.when(left >= 0)
        def _():
            if s:
                arrived(left)

            @pl.when(me < LINE - 1)
            def _():
                copy(left, me + 1, sends.at[0, s]).start()

        @pl.when(right < LINE)
        def _():
            if s:
                arrived(right)

            @pl.when(me > 0)
            def _():
                copy(right, me - 1, sends.at[1, s]).start()

        @pl.when(left >= 0)
        def _():
            each(left)

        if s:

            @pl.when(right < LINE)
            def _():
                each(right)

    for s in range(LINE):

        @pl.when((me - s >= 0) & (me < LINE - 1))
        def _():
            copy(me, me + 1, sends.at[0, s]).wait_send()

        @pl.when((me + s < LINE) & (me > 0))
        def _():
            copy(me, me - 1, sends.at[1, s]).wait_send()


def scatter_line(me, block_of, out_ref, from_left, from_right, going, sends, recv):
    def copy(j, to, side, landing):
        return pltpu.make_async_remote_copy(
            going.at[j],
            landing.at[j],
            sends.at[side, j],
            recv.at[side, j],
            device_id={"col": to},
            device_id_type=MESH_ID,
        )

    def arrived(j, side, landing):
        pltpu.make_async_copy(landing.at[j], landing.at[j], recv.at[side, j]).wait()

    for s in range(LINE - 1, 0, -1):
        ahead, behind = me + s, me - s

        @pl.when(ahead < LINE)
        def _():
            mine = block_of(ahead)

            @pl.when(me > 0)
            def _():
                arrived(ahead, 0, from_left)
                going[ahead] = (mine + from_left[ahead].astype(F32)).astype(BF16)

            @pl.when(me == 0)
            def _():
                going[ahead] = mine.astype(BF16)

            copy(ahead, me + 1, 0, from_left).start()

        @pl.when(behind >= 0)
        def _():
            mine = block_of(behind)

            @pl.when(me < LINE - 1)
            def _():
                arrived(behind, 1, from_right)
                going[behind] = (mine + from_right[behind].astype(F32)).astype(BF16)

            @pl.when(me == LINE - 1)
            def _():
                going[behind] = mine.astype(BF16)

            copy(behind, me - 1, 1, from_right).start()

    out_ref[...] = block_of(me)

    @pl.when(me > 0)
    def _():
        arrived(me, 0, from_left)
        out_ref[...] += from_left[me].astype(F32)

    @pl.when(me < LINE - 1)
    def _():
        arrived(me, 1, from_right)
        out_ref[...] += from_right[me].astype(F32)

    for s in range(1, LINE):

        @pl.when(me + s < LINE)
        def _():
            copy(me + s, me + 1, 0, from_left).wait_send()

        @pl.when(me - s >= 0)
        def _():
            copy(me - s, me - 1, 1, from_right).wait_send()


def dot(a, b, dims=(((1,), (0,)), ((), ()))):
    return lax.dot_general(a, b, dims, preferred_element_type=F32)


def turn(values):
    return pltpu.roll(values, HEAD_SIZE // 2, 1)


def norm_scale(values):
    return lax.rsqrt(jnp.sum(values * values, -1, keepdims=True) / MODEL_WIDTH + EPS)


def comm_call(body, outs, n_in, scratch, collective_id, flops, name):
    return pl.pallas_call(
        body,
        out_shape=outs,
        in_specs=[VMEM_SPEC] * n_in,
        out_specs=[VMEM_SPEC] * len(outs),
        scratch_shapes=scratch,
        compiler_params=pltpu.CompilerParams(collective_id=collective_id, has_side_effects=True),
        cost_estimate=pl.CostEstimate(flops=flops, bytes_accessed=40_000_000, transcendentals=0),
        name=name,
    )


def gather_scratch():
    return [pltpu.SemaphoreType.DMA((2, LINE)), pltpu.SemaphoreType.DMA((LINE,))]


def scatter_scratch(width=MODEL_WIDTH):
    return [pltpu.VMEM((LINE, BLOCK, width), BF16)] * 3 + [pltpu.SemaphoreType.DMA((2, LINE))] * 2


def project_body(
    x_ref, gain_ref, own_ref, other_ref, bias_ref, cos_ref, sin_ref, all_ref, query_ref, kv_ref, sends, recv
):
    me = lax.axis_index("col")
    line_barrier(me)
    x = x_ref[...].astype(F32)
    all_ref[block_rows(me)] = (x * norm_scale(x) * gain_ref[...]).astype(BF16)
    query_cols = query_ref.shape[1]

    def each(j):
        rows = block_rows(j)
        block = all_ref[rows]
        out = dot(block[:, :HALF], own_ref[...]) + dot(block[:, HALF:], other_ref[...])
        out = out + bias_ref[...]
        cosine, sine = cos_ref[rows], sin_ref[rows]
        for h in range(query_cols // HEAD_SIZE + 1):
            head = out[:, h * HEAD_SIZE : (h + 1) * HEAD_SIZE]
            turned = (head * cosine + turn(head) * sine).astype(BF16)
            if h * HEAD_SIZE < query_cols:
                query_ref[rows, h * HEAD_SIZE : (h + 1) * HEAD_SIZE] = turned
            else:
                kv_ref[rows, :HEAD_SIZE] = turned
        kv_ref[rows, HEAD_SIZE:] = out[:, query_cols + HEAD_SIZE :].astype(BF16)

    gather_line(me, all_ref, sends, recv, each)


def attend_body(query_ref, own_ref, other_ref, attended_ref, probs_ref):
    r = lax.axis_index("row")
    rows = 2 * BLOCK
    shape = (rows, rows)
    at_row = lax.broadcasted_iota(jnp.int32, shape, 0)
    at_col = lax.broadcasted_iota(jnp.int32, shape, 1)
    own_mask = at_row >= at_col
    other_mask = at_col // BLOCK < at_row // BLOCK + r
    heads = query_ref.shape[1] // HEAD_SIZE
    for s in range(2):
        part = slice(s * rows, (s + 1) * rows)
        for h in range(heads):
            cols = slice(h * HEAD_SIZE, (h + 1) * HEAD_SIZE)
            query = query_ref[part, cols]
            own = jnp.where(own_mask, dot(query, own_ref[part, :HEAD_SIZE], PAIR_COLS) * SCALE, NEG)
            other = jnp.where(
                other_mask, dot(query, other_ref[part, :HEAD_SIZE], PAIR_COLS) * SCALE, NEG
            )
            top = jnp.maximum(
                jnp.max(own, -1, keepdims=True), jnp.max(other, -1, keepdims=True)
            )
            total = jnp.sum(jnp.exp(own - top), -1, keepdims=True) + jnp.sum(
                jnp.exp(other - top), -1, keepdims=True
            )
            log_total = top + jnp.log(total)
            own = jnp.exp(own - log_total).astype(BF16)
            other = jnp.exp(other - log_total).astype(BF16)
            attended_ref[part, cols] = (
                dot(own, own_ref[part, HEAD_SIZE:]) + dot(other, other_ref[part, HEAD_SIZE:])
            ).astype(BF16)
            probs_ref[s * heads + h, :, :rows] = own
            probs_ref[s * heads + h, :, rows:] = other


def attend_back_body(
    query_ref, own_ref, other_ref, attended_ref, probs_ref, grad_ref, cos_ref, sin_ref,
    query_grad_ref, own_grad_ref, other_grad_ref,
):
    rows = 2 * BLOCK
    heads = query_ref.shape[1] // HEAD_SIZE
    for s in range(2):
        part = slice(s * rows, (s + 1) * rows)
        own_key, other_key = own_ref[part, :HEAD_SIZE], other_ref[part, :HEAD_SIZE]
        own_value, other_value = own_ref[part, HEAD_SIZE:], other_ref[part, HEAD_SIZE:]
        sums = [jnp.zeros((rows, HEAD_SIZE), F32) for _ in range(4)]
        for h in range(heads):
            cols = slice(h * HEAD_SIZE, (h + 1) * HEAD_SIZE)
            query, grad = query_ref[part, cols], grad_ref[part, cols]
            own_p = probs_ref[s * heads + h, :, :rows]
            other_p = probs_ref[s * heads + h, :, rows:]
            delta = jnp.sum(
                grad.astype(F32) * attended_ref[part, cols].astype(F32), -1, keepdims=True
            )
            own_s = (own_p.astype(F32) * (dot(grad, own_value, PAIR_COLS) - delta)).astype(BF16)
            other_s = (other_p.astype(F32) * (dot(grad, other_value, PAIR_COLS) - delta)).astype(BF16)
            query_grad = (dot(own_s, own_key) + dot(other_s, other_key)) * SCALE
            query_grad_ref[part, cols] = (
                query_grad * cos_ref[part] - turn(query_grad) * sin_ref[part]
            ).astype(BF16)
            for i, (weights, partner) in enumerate(
                ((own_s, query), (own_p, grad), (other_s, query), (other_p, grad))
            ):
                sums[i] = sums[i] + dot(weights, partner, PAIR_ROWS)
        own_grad_ref[part, :HEAD_SIZE] = sums[0] * SCALE
        own_grad_ref[part, HEAD_SIZE:] = sums[1]
        other_grad_ref[part, :HEAD_SIZE] = (sums[2] * SCALE).astype(BF16)
        other_grad_ref[part, HEAD_SIZE:] = sums[3].astype(BF16)


def residual_body(
    attended_ref, own_ref, other_ref, x_ref, gain_ref, mid_ref, all_ref,
    from_left, from_right, going, s_sends, s_recv, sends, recv,
):
    me = lax.axis_index("col")
    line_barrier(me)

    def block_of(j):
        block = attended_ref[block_rows(j)]
        return jnp.concatenate(
            [dot(block, own_ref[...], PAIR_COLS), dot(block, other_ref[...], PAIR_COLS)], 1
        )

    scatter_line(me, block_of, mid_ref, from_left, from_right, going, s_sends, s_recv)
    mid = mid_ref[...] + x_ref[...].astype(F32)
    mid_ref[...] = mid
    all_ref[block_rows(me)] = (mid * norm_scale(mid) * gain_ref[...]).astype(BF16)
    gather_line(me, all_ref, sends, recv, lambda j: None)


def middle_back_body(
    part_ref, mid_ref, cot_ref, gain_ref, own_ref, other_ref,
    mid_grad_ref, gain_grad_ref, all_ref, att_grad_ref,
    from_left, from_right, going, s_sends, s_recv, sends, recv,
):
    me = lax.axis_index("col")
    line_barrier(me)
    scatter_line(
        me, lambda j: part_ref[block_rows(j)].astype(F32), mid_grad_ref,
        from_left, from_right, going, s_sends, s_recv,
    )
    mid, grad = mid_ref[...], mid_grad_ref[...]
    rinv = norm_scale(mid)
    gain_grad_ref[...] = jnp.sum(grad * mid * rinv, 0, keepdims=True)
    scaled = grad * gain_ref[...]
    inner = jnp.sum(scaled * mid, -1, keepdims=True)
    mid_grad = cot_ref[...].astype(F32) + rinv * scaled - mid * rinv**3 * inner / MODEL_WIDTH
    mid_grad_ref[...] = mid_grad
    all_ref[block_rows(me)] = mid_grad.astype(BF16)

    def each(j):
        block = all_ref[block_rows(j)]
        att_grad_ref[block_rows(j)] = (
            dot(block[:, :HALF], own_ref[...]) + dot(block[:, HALF:], other_ref[...])
        ).astype(BF16)

    gather_line(me, all_ref, sends, recv, each)


def input_back_body(
    query_grad_ref, own_kv_ref, got_kv_ref, cos_ref, sin_ref, own_ref, other_ref, x_ref, gain_ref,
    mid_grad_ref, proj_grad_ref, bias_ref, input_grad_ref, gain_grad_ref,
    from_left, from_right, going, s_sends, s_recv,
):
    me = lax.axis_index("col")
    line_barrier(me)
    query_cols = query_grad_ref.shape[1]
    kv = own_kv_ref[...] + got_kv_ref[...].astype(F32)
    key = kv[:, :HEAD_SIZE]
    proj_grad_ref[:, :query_cols] = query_grad_ref[...]
    proj_grad_ref[:, query_cols : query_cols + HEAD_SIZE] = (
        key * cos_ref[...] - turn(key) * sin_ref[...]
    ).astype(BF16)
    proj_grad_ref[:, query_cols + HEAD_SIZE :] = kv[:, HEAD_SIZE:].astype(BF16)

    def block_of(j):
        block = proj_grad_ref[block_rows(j)]
        return jnp.concatenate(
            [dot(block, own_ref[...], PAIR_COLS), dot(block, other_ref[...], PAIR_COLS)], 1
        )

    scatter_line(me, block_of, input_grad_ref, from_left, from_right, going, s_sends, s_recv)
    bias_ref[...] = jnp.sum(proj_grad_ref[...].astype(F32), 0, keepdims=True)
    x, grad = x_ref[...].astype(F32), input_grad_ref[...]
    rinv = norm_scale(x)
    gain_grad_ref[...] = jnp.sum(grad * x * rinv, 0, keepdims=True)
    scaled = grad * gain_ref[...]
    inner = jnp.sum(scaled * x, -1, keepdims=True)
    input_grad_ref[...] = mid_grad_ref[...] + rinv * scaled - x * rinv**3 * inner / MODEL_WIDTH


def feed_body(
    normed_ref, cot_ref, gate_hbm, upper_hbm, down_hbm, other_hbm, partner_hbm,
    activated_ref, gate_grad_ref, upper_grad_ref, back_ref, out_ref,
    weights, back_sum, out_sum, sems,
):
    core = lax.rem(lax.axis_index("dp"), 2)
    hidden = activated_ref.shape[1]
    quarter = HALF // 2
    here = pl.ds(pl.multiple_of(HALF + core * quarter, quarter), quarter)
    there = pl.ds(pl.multiple_of(HALF + (1 - core) * quarter, quarter), quarter)
    copies = []
    for i, own in enumerate((gate_hbm, upper_hbm, down_hbm)):
        copies.append(pltpu.make_async_copy(own, weights.at[i, pl.ds(0, HALF)], sems.at[i, 0]))
        copies.append(pltpu.make_async_copy(other_hbm.at[i], weights.at[i, here], sems.at[i, 1]))
        copies.append(pltpu.make_async_copy(partner_hbm.at[i], weights.at[i, there], sems.at[i, 2]))
    for copy in copies:
        copy.start()
    for copy in copies:
        copy.wait()
    tile = 256
    for i, low in enumerate(range(0, hidden, tile)):
        cols = slice(low, min(low + tile, hidden))
        gate_w, upper_w, down_w = weights[0, :, cols], weights[1, :, cols], weights[2, :, cols]
        gate = dot(normed_ref[...], gate_w)
        upper = dot(normed_ref[...], upper_w)
        act_grad = dot(cot_ref[...], down_w)
        sig = jax.nn.sigmoid(gate)
        silu = gate * sig
        activated = (silu * upper).astype(BF16)
        gate_grad = (act_grad * upper * sig * (1.0 + gate * (1.0 - sig))).astype(BF16)
        upper_grad = (act_grad * silu).astype(BF16)
        activated_ref[:, cols] = activated
        gate_grad_ref[:, cols] = gate_grad
        upper_grad_ref[:, cols] = upper_grad
        back = dot(gate_grad, gate_w, PAIR_COLS) + dot(upper_grad, upper_w, PAIR_COLS)
        out = dot(activated, down_w, PAIR_COLS)
        if i == 0:
            back_sum[...] = back
            out_sum[...] = out
        else:
            back_sum[...] += back
            out_sum[...] += out
    back_ref[...] = back_sum[...].astype(BF16)
    out_ref[...] = out_sum[...].astype(BF16)


def shape(rows, cols, dtype=BF16):
    return jax.ShapeDtypeStruct((rows, cols), dtype)


def swap(values, axis, bit):
    size = lax.axis_size(axis)
    return lax.ppermute(values, axis, [(i, i ^ bit) for i in range(size)])


def reduce_blocks(grad, x_first):
    y, core = lax.axis_index("dp") // 2, lax.axis_index("dp") % 2
    width = grad.shape[1]
    parts = grad.reshape(2, 2, 2, MODEL_WIDTH // 8, width)
    pick = lambda index: lax.dynamic_index_in_dim(parts, index, 2, keepdims=False)
    part = pick(core).astype(F32) + swap(pick(1 - core), "dp", 1).astype(F32)
    part = part.astype(BF16)
    choose = lambda index: lax.dynamic_index_in_dim(part, index, 1, keepdims=False)
    if x_first:
        half = (part[0].astype(F32) + swap(part[1], "row", 1).astype(F32)).astype(BF16)
        choose = lambda index: lax.dynamic_index_in_dim(half, index, 0, keepdims=False)
        return choose(y).astype(F32) + swap(choose(1 - y), "dp", 2).astype(F32)
    half = (choose(y).astype(F32) + swap(choose(1 - y), "dp", 2).astype(F32)).astype(BF16)
    return half[0].astype(F32) + swap(half[1], "row", 1).astype(F32)


def fast_device(
    block_input,
    position_ids,
    attention_gain,
    query_weight,
    query_bias,
    key_value_weight,
    key_value_bias,
    output_weight,
    feedforward_gain,
    gate_weight,
    upper_weight,
    down_weight,
    out_cotangent,
):
    r, c = lax.axis_index("row"), lax.axis_index("col")
    core = lax.axis_index("dp") % 2
    query_cols = query_weight.shape[1]
    hidden = gate_weight.shape[1]
    proj_cols = query_cols + 2 * HEAD_SIZE
    quarter = HALF // 2
    kv_head = c // (LINE // KEYVALUE_HEADS)
    key_start = kv_head * HEAD_SIZE
    value_start = (KEYVALUE_HEADS + kv_head) * HEAD_SIZE

    def mine(values):
        keep = lax.dynamic_slice_in_dim(values, r * BLOCK, BLOCK, 1).T
        send = lax.dynamic_slice_in_dim(values, (1 - r) * BLOCK, BLOCK, 1).T
        return jnp.concatenate([keep, swap(send, "row", 1)], 1)

    x_own = mine(block_input)
    small = jnp.concatenate([attention_gain, feedforward_gain, position_ids.astype(F32)])
    got_small = swap(small, "row", 1)
    attn_gain = jnp.concatenate([attention_gain, got_small[:HALF]])[None]
    ffn_gain = jnp.concatenate([feedforward_gain, got_small[HALF : 2 * HALF]])[None]
    own_ids, other_ids = small[2 * HALF :], got_small[2 * HALF :]
    ids = jnp.stack([jnp.where(r == 0, own_ids, other_ids), jnp.where(r == 0, other_ids, own_ids)])
    ids = lax.dynamic_index_in_dim(ids.reshape(2, 2, 2, BLOCK), r, 2, keepdims=False).reshape(LOCAL)
    frequencies = THETA ** (-(jnp.arange(HEAD_SIZE // 2, dtype=F32) * 2.0 / HEAD_SIZE))
    angles = ids[:, None] * frequencies[None, :]
    cosine, sine = jnp.cos(angles), jnp.sin(angles)
    cosine = jnp.concatenate([cosine, cosine], -1)
    sine = jnp.concatenate([-sine, sine], -1)

    own_proj = jnp.concatenate(
        [
            query_weight,
            lax.dynamic_slice_in_dim(key_value_weight, key_start, HEAD_SIZE, 1),
            lax.dynamic_slice_in_dim(key_value_weight, value_start, HEAD_SIZE, 1),
            output_weight,
        ],
        1,
    )
    proj_bias = jnp.concatenate(
        [
            query_bias,
            lax.dynamic_slice_in_dim(key_value_bias, key_start, HEAD_SIZE, 0),
            lax.dynamic_slice_in_dim(key_value_bias, value_start, HEAD_SIZE, 0),
        ]
    )[None]
    here = swap(lax.dynamic_slice_in_dim(own_proj, core * quarter, quarter, 0), "row", 1)
    there = swap(here, "dp", 1)
    other_proj = jnp.where(
        core == 0, jnp.concatenate([here, there]), jnp.concatenate([there, here])
    )
    own_in, own_out = own_proj[:, :proj_cols], own_proj[:, proj_cols:]
    other_in, other_out = other_proj[:, :proj_cols], other_proj[:, proj_cols:]

    ffn_send = jnp.stack(
        [
            lax.dynamic_slice_in_dim(w, core * quarter, quarter, 0)
            for w in (gate_weight, upper_weight, down_weight)
        ]
    )
    ffn_other = swap(ffn_send, "row", 1)
    ffn_partner = swap(ffn_other, "dp", 1)

    normed_one, query_rot, kv_own = comm_call(
        project_body,
        [shape(LOCAL, MODEL_WIDTH), shape(LOCAL, query_cols), shape(LOCAL, 2 * HEAD_SIZE)],
        7,
        gather_scratch(),
        1,
        10**9,
        "project",
    )(x_own, attn_gain, own_in, other_in, proj_bias, cosine, sine)
    kv_other = swap(kv_own, "row", 1)
    heads = query_cols // HEAD_SIZE
    attended, probs = pl.pallas_call(
        attend_body,
        out_shape=[
            shape(LOCAL, query_cols),
            jax.ShapeDtypeStruct((2 * heads, 2 * BLOCK, 4 * BLOCK), BF16),
        ],
        in_specs=[VMEM_SPEC] * 3,
        out_specs=[VMEM_SPEC] * 2,
        cost_estimate=pl.CostEstimate(flops=10**9, bytes_accessed=20_000_000, transcendentals=0),
        name="attend",
    )(query_rot, kv_own, kv_other)
    cot_own = mine(out_cotangent)
    cot_all = lax.all_gather(cot_own, "col", axis=0, tiled=True)
    mid, normed_two = comm_call(
        residual_body,
        [shape(BLOCK, MODEL_WIDTH, F32), shape(LOCAL, MODEL_WIDTH)],
        5,
        scatter_scratch() + gather_scratch(),
        2,
        10**9,
        "residual",
    )(attended, own_out, other_out, x_own, ffn_gain)
    activated, gate_grad, upper_grad, back_part, out_part = pl.pallas_call(
        feed_body,
        out_shape=[shape(LOCAL, hidden)] * 3 + [shape(LOCAL, MODEL_WIDTH)] * 2,
        in_specs=[VMEM_SPEC] * 2 + [ANY_SPEC] * 5,
        out_specs=[VMEM_SPEC] * 5,
        scratch_shapes=[
            pltpu.VMEM((3, MODEL_WIDTH, hidden), BF16),
            pltpu.VMEM((LOCAL, MODEL_WIDTH), F32),
            pltpu.VMEM((LOCAL, MODEL_WIDTH), F32),
            pltpu.SemaphoreType.DMA((3, 3)),
        ],
        cost_estimate=pl.CostEstimate(
            flops=2 * 10**10, bytes_accessed=40_000_000, transcendentals=0
        ),
        name="feed",
    )(normed_two, cot_all, gate_weight, upper_weight, down_weight, ffn_other, ffn_partner)
    out_own = lax.psum_scatter(out_part, "col", scatter_dimension=0, tiled=True).astype(F32) + mid
    down_grad = lax.dot_general(cot_all, activated, PAIR_ROWS, preferred_element_type=F32).astype(
        BF16
    )
    gate_w_grad = lax.dot_general(
        normed_two, gate_grad, PAIR_ROWS, preferred_element_type=F32
    ).astype(BF16)
    upper_w_grad = lax.dot_general(
        normed_two, upper_grad, PAIR_ROWS, preferred_element_type=F32
    ).astype(BF16)
    mid_grad, ffn_gain_part, mid_half, att_grad = comm_call(
        middle_back_body,
        [
            shape(BLOCK, MODEL_WIDTH, F32),
            shape(1, MODEL_WIDTH, F32),
            shape(LOCAL, MODEL_WIDTH),
            shape(LOCAL, query_cols),
        ],
        6,
        scatter_scratch() + gather_scratch(),
        3,
        10**9,
        "middle_back",
    )(back_part, mid, cot_own, ffn_gain, own_out, other_out)
    query_grad, kv_grad_own, kv_grad_other = pl.pallas_call(
        attend_back_body,
        out_shape=[
            shape(LOCAL, query_cols),
            shape(LOCAL, 2 * HEAD_SIZE, F32),
            shape(LOCAL, 2 * HEAD_SIZE),
        ],
        in_specs=[VMEM_SPEC] * 8,
        out_specs=[VMEM_SPEC] * 3,
        cost_estimate=pl.CostEstimate(flops=10**9, bytes_accessed=20_000_000, transcendentals=0),
        name="attend_back",
    )(query_rot, kv_own, kv_other, attended, probs, att_grad, cosine, sine)
    kv_grad_got = swap(kv_grad_other, "row", 1)
    output_w_grad = lax.dot_general(
        mid_half, attended, PAIR_ROWS, preferred_element_type=F32
    ).astype(BF16)
    proj_grad, bias_part, input_grad, attn_gain_part = comm_call(
        input_back_body,
        [
            shape(LOCAL, proj_cols),
            shape(1, proj_cols, F32),
            shape(BLOCK, MODEL_WIDTH, F32),
            shape(1, MODEL_WIDTH, F32),
        ],
        10,
        scatter_scratch(),
        4,
        10**9,
        "input_back",
    )(
        query_grad, kv_grad_own, kv_grad_got, cosine, sine, own_in, other_in, x_own, attn_gain,
        mid_grad,
    )
    proj_w_grad = lax.dot_general(
        normed_one, proj_grad, PAIR_ROWS, preferred_element_type=F32
    ).astype(BF16)

    down_sum = reduce_blocks(down_grad, True)
    gate_sum = reduce_blocks(gate_w_grad, False)
    upper_sum = reduce_blocks(upper_w_grad, True)
    output_sum = reduce_blocks(output_w_grad, False)
    proj_sum = reduce_blocks(proj_w_grad, True)

    kv_sum = lax.all_gather(proj_sum[:, query_cols:].astype(BF16), "col", axis=0, tiled=False)
    group = LINE // KEYVALUE_HEADS
    kv_sum = kv_sum.reshape(KEYVALUE_HEADS, group, -1, 2, HEAD_SIZE).astype(F32).sum(1)
    kv_sum = jnp.transpose(kv_sum, (1, 2, 0, 3)).reshape(-1, 2 * KEYVALUE_HEADS * HEAD_SIZE)
    kv_weight_grad = lax.all_gather(kv_sum.astype(BF16), "dp", axis=0, tiled=True).astype(F32)

    swapped = lambda v: jnp.where(r == 0, v, jnp.roll(v, HALF))
    spread = jnp.zeros((2 * KEYVALUE_HEADS * HEAD_SIZE,), F32)
    spread = lax.dynamic_update_slice(
        spread, bias_part[0, query_cols : query_cols + HEAD_SIZE], (key_start,)
    )
    spread = lax.dynamic_update_slice(spread, bias_part[0, query_cols + HEAD_SIZE :], (value_start,))
    query_spread = lax.dynamic_update_slice(
        jnp.zeros((LINE * query_cols,), F32), bias_part[0, :query_cols], (c * query_cols,)
    )
    vector = jnp.concatenate(
        [swapped(attn_gain_part[0]), swapped(ffn_gain_part[0]), spread, query_spread]
    )
    vector = lax.psum(vector, ("dp", "row", "col"))
    attn_gain_grad = lax.dynamic_slice_in_dim(vector, r * HALF, HALF, 0)
    ffn_gain_grad = lax.dynamic_slice_in_dim(vector, MODEL_WIDTH + r * HALF, HALF, 0)
    kv_bias_grad = vector[2 * MODEL_WIDTH : 2 * MODEL_WIDTH + spread.shape[0]]
    bias_rows = query_cols // lax.axis_size("dp")
    query_bias_grad = lax.dynamic_slice_in_dim(
        vector,
        2 * MODEL_WIDTH + spread.shape[0] + c * query_cols + lax.axis_index("dp") * bias_rows,
        bias_rows,
        0,
    )

    def returned(values):
        got = swap(values[:, HALF:].astype(BF16), "row", 1).astype(F32)
        keep = values[:, :HALF]
        pair = jnp.where(
            r == 0, jnp.concatenate([keep, got]), jnp.concatenate([got, keep])
        )
        return pair.T

    return (
        returned(out_own),
        returned(input_grad),
        attn_gain_grad,
        proj_sum[:, :query_cols],
        query_bias_grad,
        kv_weight_grad,
        kv_bias_grad,
        output_sum,
        ffn_gain_grad,
        gate_sum,
        upper_sum,
        down_sum,
    )


def per_device(*arrays):
    sizes = tuple(lax.axis_size(axis) for axis in ("dp", "row", "col"))
    if sizes == (4, 2, LINE) and arrays[0].shape == (HALF, 2 * BLOCK):
        return fast_device(*arrays)
    return general_device(*arrays)


def solution(mesh):
    placed = (
        P("row", ("dp", "col")),
        P(("dp", "row")),
        P("row"),
        P("row", "col"),
        P("col"),
        P("row", None),
        P(),
        P("row", "col"),
        P("row"),
        P("row", "col"),
        P("row", "col"),
        P("row", "col"),
        P("row", ("dp", "col")),
    )
    return jax.shard_map(
        per_device,
        mesh=mesh,
        in_specs=placed,
        out_specs=(
            P("row", ("dp", "col")),
            P("row", ("dp", "col")),
            P("row"),
            P(("row", "dp"), "col"),
            P(("col", "dp")),
            P("row", None),
            P(),
            P(("row", "dp"), "col"),
            P("row"),
            P(("row", "dp"), "col"),
            P(("row", "dp"), "col"),
            P(("row", "dp"), "col"),
        ),
        check_vma=False,
    )
```

```python
import jax
import jax.numpy as jnp
from jax import lax
from jax.experimental import pallas as pl
from jax.experimental.pallas import tpu as pltpu
from jax.sharding import PartitionSpec as P

MODEL_WIDTH = 1536
KEYVALUE_HEADS = 2
HEAD_SIZE = 128


EPS = 1e-06
THETA = 1000000.0
NEG = -1e30


def rope_tables(position_ids):
    half_dim = HEAD_SIZE // 2
    frequencies = THETA ** (-(jnp.arange(half_dim, dtype=jnp.float32) * 2.0 / HEAD_SIZE))
    angles = position_ids.astype(jnp.float32)[:, None] * frequencies[None, :]
    cosine_values = jnp.cos(angles)
    sine_lookup = jnp.sin(angles)
    return (
        jnp.concatenate([cosine_values, cosine_values], -1),
        jnp.concatenate([sine_lookup, sine_lookup], -1),
    )


def apply_rotation(values, cosine_values, sine_lookup):
    half_dim = HEAD_SIZE // 2
    turned = jnp.concatenate([-values[..., half_dim:], values[..., :half_dim]], -1)
    return values * cosine_values[:, None, :] + turned * sine_lookup[:, None, :]


def unrotate(gradient, cosine_values, sine_lookup):
    half_dim = HEAD_SIZE // 2
    scaled = gradient * sine_lookup[:, None, :]
    turned = jnp.concatenate([scaled[..., half_dim:], -scaled[..., :half_dim]], -1)
    return gradient * cosine_values[:, None, :] + turned


def row_total(partial_value):
    return lax.psum(partial_value, "row")


def norm_forward(x_float, gain):
    squares = jnp.sum(x_float * x_float, -1)
    rinv = lax.rsqrt(row_total(squares) / MODEL_WIDTH + EPS)[:, None]
    return ((x_float * rinv * gain).astype(jnp.bfloat16), rinv)


def norm_backward(normed_grad, x_float, rinv, gain):
    scaled = normed_grad * gain
    inner = row_total(jnp.sum(scaled * x_float, -1))[:, None]
    input_part = rinv * scaled - x_float * rinv**3 * inner / MODEL_WIDTH
    gain_part = jnp.sum(normed_grad * x_float * rinv, 0)
    return (input_part, gain_part)


def column_gather(values):
    return lax.all_gather(values, "col", axis=0, tiled=True)


def column_sum(partial_value):
    return lax.psum_scatter(
        partial_value.astype(jnp.bfloat16), "col", scatter_dimension=0, tiled=True
    ).astype(jnp.float32)


def row_product(gathered, weight):
    return (
        lax.psum_scatter(
            jnp.dot(gathered, weight, preferred_element_type=jnp.float32).astype(jnp.bfloat16),
            "row",
            scatter_dimension=0,
            tiled=True,
        ).astype(jnp.float32),
        gathered,
    )


def row_project(local_part, weight):
    return lax.dot_general(
        lax.all_gather(local_part, "row", axis=0, tiled=True),
        weight,
        (((1,), (1,)), ((), ())),
        preferred_element_type=jnp.float32,
    )


def row_fold(local_part, partner, weight):
    pair_dims = (((0,), (0,)), ((), ()))

    def accumulate(block_rows):
        grad_sum = lax.dot_general(
            partner, block_rows, pair_dims, preferred_element_type=jnp.float32
        )
        if weight is None:
            return (grad_sum,)
        back_proj = lax.dot_general(
            block_rows, weight, (((1,), (1,)), ((), ())), preferred_element_type=jnp.float32
        )
        column_totals = jnp.sum(block_rows, 0, dtype=jnp.float32)
        return (grad_sum, back_proj, column_totals)

    return accumulate(lax.all_gather(local_part, "row", axis=0, tiled=True))


def causal_scores(query_rot, rotated_keys):
    scores = jnp.einsum(
        "ihd,jd->hij", query_rot, rotated_keys, preferred_element_type=jnp.float32
    ) * HEAD_SIZE ** (-0.5)
    length = query_rot.shape[0]
    allowed = jnp.arange(length)[:, None] >= jnp.arange(length)[None, :]
    return jnp.where(allowed[None], scores, NEG)


def attend(query_rot, rotated_keys, value_second_part):
    scores = causal_scores(query_rot, rotated_keys)
    row_max = jnp.max(scores, -1, keepdims=True)
    log_total = row_max + jnp.log(jnp.sum(jnp.exp(scores - row_max), -1, keepdims=True))
    probs_half = jnp.exp(scores - log_total).astype(jnp.bfloat16)
    attended = jnp.einsum(
        "hij,jd->ihd", probs_half, value_second_part, preferred_element_type=jnp.float32
    ).astype(jnp.bfloat16)
    return (attended, log_total)


def attend_back(query_rot, rotated_keys, value_second_part, attended, att_grad, log_total):
    scale = HEAD_SIZE ** (-0.5)
    softmax_probs = jnp.exp(causal_scores(query_rot, rotated_keys) - log_total)
    probs_half = softmax_probs.astype(jnp.bfloat16)
    prob_grad = jnp.einsum(
        "ihd,jd->hij", att_grad, value_second_part, preferred_element_type=jnp.float32
    )
    row_delta = jnp.einsum("ihd,ihd->hi", att_grad, attended, preferred_element_type=jnp.float32)
    score_half = (softmax_probs * (prob_grad - row_delta[:, :, None])).astype(jnp.bfloat16)
    query_grad = (
        jnp.einsum("hij,jd->ihd", score_half, rotated_keys, preferred_element_type=jnp.float32)
        * scale
    )
    key_grad = (
        jnp.einsum("hij,ihd->jd", score_half, query_rot, preferred_element_type=jnp.float32) * scale
    )
    value_grad = jnp.einsum("hij,ihd->jd", probs_half, att_grad, preferred_element_type=jnp.float32)
    return (query_grad, key_grad, value_grad)


def general_device(
    block_input,
    position_ids,
    attention_gain,
    query_weight,
    query_bias,
    key_value_weight,
    key_value_bias,
    output_weight,
    feedforward_gain,
    gate_weight,
    upper_weight,
    down_weight,
    out_cotangent,
):
    single_float_type = jnp.float32
    brain_float_type = jnp.bfloat16
    column_number = lax.axis_size("col")
    seq_len = position_ids.shape[0]
    heads_here = query_weight.shape[1] // HEAD_SIZE
    query_cols = query_weight.shape[1]
    hidden_cols = gate_weight.shape[1]
    key_value_head = lax.axis_index("col") // (column_number // KEYVALUE_HEADS)
    key_start = key_value_head * HEAD_SIZE
    value_offset = KEYVALUE_HEADS * HEAD_SIZE + key_value_head * HEAD_SIZE
    keyval_local = jnp.concatenate(
        [
            lax.dynamic_slice_in_dim(key_value_weight, key_start, HEAD_SIZE, 1),
            lax.dynamic_slice_in_dim(key_value_weight, value_offset, HEAD_SIZE, 1),
        ],
        1,
    )
    bias_local = jnp.concatenate(
        [
            lax.dynamic_slice_in_dim(key_value_bias, key_start, HEAD_SIZE, 0),
            lax.dynamic_slice_in_dim(key_value_bias, value_offset, HEAD_SIZE, 0),
        ],
        0,
    )
    proj_weight = jnp.concatenate([query_weight, keyval_local], 1)
    proj_bias = jnp.concatenate([query_bias, bias_local], 0)
    pair_weight = jnp.concatenate([gate_weight, upper_weight], 1)
    cosine_values, sine_lookup = rope_tables(position_ids)
    x_float = block_input.T.astype(single_float_type)
    cot_local = out_cotangent.T
    normed_one, rinv_one = norm_forward(x_float, attention_gain)
    normed_one_all = column_gather(normed_one)
    proj_out = row_product(normed_one_all, proj_weight)[0] + proj_bias
    query_rot = apply_rotation(
        proj_out[:, :query_cols].reshape(seq_len, heads_here, HEAD_SIZE), cosine_values, sine_lookup
    ).astype(brain_float_type)
    rotated_keys = apply_rotation(
        proj_out[:, query_cols : query_cols + HEAD_SIZE][:, None, :], cosine_values, sine_lookup
    )[:, 0].astype(brain_float_type)
    value_second_part = proj_out[:, query_cols + HEAD_SIZE :].astype(brain_float_type)
    attended, log_total = attend(query_rot, rotated_keys, value_second_part)
    attended_flat = attended.reshape(seq_len, query_cols)
    hidden_res = x_float + column_sum(row_project(attended_flat, output_weight))
    normed_two, rinv_two = norm_forward(hidden_res, feedforward_gain)
    normed_two_all = column_gather(normed_two)
    gate_upper, normed_two_seq = row_product(normed_two_all, pair_weight)
    gate_lin = gate_upper[:, :hidden_cols]
    upper_lin = gate_upper[:, hidden_cols:]
    sigmoid_gate = jax.nn.sigmoid(gate_lin)
    activated = (gate_lin * sigmoid_gate * upper_lin).astype(brain_float_type)
    block_output = hidden_res + column_sum(row_project(activated, down_weight))
    cotangent_all = column_gather(cot_local)
    act_grad = row_product(cotangent_all, down_weight)[0]
    down_grad = row_fold(activated, cotangent_all, None)[0]
    gate_grad = act_grad * upper_lin * sigmoid_gate * (1.0 + gate_lin * (1.0 - sigmoid_gate))
    upper_grad = act_grad * gate_lin * sigmoid_gate
    pair_grad_half = jnp.concatenate([gate_grad, upper_grad], 1).astype(brain_float_type)
    folded_two = row_fold(pair_grad_half, normed_two_all, pair_weight)
    pair_weight_grad = folded_two[0]
    spread_two = folded_two[1]
    normed_two_grad = column_sum(spread_two)
    hidden_part, ffn_gain_part = norm_backward(
        normed_two_grad, hidden_res, rinv_two, feedforward_gain
    )
    hidden_grad = cot_local.astype(single_float_type) + hidden_part
    hidden_half = hidden_grad.astype(brain_float_type)
    hidden_all = column_gather(hidden_half)
    att_grad = (
        row_product(hidden_all, output_weight)[0]
        .astype(brain_float_type)
        .reshape(seq_len, heads_here, HEAD_SIZE)
    )
    output_grad = row_fold(attended_flat, hidden_all, None)[0]
    query_grad, key_grad, value_grad = attend_back(
        query_rot, rotated_keys, value_second_part, attended, att_grad, log_total
    )
    query_half = (
        unrotate(query_grad, cosine_values, sine_lookup)
        .astype(brain_float_type)
        .reshape(seq_len, query_cols)
    )
    key_half = unrotate(key_grad[:, None, :], cosine_values, sine_lookup)[:, 0].astype(
        brain_float_type
    )
    value_grad_half = value_grad.astype(brain_float_type)
    proj_grad_half = jnp.concatenate([query_half, key_half, value_grad_half], 1)
    folded_one = row_fold(proj_grad_half, normed_one_all, proj_weight)
    projection_weight_gradient = folded_one[0]
    normed_one_grad = column_sum(folded_one[1])
    proj_bias_grad = folded_one[2]
    input_part, attn_gain_part = norm_backward(normed_one_grad, x_float, rinv_one, attention_gain)
    input_grad = hidden_grad + input_part
    key_value_gradient = jnp.zeros(
        (projection_weight_gradient.shape[0], 2 * KEYVALUE_HEADS * HEAD_SIZE), single_float_type
    )
    key_value_gradient = lax.dynamic_update_slice_in_dim(
        key_value_gradient,
        projection_weight_gradient[:, query_cols : query_cols + HEAD_SIZE],
        key_start,
        1,
    )
    key_value_gradient = lax.dynamic_update_slice_in_dim(
        key_value_gradient, projection_weight_gradient[:, query_cols + HEAD_SIZE :], value_offset, 1
    )
    key_value_bias_gradient = jnp.zeros((2 * KEYVALUE_HEADS * HEAD_SIZE,), single_float_type)
    key_value_bias_gradient = lax.dynamic_update_slice_in_dim(
        key_value_bias_gradient, proj_bias_grad[query_cols : query_cols + HEAD_SIZE], key_start, 0
    )
    key_value_bias_gradient = lax.dynamic_update_slice_in_dim(
        key_value_bias_gradient, proj_bias_grad[query_cols + HEAD_SIZE :], value_offset, 0
    )
    shared = (
        lax.psum(key_value_gradient.astype(jnp.bfloat16), ("dp", "col")).astype(jnp.float32),
        lax.psum(key_value_bias_gradient.astype(jnp.bfloat16), ("dp", "col")).astype(jnp.float32),
        lax.psum(attn_gain_part.astype(jnp.bfloat16), ("dp", "col")).astype(jnp.float32),
        lax.psum(ffn_gain_part.astype(jnp.bfloat16), ("dp", "col")).astype(jnp.float32),
    )
    summed = (
        lax.psum_scatter(
            projection_weight_gradient[:, :query_cols].astype(jnp.bfloat16),
            "dp",
            scatter_dimension=0,
            tiled=True,
        ).astype(jnp.float32),
        lax.psum_scatter(
            proj_bias_grad[:query_cols].astype(jnp.bfloat16), "dp", scatter_dimension=0, tiled=True
        ).astype(jnp.float32),
        lax.psum_scatter(
            output_grad.astype(jnp.bfloat16), "dp", scatter_dimension=0, tiled=True
        ).astype(jnp.float32),
        lax.psum_scatter(
            pair_weight_grad[:, :hidden_cols].astype(jnp.bfloat16),
            "dp",
            scatter_dimension=0,
            tiled=True,
        ).astype(jnp.float32),
        lax.psum_scatter(
            pair_weight_grad[:, hidden_cols:].astype(jnp.bfloat16),
            "dp",
            scatter_dimension=0,
            tiled=True,
        ).astype(jnp.float32),
        lax.psum_scatter(
            down_grad.astype(jnp.bfloat16), "dp", scatter_dimension=0, tiled=True
        ).astype(jnp.float32),
    )
    return (
        block_output.T,
        input_grad.T,
        shared[2],
        summed[0],
        summed[1],
        shared[0],
        shared[1],
        summed[2],
        shared[3],
        summed[3],
        summed[4],
        summed[5],
    )


MESH_ID = pl.DeviceIdType.MESH
F32 = jnp.float32
BF16 = jnp.bfloat16
LINE = 4
BLOCK = 128
LOCAL = LINE * BLOCK
HALF = MODEL_WIDTH // 2
VMEM_SPEC = pl.BlockSpec(memory_space=pltpu.VMEM)
ANY_SPEC = pl.BlockSpec(memory_space=pl.ANY)
PAIR_ROWS = (((0,), (0,)), ((), ()))
PAIR_COLS = (((1,), (1,)), ((), ()))
SCALE = HEAD_SIZE ** (-0.5)


def greet(me, others):
    barrier = pltpu.get_barrier_semaphore()
    for axis, index in others:
        pl.semaphore_signal(barrier, 1, device_id={axis: index}, device_id_type=MESH_ID)

    @pl.when(me > 0)
    def _():
        pl.semaphore_signal(barrier, 1, device_id={"col": me - 1}, device_id_type=MESH_ID)

    @pl.when(me < LINE - 1)
    def _():
        pl.semaphore_signal(barrier, 1, device_id={"col": me + 1}, device_id_type=MESH_ID)

    @pl.when((me > 0) & (me < LINE - 1))
    def _():
        pl.semaphore_wait(barrier, 2 + len(others))

    @pl.when((me == 0) | (me == LINE - 1))
    def _():
        pl.semaphore_wait(barrier, 1 + len(others))


def line_barrier(me):
    greet(me, [])


def block_rows(index):
    return pl.ds(pl.multiple_of(index * BLOCK, BLOCK), BLOCK)


def nothing(*_):
    return None


def send(src, dst, send_sem, recv_sem, axis, to):
    return pltpu.make_async_remote_copy(
        src, dst, send_sem, recv_sem, device_id={axis: to}, device_id_type=MESH_ID
    )


def landed(ref, sem):
    pltpu.make_async_copy(ref, ref, sem).wait()


class Gather:
    def __init__(self, me, rows_of, sends, recv):
        self.me, self.rows_of, self.sends, self.recv = me, rows_of, sends, recv

    def copy(self, j, to, sem):
        rows = self.rows_of(j)
        return send(rows, rows, sem, self.recv.at[j], "col", to)

    def step(self, s):
        me = self.me
        left, right = me - s, me + s

        @pl.when(left >= 0)
        def _():
            if s:
                landed(self.rows_of(left), self.recv.at[left])

            @pl.when(me < LINE - 1)
            def _():
                self.copy(left, me + 1, self.sends.at[0, s]).start()

        @pl.when(right < LINE)
        def _():
            if s:
                landed(self.rows_of(right), self.recv.at[right])

            @pl.when(me > 0)
            def _():
                self.copy(right, me - 1, self.sends.at[1, s]).start()

    def run_each(self, s, each):
        me = self.me

        @pl.when(me - s >= 0)
        def _():
            each(me - s)

        if s:

            @pl.when(me + s < LINE)
            def _():
                each(me + s)

    def drain(self):
        me = self.me
        for s in range(LINE):

            @pl.when((me - s >= 0) & (me < LINE - 1))
            def _():
                self.copy(me, me + 1, self.sends.at[0, s]).wait_send()

            @pl.when((me + s < LINE) & (me > 0))
            def _():
                self.copy(me, me - 1, self.sends.at[1, s]).wait_send()


def gather_line(me, all_ref, sends, recv, each, between=nothing):
    gather = Gather(me, lambda j: all_ref.at[block_rows(j)], sends, recv)
    for s in range(LINE):
        gather.step(s)
        gather.run_each(s, each)
        between(s)
    gather.drain()


class Scatter:
    def __init__(self, me, block_of, from_left, from_right, sends, recv):
        self.me, self.block_of = me, block_of
        self.from_left, self.from_right, self.sends, self.recv = from_left, from_right, sends, recv

    def copy(self, j, to, side):
        landing = self.from_right if side else self.from_left
        return send(
            landing.at[j], landing.at[j], self.sends.at[side, j], self.recv.at[side, j], "col", to
        )

    def arrived(self, j, side):
        landing = self.from_right if side else self.from_left
        landed(landing.at[j], self.recv.at[side, j])

    def step(self, s):
        me = self.me
        ahead, behind = me + s, me - s

        @pl.when(ahead < LINE)
        def _():
            mine = self.block_of(ahead)

            @pl.when(me > 0)
            def _():
                self.arrived(ahead, 0)
                self.from_left[ahead] = (mine + self.from_left[ahead].astype(F32)).astype(BF16)

            @pl.when(me == 0)
            def _():
                self.from_left[ahead] = mine.astype(BF16)

            self.copy(ahead, me + 1, 0).start()

        @pl.when(behind >= 0)
        def _():
            mine = self.block_of(behind)

            @pl.when(me < LINE - 1)
            def _():
                self.arrived(behind, 1)
                self.from_right[behind] = (mine + self.from_right[behind].astype(F32)).astype(BF16)

            @pl.when(me == LINE - 1)
            def _():
                self.from_right[behind] = mine.astype(BF16)

            self.copy(behind, me - 1, 1).start()

    def finish(self, out_ref):
        me = self.me
        out_ref[...] = self.block_of(me)

        @pl.when(me > 0)
        def _():
            self.arrived(me, 0)
            out_ref[...] += self.from_left[me].astype(F32)

        @pl.when(me < LINE - 1)
        def _():
            self.arrived(me, 1)
            out_ref[...] += self.from_right[me].astype(F32)

    def drain(self):
        me = self.me
        for s in range(1, LINE):

            @pl.when(me + s < LINE)
            def _():
                self.copy(me + s, me + 1, 0).wait_send()

            @pl.when(me - s >= 0)
            def _():
                self.copy(me - s, me - 1, 1).wait_send()


def scatter_line(me, block_of, out_ref, from_left, from_right, sends, recv, between=nothing):
    scatter = Scatter(me, block_of, from_left, from_right, sends, recv)
    for s in range(LINE - 1, 0, -1):
        scatter.step(s)
        between(s)
    scatter.finish(out_ref)
    scatter.drain()


def dot(a, b, dims=(((1,), (0,)), ((), ()))):
    return lax.dot_general(a, b, dims, preferred_element_type=F32)


def turn(values):
    return pltpu.roll(values, HEAD_SIZE // 2, 1)


def norm_scale(values):
    return lax.rsqrt(jnp.sum(values * values, -1, keepdims=True) / MODEL_WIDTH + EPS)


def comm_call(body, outs, n_in, scratch, collective_id, flops, name):
    return pl.pallas_call(
        body,
        out_shape=outs,
        in_specs=[VMEM_SPEC] * n_in,
        out_specs=[VMEM_SPEC] * len(outs),
        scratch_shapes=scratch,
        compiler_params=pltpu.CompilerParams(collective_id=collective_id, has_side_effects=True),
        cost_estimate=pl.CostEstimate(flops=flops, bytes_accessed=40_000_000, transcendentals=0),
        name=name,
    )


def gather_scratch():
    return [pltpu.SemaphoreType.DMA((2, LINE)), pltpu.SemaphoreType.DMA((LINE,))]


def scatter_scratch(width=MODEL_WIDTH):
    return [pltpu.VMEM((LINE, BLOCK, width), BF16)] * 2 + [pltpu.SemaphoreType.DMA((2, LINE))] * 2


def attend_local(query_ref, own_ref, other_ref, attended_ref, probs_ref, r):
    rows = 2 * BLOCK
    shape = (rows, rows)
    at_row = lax.broadcasted_iota(jnp.int32, shape, 0)
    at_col = lax.broadcasted_iota(jnp.int32, shape, 1)
    own_mask = at_row >= at_col
    other_mask = at_col // BLOCK < at_row // BLOCK + r
    heads = query_ref.shape[1] // HEAD_SIZE
    for s in range(2):
        part = slice(s * rows, (s + 1) * rows)
        for h in range(heads):
            cols = slice(h * HEAD_SIZE, (h + 1) * HEAD_SIZE)
            query = query_ref[part, cols]
            own = jnp.where(own_mask, dot(query, own_ref[part, :HEAD_SIZE], PAIR_COLS) * SCALE, NEG)
            other = jnp.where(
                other_mask, dot(query, other_ref[part, :HEAD_SIZE], PAIR_COLS) * SCALE, NEG
            )
            top = jnp.maximum(
                jnp.max(own, -1, keepdims=True), jnp.max(other, -1, keepdims=True)
            )
            total = jnp.sum(jnp.exp(own - top), -1, keepdims=True) + jnp.sum(
                jnp.exp(other - top), -1, keepdims=True
            )
            log_total = top + jnp.log(total)
            own = jnp.exp(own - log_total).astype(BF16)
            other = jnp.exp(other - log_total).astype(BF16)
            attended_ref[part, cols] = (
                dot(own, own_ref[part, HEAD_SIZE:]) + dot(other, other_ref[part, HEAD_SIZE:])
            ).astype(BF16)
            probs_ref[s * heads + h, :, :rows] = own
            probs_ref[s * heads + h, :, rows:] = other


def attend_back_body(
    query_ref, own_ref, other_ref, attended_ref, probs_ref, grad_ref, cos_ref, sin_ref,
    query_grad_ref, own_grad_ref, other_grad_ref,
):
    rows = 2 * BLOCK
    heads = query_ref.shape[1] // HEAD_SIZE
    for s in range(2):
        part = slice(s * rows, (s + 1) * rows)
        own_key, other_key = own_ref[part, :HEAD_SIZE], other_ref[part, :HEAD_SIZE]
        own_value, other_value = own_ref[part, HEAD_SIZE:], other_ref[part, HEAD_SIZE:]
        sums = [jnp.zeros((rows, HEAD_SIZE), F32) for _ in range(4)]
        for h in range(heads):
            cols = slice(h * HEAD_SIZE, (h + 1) * HEAD_SIZE)
            query, grad = query_ref[part, cols], grad_ref[part, cols]
            own_p = probs_ref[s * heads + h, :, :rows]
            other_p = probs_ref[s * heads + h, :, rows:]
            delta = jnp.sum(
                grad.astype(F32) * attended_ref[part, cols].astype(F32), -1, keepdims=True
            )
            own_s = (own_p.astype(F32) * (dot(grad, own_value, PAIR_COLS) - delta)).astype(BF16)
            other_s = (other_p.astype(F32) * (dot(grad, other_value, PAIR_COLS) - delta)).astype(BF16)
            query_grad = (dot(own_s, own_key) + dot(other_s, other_key)) * SCALE
            query_grad_ref[part, cols] = (
                query_grad * cos_ref[part] - turn(query_grad) * sin_ref[part]
            ).astype(BF16)
            for i, (weights, partner) in enumerate(
                ((own_s, query), (own_p, grad), (other_s, query), (other_p, grad))
            ):
                sums[i] = sums[i] + dot(weights, partner, PAIR_ROWS)
        own_grad_ref[part, :HEAD_SIZE] = sums[0] * SCALE
        own_grad_ref[part, HEAD_SIZE:] = sums[1]
        other_grad_ref[part, :HEAD_SIZE] = (sums[2] * SCALE).astype(BF16)
        other_grad_ref[part, HEAD_SIZE:] = sums[3].astype(BF16)


def middle_back_body(
    part_ref, mid_ref, cot_ref, gain_ref, own_ref, other_ref,
    mid_grad_ref, gain_grad_ref, all_ref, att_grad_ref,
    from_left, from_right, s_sends, s_recv, sends, recv,
):
    me = lax.axis_index("col")
    line_barrier(me)
    scatter_line(
        me, lambda j: part_ref[block_rows(j)].astype(F32), mid_grad_ref,
        from_left, from_right, s_sends, s_recv,
    )
    mid, grad = mid_ref[...], mid_grad_ref[...]
    rinv = norm_scale(mid)
    gain_grad_ref[...] = jnp.sum(grad * mid * rinv, 0, keepdims=True)
    scaled = grad * gain_ref[...]
    inner = jnp.sum(scaled * mid, -1, keepdims=True)
    mid_grad = cot_ref[...].astype(F32) + rinv * scaled - mid * rinv**3 * inner / MODEL_WIDTH
    mid_grad_ref[...] = mid_grad
    all_ref[block_rows(me)] = mid_grad.astype(BF16)

    def each(j):
        block = all_ref[block_rows(j)]
        att_grad_ref[block_rows(j)] = (
            dot(block[:, :HALF], own_ref[...]) + dot(block[:, HALF:], other_ref[...])
        ).astype(BF16)

    gather_line(me, all_ref, sends, recv, each)


def input_back_body(
    query_grad_ref, own_kv_ref, got_kv_ref, cos_ref, sin_ref, own_ref, other_ref, x_ref, gain_ref,
    mid_grad_ref, proj_grad_ref, bias_ref, input_grad_ref, gain_grad_ref,
    from_left, from_right, s_sends, s_recv,
):
    me = lax.axis_index("col")
    line_barrier(me)
    query_cols = query_grad_ref.shape[1]
    kv = own_kv_ref[...] + got_kv_ref[...].astype(F32)
    key = kv[:, :HEAD_SIZE]
    proj_grad_ref[:, :query_cols] = query_grad_ref[...]
    proj_grad_ref[:, query_cols : query_cols + HEAD_SIZE] = (
        key * cos_ref[...] - turn(key) * sin_ref[...]
    ).astype(BF16)
    proj_grad_ref[:, query_cols + HEAD_SIZE :] = kv[:, HEAD_SIZE:].astype(BF16)

    def block_of(j):
        block = proj_grad_ref[block_rows(j)]
        return jnp.concatenate(
            [dot(block, own_ref[...], PAIR_COLS), dot(block, other_ref[...], PAIR_COLS)], 1
        )

    scatter_line(me, block_of, input_grad_ref, from_left, from_right, s_sends, s_recv)
    bias_ref[...] = jnp.sum(proj_grad_ref[...].astype(F32), 0, keepdims=True)
    x, grad = x_ref[...].astype(F32), input_grad_ref[...]
    rinv = norm_scale(x)
    gain_grad_ref[...] = jnp.sum(grad * x * rinv, 0, keepdims=True)
    scaled = grad * gain_ref[...]
    inner = jnp.sum(scaled * x, -1, keepdims=True)
    input_grad_ref[...] = mid_grad_ref[...] + rinv * scaled - x * rinv**3 * inner / MODEL_WIDTH


def feed_body(
    normed_ref, cot_ref, gate_hbm, upper_hbm, down_hbm, other_hbm,
    activated_ref, gate_grad_ref, upper_grad_ref, back_ref, out_ref,
    weights, back_sum, out_sum, sems,
):
    hidden = activated_ref.shape[1]
    tile = 256
    chunk = 2 * tile
    lows = list(range(0, hidden, chunk))

    def copies(k):
        rows = pl.ds(lows[k], min(chunk, hidden - lows[k]))
        for i, own in enumerate((gate_hbm, upper_hbm, down_hbm)):
            yield pltpu.make_async_copy(
                own.at[rows], weights.at[i, rows, pl.ds(0, HALF)], sems.at[k, i, 0]
            )
            yield pltpu.make_async_copy(
                other_hbm.at[i, rows], weights.at[i, rows, pl.ds(HALF, HALF)], sems.at[k, i, 1]
            )

    for k in range(len(lows)):
        for copy in copies(k):
            copy.start()
    back_sum[...] = jnp.zeros_like(back_sum)
    out_sum[...] = jnp.zeros_like(out_sum)

    def run(low, size):
        rows = pl.ds(low, size)
        gate = dot(normed_ref[...], weights[0, rows], PAIR_COLS)
        upper = dot(normed_ref[...], weights[1, rows], PAIR_COLS)
        act_grad = dot(cot_ref[...], weights[2, rows], PAIR_COLS)
        sig = jax.nn.sigmoid(gate)
        silu = gate * sig
        activated = (silu * upper).astype(BF16)
        gate_grad = (act_grad * upper * sig * (1.0 + gate * (1.0 - sig))).astype(BF16)
        upper_grad = (act_grad * silu).astype(BF16)
        activated_ref[:, rows] = activated
        gate_grad_ref[:, rows] = gate_grad
        upper_grad_ref[:, rows] = upper_grad
        back_sum[...] += dot(gate_grad, weights[0, rows]) + dot(upper_grad, weights[1, rows])
        out_sum[...] += dot(activated, weights[2, rows])

    for k, low in enumerate(lows):
        for copy in copies(k):
            copy.wait()
        if low + chunk <= hidden:

            @pl.loop(0, 2)
            def _(t):
                run(pl.multiple_of(low + t * tile, tile), tile)
        else:
            run(low, hidden - low)
    back_ref[...] = back_sum[...].astype(BF16)
    out_ref[...] = out_sum[...].astype(BF16)


def shape(rows, cols, dtype=BF16):
    return jax.ShapeDtypeStruct((rows, cols), dtype)


def swap(values, axis, bit):
    size = lax.axis_size(axis)
    return lax.ppermute(values, axis, [(i, i ^ bit) for i in range(size)])


def reduce_blocks(grad, x_first):
    y, core = lax.axis_index("dp") // 2, lax.axis_index("dp") % 2
    width = grad.shape[1]
    parts = grad.reshape(2, 2, 2, MODEL_WIDTH // 8, width)
    pick = lambda index: lax.dynamic_index_in_dim(parts, index, 2, keepdims=False)
    part = pick(core).astype(F32) + swap(pick(1 - core), "dp", 1).astype(F32)
    part = part.astype(BF16)
    choose = lambda index: lax.dynamic_index_in_dim(part, index, 1, keepdims=False)
    if x_first:
        half = (part[0].astype(F32) + swap(part[1], "row", 1).astype(F32)).astype(BF16)
        choose = lambda index: lax.dynamic_index_in_dim(half, index, 0, keepdims=False)
        return choose(y).astype(F32) + swap(choose(1 - y), "dp", 2).astype(F32)
    half = (choose(y).astype(F32) + swap(choose(1 - y), "dp", 2).astype(F32)).astype(BF16)
    return half[0].astype(F32) + swap(half[1], "row", 1).astype(F32)


PIECES = 6


def front_body(
    keep_ref, pass_ref, cot_keep_ref, cot_pass_ref, table_ref, gains_ref, bias_ref, proj_ref,
    gate_hbm, upper_hbm, down_hbm,
    x_ref, normed_ref, query_ref, kv_ref, kv_other_ref, cos_ref, sin_ref, all_gains_ref,
    attended_ref, probs_ref, mid_ref, normed_two_ref, cot_ref, proj_other_ref, weights_other_hbm,
    tables, from_left, from_right,
    swap_sends, swap_recv, piece_sends, piece_recv, kv_sends, kv_recv,
    g_sends, g_recv, c_sends, c_recv, n_sends, n_recv, s_sends, s_recv,
):
    me, r, d = lax.axis_index("col"), lax.axis_index("row"), lax.axis_index("dp")
    y, core = d // 2, lax.rem(d, 2)
    x_to, y_to, core_to = 1 - r, 2 * (1 - y) + core, 2 * y + 1 - core
    greet(me, [("row", x_to), ("dp", y_to), ("dp", core_to)])
    proj_cols = bias_ref.shape[1]
    query_cols = query_ref.shape[1]
    quarter = HALF // 2
    my_rows = pl.ds(pl.multiple_of(core * quarter, quarter), quarter)
    its_rows = pl.ds(pl.multiple_of((1 - core) * quarter, quarter), quarter)

    swaps = [
        (pass_ref, x_ref.at[:, HALF:], "row", x_to),
        (table_ref.at[1], tables.at[1], "row", x_to),
        (gains_ref, all_gains_ref.at[:, HALF:], "row", x_to),
        (proj_ref.at[my_rows, :proj_cols], proj_other_ref.at[my_rows, :proj_cols], "row", x_to),
        (cot_pass_ref, cot_ref.at[block_rows(me), HALF:], "row", x_to),
        (proj_ref.at[my_rows, proj_cols:], proj_other_ref.at[my_rows, proj_cols:], "row", x_to),
        (
            proj_other_ref.at[my_rows, :proj_cols], proj_other_ref.at[my_rows, :proj_cols],
            "dp", core_to,
        ),
        (
            proj_other_ref.at[my_rows, proj_cols:], proj_other_ref.at[my_rows, proj_cols:],
            "dp", core_to,
        ),
    ]

    def swap_copy(i):
        src, dst, axis, to = swaps[i]
        return send(src, dst, swap_sends.at[i], swap_recv.at[i], axis, to)

    def swap_landed(i):
        swap_copy(i).wait_recv()

    rows = gate_hbm.shape[0] // 4
    owns = (gate_hbm, upper_hbm, down_hbm)
    my_cols = my_rows

    def piece(i, of_y):
        return pl.ds(pl.multiple_of((of_y * 2 + i % 2) * rows, rows), rows)

    def piece_copy(i, way):
        m = i // 2
        of_y = y if way in (0, 1, 2) else 1 - y
        at = weights_other_hbm.at[m, piece(i, of_y), my_cols]
        src = owns[m].at[piece(i, of_y), my_cols] if way == 0 else at
        axis, to = (("row", x_to), ("dp", y_to), ("dp", core_to), ("dp", core_to))[way]
        return send(src, at, piece_sends.at[way, i], piece_recv.at[way, i], axis, to)

    def relay_x(i):
        piece_copy(i, 0).wait_recv()
        piece_copy(i, 1).start()
        piece_copy(i, 2).start()

    def relay_y(i):
        piece_copy(i, 1).wait_recv()
        piece_copy(i, 3).start()

    for i in range(5):
        swap_copy(i).start()
    piece_copy(0, 0).start()
    x_ref[:, :HALF] = keep_ref[...]
    tables[0] = table_ref[0]
    all_gains_ref[:, :HALF] = gains_ref[...]
    cot_ref[block_rows(me), :HALF] = cot_keep_ref[...]
    swap_landed(0)
    swap_landed(1)
    swap_landed(2)
    x = x_ref[...].astype(F32)
    normed_ref[block_rows(me)] = (x * norm_scale(x) * all_gains_ref[0:1]).astype(BF16)
    gather = Gather(me, lambda j: normed_ref.at[block_rows(j)], g_sends, g_recv)
    gather.step(0)

    lane = lax.broadcasted_iota(jnp.int32, (2 * BLOCK, HEAD_SIZE), 1)
    first = lane < HEAD_SIZE // 2
    for i in range(2):
        table = tables[i]
        turned = turn(table)
        at = pl.ds(pl.multiple_of((r if i == 0 else 1 - r) * 2 * BLOCK, BLOCK), 2 * BLOCK)
        cos_ref[at] = jnp.where(first, table, turned)
        sin_ref[at] = jnp.where(first, -turned, table)

    swap_landed(3)
    swap_copy(6).start()
    swap_landed(6)

    def kv_copy(j):
        at = block_rows(j)
        return send(
            kv_ref.at[at], kv_other_ref.at[at], kv_sends.at[j], kv_recv.at[j], "row", x_to
        )

    def each(j):
        at = block_rows(j)
        block = normed_ref[at]
        out = dot(block[:, :HALF], proj_ref[:, :proj_cols])
        out = out + dot(block[:, HALF:], proj_other_ref[:, :proj_cols]) + bias_ref[...]
        cosine, sine = cos_ref[at], sin_ref[at]
        for h in range(query_cols // HEAD_SIZE + 1):
            head = out[:, h * HEAD_SIZE : (h + 1) * HEAD_SIZE]
            turned = (head * cosine + turn(head) * sine).astype(BF16)
            if h * HEAD_SIZE < query_cols:
                query_ref[at, h * HEAD_SIZE : (h + 1) * HEAD_SIZE] = turned
            else:
                kv_ref[at, :HEAD_SIZE] = turned
        kv_ref[at, HEAD_SIZE:] = out[:, query_cols + HEAD_SIZE :].astype(BF16)
        kv_copy(j).start()

    for s in range(LINE):
        if s:
            gather.step(s)
        gather.run_each(s, each)
    swap_copy(5).start()
    for i in range(1, PIECES):
        piece_copy(i, 0).start()
    swap_landed(4)
    cot_gather = Gather(me, lambda j: cot_ref.at[block_rows(j)], c_sends, c_recv)
    cot_gather.step(0)
    relay_x(0)
    for j in range(LINE):
        kv_copy(j).wait_recv()
    attend_local(query_ref, kv_ref, kv_other_ref, attended_ref, probs_ref, r)
    swap_landed(5)
    swap_copy(7).start()
    relay_y(0)
    swap_landed(7)

    def block_of(j):
        block = attended_ref[block_rows(j)]
        return jnp.concatenate(
            [
                dot(block, proj_ref[:, proj_cols:], PAIR_COLS),
                dot(block, proj_other_ref[:, proj_cols:], PAIR_COLS),
            ],
            1,
        )

    scatter = Scatter(me, block_of, from_left, from_right, s_sends, s_recv)
    scatter.step(3)
    scatter.step(2)
    relay_x(1)
    scatter.step(1)
    scatter.finish(mid_ref)
    mid = mid_ref[...] + x_ref[...].astype(F32)
    mid_ref[...] = mid
    normed_two_ref[block_rows(me)] = (mid * norm_scale(mid) * all_gains_ref[1:2]).astype(BF16)
    second = Gather(me, lambda j: normed_two_ref.at[block_rows(j)], n_sends, n_recv)
    second.step(0)
    relay_x(2)
    relay_y(1)
    second.step(1)
    relay_x(3)
    relay_y(2)
    second.step(2)
    relay_x(4)
    relay_y(3)
    second.step(3)
    cot_gather.step(1)
    cot_gather.step(2)
    relay_x(5)
    relay_y(4)
    cot_gather.step(3)
    relay_y(5)
    for i in range(PIECES):
        for way in (2, 3):
            of_y = y if way == 2 else 1 - y
            landed(weights_other_hbm.at[i // 2, piece(i, of_y), its_rows], piece_recv.at[way, i])
        for way in range(4):
            piece_copy(i, way).wait_send()
    for i in range(len(swaps)):
        swap_copy(i).wait_send()
    for j in range(LINE):
        kv_copy(j).wait_send()
    gather.drain()
    cot_gather.drain()
    second.drain()
    scatter.drain()


def front_call(proj_cols, query_cols, hidden, *args):
    heads = query_cols // HEAD_SIZE
    outs = [
        shape(BLOCK, MODEL_WIDTH),
        shape(LOCAL, MODEL_WIDTH),
        shape(LOCAL, query_cols),
        shape(LOCAL, 2 * HEAD_SIZE),
        shape(LOCAL, 2 * HEAD_SIZE),
        shape(LOCAL, HEAD_SIZE, F32),
        shape(LOCAL, HEAD_SIZE, F32),
        shape(8, MODEL_WIDTH, F32),
        shape(LOCAL, query_cols),
        jax.ShapeDtypeStruct((2 * heads, 2 * BLOCK, 4 * BLOCK), BF16),
        shape(BLOCK, MODEL_WIDTH, F32),
        shape(LOCAL, MODEL_WIDTH),
        shape(LOCAL, MODEL_WIDTH),
        shape(HALF, proj_cols + query_cols),
        jax.ShapeDtypeStruct((3, hidden, HALF), BF16),
    ]
    dma = pltpu.SemaphoreType.DMA
    return pl.pallas_call(
        front_body,
        out_shape=outs,
        in_specs=[VMEM_SPEC] * 8 + [ANY_SPEC] * 3,
        out_specs=[VMEM_SPEC] * (len(outs) - 1) + [ANY_SPEC],
        scratch_shapes=[
            pltpu.VMEM((2, 2 * BLOCK, HEAD_SIZE), F32),
            pltpu.VMEM((LINE, BLOCK, MODEL_WIDTH), BF16),
            pltpu.VMEM((LINE, BLOCK, MODEL_WIDTH), BF16),
            dma((8,)),
            dma((8,)),
            dma((4, PIECES)),
            dma((4, PIECES)),
            dma((LINE,)),
            dma((LINE,)),
        ]
        + [dma((2, LINE)), dma((LINE,))] * 3
        + [dma((2, LINE)), dma((2, LINE))],
        compiler_params=pltpu.CompilerParams(
            collective_id=1, has_side_effects=True, vmem_limit_bytes=60 * 1024 * 1024
        ),
        cost_estimate=pl.CostEstimate(
            flops=4 * 10**9, bytes_accessed=40_000_000, transcendentals=0
        ),
        name="front",
    )(*args)


def fast_device(
    block_input,
    position_ids,
    attention_gain,
    query_weight,
    query_bias,
    key_value_weight,
    key_value_bias,
    output_weight,
    feedforward_gain,
    gate_weight,
    upper_weight,
    down_weight,
    out_cotangent,
):
    r, c = lax.axis_index("row"), lax.axis_index("col")
    query_cols = query_weight.shape[1]
    hidden = gate_weight.shape[1]
    proj_cols = query_cols + 2 * HEAD_SIZE
    kv_head = c // (LINE // KEYVALUE_HEADS)
    key_start = kv_head * HEAD_SIZE
    value_start = (KEYVALUE_HEADS + kv_head) * HEAD_SIZE

    def parts(values):
        turned = values.T.reshape(2, BLOCK, HALF)
        pick = lambda i: lax.dynamic_index_in_dim(turned, i, 0, keepdims=False)
        return pick(r), pick(1 - r)

    x_keep, x_pass = parts(block_input)
    cot_keep, cot_pass = parts(out_cotangent)
    frequencies = THETA ** (-(jnp.arange(HEAD_SIZE // 2, dtype=F32) * 2.0 / HEAD_SIZE))
    angles = position_ids.astype(F32)[:, None] * frequencies[None, :]
    table = jnp.concatenate([jnp.cos(angles), jnp.sin(angles)], -1).reshape(2, 2, BLOCK, HEAD_SIZE)
    pick = lambda i: lax.dynamic_index_in_dim(table, i, 1, keepdims=False)
    table = jnp.stack([pick(r), pick(1 - r)]).reshape(2, 2 * BLOCK, HEAD_SIZE)
    gains = jnp.concatenate(
        [attention_gain[None], feedforward_gain[None], jnp.zeros((6, HALF), F32)]
    )
    own_proj = jnp.concatenate(
        [
            query_weight,
            lax.dynamic_slice_in_dim(key_value_weight, key_start, HEAD_SIZE, 1),
            lax.dynamic_slice_in_dim(key_value_weight, value_start, HEAD_SIZE, 1),
            output_weight,
        ],
        1,
    )
    proj_bias = jnp.concatenate(
        [
            query_bias,
            lax.dynamic_slice_in_dim(key_value_bias, key_start, HEAD_SIZE, 0),
            lax.dynamic_slice_in_dim(key_value_bias, value_start, HEAD_SIZE, 0),
        ]
    )[None]
    (
        x_own, normed_one, query_rot, kv_own, kv_other, cosine, sine, all_gains, attended, probs,
        mid, normed_two, cot_all, other_proj, ffn_other,
    ) = front_call(
        proj_cols, query_cols, hidden,
        x_keep, x_pass, cot_keep, cot_pass, table, gains, proj_bias, own_proj,
        gate_weight.T, upper_weight.T, down_weight.T,
    )
    attn_gain, ffn_gain = all_gains[:1], all_gains[1:2]
    own_in, own_out = own_proj[:, :proj_cols], own_proj[:, proj_cols:]
    other_in, other_out = other_proj[:, :proj_cols], other_proj[:, proj_cols:]
    cot_own = lax.dynamic_slice_in_dim(cot_all, c * BLOCK, BLOCK, 0)
    activated, gate_grad, upper_grad, back_part, out_part = pl.pallas_call(
        feed_body,
        out_shape=[shape(LOCAL, hidden)] * 3 + [shape(LOCAL, MODEL_WIDTH)] * 2,
        in_specs=[VMEM_SPEC] * 2 + [ANY_SPEC] * 4,
        out_specs=[VMEM_SPEC] * 5,
        scratch_shapes=[
            pltpu.VMEM((3, hidden, MODEL_WIDTH), BF16),
            pltpu.VMEM((LOCAL, MODEL_WIDTH), F32),
            pltpu.VMEM((LOCAL, MODEL_WIDTH), F32),
            pltpu.SemaphoreType.DMA((8, 3, 2)),
        ],
        cost_estimate=pl.CostEstimate(
            flops=2 * 10**10, bytes_accessed=40_000_000, transcendentals=0
        ),
        name="feed",
    )(normed_two, cot_all, gate_weight.T, upper_weight.T, down_weight.T, ffn_other)
    out_own = lax.psum_scatter(out_part, "col", scatter_dimension=0, tiled=True).astype(F32) + mid
    down_grad = lax.dot_general(cot_all, activated, PAIR_ROWS, preferred_element_type=F32).astype(
        BF16
    )
    gate_w_grad = lax.dot_general(
        normed_two, gate_grad, PAIR_ROWS, preferred_element_type=F32
    ).astype(BF16)
    upper_w_grad = lax.dot_general(
        normed_two, upper_grad, PAIR_ROWS, preferred_element_type=F32
    ).astype(BF16)
    mid_grad, ffn_gain_part, mid_half, att_grad = comm_call(
        middle_back_body,
        [
            shape(BLOCK, MODEL_WIDTH, F32),
            shape(1, MODEL_WIDTH, F32),
            shape(LOCAL, MODEL_WIDTH),
            shape(LOCAL, query_cols),
        ],
        6,
        scatter_scratch() + gather_scratch(),
        3,
        10**9,
        "middle_back",
    )(back_part, mid, cot_own, ffn_gain, own_out, other_out)
    query_grad, kv_grad_own, kv_grad_other = pl.pallas_call(
        attend_back_body,
        out_shape=[
            shape(LOCAL, query_cols),
            shape(LOCAL, 2 * HEAD_SIZE, F32),
            shape(LOCAL, 2 * HEAD_SIZE),
        ],
        in_specs=[VMEM_SPEC] * 8,
        out_specs=[VMEM_SPEC] * 3,
        cost_estimate=pl.CostEstimate(flops=10**9, bytes_accessed=20_000_000, transcendentals=0),
        name="attend_back",
    )(query_rot, kv_own, kv_other, attended, probs, att_grad, cosine, sine)
    kv_grad_got = swap(kv_grad_other, "row", 1)
    output_w_grad = lax.dot_general(
        mid_half, attended, PAIR_ROWS, preferred_element_type=F32
    ).astype(BF16)
    proj_grad, bias_part, input_grad, attn_gain_part = comm_call(
        input_back_body,
        [
            shape(LOCAL, proj_cols),
            shape(1, proj_cols, F32),
            shape(BLOCK, MODEL_WIDTH, F32),
            shape(1, MODEL_WIDTH, F32),
        ],
        10,
        scatter_scratch(),
        4,
        10**9,
        "input_back",
    )(
        query_grad, kv_grad_own, kv_grad_got, cosine, sine, own_in, other_in, x_own, attn_gain,
        mid_grad,
    )
    proj_w_grad = lax.dot_general(
        normed_one, proj_grad, PAIR_ROWS, preferred_element_type=F32
    ).astype(BF16)

    down_sum = reduce_blocks(down_grad, True)
    gate_sum = reduce_blocks(gate_w_grad, False)
    upper_sum = reduce_blocks(upper_w_grad, True)
    output_sum = reduce_blocks(output_w_grad, False)
    proj_sum = reduce_blocks(proj_w_grad, True)

    kv_sum = lax.all_gather(proj_sum[:, query_cols:].astype(BF16), "col", axis=0, tiled=False)
    group = LINE // KEYVALUE_HEADS
    kv_sum = kv_sum.reshape(KEYVALUE_HEADS, group, -1, 2, HEAD_SIZE).astype(F32).sum(1)
    kv_sum = jnp.transpose(kv_sum, (1, 2, 0, 3)).reshape(-1, 2 * KEYVALUE_HEADS * HEAD_SIZE)
    kv_weight_grad = lax.all_gather(kv_sum.astype(BF16), "dp", axis=0, tiled=True).astype(F32)

    swapped = lambda v: jnp.where(r == 0, v, jnp.roll(v, HALF))
    spread = jnp.zeros((2 * KEYVALUE_HEADS * HEAD_SIZE,), F32)
    spread = lax.dynamic_update_slice(
        spread, bias_part[0, query_cols : query_cols + HEAD_SIZE], (key_start,)
    )
    spread = lax.dynamic_update_slice(spread, bias_part[0, query_cols + HEAD_SIZE :], (value_start,))
    query_spread = lax.dynamic_update_slice(
        jnp.zeros((LINE * query_cols,), F32), bias_part[0, :query_cols], (c * query_cols,)
    )
    vector = jnp.concatenate(
        [swapped(attn_gain_part[0]), swapped(ffn_gain_part[0]), spread, query_spread]
    )
    vector = lax.psum(vector, ("dp", "row", "col"))
    attn_gain_grad = lax.dynamic_slice_in_dim(vector, r * HALF, HALF, 0)
    ffn_gain_grad = lax.dynamic_slice_in_dim(vector, MODEL_WIDTH + r * HALF, HALF, 0)
    kv_bias_grad = vector[2 * MODEL_WIDTH : 2 * MODEL_WIDTH + spread.shape[0]]
    bias_rows = query_cols // lax.axis_size("dp")
    query_bias_grad = lax.dynamic_slice_in_dim(
        vector,
        2 * MODEL_WIDTH + spread.shape[0] + c * query_cols + lax.axis_index("dp") * bias_rows,
        bias_rows,
        0,
    )

    def returned(values):
        got = swap(values[:, HALF:].astype(BF16), "row", 1).astype(F32)
        keep = values[:, :HALF]
        pair = jnp.where(
            r == 0, jnp.concatenate([keep, got]), jnp.concatenate([got, keep])
        )
        return pair.T

    return (
        returned(out_own),
        returned(input_grad),
        attn_gain_grad,
        proj_sum[:, :query_cols],
        query_bias_grad,
        kv_weight_grad,
        kv_bias_grad,
        output_sum,
        ffn_gain_grad,
        gate_sum,
        upper_sum,
        down_sum,
    )


def per_device(*arrays):
    sizes = tuple(lax.axis_size(axis) for axis in ("dp", "row", "col"))
    if sizes == (4, 2, LINE) and arrays[0].shape == (HALF, 2 * BLOCK):
        return fast_device(*arrays)
    return general_device(*arrays)


def solution(mesh):
    placed = (
        P("row", ("dp", "col")),
        P(("dp", "row")),
        P("row"),
        P("row", "col"),
        P("col"),
        P("row", None),
        P(),
        P("row", "col"),
        P("row"),
        P("row", "col"),
        P("row", "col"),
        P("row", "col"),
        P("row", ("dp", "col")),
    )
    return jax.shard_map(
        per_device,
        mesh=mesh,
        in_specs=placed,
        out_specs=(
            P("row", ("dp", "col")),
            P("row", ("dp", "col")),
            P("row"),
            P(("row", "dp"), "col"),
            P(("col", "dp")),
            P("row", None),
            P(),
            P(("row", "dp"), "col"),
            P("row"),
            P(("row", "dp"), "col"),
            P(("row", "dp"), "col"),
            P(("row", "dp"), "col"),
        ),
        check_vma=False,
    )
```

```python
import jax
import jax.numpy as jnp
from jax import lax
from jax.experimental import pallas as pl
from jax.experimental.pallas import tpu as pltpu
from jax.sharding import PartitionSpec as P

MODEL_WIDTH = 1536
KEYVALUE_HEADS = 2
HEAD_SIZE = 128


EPS = 1e-06
THETA = 1000000.0
NEG = -1e30


def rope_tables(position_ids):
    half_dim = HEAD_SIZE // 2
    frequencies = THETA ** (-(jnp.arange(half_dim, dtype=jnp.float32) * 2.0 / HEAD_SIZE))
    angles = position_ids.astype(jnp.float32)[:, None] * frequencies[None, :]
    cosine_values = jnp.cos(angles)
    sine_lookup = jnp.sin(angles)
    return (
        jnp.concatenate([cosine_values, cosine_values], -1),
        jnp.concatenate([sine_lookup, sine_lookup], -1),
    )


def apply_rotation(values, cosine_values, sine_lookup):
    half_dim = HEAD_SIZE // 2
    turned = jnp.concatenate([-values[..., half_dim:], values[..., :half_dim]], -1)
    return values * cosine_values[:, None, :] + turned * sine_lookup[:, None, :]


def unrotate(gradient, cosine_values, sine_lookup):
    half_dim = HEAD_SIZE // 2
    scaled = gradient * sine_lookup[:, None, :]
    turned = jnp.concatenate([scaled[..., half_dim:], -scaled[..., :half_dim]], -1)
    return gradient * cosine_values[:, None, :] + turned


def row_total(partial_value):
    return lax.psum(partial_value, "row")


def norm_forward(x_float, gain):
    squares = jnp.sum(x_float * x_float, -1)
    rinv = lax.rsqrt(row_total(squares) / MODEL_WIDTH + EPS)[:, None]
    return ((x_float * rinv * gain).astype(jnp.bfloat16), rinv)


def norm_backward(normed_grad, x_float, rinv, gain):
    scaled = normed_grad * gain
    inner = row_total(jnp.sum(scaled * x_float, -1))[:, None]
    input_part = rinv * scaled - x_float * rinv**3 * inner / MODEL_WIDTH
    gain_part = jnp.sum(normed_grad * x_float * rinv, 0)
    return (input_part, gain_part)


def column_gather(values):
    return lax.all_gather(values, "col", axis=0, tiled=True)


def column_sum(partial_value):
    return lax.psum_scatter(
        partial_value.astype(jnp.bfloat16), "col", scatter_dimension=0, tiled=True
    ).astype(jnp.float32)


def row_product(gathered, weight):
    return (
        lax.psum_scatter(
            jnp.dot(gathered, weight, preferred_element_type=jnp.float32).astype(jnp.bfloat16),
            "row",
            scatter_dimension=0,
            tiled=True,
        ).astype(jnp.float32),
        gathered,
    )


def row_project(local_part, weight):
    return lax.dot_general(
        lax.all_gather(local_part, "row", axis=0, tiled=True),
        weight,
        (((1,), (1,)), ((), ())),
        preferred_element_type=jnp.float32,
    )


def row_fold(local_part, partner, weight):
    pair_dims = (((0,), (0,)), ((), ()))

    def accumulate(block_rows):
        grad_sum = lax.dot_general(
            partner, block_rows, pair_dims, preferred_element_type=jnp.float32
        )
        if weight is None:
            return (grad_sum,)
        back_proj = lax.dot_general(
            block_rows, weight, (((1,), (1,)), ((), ())), preferred_element_type=jnp.float32
        )
        column_totals = jnp.sum(block_rows, 0, dtype=jnp.float32)
        return (grad_sum, back_proj, column_totals)

    return accumulate(lax.all_gather(local_part, "row", axis=0, tiled=True))


def causal_scores(query_rot, rotated_keys):
    scores = jnp.einsum(
        "ihd,jd->hij", query_rot, rotated_keys, preferred_element_type=jnp.float32
    ) * HEAD_SIZE ** (-0.5)
    length = query_rot.shape[0]
    allowed = jnp.arange(length)[:, None] >= jnp.arange(length)[None, :]
    return jnp.where(allowed[None], scores, NEG)


def attend(query_rot, rotated_keys, value_second_part):
    scores = causal_scores(query_rot, rotated_keys)
    row_max = jnp.max(scores, -1, keepdims=True)
    log_total = row_max + jnp.log(jnp.sum(jnp.exp(scores - row_max), -1, keepdims=True))
    probs_half = jnp.exp(scores - log_total).astype(jnp.bfloat16)
    attended = jnp.einsum(
        "hij,jd->ihd", probs_half, value_second_part, preferred_element_type=jnp.float32
    ).astype(jnp.bfloat16)
    return (attended, log_total)


def attend_back(query_rot, rotated_keys, value_second_part, attended, att_grad, log_total):
    scale = HEAD_SIZE ** (-0.5)
    softmax_probs = jnp.exp(causal_scores(query_rot, rotated_keys) - log_total)
    probs_half = softmax_probs.astype(jnp.bfloat16)
    prob_grad = jnp.einsum(
        "ihd,jd->hij", att_grad, value_second_part, preferred_element_type=jnp.float32
    )
    row_delta = jnp.einsum("ihd,ihd->hi", att_grad, attended, preferred_element_type=jnp.float32)
    score_half = (softmax_probs * (prob_grad - row_delta[:, :, None])).astype(jnp.bfloat16)
    query_grad = (
        jnp.einsum("hij,jd->ihd", score_half, rotated_keys, preferred_element_type=jnp.float32)
        * scale
    )
    key_grad = (
        jnp.einsum("hij,ihd->jd", score_half, query_rot, preferred_element_type=jnp.float32) * scale
    )
    value_grad = jnp.einsum("hij,ihd->jd", probs_half, att_grad, preferred_element_type=jnp.float32)
    return (query_grad, key_grad, value_grad)


def general_device(
    block_input,
    position_ids,
    attention_gain,
    query_weight,
    query_bias,
    key_value_weight,
    key_value_bias,
    output_weight,
    feedforward_gain,
    gate_weight,
    upper_weight,
    down_weight,
    out_cotangent,
):
    single_float_type = jnp.float32
    brain_float_type = jnp.bfloat16
    column_number = lax.axis_size("col")
    seq_len = position_ids.shape[0]
    heads_here = query_weight.shape[1] // HEAD_SIZE
    query_cols = query_weight.shape[1]
    hidden_cols = gate_weight.shape[1]
    key_value_head = lax.axis_index("col") // (column_number // KEYVALUE_HEADS)
    key_start = key_value_head * HEAD_SIZE
    value_offset = KEYVALUE_HEADS * HEAD_SIZE + key_value_head * HEAD_SIZE
    keyval_local = jnp.concatenate(
        [
            lax.dynamic_slice_in_dim(key_value_weight, key_start, HEAD_SIZE, 1),
            lax.dynamic_slice_in_dim(key_value_weight, value_offset, HEAD_SIZE, 1),
        ],
        1,
    )
    bias_local = jnp.concatenate(
        [
            lax.dynamic_slice_in_dim(key_value_bias, key_start, HEAD_SIZE, 0),
            lax.dynamic_slice_in_dim(key_value_bias, value_offset, HEAD_SIZE, 0),
        ],
        0,
    )
    proj_weight = jnp.concatenate([query_weight, keyval_local], 1)
    proj_bias = jnp.concatenate([query_bias, bias_local], 0)
    pair_weight = jnp.concatenate([gate_weight, upper_weight], 1)
    cosine_values, sine_lookup = rope_tables(position_ids)
    x_float = block_input.T.astype(single_float_type)
    cot_local = out_cotangent.T
    normed_one, rinv_one = norm_forward(x_float, attention_gain)
    normed_one_all = column_gather(normed_one)
    proj_out = row_product(normed_one_all, proj_weight)[0] + proj_bias
    query_rot = apply_rotation(
        proj_out[:, :query_cols].reshape(seq_len, heads_here, HEAD_SIZE), cosine_values, sine_lookup
    ).astype(brain_float_type)
    rotated_keys = apply_rotation(
        proj_out[:, query_cols : query_cols + HEAD_SIZE][:, None, :], cosine_values, sine_lookup
    )[:, 0].astype(brain_float_type)
    value_second_part = proj_out[:, query_cols + HEAD_SIZE :].astype(brain_float_type)
    attended, log_total = attend(query_rot, rotated_keys, value_second_part)
    attended_flat = attended.reshape(seq_len, query_cols)
    hidden_res = x_float + column_sum(row_project(attended_flat, output_weight))
    normed_two, rinv_two = norm_forward(hidden_res, feedforward_gain)
    normed_two_all = column_gather(normed_two)
    gate_upper, normed_two_seq = row_product(normed_two_all, pair_weight)
    gate_lin = gate_upper[:, :hidden_cols]
    upper_lin = gate_upper[:, hidden_cols:]
    sigmoid_gate = jax.nn.sigmoid(gate_lin)
    activated = (gate_lin * sigmoid_gate * upper_lin).astype(brain_float_type)
    block_output = hidden_res + column_sum(row_project(activated, down_weight))
    cotangent_all = column_gather(cot_local)
    act_grad = row_product(cotangent_all, down_weight)[0]
    down_grad = row_fold(activated, cotangent_all, None)[0]
    gate_grad = act_grad * upper_lin * sigmoid_gate * (1.0 + gate_lin * (1.0 - sigmoid_gate))
    upper_grad = act_grad * gate_lin * sigmoid_gate
    pair_grad_half = jnp.concatenate([gate_grad, upper_grad], 1).astype(brain_float_type)
    folded_two = row_fold(pair_grad_half, normed_two_all, pair_weight)
    pair_weight_grad = folded_two[0]
    spread_two = folded_two[1]
    normed_two_grad = column_sum(spread_two)
    hidden_part, ffn_gain_part = norm_backward(
        normed_two_grad, hidden_res, rinv_two, feedforward_gain
    )
    hidden_grad = cot_local.astype(single_float_type) + hidden_part
    hidden_half = hidden_grad.astype(brain_float_type)
    hidden_all = column_gather(hidden_half)
    att_grad = (
        row_product(hidden_all, output_weight)[0]
        .astype(brain_float_type)
        .reshape(seq_len, heads_here, HEAD_SIZE)
    )
    output_grad = row_fold(attended_flat, hidden_all, None)[0]
    query_grad, key_grad, value_grad = attend_back(
        query_rot, rotated_keys, value_second_part, attended, att_grad, log_total
    )
    query_half = (
        unrotate(query_grad, cosine_values, sine_lookup)
        .astype(brain_float_type)
        .reshape(seq_len, query_cols)
    )
    key_half = unrotate(key_grad[:, None, :], cosine_values, sine_lookup)[:, 0].astype(
        brain_float_type
    )
    value_grad_half = value_grad.astype(brain_float_type)
    proj_grad_half = jnp.concatenate([query_half, key_half, value_grad_half], 1)
    folded_one = row_fold(proj_grad_half, normed_one_all, proj_weight)
    projection_weight_gradient = folded_one[0]
    normed_one_grad = column_sum(folded_one[1])
    proj_bias_grad = folded_one[2]
    input_part, attn_gain_part = norm_backward(normed_one_grad, x_float, rinv_one, attention_gain)
    input_grad = hidden_grad + input_part
    key_value_gradient = jnp.zeros(
        (projection_weight_gradient.shape[0], 2 * KEYVALUE_HEADS * HEAD_SIZE), single_float_type
    )
    key_value_gradient = lax.dynamic_update_slice_in_dim(
        key_value_gradient,
        projection_weight_gradient[:, query_cols : query_cols + HEAD_SIZE],
        key_start,
        1,
    )
    key_value_gradient = lax.dynamic_update_slice_in_dim(
        key_value_gradient, projection_weight_gradient[:, query_cols + HEAD_SIZE :], value_offset, 1
    )
    key_value_bias_gradient = jnp.zeros((2 * KEYVALUE_HEADS * HEAD_SIZE,), single_float_type)
    key_value_bias_gradient = lax.dynamic_update_slice_in_dim(
        key_value_bias_gradient, proj_bias_grad[query_cols : query_cols + HEAD_SIZE], key_start, 0
    )
    key_value_bias_gradient = lax.dynamic_update_slice_in_dim(
        key_value_bias_gradient, proj_bias_grad[query_cols + HEAD_SIZE :], value_offset, 0
    )
    shared = (
        lax.psum(key_value_gradient.astype(jnp.bfloat16), ("dp", "col")).astype(jnp.float32),
        lax.psum(key_value_bias_gradient.astype(jnp.bfloat16), ("dp", "col")).astype(jnp.float32),
        lax.psum(attn_gain_part.astype(jnp.bfloat16), ("dp", "col")).astype(jnp.float32),
        lax.psum(ffn_gain_part.astype(jnp.bfloat16), ("dp", "col")).astype(jnp.float32),
    )
    summed = (
        lax.psum_scatter(
            projection_weight_gradient[:, :query_cols].astype(jnp.bfloat16),
            "dp",
            scatter_dimension=0,
            tiled=True,
        ).astype(jnp.float32),
        lax.psum_scatter(
            proj_bias_grad[:query_cols].astype(jnp.bfloat16), "dp", scatter_dimension=0, tiled=True
        ).astype(jnp.float32),
        lax.psum_scatter(
            output_grad.astype(jnp.bfloat16), "dp", scatter_dimension=0, tiled=True
        ).astype(jnp.float32),
        lax.psum_scatter(
            pair_weight_grad[:, :hidden_cols].astype(jnp.bfloat16),
            "dp",
            scatter_dimension=0,
            tiled=True,
        ).astype(jnp.float32),
        lax.psum_scatter(
            pair_weight_grad[:, hidden_cols:].astype(jnp.bfloat16),
            "dp",
            scatter_dimension=0,
            tiled=True,
        ).astype(jnp.float32),
        lax.psum_scatter(
            down_grad.astype(jnp.bfloat16), "dp", scatter_dimension=0, tiled=True
        ).astype(jnp.float32),
    )
    return (
        block_output.T,
        input_grad.T,
        shared[2],
        summed[0],
        summed[1],
        shared[0],
        shared[1],
        summed[2],
        shared[3],
        summed[3],
        summed[4],
        summed[5],
    )


MESH_ID = pl.DeviceIdType.MESH
F32 = jnp.float32
BF16 = jnp.bfloat16
LINE = 4
BLOCK = 128
LOCAL = LINE * BLOCK
HALF = MODEL_WIDTH // 2
VMEM_SPEC = pl.BlockSpec(memory_space=pltpu.VMEM)
ANY_SPEC = pl.BlockSpec(memory_space=pl.ANY)
PAIR_ROWS = (((0,), (0,)), ((), ()))
PAIR_COLS = (((1,), (1,)), ((), ()))
SCALE = HEAD_SIZE ** (-0.5)


def greet(me, others):
    barrier = pltpu.get_barrier_semaphore()
    for axis, index in others:
        pl.semaphore_signal(barrier, 1, device_id={axis: index}, device_id_type=MESH_ID)

    @pl.when(me > 0)
    def _():
        pl.semaphore_signal(barrier, 1, device_id={"col": me - 1}, device_id_type=MESH_ID)

    @pl.when(me < LINE - 1)
    def _():
        pl.semaphore_signal(barrier, 1, device_id={"col": me + 1}, device_id_type=MESH_ID)

    @pl.when((me > 0) & (me < LINE - 1))
    def _():
        pl.semaphore_wait(barrier, 2 + len(others))

    @pl.when((me == 0) | (me == LINE - 1))
    def _():
        pl.semaphore_wait(barrier, 1 + len(others))


def line_barrier(me):
    greet(me, [])


def block_rows(index):
    return pl.ds(pl.multiple_of(index * BLOCK, BLOCK), BLOCK)


def nothing(*_):
    return None


def send(src, dst, send_sem, recv_sem, axis, to):
    return pltpu.make_async_remote_copy(
        src, dst, send_sem, recv_sem, device_id={axis: to}, device_id_type=MESH_ID
    )


def landed(ref, sem):
    pltpu.make_async_copy(ref, ref, sem).wait()


class Gather:
    def __init__(self, me, rows_of, sends, recv):
        self.me, self.rows_of, self.sends, self.recv = me, rows_of, sends, recv

    def copy(self, j, to, sem):
        rows = self.rows_of(j)
        return send(rows, rows, sem, self.recv.at[j], "col", to)

    def step(self, s):
        me = self.me
        left, right = me - s, me + s

        @pl.when(left >= 0)
        def _():
            if s:
                landed(self.rows_of(left), self.recv.at[left])

            @pl.when(me < LINE - 1)
            def _():
                self.copy(left, me + 1, self.sends.at[0, s]).start()

        @pl.when(right < LINE)
        def _():
            if s:
                landed(self.rows_of(right), self.recv.at[right])

            @pl.when(me > 0)
            def _():
                self.copy(right, me - 1, self.sends.at[1, s]).start()

    def run_each(self, s, each):
        me = self.me

        @pl.when(me - s >= 0)
        def _():
            each(me - s)

        if s:

            @pl.when(me + s < LINE)
            def _():
                each(me + s)

    def drain(self):
        me = self.me
        for s in range(LINE):

            @pl.when((me - s >= 0) & (me < LINE - 1))
            def _():
                self.copy(me, me + 1, self.sends.at[0, s]).wait_send()

            @pl.when((me + s < LINE) & (me > 0))
            def _():
                self.copy(me, me - 1, self.sends.at[1, s]).wait_send()


class Scatter:
    def __init__(self, me, block_of, from_left, from_right, sends, recv):
        self.me, self.block_of = me, block_of
        self.from_left, self.from_right, self.sends, self.recv = from_left, from_right, sends, recv

    def copy(self, j, to, side):
        landing = self.from_right if side else self.from_left
        return send(
            landing.at[j], landing.at[j], self.sends.at[side, j], self.recv.at[side, j], "col", to
        )

    def arrived(self, j, side):
        landing = self.from_right if side else self.from_left
        landed(landing.at[j], self.recv.at[side, j])

    def step(self, s):
        me = self.me
        ahead, behind = me + s, me - s

        @pl.when(ahead < LINE)
        def _():
            mine = self.block_of(ahead)

            @pl.when(me > 0)
            def _():
                self.arrived(ahead, 0)
                self.from_left[ahead] = (mine + self.from_left[ahead].astype(F32)).astype(BF16)

            @pl.when(me == 0)
            def _():
                self.from_left[ahead] = mine.astype(BF16)

            self.copy(ahead, me + 1, 0).start()

        @pl.when(behind >= 0)
        def _():
            mine = self.block_of(behind)

            @pl.when(me < LINE - 1)
            def _():
                self.arrived(behind, 1)
                self.from_right[behind] = (mine + self.from_right[behind].astype(F32)).astype(BF16)

            @pl.when(me == LINE - 1)
            def _():
                self.from_right[behind] = mine.astype(BF16)

            self.copy(behind, me - 1, 1).start()

    def finish(self, out_ref):
        me = self.me
        out_ref[...] = self.block_of(me)

        @pl.when(me > 0)
        def _():
            self.arrived(me, 0)
            out_ref[...] += self.from_left[me].astype(F32)

        @pl.when(me < LINE - 1)
        def _():
            self.arrived(me, 1)
            out_ref[...] += self.from_right[me].astype(F32)

    def drain(self):
        me = self.me
        for s in range(1, LINE):

            @pl.when(me + s < LINE)
            def _():
                self.copy(me + s, me + 1, 0).wait_send()

            @pl.when(me - s >= 0)
            def _():
                self.copy(me - s, me - 1, 1).wait_send()


def dot(a, b, dims=(((1,), (0,)), ((), ()))):
    return lax.dot_general(a, b, dims, preferred_element_type=F32)


def turn(values):
    return pltpu.roll(values, HEAD_SIZE // 2, 1)


def norm_scale(values):
    return lax.rsqrt(jnp.sum(values * values, -1, keepdims=True) / MODEL_WIDTH + EPS)


def attend_local(query_ref, own_ref, other_ref, attended_ref, probs_ref, r):
    rows = 2 * BLOCK
    shape = (rows, rows)
    at_row = lax.broadcasted_iota(jnp.int32, shape, 0)
    at_col = lax.broadcasted_iota(jnp.int32, shape, 1)
    own_mask = at_row >= at_col
    other_mask = at_col // BLOCK < at_row // BLOCK + r
    heads = query_ref.shape[1] // HEAD_SIZE
    for s in range(2):
        part = slice(s * rows, (s + 1) * rows)
        for h in range(heads):
            cols = slice(h * HEAD_SIZE, (h + 1) * HEAD_SIZE)
            query = query_ref[part, cols]
            own = jnp.where(own_mask, dot(query, own_ref[part, :HEAD_SIZE], PAIR_COLS) * SCALE, NEG)
            other = jnp.where(
                other_mask, dot(query, other_ref[part, :HEAD_SIZE], PAIR_COLS) * SCALE, NEG
            )
            top = jnp.maximum(
                jnp.max(own, -1, keepdims=True), jnp.max(other, -1, keepdims=True)
            )
            total = jnp.sum(jnp.exp(own - top), -1, keepdims=True) + jnp.sum(
                jnp.exp(other - top), -1, keepdims=True
            )
            log_total = top + jnp.log(total)
            own = jnp.exp(own - log_total).astype(BF16)
            other = jnp.exp(other - log_total).astype(BF16)
            attended_ref[part, cols] = (
                dot(own, own_ref[part, HEAD_SIZE:]) + dot(other, other_ref[part, HEAD_SIZE:])
            ).astype(BF16)
            probs_ref[s * heads + h, :, :rows] = own
            probs_ref[s * heads + h, :, rows:] = other


def attend_back_body(
    query_ref, own_ref, other_ref, attended_ref, probs_ref, grad_ref, cos_ref, sin_ref,
    query_grad_ref, own_grad_ref, other_grad_ref,
):
    rows = 2 * BLOCK
    heads = query_ref.shape[1] // HEAD_SIZE
    for s in range(2):
        part = slice(s * rows, (s + 1) * rows)
        own_key, other_key = own_ref[part, :HEAD_SIZE], other_ref[part, :HEAD_SIZE]
        own_value, other_value = own_ref[part, HEAD_SIZE:], other_ref[part, HEAD_SIZE:]
        sums = [jnp.zeros((rows, HEAD_SIZE), F32) for _ in range(4)]
        for h in range(heads):
            cols = slice(h * HEAD_SIZE, (h + 1) * HEAD_SIZE)
            query, grad = query_ref[part, cols], grad_ref[part, cols]
            own_p = probs_ref[s * heads + h, :, :rows]
            other_p = probs_ref[s * heads + h, :, rows:]
            delta = jnp.sum(
                grad.astype(F32) * attended_ref[part, cols].astype(F32), -1, keepdims=True
            )
            own_s = (own_p.astype(F32) * (dot(grad, own_value, PAIR_COLS) - delta)).astype(BF16)
            other_s = (other_p.astype(F32) * (dot(grad, other_value, PAIR_COLS) - delta)).astype(BF16)
            query_grad = (dot(own_s, own_key) + dot(other_s, other_key)) * SCALE
            query_grad_ref[part, cols] = (
                query_grad * cos_ref[part] - turn(query_grad) * sin_ref[part]
            ).astype(BF16)
            for i, (weights, partner) in enumerate(
                ((own_s, query), (own_p, grad), (other_s, query), (other_p, grad))
            ):
                sums[i] = sums[i] + dot(weights, partner, PAIR_ROWS)
        own_grad_ref[part, :HEAD_SIZE] = sums[0] * SCALE
        own_grad_ref[part, HEAD_SIZE:] = sums[1]
        other_grad_ref[part, :HEAD_SIZE] = (sums[2] * SCALE).astype(BF16)
        other_grad_ref[part, HEAD_SIZE:] = sums[3].astype(BF16)


def feed_body(
    normed_ref, cot_ref, gate_hbm, upper_hbm, down_hbm, other_hbm,
    activated_ref, gate_grad_ref, upper_grad_ref, back_ref, out_ref,
    weights, back_sum, out_sum, sems,
):
    hidden = activated_ref.shape[1]
    tile = 256
    chunk = 2 * tile
    lows = list(range(0, hidden, chunk))

    def copies(k):
        rows = pl.ds(lows[k], min(chunk, hidden - lows[k]))
        for i, own in enumerate((gate_hbm, upper_hbm, down_hbm)):
            yield pltpu.make_async_copy(
                own.at[rows], weights.at[i, rows, pl.ds(0, HALF)], sems.at[k, i, 0]
            )
            yield pltpu.make_async_copy(
                other_hbm.at[i, rows], weights.at[i, rows, pl.ds(HALF, HALF)], sems.at[k, i, 1]
            )

    for k in range(len(lows)):
        for copy in copies(k):
            copy.start()
    back_sum[...] = jnp.zeros_like(back_sum)
    out_sum[...] = jnp.zeros_like(out_sum)

    def run(low, size):
        rows = pl.ds(low, size)
        gate = dot(normed_ref[...], weights[0, rows], PAIR_COLS)
        upper = dot(normed_ref[...], weights[1, rows], PAIR_COLS)
        act_grad = dot(cot_ref[...], weights[2, rows], PAIR_COLS)
        sig = jax.nn.sigmoid(gate)
        silu = gate * sig
        activated = (silu * upper).astype(BF16)
        gate_grad = (act_grad * upper * sig * (1.0 + gate * (1.0 - sig))).astype(BF16)
        upper_grad = (act_grad * silu).astype(BF16)
        activated_ref[:, rows] = activated
        gate_grad_ref[:, rows] = gate_grad
        upper_grad_ref[:, rows] = upper_grad
        back_sum[...] += dot(gate_grad, weights[0, rows]) + dot(upper_grad, weights[1, rows])
        out_sum[...] += dot(activated, weights[2, rows])

    for k, low in enumerate(lows):
        for copy in copies(k):
            copy.wait()
        if low + chunk <= hidden:

            @pl.loop(0, 2)
            def _(t):
                run(pl.multiple_of(low + t * tile, tile), tile)
        else:
            run(low, hidden - low)
    back_ref[...] = back_sum[...].astype(BF16)
    out_ref[...] = out_sum[...].astype(BF16)


def shape(rows, cols, dtype=BF16):
    return jax.ShapeDtypeStruct((rows, cols), dtype)


PIECES = 6


def front_body(
    keep_ref, pass_ref, cot_keep_ref, cot_pass_ref, table_ref, gains_ref, bias_ref, proj_ref,
    gate_hbm, upper_hbm, down_hbm,
    x_ref, normed_ref, query_ref, kv_ref, kv_other_ref, cos_ref, sin_ref, all_gains_ref,
    attended_ref, probs_ref, mid_ref, normed_two_ref, cot_ref, proj_other_ref, weights_other_hbm,
    tables, from_left, from_right,
    swap_sends, swap_recv, piece_sends, piece_recv, kv_sends, kv_recv,
    g_sends, g_recv, c_sends, c_recv, n_sends, n_recv, s_sends, s_recv,
):
    me, r, d = lax.axis_index("col"), lax.axis_index("row"), lax.axis_index("dp")
    y, core = d // 2, lax.rem(d, 2)
    x_to, y_to, core_to = 1 - r, 2 * (1 - y) + core, 2 * y + 1 - core
    greet(me, [("row", x_to), ("dp", y_to), ("dp", core_to)])
    proj_cols = bias_ref.shape[1]
    query_cols = query_ref.shape[1]
    quarter = HALF // 2
    my_rows = pl.ds(pl.multiple_of(core * quarter, quarter), quarter)
    its_rows = pl.ds(pl.multiple_of((1 - core) * quarter, quarter), quarter)

    swaps = [
        (pass_ref, x_ref.at[:, HALF:], "row", x_to),
        (table_ref.at[1], tables.at[1], "row", x_to),
        (gains_ref, all_gains_ref.at[:, HALF:], "row", x_to),
        (proj_ref.at[my_rows, :proj_cols], proj_other_ref.at[my_rows, :proj_cols], "row", x_to),
        (cot_pass_ref, cot_ref.at[block_rows(me), HALF:], "row", x_to),
        (proj_ref.at[my_rows, proj_cols:], proj_other_ref.at[my_rows, proj_cols:], "row", x_to),
        (
            proj_other_ref.at[my_rows, :proj_cols], proj_other_ref.at[my_rows, :proj_cols],
            "dp", core_to,
        ),
        (
            proj_other_ref.at[my_rows, proj_cols:], proj_other_ref.at[my_rows, proj_cols:],
            "dp", core_to,
        ),
    ]

    def swap_copy(i):
        src, dst, axis, to = swaps[i]
        return send(src, dst, swap_sends.at[i], swap_recv.at[i], axis, to)

    def swap_landed(i):
        swap_copy(i).wait_recv()

    rows = gate_hbm.shape[0] // 4
    owns = (gate_hbm, upper_hbm, down_hbm)
    my_cols = my_rows

    def piece(i, of_y):
        return pl.ds(pl.multiple_of((of_y * 2 + i % 2) * rows, rows), rows)

    def piece_copy(i, way):
        m = i // 2
        of_y = y if way in (0, 1, 2) else 1 - y
        at = weights_other_hbm.at[m, piece(i, of_y), my_cols]
        src = owns[m].at[piece(i, of_y), my_cols] if way == 0 else at
        axis, to = (("row", x_to), ("dp", y_to), ("dp", core_to), ("dp", core_to))[way]
        return send(src, at, piece_sends.at[way, i], piece_recv.at[way, i], axis, to)

    def relay_x(i):
        piece_copy(i, 0).wait_recv()
        piece_copy(i, 1).start()
        piece_copy(i, 2).start()

    def relay_y(i):
        piece_copy(i, 1).wait_recv()
        piece_copy(i, 3).start()

    for i in range(5):
        swap_copy(i).start()
    piece_copy(0, 0).start()
    x_ref[:, :HALF] = keep_ref[...]
    tables[0] = table_ref[0]
    all_gains_ref[:, :HALF] = gains_ref[...]
    cot_ref[block_rows(me), :HALF] = cot_keep_ref[...]
    swap_landed(0)
    swap_landed(1)
    swap_landed(2)
    x = x_ref[...].astype(F32)
    normed_ref[block_rows(me)] = (x * norm_scale(x) * all_gains_ref[0:1]).astype(BF16)
    gather = Gather(me, lambda j: normed_ref.at[block_rows(j)], g_sends, g_recv)
    gather.step(0)

    lane = lax.broadcasted_iota(jnp.int32, (2 * BLOCK, HEAD_SIZE), 1)
    first = lane < HEAD_SIZE // 2
    for i in range(2):
        table = tables[i]
        turned = turn(table)
        at = pl.ds(pl.multiple_of((r if i == 0 else 1 - r) * 2 * BLOCK, BLOCK), 2 * BLOCK)
        cos_ref[at] = jnp.where(first, table, turned)
        sin_ref[at] = jnp.where(first, -turned, table)

    swap_landed(3)
    swap_copy(6).start()
    swap_landed(6)

    def kv_copy(j):
        at = block_rows(j)
        return send(
            kv_ref.at[at], kv_other_ref.at[at], kv_sends.at[j], kv_recv.at[j], "row", x_to
        )

    def each(j):
        at = block_rows(j)
        block = normed_ref[at]
        out = dot(block[:, :HALF], proj_ref[:, :proj_cols])
        out = out + dot(block[:, HALF:], proj_other_ref[:, :proj_cols]) + bias_ref[...]
        cosine, sine = cos_ref[at], sin_ref[at]
        for h in range(query_cols // HEAD_SIZE + 1):
            head = out[:, h * HEAD_SIZE : (h + 1) * HEAD_SIZE]
            turned = (head * cosine + turn(head) * sine).astype(BF16)
            if h * HEAD_SIZE < query_cols:
                query_ref[at, h * HEAD_SIZE : (h + 1) * HEAD_SIZE] = turned
            else:
                kv_ref[at, :HEAD_SIZE] = turned
        kv_ref[at, HEAD_SIZE:] = out[:, query_cols + HEAD_SIZE :].astype(BF16)
        kv_copy(j).start()

    for s in range(LINE):
        if s:
            gather.step(s)
        gather.run_each(s, each)
    swap_copy(5).start()
    for i in range(1, PIECES):
        piece_copy(i, 0).start()
    swap_landed(4)
    cot_gather = Gather(me, lambda j: cot_ref.at[block_rows(j)], c_sends, c_recv)
    cot_gather.step(0)
    relay_x(0)
    for j in range(LINE):
        kv_copy(j).wait_recv()
    attend_local(query_ref, kv_ref, kv_other_ref, attended_ref, probs_ref, r)
    swap_landed(5)
    swap_copy(7).start()
    relay_y(0)
    swap_landed(7)

    def block_of(j):
        block = attended_ref[block_rows(j)]
        return jnp.concatenate(
            [
                dot(block, proj_ref[:, proj_cols:], PAIR_COLS),
                dot(block, proj_other_ref[:, proj_cols:], PAIR_COLS),
            ],
            1,
        )

    scatter = Scatter(me, block_of, from_left, from_right, s_sends, s_recv)
    scatter.step(3)
    scatter.step(2)
    relay_x(1)
    scatter.step(1)
    scatter.finish(mid_ref)
    mid = mid_ref[...] + x_ref[...].astype(F32)
    mid_ref[...] = mid
    normed_two_ref[block_rows(me)] = (mid * norm_scale(mid) * all_gains_ref[1:2]).astype(BF16)
    second = Gather(me, lambda j: normed_two_ref.at[block_rows(j)], n_sends, n_recv)
    second.step(0)
    relay_x(2)
    relay_y(1)
    second.step(1)
    relay_x(3)
    relay_y(2)
    second.step(2)
    relay_x(4)
    relay_y(3)
    second.step(3)
    cot_gather.step(1)
    cot_gather.step(2)
    relay_x(5)
    relay_y(4)
    cot_gather.step(3)
    relay_y(5)
    for i in range(PIECES):
        for way in (2, 3):
            of_y = y if way == 2 else 1 - y
            landed(weights_other_hbm.at[i // 2, piece(i, of_y), its_rows], piece_recv.at[way, i])
        for way in range(4):
            piece_copy(i, way).wait_send()
    for i in range(len(swaps)):
        swap_copy(i).wait_send()
    for j in range(LINE):
        kv_copy(j).wait_send()
    gather.drain()
    cot_gather.drain()
    second.drain()
    scatter.drain()


def front_call(proj_cols, query_cols, hidden, *args):
    heads = query_cols // HEAD_SIZE
    outs = [
        shape(BLOCK, MODEL_WIDTH),
        shape(LOCAL, MODEL_WIDTH),
        shape(LOCAL, query_cols),
        shape(LOCAL, 2 * HEAD_SIZE),
        shape(LOCAL, 2 * HEAD_SIZE),
        shape(LOCAL, HEAD_SIZE, F32),
        shape(LOCAL, HEAD_SIZE, F32),
        shape(8, MODEL_WIDTH, F32),
        shape(LOCAL, query_cols),
        jax.ShapeDtypeStruct((2 * heads, 2 * BLOCK, 4 * BLOCK), BF16),
        shape(BLOCK, MODEL_WIDTH, F32),
        shape(LOCAL, MODEL_WIDTH),
        shape(LOCAL, MODEL_WIDTH),
        shape(HALF, proj_cols + query_cols),
        jax.ShapeDtypeStruct((3, hidden, HALF), BF16),
    ]
    dma = pltpu.SemaphoreType.DMA
    return pl.pallas_call(
        front_body,
        out_shape=outs,
        in_specs=[VMEM_SPEC] * 8 + [ANY_SPEC] * 3,
        out_specs=[VMEM_SPEC] * (len(outs) - 1) + [ANY_SPEC],
        scratch_shapes=[
            pltpu.VMEM((2, 2 * BLOCK, HEAD_SIZE), F32),
            pltpu.VMEM((LINE, BLOCK, MODEL_WIDTH), BF16),
            pltpu.VMEM((LINE, BLOCK, MODEL_WIDTH), BF16),
            dma((8,)),
            dma((8,)),
            dma((4, PIECES)),
            dma((4, PIECES)),
            dma((LINE,)),
            dma((LINE,)),
        ]
        + [dma((2, LINE)), dma((LINE,))] * 3
        + [dma((2, LINE)), dma((2, LINE))],
        compiler_params=pltpu.CompilerParams(
            collective_id=1, has_side_effects=True, vmem_limit_bytes=60 * 1024 * 1024
        ),
        cost_estimate=pl.CostEstimate(
            flops=4 * 10**9, bytes_accessed=40_000_000, transcendentals=0
        ),
        name="front",
    )(*args)


UNIT = MODEL_WIDTH // 8
DOWN, GATE, UPPER = 0, 1, 2


def add_into(total_ref, term_ref):
    @pl.loop(0, total_ref.shape[0] // 32)
    def _(i):
        at = pl.ds(pl.multiple_of(i * 32, 32), 32)
        total_ref[at] = (total_ref[at].astype(F32) + term_ref[at].astype(F32)).astype(BF16)


def back_body(
    part_ref, out_part_ref, mid_ref, cot_ref, gains_ref, own_proj_ref, other_proj_ref, normed_two_ref,
    activated_ref, gate_grad_ref, upper_grad_ref, query_ref, kv_ref, kv_other_ref, attended_ref,
    probs_ref, cos_ref, sin_ref, x_ref, normed_one_ref,
    out_keep_ref, out_got_ref, in_keep_ref, in_got_ref, small_ref, chain_sum_ref, kv_all_ref,
    kept_hbm, land2_hbm, land3_hbm,
    mid_grad_ref, mid_half_ref, att_grad_ref, query_grad_ref, kv_grad_ref, kv_give_ref, kv_got_ref,
    proj_grad_ref, turned_ref, from_left, from_right, out_left, out_right, own_ref,
    sums, gives, gots,
    chain_sums, chain_gives, chain_gots, chain_land2, chain_land3, kv_line, back_give, small_buf,
    r_sends, r_recv, a_sends, a_recv, o_sends, o_recv, give_sends, give_recv, two_sends, two_recv,
    three_sends, three_recv, load_sems, kept_sems, swap_sends, swap_recv, kv_sends, kv_recv,
    kvd_sends, kvd_recv, small_sends, small_recv, credit,
):
    me, r, d = lax.axis_index("col"), lax.axis_index("row"), lax.axis_index("dp")
    y, core = d // 2, lax.rem(d, 2)
    x_to, y_to, core_to = 1 - r, 2 * (1 - y) + core, 2 * y + 1 - core
    diagonal_to = 2 * (1 - y) + 1 - core
    barrier = pltpu.get_barrier_semaphore()
    others = [("row", x_to), ("dp", y_to), ("dp", core_to), ("dp", diagonal_to)]
    for axis, index in others:
        pl.semaphore_signal(barrier, 1, device_id={axis: index}, device_id_type=MESH_ID)
    for s in range(1, LINE):
        pl.semaphore_signal(
            barrier, 1, device_id={"col": lax.rem(me + s, LINE)}, device_id_type=MESH_ID
        )
    pl.semaphore_wait(barrier, len(others) + LINE - 1)

    proj_cols, query_cols = proj_grad_ref.shape[1], query_ref.shape[1]
    hidden = activated_ref.shape[1]

    order = [
        (DOWN, 0, 1), (DOWN, 1, 1), (UPPER, 1, 0), (UPPER, 1, 1), (DOWN, 0, 0), (DOWN, 1, 0),
        (GATE, 0, 1), (GATE, 1, 1), (UPPER, 0, 0), (UPPER, 0, 1), (GATE, 0, 0), (GATE, 1, 0),
    ]
    columns_of = {DOWN: activated_ref, GATE: gate_grad_ref, UPPER: upper_grad_ref}
    x_first = {DOWN: False, GATE: False, UPPER: True}

    def slot(m, h, rel):
        return m * 4 + h * 2 + rel

    def unit_rows(h, rel):
        of_y = 1 - y if rel else y
        return pl.ds(pl.multiple_of(h * HALF + of_y * 2 * UNIT, 2 * UNIT), 2 * UNIT)

    def split(res, keep_ref, give_ref, at):
        low, high = res[:UNIT], res[UNIT:]
        keep_ref[:, at] = jnp.where(core == 0, low, high).astype(BF16)
        give_ref[:, at] = jnp.where(core == 0, high, low).astype(BF16)

    def give_copy(u):
        return send(
            gives.at[u % 2], gots.at[u % 3], give_sends.at[u], give_recv.at[u], "dp", core_to
        )

    def compute(u):
        m, h, rel = order[u]
        if u >= 2:
            give_copy(u - 2).wait_send()
        left = 0 if m == DOWN else 1
        rows = unit_rows(h, rel)
        tile = 512
        full = hidden // tile

        def run(at):
            res = dot(turned_ref[left, rows], columns_of[m][:, at])
            split(res, sums.at[slot(m, h, rel)], gives.at[u % 2], at)

        @pl.loop(0, full)
        def _(i):
            run(pl.ds(pl.multiple_of(i * tile, tile), tile))

        if hidden % tile:
            run(pl.ds(full * tile, hidden % tile))
        if u >= 3:
            pl.semaphore_wait(credit, 1)
        give_copy(u).start()

    passed = {}
    for m in (DOWN, GATE, UPPER):
        passed[m] = [(1, 0), (1, 1)] if x_first[m] else [(0, 1), (1, 1)]

    def two_copy(m, i):
        h, rel = passed[m][i]
        axis, to = ("row", x_to) if x_first[m] else ("dp", y_to)
        k = m * 2 + i
        return send(
            sums.at[slot(m, h, rel)], land2_hbm.at[k], two_sends.at[k], two_recv.at[k], axis, to
        )

    def combine(u):
        m, h, rel = order[u]
        give_copy(u).wait_recv()
        add_into(sums.at[slot(m, h, rel)], gots.at[u % 3])
        if u < len(order) - 3:
            pl.semaphore_signal(credit, 1, device_id={"dp": core_to}, device_id_type=MESH_ID)
        if (h, rel) in passed[m]:
            two_copy(m, passed[m].index((h, rel))).start()

    def kept(m):
        return [(0, 0), (0, 1)] if x_first[m] else [(0, 0), (1, 0)]

    def three_copy(m):
        axis, to = ("dp", y_to) if x_first[m] else ("row", x_to)
        return send(
            sums.at[slot(m, *kept(m)[1])], land3_hbm.at[m], three_sends.at[m], three_recv.at[m],
            axis, to,
        )

    def kept_copy(m):
        return pltpu.make_async_copy(sums.at[slot(m, 0, 0)], kept_hbm.at[m], kept_sems.at[m])

    def load(m, i):
        return pltpu.make_async_copy(land2_hbm.at[m * 2 + i], gots.at[i], load_sems.at[m, i])

    def second_stage(m):
        for i in (1, 0):
            two_copy(m, i).wait_recv()
            load(m, i).start()
        for i in (1, 0):
            load(m, i).wait()
            add_into(sums.at[slot(m, *kept(m)[i])], gots.at[i])
            if i == 1:
                three_copy(m).start()
        kept_copy(m).start()

    scatter = Scatter(
        me, lambda j: part_ref[block_rows(j)].astype(F32), from_left, from_right, r_sends, r_recv
    )
    scatter.step(3)
    turned_ref[0] = cot_ref[...].T
    compute(0)
    compute(1)
    combine(0)
    combine(1)
    scatter.step(2)
    turned_ref[1] = normed_two_ref[...].T
    compute(2)
    compute(3)
    combine(2)
    combine(3)
    scatter.step(1)
    compute(4)
    compute(5)
    combine(4)
    scatter.finish(mid_grad_ref)
    mid, grad = mid_ref[...], mid_grad_ref[...]
    rinv = norm_scale(mid)
    ffn_gain_part = jnp.sum(grad * mid * rinv, 0, keepdims=True)
    scaled = grad * gains_ref[1:2]
    inner = jnp.sum(scaled * mid, -1, keepdims=True)
    mid_grad = (
        cot_ref[block_rows(me)].astype(F32)
        + rinv * scaled
        - mid * rinv**3 * inner / MODEL_WIDTH
    )
    mid_grad_ref[...] = mid_grad
    mid_half_ref[block_rows(me)] = mid_grad.astype(BF16)
    scatter.drain()
    small_buf[0] = jnp.zeros_like(small_buf[0])
    small_buf[0, 1:2] = ffn_gain_part

    def each(j):
        block = mid_half_ref[block_rows(j)]
        att_grad_ref[block_rows(j)] = (
            dot(block[:, :HALF], own_proj_ref[:, proj_cols:])
            + dot(block[:, HALF:], other_proj_ref[:, proj_cols:])
        ).astype(BF16)

    gather = Gather(me, lambda j: mid_half_ref.at[block_rows(j)], a_sends, a_recv)
    gather.step(0)
    gather.run_each(0, each)
    combine(5)
    compute(6)
    compute(7)
    combine(6)
    combine(7)
    gather.step(1)
    gather.run_each(1, each)
    compute(8)
    compute(9)
    combine(8)
    combine(9)
    gather.step(2)
    gather.run_each(2, each)
    compute(10)
    compute(11)
    combine(10)
    combine(11)
    gather.step(3)
    gather.run_each(3, each)
    out_scatter = Scatter(
        me, lambda j: out_part_ref[block_rows(j)].astype(F32), out_left, out_right, o_sends, o_recv
    )
    out_scatter.step(3)
    attend_back_body(
        query_ref, kv_ref, kv_other_ref, attended_ref, probs_ref, att_grad_ref, cos_ref, sin_ref,
        query_grad_ref, kv_grad_ref, kv_give_ref,
    )

    def swap_copy(i):
        src, dst = (
            (kv_give_ref, kv_got_ref),
            (back_give.at[0], in_got_ref),
            (back_give.at[1], out_got_ref),
        )[i]
        return send(src, dst, swap_sends.at[i], swap_recv.at[i], "row", x_to)

    swap_copy(0).start()
    second_stage(DOWN)
    swap_copy(0).wait_recv()
    kv = kv_grad_ref[...] + kv_got_ref[...].astype(F32)
    key = kv[:, :HEAD_SIZE]
    proj_grad_ref[:, :query_cols] = query_grad_ref[...]
    proj_grad_ref[:, query_cols : query_cols + HEAD_SIZE] = (
        key * cos_ref[...] - turn(key) * sin_ref[...]
    ).astype(BF16)
    proj_grad_ref[:, query_cols + HEAD_SIZE :] = kv[:, HEAD_SIZE:].astype(BF16)

    def block_of(j):
        block = proj_grad_ref[block_rows(j)]
        return jnp.concatenate(
            [
                dot(block, own_proj_ref[:, :proj_cols], PAIR_COLS),
                dot(block, other_proj_ref[:, :proj_cols], PAIR_COLS),
            ],
            1,
        )

    def chain_give(i):
        return send(
            chain_gives.at[i], chain_gots.at[i], give_sends.at[12 + i], give_recv.at[12 + i],
            "dp", core_to,
        )

    def chain_compute(i):
        rows = unit_rows(i // 2, i % 2)
        res = dot(normed_one_ref[:, rows], proj_grad_ref[...], PAIR_ROWS)
        split(res, chain_sums.at[i], chain_gives.at[i], pl.ds(0, proj_cols))
        res = dot(mid_half_ref[:, rows], attended_ref[...], PAIR_ROWS)
        split(res, chain_sums.at[i], chain_gives.at[i], pl.ds(proj_cols, query_cols))
        chain_give(i).start()

    def chain_two(i):
        return send(
            chain_sums.at[2 + i], chain_land2.at[i], two_sends.at[6 + i], two_recv.at[6 + i],
            "row", x_to,
        )

    def chain_combine(i):
        chain_give(i).wait_recv()
        add_into(chain_sums.at[i], chain_gots.at[i])
        if i >= 2:
            chain_two(i - 2).start()

    def chain_three():
        return send(
            chain_sums.at[1], chain_land3, three_sends.at[3], three_recv.at[3], "dp", y_to
        )

    second = Scatter(me, block_of, from_left, from_right, r_sends, r_recv)
    second.step(3)
    for i in (3, 2, 1, 0):
        chain_compute(i)
    for i in (3, 2, 1, 0):
        chain_combine(i)
    small_buf[0, 2:3, :proj_cols] = jnp.sum(proj_grad_ref[...].astype(F32), 0, keepdims=True)
    second.step(2)
    second_stage(UPPER)
    out_scatter.step(2)
    second.step(1)
    for i in (1, 0):
        chain_two(i).wait_recv()
        add_into(chain_sums.at[i], chain_land2.at[i])
        if i == 1:
            chain_three().start()
    second.finish(own_ref)
    x, grad = x_ref[...].astype(F32), own_ref[...]
    rinv = norm_scale(x)
    small_buf[0, 0:1] = jnp.sum(grad * x * rinv, 0, keepdims=True)
    scaled = grad * gains_ref[0:1]
    inner = jnp.sum(scaled * x, -1, keepdims=True)
    input_grad = mid_grad_ref[...] + rinv * scaled - x * rinv**3 * inner / MODEL_WIDTH
    in_keep_ref[...] = input_grad[:, :HALF]
    back_give[0] = input_grad[:, HALF:].astype(BF16)
    swap_copy(1).start()
    out_scatter.step(1)
    second_stage(GATE)

    chain_three().wait_recv()
    total = chain_sums[0].astype(F32) + chain_land3[...].astype(F32)
    chain_sum_ref[...] = total
    kv_line[me] = total[:, query_cols:proj_cols].astype(BF16)

    def kv_line_copy(s):
        to = lax.rem(me + s, LINE)
        return send(kv_line.at[me], kv_line.at[me], kv_sends.at[s], kv_recv.at[me], "col", to)

    for s in range(1, LINE):
        kv_line_copy(s).start()
    out_scatter.finish(own_ref)
    out = own_ref[...] + mid_ref[...]
    out_keep_ref[...] = out[:, :HALF]
    back_give[1] = out[:, HALF:].astype(BF16)
    swap_copy(2).start()
    for s in range(1, LINE):
        landed(kv_line.at[me], kv_recv.at[lax.rem(me + s, LINE)])
    dp_rows = pl.ds(pl.multiple_of(d * UNIT, UNIT), UNIT)
    group = LINE // KEYVALUE_HEADS
    for h in range(KEYVALUE_HEADS):
        pair = kv_line[h * group].astype(F32)
        for i in range(1, group):
            pair = pair + kv_line[h * group + i].astype(F32)
        for i in range(2):
            at = (i * KEYVALUE_HEADS + h) * HEAD_SIZE
            kv_all_ref[dp_rows, at : at + HEAD_SIZE] = pair[
                :, i * HEAD_SIZE : (i + 1) * HEAD_SIZE
            ].astype(BF16)

    def kv_dp_copy(i):
        to = (core_to, y_to, diagonal_to)[i]
        rows = kv_all_ref.at[dp_rows]
        return send(rows, rows, kvd_sends.at[i], kvd_recv.at[i], "dp", to)

    for i in range(3):
        kv_dp_copy(i).start()

    def small_copy(i, src, dst):
        axis, to = (("row", x_to), ("dp", core_to), ("dp", y_to))[i]
        return send(src, dst, small_sends.at[i], small_recv.at[i], axis, to)

    small_buf[1, :2, :HALF] = small_buf[0, :2, HALF:]
    small_buf[1, 2:, :HALF] = small_buf[0, 2:, :HALF]
    now = small_buf.at[1, :, pl.ds(0, HALF)]
    give = small_copy(0, now, small_buf.at[2, :, pl.ds(0, HALF)])
    give.start()
    give.wait_recv()
    give.wait_send()
    small_buf[3, :, :HALF] = small_buf[0, :, :HALF] + small_buf[2, :, :HALF]
    for i, (a, b) in ((1, (3, 4)), (2, (5, 6))):
        give = small_copy(
            i, small_buf.at[a, :, pl.ds(0, HALF)], small_buf.at[b, :, pl.ds(0, HALF)]
        )
        give.start()
        give.wait_recv()
        give.wait_send()
        if i == 1:
            small_buf[5, :, :HALF] = small_buf[3, :, :HALF] + small_buf[4, :, :HALF]
        else:
            small_ref[me] = small_buf[5, :, :HALF] + small_buf[6, :, :HALF]

    def small_line_copy(s):
        to = lax.rem(me + s, LINE)
        return send(
            small_ref.at[me], small_ref.at[me], small_sends.at[2 + s], small_recv.at[3 + me],
            "col", to,
        )

    for s in range(1, LINE):
        small_line_copy(s).start()
    for s in range(1, LINE):
        landed(small_ref.at[me], small_recv.at[3 + lax.rem(me + s, LINE)])

    for i in range(3):
        rows = pl.ds(pl.multiple_of((core_to, y_to, diagonal_to)[i] * UNIT, UNIT), UNIT)
        landed(kv_all_ref.at[rows], kvd_recv.at[i])
    for i in (1, 2):
        swap_copy(i).wait_recv()
    for m in (DOWN, GATE, UPPER):
        three_copy(m).wait_recv()
        three_copy(m).wait_send()
        kept_copy(m).wait()
        for i in range(2):
            two_copy(m, i).wait_send()
    for u in (len(order) - 2, len(order) - 1):
        give_copy(u).wait_send()
    for i in range(4):
        chain_give(i).wait_send()
    for i in range(2):
        chain_two(i).wait_send()
    chain_three().wait_send()
    for i in range(3):
        swap_copy(i).wait_send()
        kv_dp_copy(i).wait_send()
        kv_line_copy(1 + i).wait_send()
        small_line_copy(1 + i).wait_send()
    gather.drain()
    out_scatter.drain()
    second.drain()


def back_call(hidden, proj_cols, query_cols, *args):
    dma = pltpu.SemaphoreType.DMA
    chain_cols = proj_cols + query_cols
    outs = [
        shape(BLOCK, HALF, F32),
        shape(BLOCK, HALF),
        shape(BLOCK, HALF, F32),
        shape(BLOCK, HALF),
        jax.ShapeDtypeStruct((LINE, 8, HALF), F32),
        shape(UNIT, chain_cols, F32),
        shape(4 * UNIT, 2 * KEYVALUE_HEADS * HEAD_SIZE),
        jax.ShapeDtypeStruct((3, UNIT, hidden), BF16),
        jax.ShapeDtypeStruct((6, UNIT, hidden), BF16),
        jax.ShapeDtypeStruct((3, UNIT, hidden), BF16),
    ]
    line = (LINE, BLOCK, MODEL_WIDTH)
    return pl.pallas_call(
        back_body,
        out_shape=outs,
        in_specs=[VMEM_SPEC] * len(args),
        out_specs=[VMEM_SPEC] * 7 + [ANY_SPEC] * 3,
        scratch_shapes=[
            pltpu.VMEM((BLOCK, MODEL_WIDTH), F32),
            pltpu.VMEM((LOCAL, MODEL_WIDTH), BF16),
            pltpu.VMEM((LOCAL, query_cols), BF16),
            pltpu.VMEM((LOCAL, query_cols), BF16),
            pltpu.VMEM((LOCAL, 2 * HEAD_SIZE), F32),
            pltpu.VMEM((LOCAL, 2 * HEAD_SIZE), BF16),
            pltpu.VMEM((LOCAL, 2 * HEAD_SIZE), BF16),
            pltpu.VMEM((LOCAL, proj_cols), BF16),
            pltpu.VMEM((2, MODEL_WIDTH, LOCAL), BF16),
        ]
        + [pltpu.VMEM(line, BF16)] * 4
        + [
            pltpu.VMEM((BLOCK, MODEL_WIDTH), F32),
            pltpu.VMEM((12, UNIT, hidden), BF16),
            pltpu.VMEM((2, UNIT, hidden), BF16),
            pltpu.VMEM((3, UNIT, hidden), BF16),
            pltpu.VMEM((4, UNIT, chain_cols), BF16),
            pltpu.VMEM((4, UNIT, chain_cols), BF16),
            pltpu.VMEM((4, UNIT, chain_cols), BF16),
            pltpu.VMEM((2, UNIT, chain_cols), BF16),
            pltpu.VMEM((UNIT, chain_cols), BF16),
            pltpu.VMEM((LINE, UNIT, 2 * HEAD_SIZE), BF16),
            pltpu.VMEM((2, BLOCK, HALF), BF16),
            pltpu.VMEM((7, 8, MODEL_WIDTH), F32),
            dma((2, LINE)), dma((2, LINE)),
            dma((2, LINE)), dma((LINE,)),
            dma((2, LINE)), dma((2, LINE)),
            dma((16,)), dma((16,)),
            dma((8,)), dma((8,)),
            dma((4,)), dma((4,)),
            dma((3, 2)), dma((3,)),
            dma((3,)), dma((3,)),
            dma((LINE,)), dma((LINE,)),
            dma((3,)), dma((3,)),
            dma((6,)), dma((3 + LINE,)),
            pltpu.SemaphoreType.REGULAR,
        ],
        compiler_params=pltpu.CompilerParams(
            collective_id=2, has_side_effects=True, vmem_limit_bytes=67_043_328
        ),
        cost_estimate=pl.CostEstimate(
            flops=2 * 10**10, bytes_accessed=80_000_000, transcendentals=0
        ),
        name="back",
    )(*args)


def fast_device(
    block_input,
    position_ids,
    attention_gain,
    query_weight,
    query_bias,
    key_value_weight,
    key_value_bias,
    output_weight,
    feedforward_gain,
    gate_weight,
    upper_weight,
    down_weight,
    out_cotangent,
):
    r, c = lax.axis_index("row"), lax.axis_index("col")
    query_cols = query_weight.shape[1]
    hidden = gate_weight.shape[1]
    proj_cols = query_cols + 2 * HEAD_SIZE
    kv_head = c // (LINE // KEYVALUE_HEADS)
    key_start = kv_head * HEAD_SIZE
    value_start = (KEYVALUE_HEADS + kv_head) * HEAD_SIZE

    def parts(values):
        turned = values.T.reshape(2, BLOCK, HALF)
        pick = lambda i: lax.dynamic_index_in_dim(turned, i, 0, keepdims=False)
        return pick(r), pick(1 - r)

    x_keep, x_pass = parts(block_input)
    cot_keep, cot_pass = parts(out_cotangent)
    frequencies = THETA ** (-(jnp.arange(HEAD_SIZE // 2, dtype=F32) * 2.0 / HEAD_SIZE))
    angles = position_ids.astype(F32)[:, None] * frequencies[None, :]
    table = jnp.concatenate([jnp.cos(angles), jnp.sin(angles)], -1).reshape(2, 2, BLOCK, HEAD_SIZE)
    pick = lambda i: lax.dynamic_index_in_dim(table, i, 1, keepdims=False)
    table = jnp.stack([pick(r), pick(1 - r)]).reshape(2, 2 * BLOCK, HEAD_SIZE)
    gains = jnp.concatenate(
        [attention_gain[None], feedforward_gain[None], jnp.zeros((6, HALF), F32)]
    )
    own_proj = jnp.concatenate(
        [
            query_weight,
            lax.dynamic_slice_in_dim(key_value_weight, key_start, HEAD_SIZE, 1),
            lax.dynamic_slice_in_dim(key_value_weight, value_start, HEAD_SIZE, 1),
            output_weight,
        ],
        1,
    )
    proj_bias = jnp.concatenate(
        [
            query_bias,
            lax.dynamic_slice_in_dim(key_value_bias, key_start, HEAD_SIZE, 0),
            lax.dynamic_slice_in_dim(key_value_bias, value_start, HEAD_SIZE, 0),
        ]
    )[None]
    (
        x_own, normed_one, query_rot, kv_own, kv_other, cosine, sine, all_gains, attended, probs,
        mid, normed_two, cot_all, other_proj, ffn_other,
    ) = front_call(
        proj_cols, query_cols, hidden,
        x_keep, x_pass, cot_keep, cot_pass, table, gains, proj_bias, own_proj,
        gate_weight.T, upper_weight.T, down_weight.T,
    )
    activated, gate_grad, upper_grad, back_part, out_part = pl.pallas_call(
        feed_body,
        out_shape=[shape(LOCAL, hidden)] * 3 + [shape(LOCAL, MODEL_WIDTH)] * 2,
        in_specs=[VMEM_SPEC] * 2 + [ANY_SPEC] * 4,
        out_specs=[VMEM_SPEC] * 5,
        scratch_shapes=[
            pltpu.VMEM((3, hidden, MODEL_WIDTH), BF16),
            pltpu.VMEM((LOCAL, MODEL_WIDTH), F32),
            pltpu.VMEM((LOCAL, MODEL_WIDTH), F32),
            pltpu.SemaphoreType.DMA((8, 3, 2)),
        ],
        cost_estimate=pl.CostEstimate(
            flops=2 * 10**10, bytes_accessed=40_000_000, transcendentals=0
        ),
        name="feed",
    )(normed_two, cot_all, gate_weight.T, upper_weight.T, down_weight.T, ffn_other)
    (
        out_keep, out_got, in_keep, in_got, small, chain, kv_all, kept, _, landing
    ) = back_call(
        hidden, proj_cols, query_cols,
        back_part, out_part, mid, cot_all, all_gains, own_proj, other_proj, normed_two,
        activated, gate_grad, upper_grad, query_rot, kv_own, kv_other, attended, probs,
        cosine, sine, x_own, normed_one,
    )
    down_sum, gate_sum, upper_sum = (kept[m].astype(F32) + landing[m].astype(F32) for m in range(3))
    gain_sums = small[:, :2].sum(0)
    query_bias_grad = lax.dynamic_slice(
        small,
        (c, 2, lax.axis_index("dp") * (query_cols // 4)),
        (1, 1, query_cols // 4),
    )[0, 0]
    pair = small[:, 2, query_cols:proj_cols].reshape(KEYVALUE_HEADS, -1, 2, HEAD_SIZE).sum(1)
    kv_bias_grad = jnp.transpose(pair, (1, 0, 2)).reshape(-1)

    def returned(keep, got):
        got = got.astype(F32)
        return jnp.concatenate(
            [jnp.where(r == 0, keep, got), jnp.where(r == 0, got, keep)]
        ).T

    return (
        returned(out_keep, out_got),
        returned(in_keep, in_got),
        gain_sums[0],
        chain[:, :query_cols],
        query_bias_grad,
        kv_all.astype(F32),
        kv_bias_grad,
        chain[:, proj_cols:],
        gain_sums[1],
        gate_sum,
        upper_sum,
        down_sum,
    )


def per_device(*arrays):
    sizes = tuple(lax.axis_size(axis) for axis in ("dp", "row", "col"))
    if sizes == (4, 2, LINE) and arrays[0].shape == (HALF, 2 * BLOCK):
        return fast_device(*arrays)
    return general_device(*arrays)


def solution(mesh):
    placed = (
        P("row", ("dp", "col")),
        P(("dp", "row")),
        P("row"),
        P("row", "col"),
        P("col"),
        P("row", None),
        P(),
        P("row", "col"),
        P("row"),
        P("row", "col"),
        P("row", "col"),
        P("row", "col"),
        P("row", ("dp", "col")),
    )
    return jax.shard_map(
        per_device,
        mesh=mesh,
        in_specs=placed,
        out_specs=(
            P("row", ("dp", "col")),
            P("row", ("dp", "col")),
            P("row"),
            P(("row", "dp"), "col"),
            P(("col", "dp")),
            P("row", None),
            P(),
            P(("row", "dp"), "col"),
            P("row"),
            P(("row", "dp"), "col"),
            P(("row", "dp"), "col"),
            P(("row", "dp"), "col"),
        ),
        check_vma=False,
    )
```

```python
import jax
import jax.numpy as jnp
from jax import lax
from jax.experimental import pallas as pl
from jax.experimental.pallas import tpu as pltpu
from jax.sharding import PartitionSpec as P

MODEL_WIDTH = 1536
KEYVALUE_HEADS = 2
HEAD_SIZE = 128


EPS = 1e-06
THETA = 1000000.0
NEG = -1e30


def rope_tables(position_ids):
    half_dim = HEAD_SIZE // 2
    frequencies = THETA ** (-(jnp.arange(half_dim, dtype=jnp.float32) * 2.0 / HEAD_SIZE))
    angles = position_ids.astype(jnp.float32)[:, None] * frequencies[None, :]
    cosine_values = jnp.cos(angles)
    sine_lookup = jnp.sin(angles)
    return (
        jnp.concatenate([cosine_values, cosine_values], -1),
        jnp.concatenate([sine_lookup, sine_lookup], -1),
    )


def apply_rotation(values, cosine_values, sine_lookup):
    half_dim = HEAD_SIZE // 2
    turned = jnp.concatenate([-values[..., half_dim:], values[..., :half_dim]], -1)
    return values * cosine_values[:, None, :] + turned * sine_lookup[:, None, :]


def unrotate(gradient, cosine_values, sine_lookup):
    half_dim = HEAD_SIZE // 2
    scaled = gradient * sine_lookup[:, None, :]
    turned = jnp.concatenate([scaled[..., half_dim:], -scaled[..., :half_dim]], -1)
    return gradient * cosine_values[:, None, :] + turned


def row_total(partial_value):
    return lax.psum(partial_value, "row")


def norm_forward(x_float, gain):
    squares = jnp.sum(x_float * x_float, -1)
    rinv = lax.rsqrt(row_total(squares) / MODEL_WIDTH + EPS)[:, None]
    return ((x_float * rinv * gain).astype(jnp.bfloat16), rinv)


def norm_backward(normed_grad, x_float, rinv, gain):
    scaled = normed_grad * gain
    inner = row_total(jnp.sum(scaled * x_float, -1))[:, None]
    input_part = rinv * scaled - x_float * rinv**3 * inner / MODEL_WIDTH
    gain_part = jnp.sum(normed_grad * x_float * rinv, 0)
    return (input_part, gain_part)


def column_gather(values):
    return lax.all_gather(values, "col", axis=0, tiled=True)


def column_sum(partial_value):
    return lax.psum_scatter(
        partial_value.astype(jnp.bfloat16), "col", scatter_dimension=0, tiled=True
    ).astype(jnp.float32)


def row_product(gathered, weight):
    return (
        lax.psum_scatter(
            jnp.dot(gathered, weight, preferred_element_type=jnp.float32).astype(jnp.bfloat16),
            "row",
            scatter_dimension=0,
            tiled=True,
        ).astype(jnp.float32),
        gathered,
    )


def row_project(local_part, weight):
    return lax.dot_general(
        lax.all_gather(local_part, "row", axis=0, tiled=True),
        weight,
        (((1,), (1,)), ((), ())),
        preferred_element_type=jnp.float32,
    )


def row_fold(local_part, partner, weight):
    pair_dims = (((0,), (0,)), ((), ()))

    def accumulate(block_rows):
        grad_sum = lax.dot_general(
            partner, block_rows, pair_dims, preferred_element_type=jnp.float32
        )
        if weight is None:
            return (grad_sum,)
        back_proj = lax.dot_general(
            block_rows, weight, (((1,), (1,)), ((), ())), preferred_element_type=jnp.float32
        )
        column_totals = jnp.sum(block_rows, 0, dtype=jnp.float32)
        return (grad_sum, back_proj, column_totals)

    return accumulate(lax.all_gather(local_part, "row", axis=0, tiled=True))


def causal_scores(query_rot, rotated_keys):
    scores = jnp.einsum(
        "ihd,jd->hij", query_rot, rotated_keys, preferred_element_type=jnp.float32
    ) * HEAD_SIZE ** (-0.5)
    length = query_rot.shape[0]
    allowed = jnp.arange(length)[:, None] >= jnp.arange(length)[None, :]
    return jnp.where(allowed[None], scores, NEG)


def attend(query_rot, rotated_keys, value_second_part):
    scores = causal_scores(query_rot, rotated_keys)
    row_max = jnp.max(scores, -1, keepdims=True)
    log_total = row_max + jnp.log(jnp.sum(jnp.exp(scores - row_max), -1, keepdims=True))
    probs_half = jnp.exp(scores - log_total).astype(jnp.bfloat16)
    attended = jnp.einsum(
        "hij,jd->ihd", probs_half, value_second_part, preferred_element_type=jnp.float32
    ).astype(jnp.bfloat16)
    return (attended, log_total)


def attend_back(query_rot, rotated_keys, value_second_part, attended, att_grad, log_total):
    scale = HEAD_SIZE ** (-0.5)
    softmax_probs = jnp.exp(causal_scores(query_rot, rotated_keys) - log_total)
    probs_half = softmax_probs.astype(jnp.bfloat16)
    prob_grad = jnp.einsum(
        "ihd,jd->hij", att_grad, value_second_part, preferred_element_type=jnp.float32
    )
    row_delta = jnp.einsum("ihd,ihd->hi", att_grad, attended, preferred_element_type=jnp.float32)
    score_half = (softmax_probs * (prob_grad - row_delta[:, :, None])).astype(jnp.bfloat16)
    query_grad = (
        jnp.einsum("hij,jd->ihd", score_half, rotated_keys, preferred_element_type=jnp.float32)
        * scale
    )
    key_grad = (
        jnp.einsum("hij,ihd->jd", score_half, query_rot, preferred_element_type=jnp.float32) * scale
    )
    value_grad = jnp.einsum("hij,ihd->jd", probs_half, att_grad, preferred_element_type=jnp.float32)
    return (query_grad, key_grad, value_grad)


def general_device(
    block_input,
    position_ids,
    attention_gain,
    query_weight,
    query_bias,
    key_value_weight,
    key_value_bias,
    output_weight,
    feedforward_gain,
    gate_weight,
    upper_weight,
    down_weight,
    out_cotangent,
):
    single_float_type = jnp.float32
    brain_float_type = jnp.bfloat16
    column_number = lax.axis_size("col")
    seq_len = position_ids.shape[0]
    heads_here = query_weight.shape[1] // HEAD_SIZE
    query_cols = query_weight.shape[1]
    hidden_cols = gate_weight.shape[1]
    key_value_head = lax.axis_index("col") // (column_number // KEYVALUE_HEADS)
    key_start = key_value_head * HEAD_SIZE
    value_offset = KEYVALUE_HEADS * HEAD_SIZE + key_value_head * HEAD_SIZE
    keyval_local = jnp.concatenate(
        [
            lax.dynamic_slice_in_dim(key_value_weight, key_start, HEAD_SIZE, 1),
            lax.dynamic_slice_in_dim(key_value_weight, value_offset, HEAD_SIZE, 1),
        ],
        1,
    )
    bias_local = jnp.concatenate(
        [
            lax.dynamic_slice_in_dim(key_value_bias, key_start, HEAD_SIZE, 0),
            lax.dynamic_slice_in_dim(key_value_bias, value_offset, HEAD_SIZE, 0),
        ],
        0,
    )
    proj_weight = jnp.concatenate([query_weight, keyval_local], 1)
    proj_bias = jnp.concatenate([query_bias, bias_local], 0)
    pair_weight = jnp.concatenate([gate_weight, upper_weight], 1)
    cosine_values, sine_lookup = rope_tables(position_ids)
    x_float = block_input.T.astype(single_float_type)
    cot_local = out_cotangent.T
    normed_one, rinv_one = norm_forward(x_float, attention_gain)
    normed_one_all = column_gather(normed_one)
    proj_out = row_product(normed_one_all, proj_weight)[0] + proj_bias
    query_rot = apply_rotation(
        proj_out[:, :query_cols].reshape(seq_len, heads_here, HEAD_SIZE), cosine_values, sine_lookup
    ).astype(brain_float_type)
    rotated_keys = apply_rotation(
        proj_out[:, query_cols : query_cols + HEAD_SIZE][:, None, :], cosine_values, sine_lookup
    )[:, 0].astype(brain_float_type)
    value_second_part = proj_out[:, query_cols + HEAD_SIZE :].astype(brain_float_type)
    attended, log_total = attend(query_rot, rotated_keys, value_second_part)
    attended_flat = attended.reshape(seq_len, query_cols)
    hidden_res = x_float + column_sum(row_project(attended_flat, output_weight))
    normed_two, rinv_two = norm_forward(hidden_res, feedforward_gain)
    normed_two_all = column_gather(normed_two)
    gate_upper, normed_two_seq = row_product(normed_two_all, pair_weight)
    gate_lin = gate_upper[:, :hidden_cols]
    upper_lin = gate_upper[:, hidden_cols:]
    sigmoid_gate = jax.nn.sigmoid(gate_lin)
    activated = (gate_lin * sigmoid_gate * upper_lin).astype(brain_float_type)
    block_output = hidden_res + column_sum(row_project(activated, down_weight))
    cotangent_all = column_gather(cot_local)
    act_grad = row_product(cotangent_all, down_weight)[0]
    down_grad = row_fold(activated, cotangent_all, None)[0]
    gate_grad = act_grad * upper_lin * sigmoid_gate * (1.0 + gate_lin * (1.0 - sigmoid_gate))
    upper_grad = act_grad * gate_lin * sigmoid_gate
    pair_grad_half = jnp.concatenate([gate_grad, upper_grad], 1).astype(brain_float_type)
    folded_two = row_fold(pair_grad_half, normed_two_all, pair_weight)
    pair_weight_grad = folded_two[0]
    spread_two = folded_two[1]
    normed_two_grad = column_sum(spread_two)
    hidden_part, ffn_gain_part = norm_backward(
        normed_two_grad, hidden_res, rinv_two, feedforward_gain
    )
    hidden_grad = cot_local.astype(single_float_type) + hidden_part
    hidden_half = hidden_grad.astype(brain_float_type)
    hidden_all = column_gather(hidden_half)
    att_grad = (
        row_product(hidden_all, output_weight)[0]
        .astype(brain_float_type)
        .reshape(seq_len, heads_here, HEAD_SIZE)
    )
    output_grad = row_fold(attended_flat, hidden_all, None)[0]
    query_grad, key_grad, value_grad = attend_back(
        query_rot, rotated_keys, value_second_part, attended, att_grad, log_total
    )
    query_half = (
        unrotate(query_grad, cosine_values, sine_lookup)
        .astype(brain_float_type)
        .reshape(seq_len, query_cols)
    )
    key_half = unrotate(key_grad[:, None, :], cosine_values, sine_lookup)[:, 0].astype(
        brain_float_type
    )
    value_grad_half = value_grad.astype(brain_float_type)
    proj_grad_half = jnp.concatenate([query_half, key_half, value_grad_half], 1)
    folded_one = row_fold(proj_grad_half, normed_one_all, proj_weight)
    projection_weight_gradient = folded_one[0]
    normed_one_grad = column_sum(folded_one[1])
    proj_bias_grad = folded_one[2]
    input_part, attn_gain_part = norm_backward(normed_one_grad, x_float, rinv_one, attention_gain)
    input_grad = hidden_grad + input_part
    key_value_gradient = jnp.zeros(
        (projection_weight_gradient.shape[0], 2 * KEYVALUE_HEADS * HEAD_SIZE), single_float_type
    )
    key_value_gradient = lax.dynamic_update_slice_in_dim(
        key_value_gradient,
        projection_weight_gradient[:, query_cols : query_cols + HEAD_SIZE],
        key_start,
        1,
    )
    key_value_gradient = lax.dynamic_update_slice_in_dim(
        key_value_gradient, projection_weight_gradient[:, query_cols + HEAD_SIZE :], value_offset, 1
    )
    key_value_bias_gradient = jnp.zeros((2 * KEYVALUE_HEADS * HEAD_SIZE,), single_float_type)
    key_value_bias_gradient = lax.dynamic_update_slice_in_dim(
        key_value_bias_gradient, proj_bias_grad[query_cols : query_cols + HEAD_SIZE], key_start, 0
    )
    key_value_bias_gradient = lax.dynamic_update_slice_in_dim(
        key_value_bias_gradient, proj_bias_grad[query_cols + HEAD_SIZE :], value_offset, 0
    )
    shared = (
        lax.psum(key_value_gradient.astype(jnp.bfloat16), ("dp", "col")).astype(jnp.float32),
        lax.psum(key_value_bias_gradient.astype(jnp.bfloat16), ("dp", "col")).astype(jnp.float32),
        lax.psum(attn_gain_part.astype(jnp.bfloat16), ("dp", "col")).astype(jnp.float32),
        lax.psum(ffn_gain_part.astype(jnp.bfloat16), ("dp", "col")).astype(jnp.float32),
    )
    summed = (
        lax.psum_scatter(
            projection_weight_gradient[:, :query_cols].astype(jnp.bfloat16),
            "dp",
            scatter_dimension=0,
            tiled=True,
        ).astype(jnp.float32),
        lax.psum_scatter(
            proj_bias_grad[:query_cols].astype(jnp.bfloat16), "dp", scatter_dimension=0, tiled=True
        ).astype(jnp.float32),
        lax.psum_scatter(
            output_grad.astype(jnp.bfloat16), "dp", scatter_dimension=0, tiled=True
        ).astype(jnp.float32),
        lax.psum_scatter(
            pair_weight_grad[:, :hidden_cols].astype(jnp.bfloat16),
            "dp",
            scatter_dimension=0,
            tiled=True,
        ).astype(jnp.float32),
        lax.psum_scatter(
            pair_weight_grad[:, hidden_cols:].astype(jnp.bfloat16),
            "dp",
            scatter_dimension=0,
            tiled=True,
        ).astype(jnp.float32),
        lax.psum_scatter(
            down_grad.astype(jnp.bfloat16), "dp", scatter_dimension=0, tiled=True
        ).astype(jnp.float32),
    )
    return (
        block_output.T,
        input_grad.T,
        shared[2],
        summed[0],
        summed[1],
        shared[0],
        shared[1],
        summed[2],
        shared[3],
        summed[3],
        summed[4],
        summed[5],
    )


MESH_ID = pl.DeviceIdType.MESH
F32 = jnp.float32
BF16 = jnp.bfloat16
LINE = 4
BLOCK = 128
SUB = 2
PART = BLOCK // SUB
LOCAL = LINE * BLOCK
HALF = MODEL_WIDTH // 2
UNIT = MODEL_WIDTH // 8
VMEM_SPEC = pl.BlockSpec(memory_space=pltpu.VMEM)
ANY_SPEC = pl.BlockSpec(memory_space=pl.ANY)
PAIR_ROWS = (((0,), (0,)), ((), ()))
PAIR_COLS = (((1,), (1,)), ((), ()))
SCALE = HEAD_SIZE ** (-0.5)
DMA = pltpu.SemaphoreType.DMA


def greet(me, others):
    barrier = pltpu.get_barrier_semaphore()
    for axis, index in others:
        pl.semaphore_signal(barrier, 1, device_id={axis: index}, device_id_type=MESH_ID)

    @pl.when(me > 0)
    def _():
        pl.semaphore_signal(barrier, 1, device_id={"col": me - 1}, device_id_type=MESH_ID)

    @pl.when(me < LINE - 1)
    def _():
        pl.semaphore_signal(barrier, 1, device_id={"col": me + 1}, device_id_type=MESH_ID)

    @pl.when((me > 0) & (me < LINE - 1))
    def _():
        pl.semaphore_wait(barrier, 2 + len(others))

    @pl.when((me == 0) | (me == LINE - 1))
    def _():
        pl.semaphore_wait(barrier, 1 + len(others))


def aligned(start, size, to=BLOCK):
    return pl.ds(pl.multiple_of(start, to), size)


def block_rows(index):
    return aligned(index * BLOCK, BLOCK)


def send(src, dst, send_sem, recv_sem, axis, to):
    return pltpu.make_async_remote_copy(
        src, dst, send_sem, recv_sem, device_id={axis: to}, device_id_type=MESH_ID
    )


def landed(ref, sem):
    pltpu.make_async_copy(ref, ref, sem).wait()


class Gather:
    def __init__(self, me, all_ref, sends, recv):
        self.me, self.all_ref, self.sends, self.recv = me, all_ref, sends, recv

    def rows(self, j, p):
        return self.all_ref.at[aligned(j * BLOCK + p * PART, PART, PART)]

    def copy(self, j, p, s, side):
        rows = self.rows(j, p)
        return send(
            rows, rows, self.sends.at[side, s, p], self.recv.at[j, p], "col",
            self.me + 1 - 2 * side,
        )

    def has_next(self, side):
        to = self.me + 1 - 2 * side
        return (to >= 0) & (to < LINE)

    def step(self, s, wait=True, forward=True):
        @pl.loop(0, 2 * SUB)
        def _(i):
            side, p = lax.rem(i, 2), i // 2
            j = self.me - (1 - 2 * side) * s

            @pl.when((j >= 0) & (j < LINE))
            def _():
                if s and wait:
                    landed(self.rows(j, p), self.recv.at[j, p])

                if forward and s < LINE - 1:

                    @pl.when(self.has_next(side))
                    def _():
                        self.copy(j, p, s, side).start()

    def run_each(self, s, each):
        if s == 0:
            each(self.me)
            return

        @pl.loop(0, 2)
        def _(side):
            j = self.me - (1 - 2 * side) * s

            @pl.when((j >= 0) & (j < LINE))
            def _():
                each(j)

    def drain(self, first=0, last=LINE - 1):
        for s in range(first, last):

            @pl.loop(0, 2)
            def _(side):
                j = self.me - (1 - 2 * side) * s

                @pl.when((j >= 0) & (j < LINE) & self.has_next(side))
                def _():
                    for p in range(SUB):
                        self.copy(self.me, p, s, side).wait_send()


class Scatter:
    def __init__(self, me, block_of, landing, sends, recv):
        self.me, self.block_of, self.landing = me, block_of, landing
        self.sends, self.recv = sends, recv

    def rows(self, side, j, p):
        return self.landing.at[side, j, pl.ds(p * PART, PART)]

    def copy(self, side, j, p):
        rows = self.rows(side, j, p)
        return send(
            rows, rows, self.sends.at[side, j, p], self.recv.at[side, j, p], "col",
            self.me + 1 - 2 * side,
        )

    def has_last(self, side):
        came = self.me - 1 + 2 * side
        return (came >= 0) & (came < LINE)

    def step(self, s):
        @pl.loop(0, 2)
        def _(side):
            j = self.me + (1 - 2 * side) * s

            @pl.when((j >= 0) & (j < LINE))
            def _():
                mine = self.block_of(j)
                for p in range(SUB):
                    term = mine[p * PART : (p + 1) * PART]
                    rows = self.rows(side, j, p)

                    @pl.when(self.has_last(side))
                    def _():
                        landed(rows, self.recv.at[side, j, p])
                        rows[...] = (term + rows[...].astype(F32)).astype(BF16)

                    @pl.when(jnp.logical_not(self.has_last(side)))
                    def _():
                        rows[...] = term.astype(BF16)

                    self.copy(side, j, p).start()

    def finish(self, out_ref):
        me = self.me
        out_ref[...] = self.block_of(me)

        @pl.loop(0, 2)
        def _(side):
            @pl.when(self.has_last(side))
            def _():
                for p in range(SUB):
                    rows = self.rows(side, me, p)
                    landed(rows, self.recv.at[side, me, p])
                    out_ref[p * PART : (p + 1) * PART] += rows[...].astype(F32)

    def drain(self):
        for s in range(1, LINE):

            @pl.loop(0, 2)
            def _(side):
                j = self.me + (1 - 2 * side) * s

                @pl.when((j >= 0) & (j < LINE))
                def _():
                    for p in range(SUB):
                        self.copy(side, j, p).wait_send()


def gather_sems():
    return [DMA((2, LINE, SUB)), DMA((LINE, SUB))]


def scatter_sems():
    return [DMA((2, LINE, SUB)), DMA((2, LINE, SUB))]


def dot(a, b, dims=(((1,), (0,)), ((), ()))):
    return lax.dot_general(a, b, dims, preferred_element_type=F32)


def turn(values):
    return pltpu.roll(values, HEAD_SIZE // 2, 1)


def norm_scale(values):
    return lax.rsqrt(jnp.sum(values * values, -1, keepdims=True) / MODEL_WIDTH + EPS)


def shape(rows, cols, dtype=BF16):
    return jax.ShapeDtypeStruct((rows, cols), dtype)


def attend_local(query_ref, own_ref, other_ref, attended_ref, probs_ref, r):
    rows = 2 * BLOCK
    shape = (rows, rows)
    at_row = lax.broadcasted_iota(jnp.int32, shape, 0)
    at_col = lax.broadcasted_iota(jnp.int32, shape, 1)
    own_mask = at_row >= at_col
    other_mask = at_col // BLOCK < at_row // BLOCK + r
    heads = query_ref.shape[1] // HEAD_SIZE
    for s in range(2):
        part = slice(s * rows, (s + 1) * rows)
        for h in range(heads):
            cols = slice(h * HEAD_SIZE, (h + 1) * HEAD_SIZE)
            query = query_ref[part, cols]
            own = jnp.where(own_mask, dot(query, own_ref[part, :HEAD_SIZE], PAIR_COLS) * SCALE, NEG)
            other = jnp.where(
                other_mask, dot(query, other_ref[part, :HEAD_SIZE], PAIR_COLS) * SCALE, NEG
            )
            top = jnp.maximum(
                jnp.max(own, -1, keepdims=True), jnp.max(other, -1, keepdims=True)
            )
            total = jnp.sum(jnp.exp(own - top), -1, keepdims=True) + jnp.sum(
                jnp.exp(other - top), -1, keepdims=True
            )
            log_total = top + jnp.log(total)
            own = jnp.exp(own - log_total).astype(BF16)
            other = jnp.exp(other - log_total).astype(BF16)
            attended_ref[part, cols] = (
                dot(own, own_ref[part, HEAD_SIZE:]) + dot(other, other_ref[part, HEAD_SIZE:])
            ).astype(BF16)
            probs_ref[s * heads + h, :, :rows] = own
            probs_ref[s * heads + h, :, rows:] = other


def attend_back_body(
    query_ref, own_ref, other_ref, attended_ref, probs_ref, grad_ref, cos_ref, sin_ref,
    query_grad_ref, own_grad_ref, other_grad_ref,
):
    rows = 2 * BLOCK
    heads = query_ref.shape[1] // HEAD_SIZE
    for s in range(2):
        part = slice(s * rows, (s + 1) * rows)
        own_key, other_key = own_ref[part, :HEAD_SIZE], other_ref[part, :HEAD_SIZE]
        own_value, other_value = own_ref[part, HEAD_SIZE:], other_ref[part, HEAD_SIZE:]
        sums = [jnp.zeros((rows, HEAD_SIZE), F32) for _ in range(4)]
        for h in range(heads):
            cols = slice(h * HEAD_SIZE, (h + 1) * HEAD_SIZE)
            query, grad = query_ref[part, cols], grad_ref[part, cols]
            own_p = probs_ref[s * heads + h, :, :rows]
            other_p = probs_ref[s * heads + h, :, rows:]
            delta = jnp.sum(
                grad.astype(F32) * attended_ref[part, cols].astype(F32), -1, keepdims=True
            )
            own_s = (own_p.astype(F32) * (dot(grad, own_value, PAIR_COLS) - delta)).astype(BF16)
            other_s = (other_p.astype(F32) * (dot(grad, other_value, PAIR_COLS) - delta)).astype(BF16)
            query_grad = (dot(own_s, own_key) + dot(other_s, other_key)) * SCALE
            query_grad_ref[part, cols] = (
                query_grad * cos_ref[part] - turn(query_grad) * sin_ref[part]
            ).astype(BF16)
            for i, (weights, partner) in enumerate(
                ((own_s, query), (own_p, grad), (other_s, query), (other_p, grad))
            ):
                sums[i] = sums[i] + dot(weights, partner, PAIR_ROWS)
        own_grad_ref[part, :HEAD_SIZE] = sums[0] * SCALE
        own_grad_ref[part, HEAD_SIZE:] = sums[1]
        other_grad_ref[part, :HEAD_SIZE] = (sums[2] * SCALE).astype(BF16)
        other_grad_ref[part, HEAD_SIZE:] = sums[3].astype(BF16)


PIECES = 6


def front_body(
    input_ref, cot_in_ref, table_ref, small_ref, query_w_ref, kv_w_ref, output_w_ref,
    gate_hbm, upper_hbm, down_hbm,
    x_ref, normed_ref, query_ref, kv_ref, kv_other_ref, cos_ref, sin_ref, gains_ref,
    attended_ref, probs_ref, mid_ref, normed_two_ref, turned_ref, cot_ref, proj_ref, proj_other_ref, weights_other_hbm,
    passing, tables, bias_ref, landing,
    swap_sends, swap_recv, piece_sends, piece_recv, kv_sends, kv_recv,
    g_sends, g_recv, c_sends, c_recv, n_sends, n_recv, s_sends, s_recv,
):
    me, r, d = lax.axis_index("col"), lax.axis_index("row"), lax.axis_index("dp")
    y, core = d // 2, lax.rem(d, 2)
    x_to, y_to, core_to = 1 - r, 2 * (1 - y) + core, 2 * y + 1 - core
    query_cols = query_ref.shape[1]
    proj_cols = query_cols + 2 * HEAD_SIZE
    quarter = HALF // 2
    my_rows = aligned(core * quarter, quarter, quarter)
    its_rows = aligned((1 - core) * quarter, quarter, quarter)
    eighth = quarter // 2
    to_y = aligned(core * quarter + y * eighth, eighth, eighth)
    in_cols, out_cols = pl.ds(0, proj_cols), pl.ds(proj_cols, query_cols)
    kv_width = KEYVALUE_HEADS * HEAD_SIZE
    kv_at = me // (LINE // KEYVALUE_HEADS) * HEAD_SIZE

    passing[0] = input_ref[:, block_rows(1 - r)].T
    x_ref[:, :HALF] = input_ref[:, block_rows(r)].T
    proj_ref[:, :query_cols] = query_w_ref[...]
    for i in range(2):
        proj_ref[:, query_cols + i * HEAD_SIZE : query_cols + (i + 1) * HEAD_SIZE] = kv_w_ref[
            :, aligned(i * kv_width + kv_at, HEAD_SIZE)
        ]
    greet(me, [("row", x_to), ("dp", y_to), ("dp", core_to)])

    swaps = [
        (passing.at[0], x_ref.at[:, HALF:], "row", x_to),
        (small_ref.at[:, :HALF], gains_ref.at[pl.ds(0, 1), HALF:], "row", x_to),
        (small_ref.at[:, HALF : 2 * HALF], gains_ref.at[pl.ds(1, 1), HALF:], "row", x_to),
        (proj_ref.at[to_y, in_cols], proj_other_ref.at[to_y, in_cols], "row", x_to),
        (table_ref.at[block_rows(1 - r)], tables.at[pl.ds(0, BLOCK)], "row", x_to),
        (table_ref.at[block_rows(3 - r)], tables.at[pl.ds(BLOCK, BLOCK)], "row", x_to),
        (passing.at[1], cot_ref.at[block_rows(me), HALF:], "row", x_to),
        (proj_ref.at[to_y, out_cols], proj_other_ref.at[to_y, out_cols], "row", x_to),
        (proj_other_ref.at[to_y, in_cols], proj_other_ref.at[to_y, in_cols], "dp", y_to),
        (proj_other_ref.at[to_y, out_cols], proj_other_ref.at[to_y, out_cols], "dp", y_to),
        (proj_other_ref.at[my_rows, in_cols], proj_other_ref.at[my_rows, in_cols], "dp", core_to),
        (proj_other_ref.at[my_rows, out_cols], proj_other_ref.at[my_rows, out_cols], "dp", core_to),
    ]

    def swap_copy(i):
        src, dst, axis, to = swaps[i]
        return send(src, dst, swap_sends.at[i], swap_recv.at[i], axis, to)

    def swap_landed(i):
        swap_copy(i).wait_recv()

    rows = gate_hbm.shape[0] // 4
    owns = (gate_hbm, upper_hbm, down_hbm)

    def piece(i, of_y):
        return aligned((of_y * 2 + i % 2) * rows, rows, rows)

    def piece_copy(i, way):
        m = i // 2
        of_y = 1 - y if way == 3 else y
        at = weights_other_hbm.at[m, piece(i, of_y), my_rows]
        src = owns[m].at[piece(i, of_y), my_rows] if way == 0 else at
        axis, to = (("row", x_to), ("dp", y_to), ("dp", core_to), ("dp", core_to))[way]
        return send(src, at, piece_sends.at[way, i], piece_recv.at[way, i], axis, to)

    def relay_x(i):
        piece_copy(i, 0).wait_recv()
        piece_copy(i, 1).start()
        piece_copy(i, 2).start()

    def relay_y(i):
        piece_copy(i, 1).wait_recv()
        piece_copy(i, 3).start()

    for i in range(6):
        swap_copy(i).start()
    passing[1] = cot_in_ref[:, block_rows(1 - r)].T
    proj_ref[:, proj_cols:] = output_w_ref[...]
    swap_copy(6).start()
    swap_copy(7).start()
    cot_ref[block_rows(me), :HALF] = cot_in_ref[:, block_rows(r)].T
    gains_ref[0:1, :HALF] = small_ref[:, :HALF]
    gains_ref[1:2, :HALF] = small_ref[:, HALF : 2 * HALF]
    bias_ref[:, :query_cols] = small_ref[:, 2 * HALF : 2 * HALF + query_cols]
    for i in range(2):
        bias_ref[:, query_cols + i * HEAD_SIZE : query_cols + (i + 1) * HEAD_SIZE] = small_ref[
            :, aligned(2 * HALF + query_cols + i * kv_width + kv_at, HEAD_SIZE)
        ]
    swap_landed(0)
    swap_landed(1)
    swap_landed(2)
    x = x_ref[...].astype(F32)
    normed_ref[block_rows(me)] = (x * norm_scale(x) * gains_ref[0:1]).astype(BF16)
    gather = Gather(me, normed_ref, g_sends, g_recv)
    gather.step(0)

    lane = lax.broadcasted_iota(jnp.int32, (BLOCK, HEAD_SIZE), 1)
    first = lane < HEAD_SIZE // 2
    swap_landed(3)
    swap_copy(8).start()
    gather.step(1)
    swap_landed(8)
    swap_copy(10).start()
    swap_landed(4)
    swap_landed(5)
    for i in range(4):
        if i < 2:
            table = table_ref[block_rows(r + 2 * i)]
        else:
            table = tables[(i - 2) * BLOCK : (i - 1) * BLOCK]
        turned = turn(table)
        at = block_rows((r if i < 2 else 1 - r) * 2 + i % 2)
        cos_ref[at] = jnp.where(first, table, turned)
        sin_ref[at] = jnp.where(first, -turned, table)
    swap_landed(10)

    def kv_copy(j):
        at = block_rows(j)
        return send(
            kv_ref.at[at], kv_other_ref.at[at], kv_sends.at[j], kv_recv.at[j], "row", x_to
        )

    def each(j):
        at = block_rows(j)
        block = normed_ref[at]
        out = dot(block[:, :HALF], proj_ref[:, :proj_cols])
        out = out + dot(block[:, HALF:], proj_other_ref[:, :proj_cols]) + bias_ref[...]
        cosine, sine = cos_ref[at], sin_ref[at]
        for h in range(query_cols // HEAD_SIZE + 1):
            head = out[:, h * HEAD_SIZE : (h + 1) * HEAD_SIZE]
            turned = (head * cosine + turn(head) * sine).astype(BF16)
            if h * HEAD_SIZE < query_cols:
                query_ref[at, h * HEAD_SIZE : (h + 1) * HEAD_SIZE] = turned
            else:
                kv_ref[at, :HEAD_SIZE] = turned
        kv_ref[at, HEAD_SIZE:] = out[:, query_cols + HEAD_SIZE :].astype(BF16)
        kv_copy(j).start()

    gather.run_each(0, each)
    gather.run_each(1, each)
    gather.step(2)
    gather.run_each(2, each)
    swap_landed(7)
    swap_copy(9).start()
    gather.step(3)
    gather.run_each(3, each)
    for i in range(PIECES):
        piece_copy(i, 0).start()
    swap_landed(6)
    cot_gather = Gather(me, cot_ref, c_sends, c_recv)
    cot_gather.step(0)
    swap_landed(9)
    swap_copy(11).start()
    for j in range(LINE):
        kv_copy(j).wait_recv()
    attend_local(query_ref, kv_ref, kv_other_ref, attended_ref, probs_ref, r)
    swap_landed(11)

    def block_of(j):
        block = attended_ref[block_rows(j)]
        return jnp.concatenate(
            [
                dot(block, proj_ref[:, proj_cols:], PAIR_COLS),
                dot(block, proj_other_ref[:, proj_cols:], PAIR_COLS),
            ],
            1,
        )

    scatter = Scatter(me, block_of, landing, s_sends, s_recv)
    scatter.step(3)
    scatter.step(2)
    scatter.step(1)
    relay_x(0)
    relay_x(1)
    scatter.finish(mid_ref)
    mid = mid_ref[...] + x_ref[...].astype(F32)
    mid_ref[...] = mid
    normed_two_ref[block_rows(me)] = (mid * norm_scale(mid) * gains_ref[1:2]).astype(BF16)

    def turn_block(j):
        turned_ref[:, block_rows(j)] = normed_two_ref[block_rows(j)].T

    second = Gather(me, normed_two_ref, n_sends, n_recv)
    second.step(0)
    second.run_each(0, turn_block)
    relay_x(2)
    relay_y(0)
    second.step(1)
    second.run_each(1, turn_block)
    relay_x(3)
    relay_y(1)
    second.step(2)
    second.run_each(2, turn_block)
    relay_x(4)
    relay_y(2)
    second.step(3)
    second.run_each(3, turn_block)
    relay_x(5)
    relay_y(3)
    relay_y(4)
    relay_y(5)
    cot_gather.step(1, forward=False)
    for i in range(PIECES):
        for way in (2, 3):
            of_y = y if way == 2 else 1 - y
            landed(weights_other_hbm.at[i // 2, piece(i, of_y), its_rows], piece_recv.at[way, i])
        for way in range(4):
            piece_copy(i, way).wait_send()
    for i in range(len(swaps)):
        swap_copy(i).wait_send()
    for j in range(LINE):
        kv_copy(j).wait_send()
    gather.drain()
    cot_gather.drain(0, 1)
    second.drain()
    scatter.drain()


def front_call(proj_cols, query_cols, hidden, *args):
    heads = query_cols // HEAD_SIZE
    outs = [
        shape(BLOCK, MODEL_WIDTH),
        shape(LOCAL, MODEL_WIDTH),
        shape(LOCAL, query_cols),
        shape(LOCAL, 2 * HEAD_SIZE),
        shape(LOCAL, 2 * HEAD_SIZE),
        shape(LOCAL, HEAD_SIZE, F32),
        shape(LOCAL, HEAD_SIZE, F32),
        shape(2, MODEL_WIDTH, F32),
        shape(LOCAL, query_cols),
        jax.ShapeDtypeStruct((2 * heads, 2 * BLOCK, 4 * BLOCK), BF16),
        shape(BLOCK, MODEL_WIDTH, F32),
        shape(LOCAL, MODEL_WIDTH),
        shape(MODEL_WIDTH, LOCAL),
        shape(LOCAL, MODEL_WIDTH),
        shape(HALF, proj_cols + query_cols),
        shape(HALF, proj_cols + query_cols),
        jax.ShapeDtypeStruct((3, hidden, HALF), BF16),
    ]
    return pl.pallas_call(
        front_body,
        out_shape=outs,
        in_specs=[VMEM_SPEC] * 7 + [ANY_SPEC] * 3,
        out_specs=[VMEM_SPEC] * (len(outs) - 1) + [ANY_SPEC],
        scratch_shapes=[
            pltpu.VMEM((2, BLOCK, HALF), BF16),
            pltpu.VMEM((2 * BLOCK, HEAD_SIZE), F32),
            pltpu.VMEM((1, proj_cols), F32),
            pltpu.VMEM((2, LINE, BLOCK, MODEL_WIDTH), BF16),
            DMA((12,)),
            DMA((12,)),
            DMA((4, PIECES)),
            DMA((4, PIECES)),
            DMA((LINE,)),
            DMA((LINE,)),
        ]
        + gather_sems() * 3
        + scatter_sems(),
        compiler_params=pltpu.CompilerParams(
            collective_id=1, has_side_effects=True, vmem_limit_bytes=67_043_328
        ),
        cost_estimate=pl.CostEstimate(
            flops=4 * 10**9, bytes_accessed=40_000_000, transcendentals=0
        ),
        name="front",
    )(*args)


DOWN, GATE, UPPER, CHAIN = 0, 1, 2, 3
UNITS = ((1, 1), (1, 0), (0, 1), (0, 0))
TILE = 256


def add_into(total_ref, term_ref, cols):
    @pl.loop(0, total_ref.shape[0] // 32)
    def _(i):
        at = aligned(i * 32, 32, 32)
        total_ref[at, cols] = (
            total_ref[at, cols].astype(F32) + term_ref[at, cols].astype(F32)
        ).astype(BF16)


def rear_body(
    mid_ref, gains_ref,
    normed_two_hbm, turned_hbm, cot_hbm, gate_hbm, upper_hbm, down_hbm, other_hbm, proj_hbm, proj_other_hbm, query_hbm, kv_hbm,
    kv_other_hbm, attended_hbm, probs_hbm, cos_hbm, sin_hbm, x_hbm, normed_one_hbm,
    out_ref, in_ref, small_ref, query_w_ref, output_w_ref, kv_all_ref, kept_hbm, land2_hbm, land3_hbm,
    cot_ref, activated_ref, gate_grad_ref, upper_grad_ref, out_part_ref, back_part_ref, turned_ref,
    kv_got_ref, got_ref, out_landing, landing, sums, gives, gots,
    chain_gots, chain_land2, chain_land3, kv_line, small_line, small_swap,
    load_sems, w_sems, c_sends, c_recv, o_sends, o_recv, r_sends, r_recv, a_sends, a_recv,
    give_sends, give_recv, two_sends, two_recv, three_sends, three_recv, stage_sem, kept_sems,
    swap_sends, swap_recv, kv_sends, kv_recv, kvd_sends, kvd_recv, line_sends, line_recv,
    small_sends, small_recv, credit,
):
    me, r, d = lax.axis_index("col"), lax.axis_index("row"), lax.axis_index("dp")
    y, core = d // 2, lax.rem(d, 2)
    x_to, y_to, core_to = 1 - r, 2 * (1 - y) + core, 2 * y + 1 - core
    diagonal_to = 2 * (1 - y) + 1 - core
    hidden = activated_ref.shape[1]
    query_cols = query_w_ref.shape[1]
    proj_cols = query_cols + 2 * HEAD_SIZE
    chain_cols = proj_cols + query_cols
    owns = (gate_hbm, upper_hbm, down_hbm)

    def cot_loads(act):
        for i in range(3):
            j = me - 1 + i

            @pl.when((j >= 0) & (j < LINE))
            def _():
                rows = block_rows(j)
                act(pltpu.make_async_copy(cot_hbm.at[rows], cot_ref.at[rows], load_sems.at[i]))

    turned_load = pltpu.make_async_copy(turned_hbm, turned_ref.at[1], load_sems.at[14])
    turned_load.start()
    cot_loads(lambda copy: copy.start())

    halves = {m: (hidden // 2 + BLOCK - 1) // BLOCK * BLOCK for m in (DOWN, GATE, UPPER)}
    halves[CHAIN] = chain_cols // 2

    def columns(m, axis):
        width = chain_cols if m == CHAIN else hidden
        return pl.ds(0, halves[m]) if axis == "row" else pl.ds(halves[m], width - halves[m])

    def unit_rows(h, rel):
        of_y = 1 - y if rel else y
        return aligned(h * HALF + of_y * 2 * UNIT, 2 * UNIT)

    def split(res, keep_ref, give_ref, at):
        low, high = res[:UNIT], res[UNIT:]
        keep_ref[:, at] = jnp.where(core == 0, low, high).astype(BF16)
        give_ref[:, at] = jnp.where(core == 0, high, low).astype(BF16)

    order = [
        (DOWN, 0), (DOWN, 1), (DOWN, 2), (UPPER, 0), (UPPER, 1), (UPPER, 2), (DOWN, 3),
        (GATE, 0), (GATE, 1), (GATE, 2), (UPPER, 3), (GATE, 3),
    ]
    columns_of = {DOWN: activated_ref, GATE: gate_grad_ref, UPPER: upper_grad_ref}
    ring = 3

    def total_of(m, h, rel):
        return sums.at[m * 4 + h * 2 + rel]

    def give_copy(u):
        return send(
            gives.at[u % 2], gots.at[u % ring], give_sends.at[u], give_recv.at[u], "dp", core_to
        )

    def compute(u):
        m, i = order[u]
        h, rel = UNITS[i]
        if u >= 2:
            give_copy(u - 2).wait_send()
        left = 0 if m == DOWN else 1
        rows = unit_rows(h, rel)
        tile = 512

        def run(at):
            res = dot(turned_ref[left, rows], columns_of[m][:, at])
            split(res, total_of(m, h, rel), gives.at[u % 2], at)

        @pl.loop(0, hidden // tile)
        def _(i):
            run(aligned(i * tile, tile))

        if hidden % tile:
            run(pl.ds(hidden // tile * tile, hidden % tile))
        if u >= ring:
            pl.semaphore_wait(credit, 1)
        give_copy(u).start()

    def two_copy(m, k, chain_sums=None):
        h, rel = ((1, 0), (1, 1), (0, 1), (1, 1))[k]
        axis, to = (("row", x_to), ("dp", y_to))[k // 2]
        at = columns(m, axis)
        if m == CHAIN:
            src, dst = chain_sums.at[h * 2 + rel, :, at], chain_land2.at[k % 2, :, at]
        else:
            src, dst = total_of(m, h, rel).at[:, at], land2_hbm.at[m * 2 + k % 2, :, at]
        return send(src, dst, two_sends.at[m, k], two_recv.at[m, k], axis, to)

    def combine(u):
        m, i = order[u]
        h, rel = UNITS[i]
        give_copy(u).wait_recv()
        add_into(total_of(m, h, rel), gots.at[u % ring], pl.ds(0, hidden))
        if u < len(order) - ring:
            pl.semaphore_signal(credit, 1, device_id={"dp": core_to}, device_id_type=MESH_ID)
        for k in {(1, 1): (1, 3), (1, 0): (0,), (0, 1): (2,), (0, 0): ()}[h, rel]:
            two_copy(m, k).start()

    def three_copy(m, k, chain_sums=None):
        h, rel = ((0, 1), (1, 0))[k]
        axis, to = (("dp", y_to), ("row", x_to))[k]
        at = columns(m, ("row", "dp")[k])
        if m == CHAIN:
            src, dst = chain_sums.at[h * 2 + rel, :, at], chain_land3.at[:, at]
        else:
            src, dst = total_of(m, h, rel).at[:, at], land3_hbm.at[m, :, at]
        return send(src, dst, three_sends.at[m, k], three_recv.at[m, k], axis, to)

    def kept_copy(m):
        return pltpu.make_async_copy(total_of(m, 0, 0), kept_hbm.at[m], kept_sems.at[m])

    def stage(m, i):
        return pltpu.make_async_copy(land2_hbm.at[m * 2 + i], gots.at[i], stage_sem.at[m, i])

    def second_stage(m):
        for k in range(4):
            two_copy(m, k).wait_recv()
        for i in (1, 0):
            stage(m, i).start()
        stage(m, 1).wait()
        add_into(total_of(m, 0, 1), gots.at[1], columns(m, "row"))
        three_copy(m, 0).start()
        add_into(total_of(m, 1, 0), gots.at[1], columns(m, "dp"))
        three_copy(m, 1).start()
        stage(m, 0).wait()
        add_into(total_of(m, 0, 0), gots.at[0], pl.ds(0, hidden))
        kept_copy(m).start()

    barrier = pltpu.get_barrier_semaphore()
    others = [("row", x_to), ("dp", y_to), ("dp", core_to)]
    for axis, index in others:
        pl.semaphore_signal(barrier, 1, device_id={axis: index}, device_id_type=MESH_ID)
    for s in range(1, LINE):
        pl.semaphore_signal(
            barrier, 1, device_id={"col": lax.rem(me + s, LINE)}, device_id_type=MESH_ID
        )

    cot_gather = Gather(me, cot_ref, c_sends, c_recv)
    out_scatter = Scatter(
        me, lambda j: out_part_ref[block_rows(j)].astype(F32), out_landing, o_sends, o_recv
    )

    def feed(weights, gates, total, normed_two_ref):
        tiles = hidden // TILE
        rest = hidden % TILE

        def loads(t, slot, size):
            rows = aligned(t * TILE, size, TILE)
            for m in range(3):
                for i, src in enumerate((owns[m].at[rows], other_hbm.at[m, rows])):
                    yield pltpu.make_async_copy(
                        src,
                        weights.at[slot, m, pl.ds(0, size), pl.ds(i * HALF, HALF)],
                        w_sems.at[slot, m, i],
                    )

        def start(t, slot, size):
            for copy in loads(t, slot, size):
                copy.start()

        def ready(t, slot, size):
            for copy in loads(t, slot, size):
                copy.wait()

        def sweep(body, first_slot, hooks, again):
            @pl.loop(0, tiles)
            def _(t):
                slot = lax.rem(t + first_slot, 2)
                ready(t, slot, TILE)

                @pl.when(t < tiles - 1)
                def _():
                    start(t + 1, 1 - slot, TILE)

                @pl.when(t == tiles - 1)
                def _():
                    start(tiles, 1 - slot, rest)

                body(aligned(t * TILE, TILE), slot, TILE)
                for at, hook in hooks:
                    pl.when(t == at)(hook)

            slot = (tiles + first_slot) % 2
            ready(tiles, slot, rest)
            if again:
                start(0, 1 - slot, TILE)
            body(pl.ds(tiles * TILE, rest), slot, rest)

        def add_products(slot, size, factors, cols):
            width = 512

            @pl.loop(0, MODEL_WIDTH // width)
            def _(i):
                at = aligned(i * width, width)
                term = sum(
                    dot(factor[:, cols], weights[slot, m, pl.ds(0, size), at])
                    for factor, m in factors
                )
                total[:, at] += term

        def forward(cols, slot, size):
            here = pl.ds(0, size)
            gate = dot(normed_two_ref[...], weights[slot, 0, here], PAIR_COLS)
            upper = dot(normed_two_ref[...], weights[slot, 1, here], PAIR_COLS)
            activated = (gate * jax.nn.sigmoid(gate) * upper).astype(BF16)
            gates[0, :, cols] = gate.astype(BF16)
            gates[1, :, cols] = upper.astype(BF16)
            activated_ref[:, cols] = activated
            total[...] += dot(activated, weights[slot, 2, here])

        def backward(cols, slot, size):
            here = pl.ds(0, size)
            act_grad = dot(cot_ref[...], weights[slot, 2, here], PAIR_COLS)
            gate, upper = gates[0, :, cols].astype(F32), gates[1, :, cols].astype(F32)
            sig = jax.nn.sigmoid(gate)
            gate_grad = (act_grad * upper * sig * (1.0 + gate * (1.0 - sig))).astype(BF16)
            upper_grad = (act_grad * gate * sig).astype(BF16)
            gate_grad_ref[:, cols] = gate_grad
            upper_grad_ref[:, cols] = upper_grad
            add_products(slot, size, ((gate_grad_ref, 0), (upper_grad_ref, 1)), cols)

        load = pltpu.make_async_copy(normed_two_hbm, normed_two_ref, load_sems.at[15])
        load.start()
        start(0, 0, TILE)
        total[...] = jnp.zeros_like(total)
        pl.semaphore_wait(barrier, len(others) + LINE - 1)
        cot_loads(lambda copy: copy.wait())
        cot_gather.step(1, wait=False)
        load.wait()
        turned_load.wait()
        sweep(forward, 0, [(4, lambda: cot_gather.step(2))], True)
        out_part_ref[...] = total[...].astype(BF16)
        out_scatter.step(3)
        cot_gather.step(3)
        turned_ref[0] = cot_ref[...].T
        total[...] = jnp.zeros_like(total)
        compute(0)
        compute(1)
        combine(0)
        combine(1)
        sweep(backward, (tiles + 1) % 2, [(3, lambda: out_scatter.step(2))], False)
        back_part_ref[...] = total[...].astype(BF16)
        cot_gather.drain(1, LINE - 1)

    pl.run_scoped(
        feed,
        pltpu.VMEM((2, 3, TILE, MODEL_WIDTH), BF16),
        pltpu.VMEM((2, LOCAL, hidden), BF16),
        pltpu.VMEM((LOCAL, MODEL_WIDTH), F32),
        pltpu.VMEM((LOCAL, MODEL_WIDTH), BF16),
    )

    def rest(
        proj_ref, proj_other_ref, query_ref, kv_ref, kv_other_ref, attended_ref, probs_ref, cos_ref,
        sin_ref, x_ref, normed_one_ref, mid_grad_ref, own_ref, att_grad_ref,
        kv_grad_ref, kv_give_ref, proj_grad_ref, chain_sums, back_give,
    ):
        pairs = (
            (proj_hbm, proj_ref), (proj_other_hbm, proj_other_ref), (query_hbm, query_ref),
            (kv_hbm, kv_ref), (kv_other_hbm, kv_other_ref), (attended_hbm, attended_ref),
            (probs_hbm, probs_ref), (cos_hbm, cos_ref), (sin_hbm, sin_ref), (x_hbm, x_ref),
            (normed_one_hbm, normed_one_ref),
        )
        reads = [
            pltpu.make_async_copy(src, dst, load_sems.at[3 + i])
            for i, (src, dst) in enumerate(pairs)
        ]

        mid_half_ref = cot_ref

        scatter = Scatter(
            me, lambda j: back_part_ref[block_rows(j)].astype(F32), landing, r_sends, r_recv
        )
        scatter.step(3)
        for read in reads:
            read.start()
        compute(2)
        compute(3)
        combine(2)
        scatter.step(2)
        compute(4)
        combine(3)
        compute(5)
        combine(4)
        scatter.step(1)
        compute(6)
        combine(5)
        compute(7)
        combine(6)
        scatter.finish(mid_grad_ref)
        mid, grad = mid_ref[...], mid_grad_ref[...]
        rinv = norm_scale(mid)
        small_line[me] = jnp.zeros_like(small_line[me])
        small_line[me, 1:2] = jnp.sum(grad * mid * rinv, 0, keepdims=True)
        scaled = grad * gains_ref[1:2]
        inner = jnp.sum(scaled * mid, -1, keepdims=True)
        mid_grad = (
            cot_ref[block_rows(me)].astype(F32)
            + rinv * scaled
            - mid * rinv**3 * inner / MODEL_WIDTH
        )
        mid_grad_ref[...] = mid_grad
        mid_half_ref[block_rows(me)] = mid_grad.astype(BF16)

        gather = Gather(me, mid_half_ref, a_sends, a_recv)
        gather.step(0)
        scatter.drain()
        for read in reads:
            read.wait()

        def each(j):
            block = mid_half_ref[block_rows(j)]
            att_grad_ref[block_rows(j)] = (
                dot(block[:, :HALF], proj_ref[:, proj_cols:])
                + dot(block[:, HALF:], proj_other_ref[:, proj_cols:])
            ).astype(BF16)

        gather.run_each(0, each)
        compute(8)
        combine(7)
        compute(9)
        combine(8)
        gather.step(1)
        gather.run_each(1, each)
        compute(10)
        combine(9)
        compute(11)
        combine(10)
        combine(11)
        gather.step(2)
        gather.run_each(2, each)
        second_stage(DOWN)
        gather.step(3)
        gather.run_each(3, each)
        out_scatter.step(1)
        attend_back_body(
            query_ref, kv_ref, kv_other_ref, attended_ref, probs_ref, att_grad_ref, cos_ref,
            sin_ref, proj_grad_ref, kv_grad_ref, kv_give_ref,
        )

        def swap_copy(i):
            src, dst = (
                (kv_give_ref, kv_got_ref),
                (back_give.at[0], got_ref.at[0]),
                (back_give.at[1], got_ref.at[1]),
            )[i]
            return send(src, dst, swap_sends.at[i], swap_recv.at[i], "row", x_to)

        swap_copy(0).start()
        second_stage(UPPER)
        swap_copy(0).wait_recv()
        kv = kv_grad_ref[...] + kv_got_ref[...].astype(F32)
        key = kv[:, :HEAD_SIZE]
        proj_grad_ref[:, query_cols : query_cols + HEAD_SIZE] = (
            key * cos_ref[...] - turn(key) * sin_ref[...]
        ).astype(BF16)
        proj_grad_ref[:, query_cols + HEAD_SIZE :] = kv[:, HEAD_SIZE:].astype(BF16)

        def block_of(j):
            block = proj_grad_ref[block_rows(j)]
            return jnp.concatenate(
                [
                    dot(block, proj_ref[:, :proj_cols], PAIR_COLS),
                    dot(block, proj_other_ref[:, :proj_cols], PAIR_COLS),
                ],
                1,
            )

        def chain_from(i):
            return gives.at[i // 2, :, pl.ds(i % 2 * chain_cols, chain_cols)]

        def chain_give(i):
            return send(
                chain_from(i), chain_gots.at[i], give_sends.at[12 + i], give_recv.at[12 + i],
                "dp", core_to,
            )

        def chain_compute(i):
            h, rel = UNITS[i]
            rows = unit_rows(h, rel)
            keep = chain_sums.at[h * 2 + rel]
            res = dot(normed_one_ref[:, rows], proj_grad_ref[...], PAIR_ROWS)
            split(res, keep, chain_from(i), pl.ds(0, proj_cols))
            res = dot(mid_half_ref[:, rows], attended_ref[...], PAIR_ROWS)
            split(res, keep, chain_from(i), pl.ds(proj_cols, query_cols))
            chain_give(i).start()

        def chain_combine(i):
            h, rel = UNITS[i]
            chain_give(i).wait_recv()
            add_into(chain_sums.at[h * 2 + rel], chain_gots.at[i], pl.ds(0, chain_cols))
            for k in {(1, 1): (1, 3), (1, 0): (0,), (0, 1): (2,), (0, 0): ()}[h, rel]:
                two_copy(CHAIN, k, chain_sums).start()

        second = Scatter(me, block_of, landing, r_sends, r_recv)
        second.step(3)
        for u in (len(order) - 2, len(order) - 1):
            give_copy(u).wait_send()
        for i in range(4):
            chain_compute(i)
        for i in range(4):
            chain_combine(i)
        small_line[me, 2:3, :proj_cols] = jnp.sum(
            proj_grad_ref[...].astype(F32), 0, keepdims=True
        )
        second.step(2)
        second_stage(GATE)
        out_scatter.finish(own_ref)
        out = own_ref[...] + mid_ref[...]
        out_ref[:, block_rows(r)] = out[:, :HALF].T
        back_give[1] = out[:, HALF:].astype(BF16)
        second.step(1)
        swap_copy(2).start()
        for k in range(4):
            two_copy(CHAIN, k, chain_sums).wait_recv()
        add_into(chain_sums.at[1], chain_land2.at[1], columns(CHAIN, "row"))
        three_copy(CHAIN, 0, chain_sums).start()
        add_into(chain_sums.at[2], chain_land2.at[1], columns(CHAIN, "dp"))
        three_copy(CHAIN, 1, chain_sums).start()
        add_into(chain_sums.at[0], chain_land2.at[0], pl.ds(0, chain_cols))
        second.finish(own_ref)
        x, grad = x_ref[...].astype(F32), own_ref[...]
        rinv = norm_scale(x)
        scaled = grad * gains_ref[0:1]
        inner = jnp.sum(scaled * x, -1, keepdims=True)
        input_grad = mid_grad_ref[...] + rinv * scaled - x * rinv**3 * inner / MODEL_WIDTH
        back_give[0] = input_grad[:, HALF:].astype(BF16)
        swap_copy(1).start()
        small_line[me, 0:1] = jnp.sum(grad * x * rinv, 0, keepdims=True)

        def small_line_copy(s):
            to = lax.rem(me + s, LINE)
            return send(
                small_line.at[me], small_line.at[me], line_sends.at[s], line_recv.at[me], "col", to
            )

        for s in range(1, LINE):
            small_line_copy(s).start()
        in_ref[:, block_rows(r)] = input_grad[:, :HALF].T

        for s in range(1, LINE):
            landed(small_line.at[me], line_recv.at[lax.rem(me + s, LINE)])
        group = LINE // KEYVALUE_HEADS
        lines = [small_line[j] for j in range(LINE)]
        gain_sum = lines[0][:2] + lines[1][:2] + lines[2][:2] + lines[3][:2]
        small_swap[0] = jnp.zeros_like(small_swap[0])
        small_swap[0, 0:2] = gain_sum
        small_swap[0, 2:3, :query_cols] = small_line[me, 2:3, :query_cols]
        for i in range(2):
            for h in range(KEYVALUE_HEADS):
                at = query_cols + i * HEAD_SIZE
                part = lines[h * group][2:3, at : at + HEAD_SIZE]
                for j in range(1, group):
                    part = part + lines[h * group + j][2:3, at : at + HEAD_SIZE]
                at = (i * KEYVALUE_HEADS + h) * HEAD_SIZE
                small_swap[0, 3:4, at : at + HEAD_SIZE] = part

        def small_copy(i):
            axis, to = (("dp", core_to), ("dp", y_to), ("row", x_to))[i]
            return send(
                small_swap.at[2 * i], small_swap.at[2 * i + 1], small_sends.at[i],
                small_recv.at[i], axis, to,
            )

        small_copy(0).start()
        small_copy(0).wait_recv()
        small_swap[2] = small_swap[0] + small_swap[1]
        small_copy(1).start()

        for k in range(2):
            three_copy(CHAIN, k, chain_sums).wait_recv()
        total = chain_sums[0].astype(F32) + chain_land3[...].astype(F32)
        query_w_ref[...] = total[:, :query_cols]
        output_w_ref[...] = total[:, proj_cols:]
        kv_line[me] = total[:, query_cols:proj_cols].astype(BF16)

        def kv_line_copy(s):
            to = lax.rem(me + s, LINE)
            return send(kv_line.at[me], kv_line.at[me], kv_sends.at[s], kv_recv.at[me], "col", to)

        for s in range(1, LINE):
            kv_line_copy(s).start()
        small_copy(1).wait_recv()
        both = small_swap[2] + small_swap[3]
        small_swap[4, :2, :HALF] = both[:2, HALF:]
        small_swap[4, 2:, :HALF] = both[2:, :HALF]
        small_copy(2).start()
        for s in range(1, LINE):
            landed(kv_line.at[me], kv_recv.at[lax.rem(me + s, LINE)])
        dp_rows = aligned(d * UNIT, UNIT, UNIT)
        for h in range(KEYVALUE_HEADS):
            pair = kv_line[h * group].astype(F32)
            for i in range(1, group):
                pair = pair + kv_line[h * group + i].astype(F32)
            for i in range(2):
                at = (i * KEYVALUE_HEADS + h) * HEAD_SIZE
                kv_all_ref[dp_rows, at : at + HEAD_SIZE] = pair[
                    :, i * HEAD_SIZE : (i + 1) * HEAD_SIZE
                ].astype(BF16)

        def kv_rows(of):
            return kv_all_ref.at[aligned(of * UNIT, UNIT, UNIT)]

        def kv_dp_copy(i):
            rows = kv_rows(y_to if i == 2 else d)
            to = y_to if i == 1 else core_to
            return send(rows, rows, kvd_sends.at[i], kvd_recv.at[i], "dp", to)

        kv_dp_copy(1).start()
        kv_dp_copy(0).start()
        for i in (2, 1):
            swap_copy(i).wait_recv()
            to_ref = (in_ref, out_ref)[i - 1]
            to_ref[:, block_rows(1 - r)] = got_ref[i - 1].astype(F32).T
        small_copy(2).wait_recv()
        small_ref[...] = both[:, :HALF] + small_swap[5, :, :HALF]

        landed(kv_rows(y_to), kvd_recv.at[1])
        kv_dp_copy(2).start()
        landed(kv_rows(core_to), kvd_recv.at[0])
        landed(kv_rows(diagonal_to), kvd_recv.at[2])
        for m in (DOWN, GATE, UPPER):
            for k in range(2):
                three_copy(m, k).wait_recv()
                three_copy(m, k).wait_send()
            kept_copy(m).wait()
            for k in range(4):
                two_copy(m, k).wait_send()
        for i in range(4):
            chain_give(i).wait_send()
            two_copy(CHAIN, i, chain_sums).wait_send()
        for k in range(2):
            three_copy(CHAIN, k, chain_sums).wait_send()
        for i in range(3):
            swap_copy(i).wait_send()
            small_copy(i).wait_send()
            kv_dp_copy(i).wait_send()
            kv_line_copy(1 + i).wait_send()
            small_line_copy(1 + i).wait_send()
        gather.drain()
        out_scatter.drain()
        second.drain()

    wide = (HALF, chain_cols)
    pl.run_scoped(
        rest,
        pltpu.VMEM(wide, BF16),
        pltpu.VMEM(wide, BF16),
        pltpu.VMEM((LOCAL, query_cols), BF16),
        pltpu.VMEM((LOCAL, 2 * HEAD_SIZE), BF16),
        pltpu.VMEM((LOCAL, 2 * HEAD_SIZE), BF16),
        pltpu.VMEM((LOCAL, query_cols), BF16),
        pltpu.VMEM(probs_hbm.shape, BF16),
        pltpu.VMEM((LOCAL, HEAD_SIZE), F32),
        pltpu.VMEM((LOCAL, HEAD_SIZE), F32),
        pltpu.VMEM((BLOCK, MODEL_WIDTH), BF16),
        pltpu.VMEM((LOCAL, MODEL_WIDTH), BF16),
        pltpu.VMEM((BLOCK, MODEL_WIDTH), F32),
        pltpu.VMEM((BLOCK, MODEL_WIDTH), F32),
        pltpu.VMEM((LOCAL, query_cols), BF16),
        pltpu.VMEM((LOCAL, 2 * HEAD_SIZE), F32),
        pltpu.VMEM((LOCAL, 2 * HEAD_SIZE), BF16),
        pltpu.VMEM((LOCAL, proj_cols), BF16),
        pltpu.VMEM((4, UNIT, chain_cols), BF16),
        pltpu.VMEM((2, BLOCK, HALF), BF16),
    )


def rear_call(hidden, proj_cols, query_cols, *args):
    chain_cols = proj_cols + query_cols
    outs = [
        shape(HALF, 2 * BLOCK, F32),
        shape(HALF, 2 * BLOCK, F32),
        shape(8, HALF, F32),
        shape(UNIT, query_cols, F32),
        shape(UNIT, query_cols, F32),
        shape(4 * UNIT, 2 * KEYVALUE_HEADS * HEAD_SIZE),
        jax.ShapeDtypeStruct((3, UNIT, hidden), BF16),
        jax.ShapeDtypeStruct((6, UNIT, hidden), BF16),
        jax.ShapeDtypeStruct((3, UNIT, hidden), BF16),
    ]
    local = (LOCAL, MODEL_WIDTH)
    line = (2, LINE, BLOCK, MODEL_WIDTH)
    return pl.pallas_call(
        rear_body,
        out_shape=outs,
        in_specs=[VMEM_SPEC] * 2 + [ANY_SPEC] * (len(args) - 2),
        out_specs=[VMEM_SPEC] * 6 + [ANY_SPEC] * 3,
        scratch_shapes=[
            pltpu.VMEM(local, BF16),
            pltpu.VMEM((LOCAL, hidden), BF16),
            pltpu.VMEM((LOCAL, hidden), BF16),
            pltpu.VMEM((LOCAL, hidden), BF16),
            pltpu.VMEM(local, BF16),
            pltpu.VMEM(local, BF16),
            pltpu.VMEM((2, MODEL_WIDTH, LOCAL), BF16),
            pltpu.VMEM((LOCAL, 2 * HEAD_SIZE), BF16),
            pltpu.VMEM((2, BLOCK, HALF), BF16),
            pltpu.VMEM(line, BF16),
            pltpu.VMEM(line, BF16),
            pltpu.VMEM((12, UNIT, hidden), BF16),
            pltpu.VMEM((2, UNIT, hidden), BF16),
            pltpu.VMEM((3, UNIT, hidden), BF16),
            pltpu.VMEM((4, UNIT, chain_cols), BF16),
            pltpu.VMEM((2, UNIT, chain_cols), BF16),
            pltpu.VMEM((UNIT, chain_cols), BF16),
            pltpu.VMEM((LINE, UNIT, 2 * HEAD_SIZE), BF16),
            pltpu.VMEM((LINE, 8, MODEL_WIDTH), F32),
            pltpu.VMEM((6, 8, MODEL_WIDTH), F32),
            DMA((16,)),
            DMA((2, 3, 2)),
        ]
        + gather_sems()
        + scatter_sems()
        + scatter_sems()
        + gather_sems()
        + [
            DMA((16,)), DMA((16,)),
            DMA((4, 4)), DMA((4, 4)),
            DMA((4, 2)), DMA((4, 2)),
            DMA((3, 2)), DMA((3,)),
            DMA((3,)), DMA((3,)),
            DMA((LINE,)), DMA((LINE,)),
            DMA((3,)), DMA((3,)),
            DMA((LINE,)), DMA((LINE,)),
            DMA((3,)), DMA((3,)),
            pltpu.SemaphoreType.REGULAR,
        ],
        compiler_params=pltpu.CompilerParams(
            collective_id=2, has_side_effects=True, vmem_limit_bytes=67_043_328
        ),
        cost_estimate=pl.CostEstimate(
            flops=4 * 10**10, bytes_accessed=80_000_000, transcendentals=0
        ),
        name="rear",
    )(*args)


def fast_device(
    block_input,
    position_ids,
    attention_gain,
    query_weight,
    query_bias,
    key_value_weight,
    key_value_bias,
    output_weight,
    feedforward_gain,
    gate_weight,
    upper_weight,
    down_weight,
    out_cotangent,
):
    query_cols = query_weight.shape[1]
    hidden = gate_weight.shape[1]
    proj_cols = query_cols + 2 * HEAD_SIZE
    frequencies = THETA ** (-(jnp.arange(HEAD_SIZE // 2, dtype=F32) * 2.0 / HEAD_SIZE))
    angles = position_ids.astype(F32)[:, None] * frequencies[None, :]
    table = jnp.concatenate([jnp.cos(angles), jnp.sin(angles)], -1)
    small = jnp.concatenate([attention_gain, feedforward_gain, query_bias, key_value_bias])[None]
    gate_t, upper_t, down_t = gate_weight.T, upper_weight.T, down_weight.T
    (
        x_own, normed_one, query_rot, kv_own, kv_other, cosine, sine, gains, attended, probs,
        mid, normed_two, normed_turned, cot_part, own_proj, other_proj, other_weights,
    ) = front_call(
        proj_cols, query_cols, hidden,
        block_input, out_cotangent, table, small, query_weight, key_value_weight, output_weight,
        gate_t, upper_t, down_t,
    )
    out, input_grad, sums, query_sum, output_sum, kv_all, kept, _, landing = rear_call(
        hidden, proj_cols, query_cols,
        mid, gains,
        normed_two, normed_turned, cot_part, gate_t, upper_t, down_t, other_weights, own_proj, other_proj, query_rot, kv_own,
        kv_other, attended, probs, cosine, sine, x_own, normed_one,
    )
    down_sum, gate_sum, upper_sum = (
        kept[m].astype(F32) + landing[m].astype(F32) for m in range(3)
    )
    bias_rows = query_cols // lax.axis_size("dp")
    query_bias_grad = lax.dynamic_slice_in_dim(
        sums[2], lax.axis_index("dp") * bias_rows, bias_rows, 0
    )
    return (
        out,
        input_grad,
        sums[0],
        query_sum,
        query_bias_grad,
        kv_all.astype(F32),
        sums[3, : 2 * KEYVALUE_HEADS * HEAD_SIZE],
        output_sum,
        sums[1],
        gate_sum,
        upper_sum,
        down_sum,
    )


def per_device(*arrays):
    sizes = tuple(lax.axis_size(axis) for axis in ("dp", "row", "col"))
    if sizes == (4, 2, LINE) and arrays[0].shape == (HALF, 2 * BLOCK):
        return fast_device(*arrays)
    return general_device(*arrays)


def solution(mesh):
    placed = (
        P("row", ("dp", "col")),
        P(("dp", "row")),
        P("row"),
        P("row", "col"),
        P("col"),
        P("row", None),
        P(),
        P("row", "col"),
        P("row"),
        P("row", "col"),
        P("row", "col"),
        P("row", "col"),
        P("row", ("dp", "col")),
    )
    return jax.shard_map(
        per_device,
        mesh=mesh,
        in_specs=placed,
        out_specs=(
            P("row", ("dp", "col")),
            P("row", ("dp", "col")),
            P("row"),
            P(("row", "dp"), "col"),
            P(("col", "dp")),
            P("row", None),
            P(),
            P(("row", "dp"), "col"),
            P("row"),
            P(("row", "dp"), "col"),
            P(("row", "dp"), "col"),
            P(("row", "dp"), "col"),
        ),
        check_vma=False,
    )
```

```python
import jax
import jax.numpy as jnp
from jax import lax
from jax.experimental import pallas as pl
from jax.experimental.pallas import tpu as pltpu
from jax.sharding import PartitionSpec as P

MODEL_WIDTH = 1536
KEYVALUE_HEADS = 2
HEAD_SIZE = 128


EPS = 1e-06
THETA = 1000000.0
NEG = -1e30


def rope_tables(position_ids):
    half_dim = HEAD_SIZE // 2
    frequencies = THETA ** (-(jnp.arange(half_dim, dtype=jnp.float32) * 2.0 / HEAD_SIZE))
    angles = position_ids.astype(jnp.float32)[:, None] * frequencies[None, :]
    cosine_values = jnp.cos(angles)
    sine_lookup = jnp.sin(angles)
    return (
        jnp.concatenate([cosine_values, cosine_values], -1),
        jnp.concatenate([sine_lookup, sine_lookup], -1),
    )


def apply_rotation(values, cosine_values, sine_lookup):
    half_dim = HEAD_SIZE // 2
    turned = jnp.concatenate([-values[..., half_dim:], values[..., :half_dim]], -1)
    return values * cosine_values[:, None, :] + turned * sine_lookup[:, None, :]


def unrotate(gradient, cosine_values, sine_lookup):
    half_dim = HEAD_SIZE // 2
    scaled = gradient * sine_lookup[:, None, :]
    turned = jnp.concatenate([scaled[..., half_dim:], -scaled[..., :half_dim]], -1)
    return gradient * cosine_values[:, None, :] + turned


def row_total(partial_value):
    return lax.psum(partial_value, "row")


def norm_forward(x_float, gain):
    squares = jnp.sum(x_float * x_float, -1)
    rinv = lax.rsqrt(row_total(squares) / MODEL_WIDTH + EPS)[:, None]
    return ((x_float * rinv * gain).astype(jnp.bfloat16), rinv)


def norm_backward(normed_grad, x_float, rinv, gain):
    scaled = normed_grad * gain
    inner = row_total(jnp.sum(scaled * x_float, -1))[:, None]
    input_part = rinv * scaled - x_float * rinv**3 * inner / MODEL_WIDTH
    gain_part = jnp.sum(normed_grad * x_float * rinv, 0)
    return (input_part, gain_part)


def column_gather(values):
    return lax.all_gather(values, "col", axis=0, tiled=True)


def column_sum(partial_value):
    return lax.psum_scatter(
        partial_value.astype(jnp.bfloat16), "col", scatter_dimension=0, tiled=True
    ).astype(jnp.float32)


def row_product(gathered, weight):
    return (
        lax.psum_scatter(
            jnp.dot(gathered, weight, preferred_element_type=jnp.float32).astype(jnp.bfloat16),
            "row",
            scatter_dimension=0,
            tiled=True,
        ).astype(jnp.float32),
        gathered,
    )


def row_project(local_part, weight):
    return lax.dot_general(
        lax.all_gather(local_part, "row", axis=0, tiled=True),
        weight,
        (((1,), (1,)), ((), ())),
        preferred_element_type=jnp.float32,
    )


def row_fold(local_part, partner, weight):
    pair_dims = (((0,), (0,)), ((), ()))

    def accumulate(block_rows):
        grad_sum = lax.dot_general(
            partner, block_rows, pair_dims, preferred_element_type=jnp.float32
        )
        if weight is None:
            return (grad_sum,)
        back_proj = lax.dot_general(
            block_rows, weight, (((1,), (1,)), ((), ())), preferred_element_type=jnp.float32
        )
        column_totals = jnp.sum(block_rows, 0, dtype=jnp.float32)
        return (grad_sum, back_proj, column_totals)

    return accumulate(lax.all_gather(local_part, "row", axis=0, tiled=True))


def causal_scores(query_rot, rotated_keys):
    scores = jnp.einsum(
        "ihd,jd->hij", query_rot, rotated_keys, preferred_element_type=jnp.float32
    ) * HEAD_SIZE ** (-0.5)
    length = query_rot.shape[0]
    allowed = jnp.arange(length)[:, None] >= jnp.arange(length)[None, :]
    return jnp.where(allowed[None], scores, NEG)


def attend(query_rot, rotated_keys, value_second_part):
    scores = causal_scores(query_rot, rotated_keys)
    row_max = jnp.max(scores, -1, keepdims=True)
    log_total = row_max + jnp.log(jnp.sum(jnp.exp(scores - row_max), -1, keepdims=True))
    probs_half = jnp.exp(scores - log_total).astype(jnp.bfloat16)
    attended = jnp.einsum(
        "hij,jd->ihd", probs_half, value_second_part, preferred_element_type=jnp.float32
    ).astype(jnp.bfloat16)
    return (attended, log_total)


def attend_back(query_rot, rotated_keys, value_second_part, attended, att_grad, log_total):
    scale = HEAD_SIZE ** (-0.5)
    softmax_probs = jnp.exp(causal_scores(query_rot, rotated_keys) - log_total)
    probs_half = softmax_probs.astype(jnp.bfloat16)
    prob_grad = jnp.einsum(
        "ihd,jd->hij", att_grad, value_second_part, preferred_element_type=jnp.float32
    )
    row_delta = jnp.einsum("ihd,ihd->hi", att_grad, attended, preferred_element_type=jnp.float32)
    score_half = (softmax_probs * (prob_grad - row_delta[:, :, None])).astype(jnp.bfloat16)
    query_grad = (
        jnp.einsum("hij,jd->ihd", score_half, rotated_keys, preferred_element_type=jnp.float32)
        * scale
    )
    key_grad = (
        jnp.einsum("hij,ihd->jd", score_half, query_rot, preferred_element_type=jnp.float32) * scale
    )
    value_grad = jnp.einsum("hij,ihd->jd", probs_half, att_grad, preferred_element_type=jnp.float32)
    return (query_grad, key_grad, value_grad)


def general_device(
    block_input,
    position_ids,
    attention_gain,
    query_weight,
    query_bias,
    key_value_weight,
    key_value_bias,
    output_weight,
    feedforward_gain,
    gate_weight,
    upper_weight,
    down_weight,
    out_cotangent,
):
    single_float_type = jnp.float32
    brain_float_type = jnp.bfloat16
    column_number = lax.axis_size("col")
    seq_len = position_ids.shape[0]
    heads_here = query_weight.shape[1] // HEAD_SIZE
    query_cols = query_weight.shape[1]
    hidden_cols = gate_weight.shape[1]
    key_value_head = lax.axis_index("col") // (column_number // KEYVALUE_HEADS)
    key_start = key_value_head * HEAD_SIZE
    value_offset = KEYVALUE_HEADS * HEAD_SIZE + key_value_head * HEAD_SIZE
    keyval_local = jnp.concatenate(
        [
            lax.dynamic_slice_in_dim(key_value_weight, key_start, HEAD_SIZE, 1),
            lax.dynamic_slice_in_dim(key_value_weight, value_offset, HEAD_SIZE, 1),
        ],
        1,
    )
    bias_local = jnp.concatenate(
        [
            lax.dynamic_slice_in_dim(key_value_bias, key_start, HEAD_SIZE, 0),
            lax.dynamic_slice_in_dim(key_value_bias, value_offset, HEAD_SIZE, 0),
        ],
        0,
    )
    proj_weight = jnp.concatenate([query_weight, keyval_local], 1)
    proj_bias = jnp.concatenate([query_bias, bias_local], 0)
    pair_weight = jnp.concatenate([gate_weight, upper_weight], 1)
    cosine_values, sine_lookup = rope_tables(position_ids)
    x_float = block_input.T.astype(single_float_type)
    cot_local = out_cotangent.T
    normed_one, rinv_one = norm_forward(x_float, attention_gain)
    normed_one_all = column_gather(normed_one)
    proj_out = row_product(normed_one_all, proj_weight)[0] + proj_bias
    query_rot = apply_rotation(
        proj_out[:, :query_cols].reshape(seq_len, heads_here, HEAD_SIZE), cosine_values, sine_lookup
    ).astype(brain_float_type)
    rotated_keys = apply_rotation(
        proj_out[:, query_cols : query_cols + HEAD_SIZE][:, None, :], cosine_values, sine_lookup
    )[:, 0].astype(brain_float_type)
    value_second_part = proj_out[:, query_cols + HEAD_SIZE :].astype(brain_float_type)
    attended, log_total = attend(query_rot, rotated_keys, value_second_part)
    attended_flat = attended.reshape(seq_len, query_cols)
    hidden_res = x_float + column_sum(row_project(attended_flat, output_weight))
    normed_two, rinv_two = norm_forward(hidden_res, feedforward_gain)
    normed_two_all = column_gather(normed_two)
    gate_upper, normed_two_seq = row_product(normed_two_all, pair_weight)
    gate_lin = gate_upper[:, :hidden_cols]
    upper_lin = gate_upper[:, hidden_cols:]
    sigmoid_gate = jax.nn.sigmoid(gate_lin)
    activated = (gate_lin * sigmoid_gate * upper_lin).astype(brain_float_type)
    block_output = hidden_res + column_sum(row_project(activated, down_weight))
    cotangent_all = column_gather(cot_local)
    act_grad = row_product(cotangent_all, down_weight)[0]
    down_grad = row_fold(activated, cotangent_all, None)[0]
    gate_grad = act_grad * upper_lin * sigmoid_gate * (1.0 + gate_lin * (1.0 - sigmoid_gate))
    upper_grad = act_grad * gate_lin * sigmoid_gate
    pair_grad_half = jnp.concatenate([gate_grad, upper_grad], 1).astype(brain_float_type)
    folded_two = row_fold(pair_grad_half, normed_two_all, pair_weight)
    pair_weight_grad = folded_two[0]
    spread_two = folded_two[1]
    normed_two_grad = column_sum(spread_two)
    hidden_part, ffn_gain_part = norm_backward(
        normed_two_grad, hidden_res, rinv_two, feedforward_gain
    )
    hidden_grad = cot_local.astype(single_float_type) + hidden_part
    hidden_half = hidden_grad.astype(brain_float_type)
    hidden_all = column_gather(hidden_half)
    att_grad = (
        row_product(hidden_all, output_weight)[0]
        .astype(brain_float_type)
        .reshape(seq_len, heads_here, HEAD_SIZE)
    )
    output_grad = row_fold(attended_flat, hidden_all, None)[0]
    query_grad, key_grad, value_grad = attend_back(
        query_rot, rotated_keys, value_second_part, attended, att_grad, log_total
    )
    query_half = (
        unrotate(query_grad, cosine_values, sine_lookup)
        .astype(brain_float_type)
        .reshape(seq_len, query_cols)
    )
    key_half = unrotate(key_grad[:, None, :], cosine_values, sine_lookup)[:, 0].astype(
        brain_float_type
    )
    value_grad_half = value_grad.astype(brain_float_type)
    proj_grad_half = jnp.concatenate([query_half, key_half, value_grad_half], 1)
    folded_one = row_fold(proj_grad_half, normed_one_all, proj_weight)
    projection_weight_gradient = folded_one[0]
    normed_one_grad = column_sum(folded_one[1])
    proj_bias_grad = folded_one[2]
    input_part, attn_gain_part = norm_backward(normed_one_grad, x_float, rinv_one, attention_gain)
    input_grad = hidden_grad + input_part
    key_value_gradient = jnp.zeros(
        (projection_weight_gradient.shape[0], 2 * KEYVALUE_HEADS * HEAD_SIZE), single_float_type
    )
    key_value_gradient = lax.dynamic_update_slice_in_dim(
        key_value_gradient,
        projection_weight_gradient[:, query_cols : query_cols + HEAD_SIZE],
        key_start,
        1,
    )
    key_value_gradient = lax.dynamic_update_slice_in_dim(
        key_value_gradient, projection_weight_gradient[:, query_cols + HEAD_SIZE :], value_offset, 1
    )
    key_value_bias_gradient = jnp.zeros((2 * KEYVALUE_HEADS * HEAD_SIZE,), single_float_type)
    key_value_bias_gradient = lax.dynamic_update_slice_in_dim(
        key_value_bias_gradient, proj_bias_grad[query_cols : query_cols + HEAD_SIZE], key_start, 0
    )
    key_value_bias_gradient = lax.dynamic_update_slice_in_dim(
        key_value_bias_gradient, proj_bias_grad[query_cols + HEAD_SIZE :], value_offset, 0
    )
    shared = (
        lax.psum(key_value_gradient.astype(jnp.bfloat16), ("dp", "col")).astype(jnp.float32),
        lax.psum(key_value_bias_gradient.astype(jnp.bfloat16), ("dp", "col")).astype(jnp.float32),
        lax.psum(attn_gain_part.astype(jnp.bfloat16), ("dp", "col")).astype(jnp.float32),
        lax.psum(ffn_gain_part.astype(jnp.bfloat16), ("dp", "col")).astype(jnp.float32),
    )
    summed = (
        lax.psum_scatter(
            projection_weight_gradient[:, :query_cols].astype(jnp.bfloat16),
            "dp",
            scatter_dimension=0,
            tiled=True,
        ).astype(jnp.float32),
        lax.psum_scatter(
            proj_bias_grad[:query_cols].astype(jnp.bfloat16), "dp", scatter_dimension=0, tiled=True
        ).astype(jnp.float32),
        lax.psum_scatter(
            output_grad.astype(jnp.bfloat16), "dp", scatter_dimension=0, tiled=True
        ).astype(jnp.float32),
        lax.psum_scatter(
            pair_weight_grad[:, :hidden_cols].astype(jnp.bfloat16),
            "dp",
            scatter_dimension=0,
            tiled=True,
        ).astype(jnp.float32),
        lax.psum_scatter(
            pair_weight_grad[:, hidden_cols:].astype(jnp.bfloat16),
            "dp",
            scatter_dimension=0,
            tiled=True,
        ).astype(jnp.float32),
        lax.psum_scatter(
            down_grad.astype(jnp.bfloat16), "dp", scatter_dimension=0, tiled=True
        ).astype(jnp.float32),
    )
    return (
        block_output.T,
        input_grad.T,
        shared[2],
        summed[0],
        summed[1],
        shared[0],
        shared[1],
        summed[2],
        shared[3],
        summed[3],
        summed[4],
        summed[5],
    )


MESH_ID = pl.DeviceIdType.MESH
F32 = jnp.float32
BF16 = jnp.bfloat16
LINE = 4
BLOCK = 128
SUB = 2
PART = BLOCK // SUB
LOCAL = LINE * BLOCK
HALF = MODEL_WIDTH // 2
UNIT = MODEL_WIDTH // 8
VMEM_SPEC = pl.BlockSpec(memory_space=pltpu.VMEM)
ANY_SPEC = pl.BlockSpec(memory_space=pl.ANY)
PAIR_ROWS = (((0,), (0,)), ((), ()))
PAIR_COLS = (((1,), (1,)), ((), ()))
SCALE = HEAD_SIZE ** (-0.5)
DMA = pltpu.SemaphoreType.DMA


def greet(me, others):
    barrier = pltpu.get_barrier_semaphore()
    for axis, index in others:
        pl.semaphore_signal(barrier, 1, device_id={axis: index}, device_id_type=MESH_ID)

    @pl.when(me > 0)
    def _():
        pl.semaphore_signal(barrier, 1, device_id={"col": me - 1}, device_id_type=MESH_ID)

    @pl.when(me < LINE - 1)
    def _():
        pl.semaphore_signal(barrier, 1, device_id={"col": me + 1}, device_id_type=MESH_ID)

    @pl.when((me > 0) & (me < LINE - 1))
    def _():
        pl.semaphore_wait(barrier, 2 + len(others))

    @pl.when((me == 0) | (me == LINE - 1))
    def _():
        pl.semaphore_wait(barrier, 1 + len(others))


def aligned(start, size, to=BLOCK):
    return pl.ds(pl.multiple_of(start, to), size)


def block_rows(index):
    return aligned(index * BLOCK, BLOCK)


def send(src, dst, send_sem, recv_sem, axis, to):
    return pltpu.make_async_remote_copy(
        src, dst, send_sem, recv_sem, device_id={axis: to}, device_id_type=MESH_ID
    )


def landed(ref, sem):
    pltpu.make_async_copy(ref, ref, sem).wait()


class Gather:
    def __init__(self, me, all_ref, sends, recv):
        self.me, self.all_ref, self.sends, self.recv = me, all_ref, sends, recv

    def rows(self, j, p):
        return self.all_ref.at[aligned(j * BLOCK + p * PART, PART, PART)]

    def copy(self, j, p, s, side):
        rows = self.rows(j, p)
        return send(
            rows, rows, self.sends.at[side, s, p], self.recv.at[j, p], "col",
            self.me + 1 - 2 * side,
        )

    def has_next(self, side):
        to = self.me + 1 - 2 * side
        return (to >= 0) & (to < LINE)

    def step(self, s, wait=True, forward=True):
        @pl.loop(0, 2 * SUB)
        def _(i):
            side, p = lax.rem(i, 2), i // 2
            j = self.me - (1 - 2 * side) * s

            @pl.when((j >= 0) & (j < LINE))
            def _():
                if s and wait:
                    landed(self.rows(j, p), self.recv.at[j, p])

                if forward and s < LINE - 1:

                    @pl.when(self.has_next(side))
                    def _():
                        self.copy(j, p, s, side).start()

    def run_each(self, s, each):
        if s == 0:
            each(self.me)
            return

        @pl.loop(0, 2)
        def _(side):
            j = self.me - (1 - 2 * side) * s

            @pl.when((j >= 0) & (j < LINE))
            def _():
                each(j)

    def drain(self, first=0, last=LINE - 1):
        for s in range(first, last):

            @pl.loop(0, 2)
            def _(side):
                j = self.me - (1 - 2 * side) * s

                @pl.when((j >= 0) & (j < LINE) & self.has_next(side))
                def _():
                    for p in range(SUB):
                        self.copy(self.me, p, s, side).wait_send()


class Scatter:
    def __init__(self, me, block_of, landing, sends, recv):
        self.me, self.block_of, self.landing = me, block_of, landing
        self.sends, self.recv = sends, recv

    def rows(self, side, j, p):
        return self.landing.at[side, j, pl.ds(p * PART, PART)]

    def copy(self, side, j, p):
        rows = self.rows(side, j, p)
        return send(
            rows, rows, self.sends.at[side, j, p], self.recv.at[side, j, p], "col",
            self.me + 1 - 2 * side,
        )

    def has_last(self, side):
        came = self.me - 1 + 2 * side
        return (came >= 0) & (came < LINE)

    def step(self, s):
        @pl.loop(0, 2)
        def _(side):
            j = self.me + (1 - 2 * side) * s

            @pl.when((j >= 0) & (j < LINE))
            def _():
                mine = self.block_of(j)
                for p in range(SUB):
                    term = mine[p * PART : (p + 1) * PART]
                    rows = self.rows(side, j, p)

                    @pl.when(self.has_last(side))
                    def _():
                        landed(rows, self.recv.at[side, j, p])
                        rows[...] = (term + rows[...].astype(F32)).astype(BF16)

                    @pl.when(jnp.logical_not(self.has_last(side)))
                    def _():
                        rows[...] = term.astype(BF16)

                    self.copy(side, j, p).start()

    def finish(self, out_ref):
        me = self.me
        out_ref[...] = self.block_of(me)

        @pl.loop(0, 2)
        def _(side):
            @pl.when(self.has_last(side))
            def _():
                for p in range(SUB):
                    rows = self.rows(side, me, p)
                    landed(rows, self.recv.at[side, me, p])
                    out_ref[p * PART : (p + 1) * PART] += rows[...].astype(F32)

    def drain(self):
        for s in range(1, LINE):

            @pl.loop(0, 2)
            def _(side):
                j = self.me + (1 - 2 * side) * s

                @pl.when((j >= 0) & (j < LINE))
                def _():
                    for p in range(SUB):
                        self.copy(side, j, p).wait_send()


def gather_sems():
    return [DMA((2, LINE, SUB)), DMA((LINE, SUB))]


def scatter_sems():
    return [DMA((2, LINE, SUB)), DMA((2, LINE, SUB))]


def dot(a, b, dims=(((1,), (0,)), ((), ()))):
    return lax.dot_general(a, b, dims, preferred_element_type=F32)


def turn(values):
    return pltpu.roll(values, HEAD_SIZE // 2, 1)


def norm_scale(values):
    return lax.rsqrt(jnp.sum(values * values, -1, keepdims=True) / MODEL_WIDTH + EPS)


def shape(rows, cols, dtype=BF16):
    return jax.ShapeDtypeStruct((rows, cols), dtype)


def attend_local(query_ref, own_ref, other_ref, attended_ref, probs_ref, r):
    rows = 2 * BLOCK
    shape = (rows, rows)
    at_row = lax.broadcasted_iota(jnp.int32, shape, 0)
    at_col = lax.broadcasted_iota(jnp.int32, shape, 1)
    own_mask = at_row >= at_col
    other_mask = at_col // BLOCK < at_row // BLOCK + r
    heads = query_ref.shape[1] // HEAD_SIZE
    for s in range(2):
        part = slice(s * rows, (s + 1) * rows)
        for h in range(heads):
            cols = slice(h * HEAD_SIZE, (h + 1) * HEAD_SIZE)
            query = query_ref[part, cols]
            own = jnp.where(own_mask, dot(query, own_ref[part, :HEAD_SIZE], PAIR_COLS) * SCALE, NEG)
            other = jnp.where(
                other_mask, dot(query, other_ref[part, :HEAD_SIZE], PAIR_COLS) * SCALE, NEG
            )
            top = jnp.maximum(
                jnp.max(own, -1, keepdims=True), jnp.max(other, -1, keepdims=True)
            )
            total = jnp.sum(jnp.exp(own - top), -1, keepdims=True) + jnp.sum(
                jnp.exp(other - top), -1, keepdims=True
            )
            log_total = top + jnp.log(total)
            own = jnp.exp(own - log_total).astype(BF16)
            other = jnp.exp(other - log_total).astype(BF16)
            attended_ref[part, cols] = (
                dot(own, own_ref[part, HEAD_SIZE:]) + dot(other, other_ref[part, HEAD_SIZE:])
            ).astype(BF16)
            probs_ref[s * heads + h, :, :rows] = own
            probs_ref[s * heads + h, :, rows:] = other


def attend_back_body(
    query_ref, own_ref, other_ref, attended_ref, probs_ref, grad_ref, cos_ref, sin_ref,
    query_grad_ref, own_grad_ref, other_grad_ref,
):
    rows = 2 * BLOCK
    heads = query_ref.shape[1] // HEAD_SIZE
    for s in range(2):
        part = slice(s * rows, (s + 1) * rows)
        own_key, other_key = own_ref[part, :HEAD_SIZE], other_ref[part, :HEAD_SIZE]
        own_value, other_value = own_ref[part, HEAD_SIZE:], other_ref[part, HEAD_SIZE:]
        sums = [jnp.zeros((rows, HEAD_SIZE), F32) for _ in range(4)]
        for h in range(heads):
            cols = slice(h * HEAD_SIZE, (h + 1) * HEAD_SIZE)
            query, grad = query_ref[part, cols], grad_ref[part, cols]
            own_p = probs_ref[s * heads + h, :, :rows]
            other_p = probs_ref[s * heads + h, :, rows:]
            delta = jnp.sum(
                grad.astype(F32) * attended_ref[part, cols].astype(F32), -1, keepdims=True
            )
            own_s = (own_p.astype(F32) * (dot(grad, own_value, PAIR_COLS) - delta)).astype(BF16)
            other_s = (other_p.astype(F32) * (dot(grad, other_value, PAIR_COLS) - delta)).astype(BF16)
            query_grad = (dot(own_s, own_key) + dot(other_s, other_key)) * SCALE
            query_grad_ref[part, cols] = (
                query_grad * cos_ref[part] - turn(query_grad) * sin_ref[part]
            ).astype(BF16)
            for i, (weights, partner) in enumerate(
                ((own_s, query), (own_p, grad), (other_s, query), (other_p, grad))
            ):
                sums[i] = sums[i] + dot(weights, partner, PAIR_ROWS)
        own_grad_ref[part, :HEAD_SIZE] = sums[0] * SCALE
        own_grad_ref[part, HEAD_SIZE:] = sums[1]
        other_grad_ref[part, :HEAD_SIZE] = (sums[2] * SCALE).astype(BF16)
        other_grad_ref[part, HEAD_SIZE:] = sums[3].astype(BF16)


PIECES = 6


def front_body(
    input_ref, cot_in_ref, table_ref, small_ref, query_w_ref, kv_w_ref, output_w_ref,
    gate_hbm, upper_hbm, down_hbm,
    x_hbm, normed_hbm, query_hbm, kv_hbm, kv_other_hbm, cos_hbm, sin_hbm, gains_ref,
    attended_hbm, probs_hbm, mid_hbm, normed_two_hbm, turned_hbm, cot_hbm, proj_hbm, proj_other_hbm,
    weights_other_hbm,
    x_ref, normed_ref, query_ref, kv_ref, kv_other_ref, cos_ref, sin_ref,
    attended_ref, probs_ref, mid_ref, normed_two_ref, turned_ref, cot_ref, proj_ref, proj_other_ref,
    passing, tables, bias_ref, landing, store_sems,
    swap_sends, swap_recv, piece_sends, piece_recv, kv_sends, kv_recv,
    g_sends, g_recv, c_sends, c_recv, n_sends, n_recv, s_sends, s_recv,
):
    me, r, d = lax.axis_index("col"), lax.axis_index("row"), lax.axis_index("dp")
    y, core = d // 2, lax.rem(d, 2)
    x_to, y_to, core_to = 1 - r, 2 * (1 - y) + core, 2 * y + 1 - core
    query_cols = query_ref.shape[1]
    proj_cols = query_cols + 2 * HEAD_SIZE
    quarter = HALF // 2
    my_rows = aligned(core * quarter, quarter, quarter)
    its_rows = aligned((1 - core) * quarter, quarter, quarter)
    eighth = quarter // 2
    to_y = aligned(core * quarter + y * eighth, eighth, eighth)
    in_cols, out_cols = pl.ds(0, proj_cols), pl.ds(proj_cols, query_cols)
    kv_width = KEYVALUE_HEADS * HEAD_SIZE
    kv_at = me // (LINE // KEYVALUE_HEADS) * HEAD_SIZE

    stores = [
        pltpu.make_async_copy(src, dst, store_sems.at[i])
        for i, (src, dst) in enumerate(
            (
                (x_ref, x_hbm), (cos_ref, cos_hbm), (sin_ref, sin_hbm), (proj_ref, proj_hbm),
                (normed_ref, normed_hbm), (query_ref, query_hbm), (kv_ref, kv_hbm),
                (kv_other_ref, kv_other_hbm), (probs_ref, probs_hbm), (attended_ref, attended_hbm),
                (proj_other_ref, proj_other_hbm), (mid_ref, mid_hbm),
                (normed_two_ref, normed_two_hbm), (turned_ref, turned_hbm), (cot_ref, cot_hbm),
            )
        )
    ]

    passing[0] = input_ref[:, block_rows(1 - r)].T
    x_ref[:, :HALF] = input_ref[:, block_rows(r)].T
    proj_ref[:, :query_cols] = query_w_ref[...]
    for i in range(2):
        proj_ref[:, query_cols + i * HEAD_SIZE : query_cols + (i + 1) * HEAD_SIZE] = kv_w_ref[
            :, aligned(i * kv_width + kv_at, HEAD_SIZE)
        ]
    greet(me, [("row", x_to), ("dp", y_to), ("dp", core_to)])

    swaps = [
        (passing.at[0], x_ref.at[:, HALF:], "row", x_to),
        (small_ref.at[:, :HALF], gains_ref.at[pl.ds(0, 1), HALF:], "row", x_to),
        (small_ref.at[:, HALF : 2 * HALF], gains_ref.at[pl.ds(1, 1), HALF:], "row", x_to),
        (proj_ref.at[to_y, in_cols], proj_other_ref.at[to_y, in_cols], "row", x_to),
        (table_ref.at[block_rows(1 - r)], tables.at[pl.ds(0, BLOCK)], "row", x_to),
        (table_ref.at[block_rows(3 - r)], tables.at[pl.ds(BLOCK, BLOCK)], "row", x_to),
        (passing.at[1], cot_ref.at[block_rows(me), HALF:], "row", x_to),
        (proj_ref.at[to_y, out_cols], proj_other_ref.at[to_y, out_cols], "row", x_to),
        (proj_other_ref.at[to_y, in_cols], proj_other_ref.at[to_y, in_cols], "dp", y_to),
        (proj_other_ref.at[to_y, out_cols], proj_other_ref.at[to_y, out_cols], "dp", y_to),
        (proj_other_ref.at[my_rows, in_cols], proj_other_ref.at[my_rows, in_cols], "dp", core_to),
        (proj_other_ref.at[my_rows, out_cols], proj_other_ref.at[my_rows, out_cols], "dp", core_to),
    ]

    def swap_copy(i):
        src, dst, axis, to = swaps[i]
        return send(src, dst, swap_sends.at[i], swap_recv.at[i], axis, to)

    def swap_landed(i):
        swap_copy(i).wait_recv()

    rows = gate_hbm.shape[0] // 4
    owns = (gate_hbm, upper_hbm, down_hbm)

    def piece(i, of_y):
        return aligned((of_y * 2 + i % 2) * rows, rows, rows)

    def piece_copy(i, way):
        m = i // 2
        of_y = 1 - y if way == 3 else y
        at = weights_other_hbm.at[m, piece(i, of_y), my_rows]
        src = owns[m].at[piece(i, of_y), my_rows] if way == 0 else at
        axis, to = (("row", x_to), ("dp", y_to), ("dp", core_to), ("dp", core_to))[way]
        return send(src, at, piece_sends.at[way, i], piece_recv.at[way, i], axis, to)

    def relay_x(i):
        piece_copy(i, 0).wait_recv()
        piece_copy(i, 1).start()
        piece_copy(i, 2).start()

    def relay_y(i):
        piece_copy(i, 1).wait_recv()
        piece_copy(i, 3).start()

    for i in range(6):
        swap_copy(i).start()
    passing[1] = cot_in_ref[:, block_rows(1 - r)].T
    proj_ref[:, proj_cols:] = output_w_ref[...]
    swap_copy(6).start()
    swap_copy(7).start()
    piece_copy(0, 0).start()
    cot_ref[block_rows(me), :HALF] = cot_in_ref[:, block_rows(r)].T
    gains_ref[0:1, :HALF] = small_ref[:, :HALF]
    gains_ref[1:2, :HALF] = small_ref[:, HALF : 2 * HALF]
    bias_ref[:, :query_cols] = small_ref[:, 2 * HALF : 2 * HALF + query_cols]
    for i in range(2):
        bias_ref[:, query_cols + i * HEAD_SIZE : query_cols + (i + 1) * HEAD_SIZE] = small_ref[
            :, aligned(2 * HALF + query_cols + i * kv_width + kv_at, HEAD_SIZE)
        ]
    swap_landed(0)
    swap_landed(1)
    swap_landed(2)
    x = x_ref[...].astype(F32)
    normed_ref[block_rows(me)] = (x * norm_scale(x) * gains_ref[0:1]).astype(BF16)
    gather = Gather(me, normed_ref, g_sends, g_recv)
    gather.step(0)

    lane = lax.broadcasted_iota(jnp.int32, (BLOCK, HEAD_SIZE), 1)
    first = lane < HEAD_SIZE // 2
    swap_landed(3)
    swap_copy(8).start()
    gather.step(1)
    swap_landed(8)
    swap_copy(10).start()
    swap_landed(4)
    swap_landed(5)
    for i in range(4):
        if i < 2:
            table = table_ref[block_rows(r + 2 * i)]
        else:
            table = tables[(i - 2) * BLOCK : (i - 1) * BLOCK]
        turned = turn(table)
        at = block_rows((r if i < 2 else 1 - r) * 2 + i % 2)
        cos_ref[at] = jnp.where(first, table, turned)
        sin_ref[at] = jnp.where(first, -turned, table)
    swap_landed(10)

    def kv_copy(j):
        at = block_rows(j)
        return send(
            kv_ref.at[at], kv_other_ref.at[at], kv_sends.at[j], kv_recv.at[j], "row", x_to
        )

    def each(j):
        at = block_rows(j)
        block = normed_ref[at]
        out = dot(block[:, :HALF], proj_ref[:, :proj_cols])
        out = out + dot(block[:, HALF:], proj_other_ref[:, :proj_cols]) + bias_ref[...]
        cosine, sine = cos_ref[at], sin_ref[at]
        for h in range(query_cols // HEAD_SIZE + 1):
            head = out[:, h * HEAD_SIZE : (h + 1) * HEAD_SIZE]
            turned = (head * cosine + turn(head) * sine).astype(BF16)
            if h * HEAD_SIZE < query_cols:
                query_ref[at, h * HEAD_SIZE : (h + 1) * HEAD_SIZE] = turned
            else:
                kv_ref[at, :HEAD_SIZE] = turned
        kv_ref[at, HEAD_SIZE:] = out[:, query_cols + HEAD_SIZE :].astype(BF16)
        kv_copy(j).start()

    gather.run_each(0, each)
    gather.run_each(1, each)
    gather.step(2)
    gather.run_each(2, each)
    swap_landed(7)
    swap_copy(9).start()
    gather.step(3)
    gather.run_each(3, each)
    for i in range(1, PIECES):
        piece_copy(i, 0).start()
    swap_landed(6)
    cot_gather = Gather(me, cot_ref, c_sends, c_recv)
    cot_gather.step(0)
    swap_landed(9)
    swap_copy(11).start()
    relay_x(0)
    for j in range(LINE):
        kv_copy(j).wait_recv()
    attend_local(query_ref, kv_ref, kv_other_ref, attended_ref, probs_ref, r)
    swap_landed(11)

    def block_of(j):
        block = attended_ref[block_rows(j)]
        return jnp.concatenate(
            [
                dot(block, proj_ref[:, proj_cols:], PAIR_COLS),
                dot(block, proj_other_ref[:, proj_cols:], PAIR_COLS),
            ],
            1,
        )

    scatter = Scatter(me, block_of, landing, s_sends, s_recv)
    scatter.step(3)
    for store in stores[:11]:
        store.start()
    relay_x(1)
    scatter.step(2)
    relay_x(2)
    scatter.step(1)
    relay_y(0)
    relay_x(3)
    scatter.finish(mid_ref)
    mid = mid_ref[...] + x_ref[...].astype(F32)
    mid_ref[...] = mid
    normed_two_ref[block_rows(me)] = (mid * norm_scale(mid) * gains_ref[1:2]).astype(BF16)

    def turn_block(j):
        turned_ref[:, block_rows(j)] = normed_two_ref[block_rows(j)].T

    second = Gather(me, normed_two_ref, n_sends, n_recv)
    second.step(0)
    stores[11].start()
    second.run_each(0, turn_block)
    relay_y(1)
    relay_x(4)
    second.step(1)
    second.run_each(1, turn_block)
    relay_y(2)
    relay_x(5)
    second.step(2)
    second.run_each(2, turn_block)
    relay_y(3)
    second.step(3)
    second.run_each(3, turn_block)
    relay_y(4)
    stores[12].start()
    stores[13].start()
    cot_gather.step(1, forward=False)
    stores[14].start()
    relay_y(5)
    for i in range(PIECES):
        for way in (2, 3):
            of_y = y if way == 2 else 1 - y
            landed(weights_other_hbm.at[i // 2, piece(i, of_y), its_rows], piece_recv.at[way, i])
        for way in range(4):
            piece_copy(i, way).wait_send()
    for i in range(len(swaps)):
        swap_copy(i).wait_send()
    for j in range(LINE):
        kv_copy(j).wait_send()
    for store in stores:
        store.wait()
    gather.drain()
    cot_gather.drain(0, 1)
    second.drain()
    scatter.drain()


def front_call(proj_cols, query_cols, hidden, *args):
    heads = query_cols // HEAD_SIZE
    gains = shape(2, MODEL_WIDTH, F32)
    outs = [
        shape(BLOCK, MODEL_WIDTH),
        shape(LOCAL, MODEL_WIDTH),
        shape(LOCAL, query_cols),
        shape(LOCAL, 2 * HEAD_SIZE),
        shape(LOCAL, 2 * HEAD_SIZE),
        shape(LOCAL, HEAD_SIZE, F32),
        shape(LOCAL, HEAD_SIZE, F32),
        gains,
        shape(LOCAL, query_cols),
        jax.ShapeDtypeStruct((2 * heads, 2 * BLOCK, 4 * BLOCK), BF16),
        shape(BLOCK, MODEL_WIDTH, F32),
        shape(LOCAL, MODEL_WIDTH),
        shape(MODEL_WIDTH, LOCAL),
        shape(LOCAL, MODEL_WIDTH),
        shape(HALF, proj_cols + query_cols),
        shape(HALF, proj_cols + query_cols),
        jax.ShapeDtypeStruct((3, hidden, HALF), BF16),
    ]
    return pl.pallas_call(
        front_body,
        out_shape=outs,
        in_specs=[VMEM_SPEC] * 7 + [ANY_SPEC] * 3,
        out_specs=[VMEM_SPEC if out is gains else ANY_SPEC for out in outs],
        scratch_shapes=[pltpu.VMEM(out.shape, out.dtype) for out in outs[:-1] if out is not gains]
        + [
            pltpu.VMEM((2, BLOCK, HALF), BF16),
            pltpu.VMEM((2 * BLOCK, HEAD_SIZE), F32),
            pltpu.VMEM((1, proj_cols), F32),
            pltpu.VMEM((2, LINE, BLOCK, MODEL_WIDTH), BF16),
            DMA((15,)),
            DMA((12,)),
            DMA((12,)),
            DMA((4, PIECES)),
            DMA((4, PIECES)),
            DMA((LINE,)),
            DMA((LINE,)),
        ]
        + gather_sems() * 3
        + scatter_sems(),
        compiler_params=pltpu.CompilerParams(
            collective_id=1, has_side_effects=True, vmem_limit_bytes=67_043_328
        ),
        cost_estimate=pl.CostEstimate(
            flops=4 * 10**9, bytes_accessed=40_000_000, transcendentals=0
        ),
        name="front",
    )(*args)


DOWN, GATE, UPPER, CHAIN = 0, 1, 2, 3
UNITS = ((1, 1), (1, 0), (0, 1), (0, 0))
TILE = 256


def add_into(total_ref, term_ref, cols):
    @pl.loop(0, total_ref.shape[0] // 32)
    def _(i):
        at = aligned(i * 32, 32, 32)
        total_ref[at, cols] = (
            total_ref[at, cols].astype(F32) + term_ref[at, cols].astype(F32)
        ).astype(BF16)


def rear_body(
    mid_ref, gains_ref,
    normed_two_hbm, turned_hbm, cot_hbm, gate_hbm, upper_hbm, down_hbm, other_hbm, proj_hbm, proj_other_hbm, query_hbm, kv_hbm,
    kv_other_hbm, attended_hbm, probs_hbm, cos_hbm, sin_hbm, x_hbm, normed_one_hbm,
    out_ref, in_ref, small_ref, query_w_ref, output_w_ref, kv_all_ref, kept_hbm, land2_hbm, land3_hbm,
    cot_ref, activated_ref, gate_grad_ref, upper_grad_ref, out_part_ref, back_part_ref, turned_ref,
    kv_got_ref, got_ref, out_landing, landing, sums, gives, gots,
    chain_gots, chain_land2, chain_land3, kv_line, small_line, small_swap,
    load_sems, w_sems, c_sends, c_recv, o_sends, o_recv, r_sends, r_recv, a_sends, a_recv,
    give_sends, give_recv, two_sends, two_recv, three_sends, three_recv, stage_sem, kept_sems,
    swap_sends, swap_recv, kv_sends, kv_recv, kvd_sends, kvd_recv, line_sends, line_recv,
    small_sends, small_recv, credit,
):
    me, r, d = lax.axis_index("col"), lax.axis_index("row"), lax.axis_index("dp")
    y, core = d // 2, lax.rem(d, 2)
    x_to, y_to, core_to = 1 - r, 2 * (1 - y) + core, 2 * y + 1 - core
    diagonal_to = 2 * (1 - y) + 1 - core
    hidden = activated_ref.shape[1]
    query_cols = query_w_ref.shape[1]
    proj_cols = query_cols + 2 * HEAD_SIZE
    chain_cols = proj_cols + query_cols
    owns = (gate_hbm, upper_hbm, down_hbm)

    def cot_loads(act):
        for i in range(3):
            j = me - 1 + i

            @pl.when((j >= 0) & (j < LINE))
            def _():
                rows = block_rows(j)
                act(pltpu.make_async_copy(cot_hbm.at[rows], cot_ref.at[rows], load_sems.at[i]))

    turned_load = pltpu.make_async_copy(turned_hbm, turned_ref.at[1], load_sems.at[14])
    turned_load.start()
    cot_loads(lambda copy: copy.start())

    halves = {m: (hidden // 2 + BLOCK - 1) // BLOCK * BLOCK for m in (DOWN, GATE, UPPER)}
    halves[CHAIN] = chain_cols // 2

    def columns(m, axis):
        width = chain_cols if m == CHAIN else hidden
        return pl.ds(0, halves[m]) if axis == "row" else pl.ds(halves[m], width - halves[m])

    def unit_rows(h, rel):
        of_y = 1 - y if rel else y
        return aligned(h * HALF + of_y * 2 * UNIT, 2 * UNIT)

    def split(res, keep_ref, give_ref, at):
        low, high = res[:UNIT], res[UNIT:]
        keep_ref[:, at] = jnp.where(core == 0, low, high).astype(BF16)
        give_ref[:, at] = jnp.where(core == 0, high, low).astype(BF16)

    order = [
        (DOWN, 0), (DOWN, 1), (DOWN, 2), (UPPER, 0), (UPPER, 1), (UPPER, 2), (DOWN, 3),
        (GATE, 0), (GATE, 1), (GATE, 2), (UPPER, 3), (GATE, 3),
    ]
    columns_of = {DOWN: activated_ref, GATE: gate_grad_ref, UPPER: upper_grad_ref}
    ring = 3

    def total_of(m, h, rel):
        return sums.at[m * 4 + h * 2 + rel]

    def give_copy(u):
        return send(
            gives.at[u % 2], gots.at[u % ring], give_sends.at[u], give_recv.at[u], "dp", core_to
        )

    def compute(u):
        m, i = order[u]
        h, rel = UNITS[i]
        if u >= 2:
            give_copy(u - 2).wait_send()
        left = 0 if m == DOWN else 1
        rows = unit_rows(h, rel)
        tile = 512

        def run(at):
            res = dot(turned_ref[left, rows], columns_of[m][:, at])
            split(res, total_of(m, h, rel), gives.at[u % 2], at)

        @pl.loop(0, hidden // tile)
        def _(i):
            run(aligned(i * tile, tile))

        if hidden % tile:
            run(pl.ds(hidden // tile * tile, hidden % tile))
        if u >= ring:
            pl.semaphore_wait(credit, 1)
        give_copy(u).start()

    def two_copy(m, k, chain_sums=None):
        h, rel = ((1, 0), (1, 1), (0, 1), (1, 1))[k]
        axis, to = (("row", x_to), ("dp", y_to))[k // 2]
        at = columns(m, axis)
        if m == CHAIN:
            src, dst = chain_sums.at[h * 2 + rel, :, at], chain_land2.at[k % 2, :, at]
        else:
            src, dst = total_of(m, h, rel).at[:, at], land2_hbm.at[m * 2 + k % 2, :, at]
        return send(src, dst, two_sends.at[m, k], two_recv.at[m, k], axis, to)

    def combine(u):
        m, i = order[u]
        h, rel = UNITS[i]
        give_copy(u).wait_recv()
        add_into(total_of(m, h, rel), gots.at[u % ring], pl.ds(0, hidden))
        if u < len(order) - ring:
            pl.semaphore_signal(credit, 1, device_id={"dp": core_to}, device_id_type=MESH_ID)
        for k in {(1, 1): (1, 3), (1, 0): (0,), (0, 1): (2,), (0, 0): ()}[h, rel]:
            two_copy(m, k).start()

    def three_copy(m, k, chain_sums=None):
        h, rel = ((0, 1), (1, 0))[k]
        axis, to = (("dp", y_to), ("row", x_to))[k]
        at = columns(m, ("row", "dp")[k])
        if m == CHAIN:
            src, dst = chain_sums.at[h * 2 + rel, :, at], chain_land3.at[:, at]
        else:
            src, dst = total_of(m, h, rel).at[:, at], land3_hbm.at[m, :, at]
        return send(src, dst, three_sends.at[m, k], three_recv.at[m, k], axis, to)

    def kept_copy(m):
        return pltpu.make_async_copy(total_of(m, 0, 0), kept_hbm.at[m], kept_sems.at[m])

    def stage(m, i):
        return pltpu.make_async_copy(land2_hbm.at[m * 2 + i], gots.at[i], stage_sem.at[m, i])

    def second_stage(m, over_row=True):
        for k in range(4):
            two_copy(m, k).wait_recv()
        for i in (1, 0):
            stage(m, i).start()
        stage(m, 1).wait()
        add_into(total_of(m, 0, 1), gots.at[1], columns(m, "row"))
        three_copy(m, 0).start()
        add_into(total_of(m, 1, 0), gots.at[1], columns(m, "dp"))
        if over_row:
            three_copy(m, 1).start()
        stage(m, 0).wait()
        add_into(total_of(m, 0, 0), gots.at[0], pl.ds(0, hidden))
        kept_copy(m).start()

    barrier = pltpu.get_barrier_semaphore()
    others = [("row", x_to), ("dp", y_to), ("dp", core_to)]
    for axis, index in others:
        pl.semaphore_signal(barrier, 1, device_id={axis: index}, device_id_type=MESH_ID)
    for s in range(1, LINE):
        pl.semaphore_signal(
            barrier, 1, device_id={"col": lax.rem(me + s, LINE)}, device_id_type=MESH_ID
        )

    cot_gather = Gather(me, cot_ref, c_sends, c_recv)
    out_scatter = Scatter(
        me, lambda j: out_part_ref[block_rows(j)].astype(F32), out_landing, o_sends, o_recv
    )

    def feed(weights, gates, total, normed_two_ref):
        tiles = hidden // TILE
        rest = hidden % TILE

        def loads(t, slot, size):
            rows = aligned(t * TILE, size, TILE)
            for m in range(3):
                for i, src in enumerate((owns[m].at[rows], other_hbm.at[m, rows])):
                    yield pltpu.make_async_copy(
                        src,
                        weights.at[slot, m, pl.ds(0, size), pl.ds(i * HALF, HALF)],
                        w_sems.at[slot, m, i],
                    )

        def start(t, slot, size):
            for copy in loads(t, slot, size):
                copy.start()

        def ready(t, slot, size):
            for copy in loads(t, slot, size):
                copy.wait()

        def sweep(body, first_slot, hooks, again):
            @pl.loop(0, tiles)
            def _(t):
                slot = lax.rem(t + first_slot, 2)
                ready(t, slot, TILE)

                @pl.when(t < tiles - 1)
                def _():
                    start(t + 1, 1 - slot, TILE)

                @pl.when(t == tiles - 1)
                def _():
                    start(tiles, 1 - slot, rest)

                body(aligned(t * TILE, TILE), slot, TILE)
                for at, hook in hooks:
                    pl.when(t == at)(hook)

            slot = (tiles + first_slot) % 2
            ready(tiles, slot, rest)
            if again:
                start(0, 1 - slot, TILE)
            body(pl.ds(tiles * TILE, rest), slot, rest)

        def add_products(slot, size, factors, cols):
            width = 512

            @pl.loop(0, MODEL_WIDTH // width)
            def _(i):
                at = aligned(i * width, width)
                term = sum(
                    dot(factor[:, cols], weights[slot, m, pl.ds(0, size), at])
                    for factor, m in factors
                )
                total[:, at] += term

        def forward(cols, slot, size):
            here = pl.ds(0, size)
            gate = dot(normed_two_ref[...], weights[slot, 0, here], PAIR_COLS)
            upper = dot(normed_two_ref[...], weights[slot, 1, here], PAIR_COLS)
            activated = (gate * jax.nn.sigmoid(gate) * upper).astype(BF16)
            gates[0, :, cols] = gate.astype(BF16)
            gates[1, :, cols] = upper.astype(BF16)
            activated_ref[:, cols] = activated
            total[...] += dot(activated, weights[slot, 2, here])

        def backward(cols, slot, size):
            here = pl.ds(0, size)
            act_grad = dot(cot_ref[...], weights[slot, 2, here], PAIR_COLS)
            gate, upper = gates[0, :, cols].astype(F32), gates[1, :, cols].astype(F32)
            sig = jax.nn.sigmoid(gate)
            gate_grad = (act_grad * upper * sig * (1.0 + gate * (1.0 - sig))).astype(BF16)
            upper_grad = (act_grad * gate * sig).astype(BF16)
            gate_grad_ref[:, cols] = gate_grad
            upper_grad_ref[:, cols] = upper_grad
            add_products(slot, size, ((gate_grad_ref, 0), (upper_grad_ref, 1)), cols)

        load = pltpu.make_async_copy(normed_two_hbm, normed_two_ref, load_sems.at[15])
        load.start()
        start(0, 0, TILE)
        total[...] = jnp.zeros_like(total)
        pl.semaphore_wait(barrier, len(others) + LINE - 1)
        cot_loads(lambda copy: copy.wait())
        cot_gather.step(1, wait=False)
        load.wait()
        turned_load.wait()
        sweep(forward, 0, [(4, lambda: cot_gather.step(2))], True)
        out_part_ref[...] = total[...].astype(BF16)
        out_scatter.step(3)
        cot_gather.step(3)
        turned_ref[0] = cot_ref[...].T
        total[...] = jnp.zeros_like(total)
        compute(0)
        compute(1)
        combine(0)
        combine(1)
        sweep(backward, (tiles + 1) % 2, [(3, lambda: out_scatter.step(2))], False)
        back_part_ref[...] = total[...].astype(BF16)
        cot_gather.drain(1, LINE - 1)

    pl.run_scoped(
        feed,
        pltpu.VMEM((2, 3, TILE, MODEL_WIDTH), BF16),
        pltpu.VMEM((2, LOCAL, hidden), BF16),
        pltpu.VMEM((LOCAL, MODEL_WIDTH), F32),
        pltpu.VMEM((LOCAL, MODEL_WIDTH), BF16),
    )

    def rest(
        proj_ref, proj_other_ref, query_ref, kv_ref, kv_other_ref, attended_ref, probs_ref, cos_ref,
        sin_ref, x_ref, normed_one_ref, mid_grad_ref, own_ref, att_grad_ref,
        kv_grad_ref, kv_give_ref, proj_grad_ref, chain_sums, back_give,
    ):
        pairs = (
            (proj_hbm, proj_ref), (proj_other_hbm, proj_other_ref), (query_hbm, query_ref),
            (kv_hbm, kv_ref), (kv_other_hbm, kv_other_ref), (attended_hbm, attended_ref),
            (probs_hbm, probs_ref), (cos_hbm, cos_ref), (sin_hbm, sin_ref), (x_hbm, x_ref),
            (normed_one_hbm, normed_one_ref),
        )
        reads = [
            pltpu.make_async_copy(src, dst, load_sems.at[3 + i])
            for i, (src, dst) in enumerate(pairs)
        ]

        mid_half_ref = cot_ref

        scatter = Scatter(
            me, lambda j: back_part_ref[block_rows(j)].astype(F32), landing, r_sends, r_recv
        )
        scatter.step(3)
        for read in reads:
            read.start()
        compute(2)
        for u in (3, 4, 5):
            compute(u)
            combine(u - 1)
        scatter.step(2)
        for u in (6, 7):
            compute(u)
            combine(u - 1)
        scatter.step(1)
        for u in (8, 9):
            compute(u)
            combine(u - 1)
        scatter.finish(mid_grad_ref)
        mid, grad = mid_ref[...], mid_grad_ref[...]
        rinv = norm_scale(mid)
        small_line[me] = jnp.zeros_like(small_line[me])
        small_line[me, 1:2] = jnp.sum(grad * mid * rinv, 0, keepdims=True)
        scaled = grad * gains_ref[1:2]
        inner = jnp.sum(scaled * mid, -1, keepdims=True)
        mid_grad = (
            cot_ref[block_rows(me)].astype(F32)
            + rinv * scaled
            - mid * rinv**3 * inner / MODEL_WIDTH
        )
        mid_grad_ref[...] = mid_grad
        mid_half_ref[block_rows(me)] = mid_grad.astype(BF16)

        gather = Gather(me, mid_half_ref, a_sends, a_recv)
        gather.step(0)
        scatter.drain()
        for read in reads:
            read.wait()

        def each(j):
            block = mid_half_ref[block_rows(j)]
            att_grad_ref[block_rows(j)] = (
                dot(block[:, :HALF], proj_ref[:, proj_cols:])
                + dot(block[:, HALF:], proj_other_ref[:, proj_cols:])
            ).astype(BF16)

        gather.run_each(0, each)
        for u in (10, 11):
            compute(u)
            combine(u - 1)
        combine(11)
        gather.step(1)
        gather.run_each(1, each)
        second_stage(DOWN)
        gather.step(2)
        gather.run_each(2, each)
        second_stage(UPPER, False)
        gather.step(3)
        gather.run_each(3, each)
        out_scatter.step(1)
        attend_back_body(
            query_ref, kv_ref, kv_other_ref, attended_ref, probs_ref, att_grad_ref, cos_ref,
            sin_ref, proj_grad_ref, kv_grad_ref, kv_give_ref,
        )

        def swap_copy(i):
            src, dst = (
                (kv_give_ref, kv_got_ref),
                (back_give.at[0], got_ref.at[0]),
                (back_give.at[1], got_ref.at[1]),
            )[i]
            return send(src, dst, swap_sends.at[i], swap_recv.at[i], "row", x_to)

        swap_copy(0).start()
        swap_copy(0).wait_recv()
        kv = kv_grad_ref[...] + kv_got_ref[...].astype(F32)
        key = kv[:, :HEAD_SIZE]
        proj_grad_ref[:, query_cols : query_cols + HEAD_SIZE] = (
            key * cos_ref[...] - turn(key) * sin_ref[...]
        ).astype(BF16)
        proj_grad_ref[:, query_cols + HEAD_SIZE :] = kv[:, HEAD_SIZE:].astype(BF16)

        def block_of(j):
            block = proj_grad_ref[block_rows(j)]
            return jnp.concatenate(
                [
                    dot(block, proj_ref[:, :proj_cols], PAIR_COLS),
                    dot(block, proj_other_ref[:, :proj_cols], PAIR_COLS),
                ],
                1,
            )

        def chain_from(i):
            return gives.at[i // 2, :, pl.ds(i % 2 * chain_cols, chain_cols)]

        def chain_give(i):
            return send(
                chain_from(i), chain_gots.at[i], give_sends.at[12 + i], give_recv.at[12 + i],
                "dp", core_to,
            )

        def chain_compute(i):
            h, rel = UNITS[i]
            rows = unit_rows(h, rel)
            keep = chain_sums.at[h * 2 + rel]
            res = dot(normed_one_ref[:, rows], proj_grad_ref[...], PAIR_ROWS)
            split(res, keep, chain_from(i), pl.ds(0, proj_cols))
            res = dot(mid_half_ref[:, rows], attended_ref[...], PAIR_ROWS)
            split(res, keep, chain_from(i), pl.ds(proj_cols, query_cols))
            chain_give(i).start()

        def chain_combine(i):
            h, rel = UNITS[i]
            chain_give(i).wait_recv()
            add_into(chain_sums.at[h * 2 + rel], chain_gots.at[i], pl.ds(0, chain_cols))
            for k in {(1, 1): (1, 3), (1, 0): (0,), (0, 1): (2,), (0, 0): ()}[h, rel]:
                two_copy(CHAIN, k, chain_sums).start()

        second = Scatter(me, block_of, landing, r_sends, r_recv)
        second.step(3)
        for u in (len(order) - 2, len(order) - 1):
            give_copy(u).wait_send()
        for i in range(4):
            chain_compute(i)
        for i in range(4):
            chain_combine(i)
        three_copy(UPPER, 1).start()
        small_line[me, 2:3, :proj_cols] = jnp.sum(
            proj_grad_ref[...].astype(F32), 0, keepdims=True
        )
        second.step(2)
        second_stage(GATE, False)
        out_scatter.finish(own_ref)
        out = own_ref[...] + mid_ref[...]
        out_ref[:, block_rows(r)] = out[:, :HALF].T
        back_give[1] = out[:, HALF:].astype(BF16)
        second.step(1)
        for k in range(4):
            two_copy(CHAIN, k, chain_sums).wait_recv()
        add_into(chain_sums.at[1], chain_land2.at[1], columns(CHAIN, "row"))
        three_copy(CHAIN, 0, chain_sums).start()
        add_into(chain_sums.at[2], chain_land2.at[1], columns(CHAIN, "dp"))
        three_copy(CHAIN, 1, chain_sums).start()
        add_into(chain_sums.at[0], chain_land2.at[0], pl.ds(0, chain_cols))
        three_copy(GATE, 1).start()
        swap_copy(2).start()
        second.finish(own_ref)
        x, grad = x_ref[...].astype(F32), own_ref[...]
        rinv = norm_scale(x)
        scaled = grad * gains_ref[0:1]
        inner = jnp.sum(scaled * x, -1, keepdims=True)
        input_grad = mid_grad_ref[...] + rinv * scaled - x * rinv**3 * inner / MODEL_WIDTH
        back_give[0] = input_grad[:, HALF:].astype(BF16)
        swap_copy(1).start()
        small_line[me, 0:1] = jnp.sum(grad * x * rinv, 0, keepdims=True)

        def small_line_copy(s):
            to = lax.rem(me + s, LINE)
            return send(
                small_line.at[me], small_line.at[me], line_sends.at[s], line_recv.at[me], "col", to
            )

        for s in range(1, LINE):
            small_line_copy(s).start()
        in_ref[:, block_rows(r)] = input_grad[:, :HALF].T

        for s in range(1, LINE):
            landed(small_line.at[me], line_recv.at[lax.rem(me + s, LINE)])
        group = LINE // KEYVALUE_HEADS
        lines = [small_line[j] for j in range(LINE)]
        gain_sum = lines[0][:2] + lines[1][:2] + lines[2][:2] + lines[3][:2]
        small_swap[0] = jnp.zeros_like(small_swap[0])
        small_swap[0, 0:2] = gain_sum
        small_swap[0, 2:3, :query_cols] = small_line[me, 2:3, :query_cols]
        for i in range(2):
            for h in range(KEYVALUE_HEADS):
                at = query_cols + i * HEAD_SIZE
                part = lines[h * group][2:3, at : at + HEAD_SIZE]
                for j in range(1, group):
                    part = part + lines[h * group + j][2:3, at : at + HEAD_SIZE]
                at = (i * KEYVALUE_HEADS + h) * HEAD_SIZE
                small_swap[0, 3:4, at : at + HEAD_SIZE] = part

        def small_copy(i):
            axis, to = (("dp", core_to), ("dp", y_to), ("row", x_to))[i]
            return send(
                small_swap.at[2 * i], small_swap.at[2 * i + 1], small_sends.at[i],
                small_recv.at[i], axis, to,
            )

        small_copy(0).start()
        small_copy(0).wait_recv()
        small_swap[2] = small_swap[0] + small_swap[1]
        small_copy(1).start()

        for k in range(2):
            three_copy(CHAIN, k, chain_sums).wait_recv()
        total = chain_sums[0].astype(F32) + chain_land3[...].astype(F32)
        query_w_ref[...] = total[:, :query_cols]
        output_w_ref[...] = total[:, proj_cols:]
        kv_line[me] = total[:, query_cols:proj_cols].astype(BF16)

        def kv_line_copy(s):
            to = lax.rem(me + s, LINE)
            return send(kv_line.at[me], kv_line.at[me], kv_sends.at[s], kv_recv.at[me], "col", to)

        for s in range(1, LINE):
            kv_line_copy(s).start()
        small_copy(1).wait_recv()
        both = small_swap[2] + small_swap[3]
        small_swap[4, :2, :HALF] = both[:2, HALF:]
        small_swap[4, 2:, :HALF] = both[2:, :HALF]
        small_copy(2).start()
        for s in range(1, LINE):
            landed(kv_line.at[me], kv_recv.at[lax.rem(me + s, LINE)])
        dp_rows = aligned(d * UNIT, UNIT, UNIT)
        for h in range(KEYVALUE_HEADS):
            pair = kv_line[h * group].astype(F32)
            for i in range(1, group):
                pair = pair + kv_line[h * group + i].astype(F32)
            for i in range(2):
                at = (i * KEYVALUE_HEADS + h) * HEAD_SIZE
                kv_all_ref[dp_rows, at : at + HEAD_SIZE] = pair[
                    :, i * HEAD_SIZE : (i + 1) * HEAD_SIZE
                ].astype(BF16)

        def kv_rows(of):
            return kv_all_ref.at[aligned(of * UNIT, UNIT, UNIT)]

        def kv_dp_copy(i):
            rows = kv_rows(y_to if i == 2 else d)
            to = y_to if i == 1 else core_to
            return send(rows, rows, kvd_sends.at[i], kvd_recv.at[i], "dp", to)

        kv_dp_copy(1).start()
        kv_dp_copy(0).start()
        for i in (2, 1):
            swap_copy(i).wait_recv()
            to_ref = (in_ref, out_ref)[i - 1]
            to_ref[:, block_rows(1 - r)] = got_ref[i - 1].astype(F32).T
        small_copy(2).wait_recv()
        small_ref[...] = both[:, :HALF] + small_swap[5, :, :HALF]

        landed(kv_rows(y_to), kvd_recv.at[1])
        kv_dp_copy(2).start()
        landed(kv_rows(core_to), kvd_recv.at[0])
        landed(kv_rows(diagonal_to), kvd_recv.at[2])
        for m in (DOWN, GATE, UPPER):
            for k in range(2):
                three_copy(m, k).wait_recv()
                three_copy(m, k).wait_send()
            kept_copy(m).wait()
            for k in range(4):
                two_copy(m, k).wait_send()
        for i in range(4):
            chain_give(i).wait_send()
            two_copy(CHAIN, i, chain_sums).wait_send()
        for k in range(2):
            three_copy(CHAIN, k, chain_sums).wait_send()
        for i in range(3):
            swap_copy(i).wait_send()
            small_copy(i).wait_send()
            kv_dp_copy(i).wait_send()
            kv_line_copy(1 + i).wait_send()
            small_line_copy(1 + i).wait_send()
        gather.drain()
        out_scatter.drain()
        second.drain()

    wide = (HALF, chain_cols)
    pl.run_scoped(
        rest,
        pltpu.VMEM(wide, BF16),
        pltpu.VMEM(wide, BF16),
        pltpu.VMEM((LOCAL, query_cols), BF16),
        pltpu.VMEM((LOCAL, 2 * HEAD_SIZE), BF16),
        pltpu.VMEM((LOCAL, 2 * HEAD_SIZE), BF16),
        pltpu.VMEM((LOCAL, query_cols), BF16),
        pltpu.VMEM(probs_hbm.shape, BF16),
        pltpu.VMEM((LOCAL, HEAD_SIZE), F32),
        pltpu.VMEM((LOCAL, HEAD_SIZE), F32),
        pltpu.VMEM((BLOCK, MODEL_WIDTH), BF16),
        pltpu.VMEM((LOCAL, MODEL_WIDTH), BF16),
        pltpu.VMEM((BLOCK, MODEL_WIDTH), F32),
        pltpu.VMEM((BLOCK, MODEL_WIDTH), F32),
        pltpu.VMEM((LOCAL, query_cols), BF16),
        pltpu.VMEM((LOCAL, 2 * HEAD_SIZE), F32),
        pltpu.VMEM((LOCAL, 2 * HEAD_SIZE), BF16),
        pltpu.VMEM((LOCAL, proj_cols), BF16),
        pltpu.VMEM((4, UNIT, chain_cols), BF16),
        pltpu.VMEM((2, BLOCK, HALF), BF16),
    )


def rear_call(hidden, proj_cols, query_cols, *args):
    chain_cols = proj_cols + query_cols
    outs = [
        shape(HALF, 2 * BLOCK, F32),
        shape(HALF, 2 * BLOCK, F32),
        shape(8, HALF, F32),
        shape(UNIT, query_cols, F32),
        shape(UNIT, query_cols, F32),
        shape(4 * UNIT, 2 * KEYVALUE_HEADS * HEAD_SIZE),
        jax.ShapeDtypeStruct((3, UNIT, hidden), BF16),
        jax.ShapeDtypeStruct((6, UNIT, hidden), BF16),
        jax.ShapeDtypeStruct((3, UNIT, hidden), BF16),
    ]
    local = (LOCAL, MODEL_WIDTH)
    line = (2, LINE, BLOCK, MODEL_WIDTH)
    return pl.pallas_call(
        rear_body,
        out_shape=outs,
        in_specs=[VMEM_SPEC] * 2 + [ANY_SPEC] * (len(args) - 2),
        out_specs=[VMEM_SPEC] * 6 + [ANY_SPEC] * 3,
        scratch_shapes=[
            pltpu.VMEM(local, BF16),
            pltpu.VMEM((LOCAL, hidden), BF16),
            pltpu.VMEM((LOCAL, hidden), BF16),
            pltpu.VMEM((LOCAL, hidden), BF16),
            pltpu.VMEM(local, BF16),
            pltpu.VMEM(local, BF16),
            pltpu.VMEM((2, MODEL_WIDTH, LOCAL), BF16),
            pltpu.VMEM((LOCAL, 2 * HEAD_SIZE), BF16),
            pltpu.VMEM((2, BLOCK, HALF), BF16),
            pltpu.VMEM(line, BF16),
            pltpu.VMEM(line, BF16),
            pltpu.VMEM((12, UNIT, hidden), BF16),
            pltpu.VMEM((2, UNIT, hidden), BF16),
            pltpu.VMEM((3, UNIT, hidden), BF16),
            pltpu.VMEM((4, UNIT, chain_cols), BF16),
            pltpu.VMEM((2, UNIT, chain_cols), BF16),
            pltpu.VMEM((UNIT, chain_cols), BF16),
            pltpu.VMEM((LINE, UNIT, 2 * HEAD_SIZE), BF16),
            pltpu.VMEM((LINE, 8, MODEL_WIDTH), F32),
            pltpu.VMEM((6, 8, MODEL_WIDTH), F32),
            DMA((16,)),
            DMA((2, 3, 2)),
        ]
        + gather_sems()
        + scatter_sems()
        + scatter_sems()
        + gather_sems()
        + [
            DMA((16,)), DMA((16,)),
            DMA((4, 4)), DMA((4, 4)),
            DMA((4, 2)), DMA((4, 2)),
            DMA((3, 2)), DMA((3,)),
            DMA((3,)), DMA((3,)),
            DMA((LINE,)), DMA((LINE,)),
            DMA((3,)), DMA((3,)),
            DMA((LINE,)), DMA((LINE,)),
            DMA((3,)), DMA((3,)),
            pltpu.SemaphoreType.REGULAR,
        ],
        compiler_params=pltpu.CompilerParams(
            collective_id=2, has_side_effects=True, vmem_limit_bytes=67_043_328
        ),
        cost_estimate=pl.CostEstimate(
            flops=4 * 10**10, bytes_accessed=80_000_000, transcendentals=0
        ),
        name="rear",
    )(*args)


def fast_device(
    block_input,
    position_ids,
    attention_gain,
    query_weight,
    query_bias,
    key_value_weight,
    key_value_bias,
    output_weight,
    feedforward_gain,
    gate_weight,
    upper_weight,
    down_weight,
    out_cotangent,
):
    query_cols = query_weight.shape[1]
    hidden = gate_weight.shape[1]
    proj_cols = query_cols + 2 * HEAD_SIZE
    frequencies = THETA ** (-(jnp.arange(HEAD_SIZE // 2, dtype=F32) * 2.0 / HEAD_SIZE))
    angles = position_ids.astype(F32)[:, None] * frequencies[None, :]
    table = jnp.concatenate([jnp.cos(angles), jnp.sin(angles)], -1)
    small = jnp.concatenate([attention_gain, feedforward_gain, query_bias, key_value_bias])[None]
    gate_t, upper_t, down_t = gate_weight.T, upper_weight.T, down_weight.T
    (
        x_own, normed_one, query_rot, kv_own, kv_other, cosine, sine, gains, attended, probs,
        mid, normed_two, normed_turned, cot_part, own_proj, other_proj, other_weights,
    ) = front_call(
        proj_cols, query_cols, hidden,
        block_input, out_cotangent, table, small, query_weight, key_value_weight, output_weight,
        gate_t, upper_t, down_t,
    )
    out, input_grad, sums, query_sum, output_sum, kv_all, kept, _, landing = rear_call(
        hidden, proj_cols, query_cols,
        mid, gains,
        normed_two, normed_turned, cot_part, gate_t, upper_t, down_t, other_weights, own_proj, other_proj, query_rot, kv_own,
        kv_other, attended, probs, cosine, sine, x_own, normed_one,
    )
    down_sum, gate_sum, upper_sum = (
        kept[m].astype(F32) + landing[m].astype(F32) for m in range(3)
    )
    bias_rows = query_cols // lax.axis_size("dp")
    query_bias_grad = lax.dynamic_slice_in_dim(
        sums[2], lax.axis_index("dp") * bias_rows, bias_rows, 0
    )
    return (
        out,
        input_grad,
        sums[0],
        query_sum,
        query_bias_grad,
        kv_all.astype(F32),
        sums[3, : 2 * KEYVALUE_HEADS * HEAD_SIZE],
        output_sum,
        sums[1],
        gate_sum,
        upper_sum,
        down_sum,
    )


def per_device(*arrays):
    sizes = tuple(lax.axis_size(axis) for axis in ("dp", "row", "col"))
    if sizes == (4, 2, LINE) and arrays[0].shape == (HALF, 2 * BLOCK):
        return fast_device(*arrays)
    return general_device(*arrays)


def solution(mesh):
    placed = (
        P("row", ("dp", "col")),
        P(("dp", "row")),
        P("row"),
        P("row", "col"),
        P("col"),
        P("row", None),
        P(),
        P("row", "col"),
        P("row"),
        P("row", "col"),
        P("row", "col"),
        P("row", "col"),
        P("row", ("dp", "col")),
    )
    return jax.shard_map(
        per_device,
        mesh=mesh,
        in_specs=placed,
        out_specs=(
            P("row", ("dp", "col")),
            P("row", ("dp", "col")),
            P("row"),
            P(("row", "dp"), "col"),
            P(("col", "dp")),
            P("row", None),
            P(),
            P(("row", "dp"), "col"),
            P("row"),
            P(("row", "dp"), "col"),
            P(("row", "dp"), "col"),
            P(("row", "dp"), "col"),
        ),
        check_vma=False,
    )
```

```python
import jax
import jax.numpy as jnp
from jax import lax
from jax.experimental import pallas as pl
from jax.experimental.pallas import tpu as pltpu
from jax.sharding import PartitionSpec as P

MODEL_WIDTH = 1536
KEYVALUE_HEADS = 2
HEAD_SIZE = 128


EPS = 1e-06
THETA = 1000000.0
NEG = -1e30


def rope_tables(position_ids):
    half_dim = HEAD_SIZE // 2
    frequencies = THETA ** (-(jnp.arange(half_dim, dtype=jnp.float32) * 2.0 / HEAD_SIZE))
    angles = position_ids.astype(jnp.float32)[:, None] * frequencies[None, :]
    cosine_values = jnp.cos(angles)
    sine_lookup = jnp.sin(angles)
    return (
        jnp.concatenate([cosine_values, cosine_values], -1),
        jnp.concatenate([sine_lookup, sine_lookup], -1),
    )


def apply_rotation(values, cosine_values, sine_lookup):
    half_dim = HEAD_SIZE // 2
    turned = jnp.concatenate([-values[..., half_dim:], values[..., :half_dim]], -1)
    return values * cosine_values[:, None, :] + turned * sine_lookup[:, None, :]


def unrotate(gradient, cosine_values, sine_lookup):
    half_dim = HEAD_SIZE // 2
    scaled = gradient * sine_lookup[:, None, :]
    turned = jnp.concatenate([scaled[..., half_dim:], -scaled[..., :half_dim]], -1)
    return gradient * cosine_values[:, None, :] + turned


def row_total(partial_value):
    return lax.psum(partial_value, "row")


def norm_forward(x_float, gain):
    squares = jnp.sum(x_float * x_float, -1)
    rinv = lax.rsqrt(row_total(squares) / MODEL_WIDTH + EPS)[:, None]
    return ((x_float * rinv * gain).astype(jnp.bfloat16), rinv)


def norm_backward(normed_grad, x_float, rinv, gain):
    scaled = normed_grad * gain
    inner = row_total(jnp.sum(scaled * x_float, -1))[:, None]
    input_part = rinv * scaled - x_float * rinv**3 * inner / MODEL_WIDTH
    gain_part = jnp.sum(normed_grad * x_float * rinv, 0)
    return (input_part, gain_part)


def column_gather(values):
    return lax.all_gather(values, "col", axis=0, tiled=True)


def column_sum(partial_value):
    return lax.psum_scatter(
        partial_value.astype(jnp.bfloat16), "col", scatter_dimension=0, tiled=True
    ).astype(jnp.float32)


def row_product(gathered, weight):
    return (
        lax.psum_scatter(
            jnp.dot(gathered, weight, preferred_element_type=jnp.float32).astype(jnp.bfloat16),
            "row",
            scatter_dimension=0,
            tiled=True,
        ).astype(jnp.float32),
        gathered,
    )


def row_project(local_part, weight):
    return lax.dot_general(
        lax.all_gather(local_part, "row", axis=0, tiled=True),
        weight,
        (((1,), (1,)), ((), ())),
        preferred_element_type=jnp.float32,
    )


def row_fold(local_part, partner, weight):
    pair_dims = (((0,), (0,)), ((), ()))

    def accumulate(block_rows):
        grad_sum = lax.dot_general(
            partner, block_rows, pair_dims, preferred_element_type=jnp.float32
        )
        if weight is None:
            return (grad_sum,)
        back_proj = lax.dot_general(
            block_rows, weight, (((1,), (1,)), ((), ())), preferred_element_type=jnp.float32
        )
        column_totals = jnp.sum(block_rows, 0, dtype=jnp.float32)
        return (grad_sum, back_proj, column_totals)

    return accumulate(lax.all_gather(local_part, "row", axis=0, tiled=True))


def causal_scores(query_rot, rotated_keys):
    scores = jnp.einsum(
        "ihd,jd->hij", query_rot, rotated_keys, preferred_element_type=jnp.float32
    ) * HEAD_SIZE ** (-0.5)
    length = query_rot.shape[0]
    allowed = jnp.arange(length)[:, None] >= jnp.arange(length)[None, :]
    return jnp.where(allowed[None], scores, NEG)


def attend(query_rot, rotated_keys, value_second_part):
    scores = causal_scores(query_rot, rotated_keys)
    row_max = jnp.max(scores, -1, keepdims=True)
    log_total = row_max + jnp.log(jnp.sum(jnp.exp(scores - row_max), -1, keepdims=True))
    probs_half = jnp.exp(scores - log_total).astype(jnp.bfloat16)
    attended = jnp.einsum(
        "hij,jd->ihd", probs_half, value_second_part, preferred_element_type=jnp.float32
    ).astype(jnp.bfloat16)
    return (attended, log_total)


def attend_back(query_rot, rotated_keys, value_second_part, attended, att_grad, log_total):
    scale = HEAD_SIZE ** (-0.5)
    softmax_probs = jnp.exp(causal_scores(query_rot, rotated_keys) - log_total)
    probs_half = softmax_probs.astype(jnp.bfloat16)
    prob_grad = jnp.einsum(
        "ihd,jd->hij", att_grad, value_second_part, preferred_element_type=jnp.float32
    )
    row_delta = jnp.einsum("ihd,ihd->hi", att_grad, attended, preferred_element_type=jnp.float32)
    score_half = (softmax_probs * (prob_grad - row_delta[:, :, None])).astype(jnp.bfloat16)
    query_grad = (
        jnp.einsum("hij,jd->ihd", score_half, rotated_keys, preferred_element_type=jnp.float32)
        * scale
    )
    key_grad = (
        jnp.einsum("hij,ihd->jd", score_half, query_rot, preferred_element_type=jnp.float32) * scale
    )
    value_grad = jnp.einsum("hij,ihd->jd", probs_half, att_grad, preferred_element_type=jnp.float32)
    return (query_grad, key_grad, value_grad)


def general_device(
    block_input,
    position_ids,
    attention_gain,
    query_weight,
    query_bias,
    key_value_weight,
    key_value_bias,
    output_weight,
    feedforward_gain,
    gate_weight,
    upper_weight,
    down_weight,
    out_cotangent,
):
    single_float_type = jnp.float32
    brain_float_type = jnp.bfloat16
    column_number = lax.axis_size("col")
    seq_len = position_ids.shape[0]
    heads_here = query_weight.shape[1] // HEAD_SIZE
    query_cols = query_weight.shape[1]
    hidden_cols = gate_weight.shape[1]
    key_value_head = lax.axis_index("col") // (column_number // KEYVALUE_HEADS)
    key_start = key_value_head * HEAD_SIZE
    value_offset = KEYVALUE_HEADS * HEAD_SIZE + key_value_head * HEAD_SIZE
    keyval_local = jnp.concatenate(
        [
            lax.dynamic_slice_in_dim(key_value_weight, key_start, HEAD_SIZE, 1),
            lax.dynamic_slice_in_dim(key_value_weight, value_offset, HEAD_SIZE, 1),
        ],
        1,
    )
    bias_local = jnp.concatenate(
        [
            lax.dynamic_slice_in_dim(key_value_bias, key_start, HEAD_SIZE, 0),
            lax.dynamic_slice_in_dim(key_value_bias, value_offset, HEAD_SIZE, 0),
        ],
        0,
    )
    proj_weight = jnp.concatenate([query_weight, keyval_local], 1)
    proj_bias = jnp.concatenate([query_bias, bias_local], 0)
    pair_weight = jnp.concatenate([gate_weight, upper_weight], 1)
    cosine_values, sine_lookup = rope_tables(position_ids)
    x_float = block_input.T.astype(single_float_type)
    cot_local = out_cotangent.T
    normed_one, rinv_one = norm_forward(x_float, attention_gain)
    normed_one_all = column_gather(normed_one)
    proj_out = row_product(normed_one_all, proj_weight)[0] + proj_bias
    query_rot = apply_rotation(
        proj_out[:, :query_cols].reshape(seq_len, heads_here, HEAD_SIZE), cosine_values, sine_lookup
    ).astype(brain_float_type)
    rotated_keys = apply_rotation(
        proj_out[:, query_cols : query_cols + HEAD_SIZE][:, None, :], cosine_values, sine_lookup
    )[:, 0].astype(brain_float_type)
    value_second_part = proj_out[:, query_cols + HEAD_SIZE :].astype(brain_float_type)
    attended, log_total = attend(query_rot, rotated_keys, value_second_part)
    attended_flat = attended.reshape(seq_len, query_cols)
    hidden_res = x_float + column_sum(row_project(attended_flat, output_weight))
    normed_two, rinv_two = norm_forward(hidden_res, feedforward_gain)
    normed_two_all = column_gather(normed_two)
    gate_upper, normed_two_seq = row_product(normed_two_all, pair_weight)
    gate_lin = gate_upper[:, :hidden_cols]
    upper_lin = gate_upper[:, hidden_cols:]
    sigmoid_gate = jax.nn.sigmoid(gate_lin)
    activated = (gate_lin * sigmoid_gate * upper_lin).astype(brain_float_type)
    block_output = hidden_res + column_sum(row_project(activated, down_weight))
    cotangent_all = column_gather(cot_local)
    act_grad = row_product(cotangent_all, down_weight)[0]
    down_grad = row_fold(activated, cotangent_all, None)[0]
    gate_grad = act_grad * upper_lin * sigmoid_gate * (1.0 + gate_lin * (1.0 - sigmoid_gate))
    upper_grad = act_grad * gate_lin * sigmoid_gate
    pair_grad_half = jnp.concatenate([gate_grad, upper_grad], 1).astype(brain_float_type)
    folded_two = row_fold(pair_grad_half, normed_two_all, pair_weight)
    pair_weight_grad = folded_two[0]
    spread_two = folded_two[1]
    normed_two_grad = column_sum(spread_two)
    hidden_part, ffn_gain_part = norm_backward(
        normed_two_grad, hidden_res, rinv_two, feedforward_gain
    )
    hidden_grad = cot_local.astype(single_float_type) + hidden_part
    hidden_half = hidden_grad.astype(brain_float_type)
    hidden_all = column_gather(hidden_half)
    att_grad = (
        row_product(hidden_all, output_weight)[0]
        .astype(brain_float_type)
        .reshape(seq_len, heads_here, HEAD_SIZE)
    )
    output_grad = row_fold(attended_flat, hidden_all, None)[0]
    query_grad, key_grad, value_grad = attend_back(
        query_rot, rotated_keys, value_second_part, attended, att_grad, log_total
    )
    query_half = (
        unrotate(query_grad, cosine_values, sine_lookup)
        .astype(brain_float_type)
        .reshape(seq_len, query_cols)
    )
    key_half = unrotate(key_grad[:, None, :], cosine_values, sine_lookup)[:, 0].astype(
        brain_float_type
    )
    value_grad_half = value_grad.astype(brain_float_type)
    proj_grad_half = jnp.concatenate([query_half, key_half, value_grad_half], 1)
    folded_one = row_fold(proj_grad_half, normed_one_all, proj_weight)
    projection_weight_gradient = folded_one[0]
    normed_one_grad = column_sum(folded_one[1])
    proj_bias_grad = folded_one[2]
    input_part, attn_gain_part = norm_backward(normed_one_grad, x_float, rinv_one, attention_gain)
    input_grad = hidden_grad + input_part
    key_value_gradient = jnp.zeros(
        (projection_weight_gradient.shape[0], 2 * KEYVALUE_HEADS * HEAD_SIZE), single_float_type
    )
    key_value_gradient = lax.dynamic_update_slice_in_dim(
        key_value_gradient,
        projection_weight_gradient[:, query_cols : query_cols + HEAD_SIZE],
        key_start,
        1,
    )
    key_value_gradient = lax.dynamic_update_slice_in_dim(
        key_value_gradient, projection_weight_gradient[:, query_cols + HEAD_SIZE :], value_offset, 1
    )
    key_value_bias_gradient = jnp.zeros((2 * KEYVALUE_HEADS * HEAD_SIZE,), single_float_type)
    key_value_bias_gradient = lax.dynamic_update_slice_in_dim(
        key_value_bias_gradient, proj_bias_grad[query_cols : query_cols + HEAD_SIZE], key_start, 0
    )
    key_value_bias_gradient = lax.dynamic_update_slice_in_dim(
        key_value_bias_gradient, proj_bias_grad[query_cols + HEAD_SIZE :], value_offset, 0
    )
    shared = (
        lax.psum(key_value_gradient.astype(jnp.bfloat16), ("dp", "col")).astype(jnp.float32),
        lax.psum(key_value_bias_gradient.astype(jnp.bfloat16), ("dp", "col")).astype(jnp.float32),
        lax.psum(attn_gain_part.astype(jnp.bfloat16), ("dp", "col")).astype(jnp.float32),
        lax.psum(ffn_gain_part.astype(jnp.bfloat16), ("dp", "col")).astype(jnp.float32),
    )
    summed = (
        lax.psum_scatter(
            projection_weight_gradient[:, :query_cols].astype(jnp.bfloat16),
            "dp",
            scatter_dimension=0,
            tiled=True,
        ).astype(jnp.float32),
        lax.psum_scatter(
            proj_bias_grad[:query_cols].astype(jnp.bfloat16), "dp", scatter_dimension=0, tiled=True
        ).astype(jnp.float32),
        lax.psum_scatter(
            output_grad.astype(jnp.bfloat16), "dp", scatter_dimension=0, tiled=True
        ).astype(jnp.float32),
        lax.psum_scatter(
            pair_weight_grad[:, :hidden_cols].astype(jnp.bfloat16),
            "dp",
            scatter_dimension=0,
            tiled=True,
        ).astype(jnp.float32),
        lax.psum_scatter(
            pair_weight_grad[:, hidden_cols:].astype(jnp.bfloat16),
            "dp",
            scatter_dimension=0,
            tiled=True,
        ).astype(jnp.float32),
        lax.psum_scatter(
            down_grad.astype(jnp.bfloat16), "dp", scatter_dimension=0, tiled=True
        ).astype(jnp.float32),
    )
    return (
        block_output.T,
        input_grad.T,
        shared[2],
        summed[0],
        summed[1],
        shared[0],
        shared[1],
        summed[2],
        shared[3],
        summed[3],
        summed[4],
        summed[5],
    )


MESH_ID = pl.DeviceIdType.MESH
F32 = jnp.float32
BF16 = jnp.bfloat16
LINE = 4
BLOCK = 128
SUB = 2
PART = BLOCK // SUB
LOCAL = LINE * BLOCK
HALF = MODEL_WIDTH // 2
UNIT = MODEL_WIDTH // 8
VMEM_SPEC = pl.BlockSpec(memory_space=pltpu.VMEM)
ANY_SPEC = pl.BlockSpec(memory_space=pl.ANY)
PAIR_ROWS = (((0,), (0,)), ((), ()))
PAIR_COLS = (((1,), (1,)), ((), ()))
SCALE = HEAD_SIZE ** (-0.5)
DMA = pltpu.SemaphoreType.DMA


def greet(me, others):
    barrier = pltpu.get_barrier_semaphore()
    for axis, index in others:
        pl.semaphore_signal(barrier, 1, device_id={axis: index}, device_id_type=MESH_ID)

    @pl.when(me > 0)
    def _():
        pl.semaphore_signal(barrier, 1, device_id={"col": me - 1}, device_id_type=MESH_ID)

    @pl.when(me < LINE - 1)
    def _():
        pl.semaphore_signal(barrier, 1, device_id={"col": me + 1}, device_id_type=MESH_ID)

    @pl.when((me > 0) & (me < LINE - 1))
    def _():
        pl.semaphore_wait(barrier, 2 + len(others))

    @pl.when((me == 0) | (me == LINE - 1))
    def _():
        pl.semaphore_wait(barrier, 1 + len(others))


def aligned(start, size, to=BLOCK):
    return pl.ds(pl.multiple_of(start, to), size)


def block_rows(index):
    return aligned(index * BLOCK, BLOCK)


def send(src, dst, send_sem, recv_sem, axis, to):
    return pltpu.make_async_remote_copy(
        src, dst, send_sem, recv_sem, device_id={axis: to}, device_id_type=MESH_ID
    )


def landed(ref, sem):
    pltpu.make_async_copy(ref, ref, sem).wait()


class Gather:
    def __init__(self, me, all_ref, sends, recv):
        self.me, self.all_ref, self.sends, self.recv = me, all_ref, sends, recv

    def rows(self, j, p):
        return self.all_ref.at[aligned(j * BLOCK + p * PART, PART, PART)]

    def copy(self, j, p, s, side):
        rows = self.rows(j, p)
        return send(
            rows, rows, self.sends.at[side, s, p], self.recv.at[j, p], "col",
            self.me + 1 - 2 * side,
        )

    def has_next(self, side):
        to = self.me + 1 - 2 * side
        return (to >= 0) & (to < LINE)

    def step(self, s, wait=True, forward=True):
        @pl.loop(0, 2 * SUB)
        def _(i):
            side, p = lax.rem(i, 2), i // 2
            j = self.me - (1 - 2 * side) * s

            @pl.when((j >= 0) & (j < LINE))
            def _():
                if s and wait:
                    landed(self.rows(j, p), self.recv.at[j, p])

                if forward and s < LINE - 1:

                    @pl.when(self.has_next(side))
                    def _():
                        self.copy(j, p, s, side).start()

    def run_each(self, s, each):
        if s == 0:
            each(self.me)
            return

        @pl.loop(0, 2)
        def _(side):
            j = self.me - (1 - 2 * side) * s

            @pl.when((j >= 0) & (j < LINE))
            def _():
                each(j)

    def drain(self, first=0, last=LINE - 1):
        for s in range(first, last):

            @pl.loop(0, 2)
            def _(side):
                j = self.me - (1 - 2 * side) * s

                @pl.when((j >= 0) & (j < LINE) & self.has_next(side))
                def _():
                    for p in range(SUB):
                        self.copy(self.me, p, s, side).wait_send()


class Scatter:
    def __init__(self, me, block_of, landing, sends, recv):
        self.me, self.block_of, self.landing = me, block_of, landing
        self.sends, self.recv = sends, recv

    def rows(self, side, j, p):
        return self.landing.at[side, j, pl.ds(p * PART, PART)]

    def copy(self, side, j, p):
        rows = self.rows(side, j, p)
        return send(
            rows, rows, self.sends.at[side, j, p], self.recv.at[side, j, p], "col",
            self.me + 1 - 2 * side,
        )

    def has_last(self, side):
        came = self.me - 1 + 2 * side
        return (came >= 0) & (came < LINE)

    def step(self, s):
        far = jnp.where(self.me < LINE // 2, 1, 0)

        @pl.loop(0, 2)
        def _(i):
            side = lax.rem(i + far, 2)
            j = self.me + (1 - 2 * side) * s

            @pl.when((j >= 0) & (j < LINE))
            def _():
                mine = self.block_of(j)
                for p in range(SUB):
                    term = mine[p * PART : (p + 1) * PART]
                    rows = self.rows(side, j, p)

                    @pl.when(self.has_last(side))
                    def _():
                        landed(rows, self.recv.at[side, j, p])
                        rows[...] = (term + rows[...].astype(F32)).astype(BF16)

                    @pl.when(jnp.logical_not(self.has_last(side)))
                    def _():
                        rows[...] = term.astype(BF16)

                    self.copy(side, j, p).start()

    def finish(self, out_ref):
        me = self.me
        out_ref[...] = self.block_of(me)

        @pl.loop(0, 2)
        def _(side):
            @pl.when(self.has_last(side))
            def _():
                for p in range(SUB):
                    rows = self.rows(side, me, p)
                    landed(rows, self.recv.at[side, me, p])
                    out_ref[p * PART : (p + 1) * PART] += rows[...].astype(F32)

    def drain(self):
        for s in range(1, LINE):

            @pl.loop(0, 2)
            def _(side):
                j = self.me + (1 - 2 * side) * s

                @pl.when((j >= 0) & (j < LINE))
                def _():
                    for p in range(SUB):
                        self.copy(side, j, p).wait_send()


def gather_sems():
    return [DMA((2, LINE, SUB)), DMA((LINE, SUB))]


def scatter_sems():
    return [DMA((2, LINE, SUB)), DMA((2, LINE, SUB))]


def dot(a, b, dims=(((1,), (0,)), ((), ()))):
    return lax.dot_general(a, b, dims, preferred_element_type=F32)


def turn(values):
    return pltpu.roll(values, HEAD_SIZE // 2, 1)


def norm_scale(values):
    return lax.rsqrt(jnp.sum(values * values, -1, keepdims=True) / MODEL_WIDTH + EPS)


def shape(rows, cols, dtype=BF16):
    return jax.ShapeDtypeStruct((rows, cols), dtype)


def attend_local(query_ref, own_ref, other_ref, attended_ref, probs_ref, r):
    rows = 2 * BLOCK
    shape = (rows, rows)
    at_row = lax.broadcasted_iota(jnp.int32, shape, 0)
    at_col = lax.broadcasted_iota(jnp.int32, shape, 1)
    own_mask = at_row >= at_col
    other_mask = at_col // BLOCK < at_row // BLOCK + r
    heads = query_ref.shape[1] // HEAD_SIZE
    for s in range(2):
        part = slice(s * rows, (s + 1) * rows)
        for h in range(heads):
            cols = slice(h * HEAD_SIZE, (h + 1) * HEAD_SIZE)
            query = query_ref[part, cols]
            own = jnp.where(own_mask, dot(query, own_ref[part, :HEAD_SIZE], PAIR_COLS) * SCALE, NEG)
            other = jnp.where(
                other_mask, dot(query, other_ref[part, :HEAD_SIZE], PAIR_COLS) * SCALE, NEG
            )
            top = jnp.maximum(
                jnp.max(own, -1, keepdims=True), jnp.max(other, -1, keepdims=True)
            )
            total = jnp.sum(jnp.exp(own - top), -1, keepdims=True) + jnp.sum(
                jnp.exp(other - top), -1, keepdims=True
            )
            log_total = top + jnp.log(total)
            own = jnp.exp(own - log_total).astype(BF16)
            other = jnp.exp(other - log_total).astype(BF16)
            attended_ref[part, cols] = (
                dot(own, own_ref[part, HEAD_SIZE:]) + dot(other, other_ref[part, HEAD_SIZE:])
            ).astype(BF16)
            probs_ref[s * heads + h, :, :rows] = own
            probs_ref[s * heads + h, :, rows:] = other


def attend_back_body(
    query_ref, own_ref, other_ref, attended_ref, probs_ref, grad_ref, cos_ref, sin_ref,
    query_grad_ref, own_grad_ref, other_grad_ref,
):
    rows = 2 * BLOCK
    heads = query_ref.shape[1] // HEAD_SIZE
    for s in range(2):
        part = slice(s * rows, (s + 1) * rows)
        own_key, other_key = own_ref[part, :HEAD_SIZE], other_ref[part, :HEAD_SIZE]
        own_value, other_value = own_ref[part, HEAD_SIZE:], other_ref[part, HEAD_SIZE:]
        sums = [jnp.zeros((rows, HEAD_SIZE), F32) for _ in range(4)]
        for h in range(heads):
            cols = slice(h * HEAD_SIZE, (h + 1) * HEAD_SIZE)
            query, grad = query_ref[part, cols], grad_ref[part, cols]
            own_p = probs_ref[s * heads + h, :, :rows]
            other_p = probs_ref[s * heads + h, :, rows:]
            delta = jnp.sum(
                grad.astype(F32) * attended_ref[part, cols].astype(F32), -1, keepdims=True
            )
            own_s = (own_p.astype(F32) * (dot(grad, own_value, PAIR_COLS) - delta)).astype(BF16)
            other_s = (other_p.astype(F32) * (dot(grad, other_value, PAIR_COLS) - delta)).astype(BF16)
            query_grad = (dot(own_s, own_key) + dot(other_s, other_key)) * SCALE
            query_grad_ref[part, cols] = (
                query_grad * cos_ref[part] - turn(query_grad) * sin_ref[part]
            ).astype(BF16)
            for i, (weights, partner) in enumerate(
                ((own_s, query), (own_p, grad), (other_s, query), (other_p, grad))
            ):
                sums[i] = sums[i] + dot(weights, partner, PAIR_ROWS)
        own_grad_ref[part, :HEAD_SIZE] = sums[0] * SCALE
        own_grad_ref[part, HEAD_SIZE:] = sums[1]
        other_grad_ref[part, :HEAD_SIZE] = (sums[2] * SCALE).astype(BF16)
        other_grad_ref[part, HEAD_SIZE:] = sums[3].astype(BF16)


PIECES = 6


def front_body(
    input_ref, cot_in_ref, table_ref, small_ref, query_w_ref, kv_w_ref, output_w_ref,
    gate_hbm, upper_hbm, down_hbm,
    x_hbm, normed_hbm, query_hbm, kv_hbm, kv_other_hbm, cos_hbm, sin_hbm, gains_ref,
    attended_hbm, probs_hbm, mid_hbm, normed_two_hbm, turned_hbm, cot_hbm, proj_hbm, proj_other_hbm,
    weights_other_hbm,
    x_ref, normed_ref, query_ref, kv_ref, kv_other_ref, cos_ref, sin_ref,
    attended_ref, probs_ref, mid_ref, normed_two_ref, turned_ref, cot_ref, proj_ref, proj_other_ref,
    passing, tables, bias_ref, landing, store_sems,
    swap_sends, swap_recv, piece_sends, piece_recv, kv_sends, kv_recv,
    g_sends, g_recv, c_sends, c_recv, n_sends, n_recv, s_sends, s_recv,
):
    me, r, d = lax.axis_index("col"), lax.axis_index("row"), lax.axis_index("dp")
    y, core = d // 2, lax.rem(d, 2)
    x_to, y_to, core_to = 1 - r, 2 * (1 - y) + core, 2 * y + 1 - core
    query_cols = query_ref.shape[1]
    proj_cols = query_cols + 2 * HEAD_SIZE
    quarter = HALF // 2
    my_rows = aligned(core * quarter, quarter, quarter)
    its_rows = aligned((1 - core) * quarter, quarter, quarter)
    eighth = quarter // 2
    to_y = aligned(core * quarter + y * eighth, eighth, eighth)
    in_cols, out_cols = pl.ds(0, proj_cols), pl.ds(proj_cols, query_cols)
    kv_width = KEYVALUE_HEADS * HEAD_SIZE
    kv_at = me // (LINE // KEYVALUE_HEADS) * HEAD_SIZE

    stores = [
        pltpu.make_async_copy(src, dst, store_sems.at[i])
        for i, (src, dst) in enumerate(
            (
                (x_ref, x_hbm), (cos_ref, cos_hbm), (sin_ref, sin_hbm), (proj_ref, proj_hbm),
                (normed_ref, normed_hbm), (query_ref, query_hbm), (kv_ref, kv_hbm),
                (kv_other_ref, kv_other_hbm), (probs_ref, probs_hbm), (attended_ref, attended_hbm),
                (proj_other_ref, proj_other_hbm), (mid_ref, mid_hbm),
                (normed_two_ref, normed_two_hbm), (turned_ref, turned_hbm), (cot_ref, cot_hbm),
            )
        )
    ]

    passing[0] = input_ref[:, block_rows(1 - r)].T
    x_ref[:, :HALF] = input_ref[:, block_rows(r)].T
    proj_ref[:, :query_cols] = query_w_ref[...]
    for i in range(2):
        proj_ref[:, query_cols + i * HEAD_SIZE : query_cols + (i + 1) * HEAD_SIZE] = kv_w_ref[
            :, aligned(i * kv_width + kv_at, HEAD_SIZE)
        ]
    greet(me, [("row", x_to), ("dp", y_to), ("dp", core_to)])

    swaps = [
        (passing.at[0], x_ref.at[:, HALF:], "row", x_to),
        (small_ref.at[:, :HALF], gains_ref.at[pl.ds(0, 1), HALF:], "row", x_to),
        (small_ref.at[:, HALF : 2 * HALF], gains_ref.at[pl.ds(1, 1), HALF:], "row", x_to),
        (proj_ref.at[to_y, in_cols], proj_other_ref.at[to_y, in_cols], "row", x_to),
        (table_ref.at[block_rows(1 - r)], tables.at[pl.ds(0, BLOCK)], "row", x_to),
        (table_ref.at[block_rows(3 - r)], tables.at[pl.ds(BLOCK, BLOCK)], "row", x_to),
        (passing.at[1], cot_ref.at[block_rows(me), HALF:], "row", x_to),
        (proj_ref.at[to_y, out_cols], proj_other_ref.at[to_y, out_cols], "row", x_to),
        (proj_other_ref.at[to_y, in_cols], proj_other_ref.at[to_y, in_cols], "dp", y_to),
        (proj_other_ref.at[to_y, out_cols], proj_other_ref.at[to_y, out_cols], "dp", y_to),
        (proj_other_ref.at[my_rows, in_cols], proj_other_ref.at[my_rows, in_cols], "dp", core_to),
        (proj_other_ref.at[my_rows, out_cols], proj_other_ref.at[my_rows, out_cols], "dp", core_to),
    ]

    def swap_copy(i):
        src, dst, axis, to = swaps[i]
        return send(src, dst, swap_sends.at[i], swap_recv.at[i], axis, to)

    def swap_landed(i):
        swap_copy(i).wait_recv()

    rows = gate_hbm.shape[0] // 4
    owns = (gate_hbm, upper_hbm, down_hbm)

    def piece(i, of_y):
        return aligned((of_y * 2 + i % 2) * rows, rows, rows)

    def piece_copy(i, way):
        m = i // 2
        of_y = 1 - y if way == 3 else y
        at = weights_other_hbm.at[m, piece(i, of_y), my_rows]
        src = owns[m].at[piece(i, of_y), my_rows] if way == 0 else at
        axis, to = (("row", x_to), ("dp", y_to), ("dp", core_to), ("dp", core_to))[way]
        return send(src, at, piece_sends.at[way, i], piece_recv.at[way, i], axis, to)

    def relay_x(i):
        piece_copy(i, 0).wait_recv()
        piece_copy(i, 1).start()
        piece_copy(i, 2).start()

    def relay_y(i):
        piece_copy(i, 1).wait_recv()
        piece_copy(i, 3).start()

    for i in range(6):
        swap_copy(i).start()
    passing[1] = cot_in_ref[:, block_rows(1 - r)].T
    proj_ref[:, proj_cols:] = output_w_ref[...]
    swap_copy(6).start()
    swap_copy(7).start()
    piece_copy(0, 0).start()
    cot_ref[block_rows(me), :HALF] = cot_in_ref[:, block_rows(r)].T
    gains_ref[0:1, :HALF] = small_ref[:, :HALF]
    gains_ref[1:2, :HALF] = small_ref[:, HALF : 2 * HALF]
    bias_ref[:, :query_cols] = small_ref[:, 2 * HALF : 2 * HALF + query_cols]
    for i in range(2):
        bias_ref[:, query_cols + i * HEAD_SIZE : query_cols + (i + 1) * HEAD_SIZE] = small_ref[
            :, aligned(2 * HALF + query_cols + i * kv_width + kv_at, HEAD_SIZE)
        ]
    swap_landed(0)
    swap_landed(1)
    swap_landed(2)
    x = x_ref[...].astype(F32)
    normed_ref[block_rows(me)] = (x * norm_scale(x) * gains_ref[0:1]).astype(BF16)
    gather = Gather(me, normed_ref, g_sends, g_recv)
    gather.step(0)

    lane = lax.broadcasted_iota(jnp.int32, (BLOCK, HEAD_SIZE), 1)
    first = lane < HEAD_SIZE // 2
    swap_landed(3)
    swap_copy(8).start()
    gather.step(1)
    swap_landed(8)
    swap_copy(10).start()
    swap_landed(4)
    swap_landed(5)
    for i in range(4):
        if i < 2:
            table = table_ref[block_rows(r + 2 * i)]
        else:
            table = tables[(i - 2) * BLOCK : (i - 1) * BLOCK]
        turned = turn(table)
        at = block_rows((r if i < 2 else 1 - r) * 2 + i % 2)
        cos_ref[at] = jnp.where(first, table, turned)
        sin_ref[at] = jnp.where(first, -turned, table)
    swap_landed(10)

    def kv_copy(j):
        at = block_rows(j)
        return send(
            kv_ref.at[at], kv_other_ref.at[at], kv_sends.at[j], kv_recv.at[j], "row", x_to
        )

    def each(j):
        at = block_rows(j)
        block = normed_ref[at]
        out = dot(block[:, :HALF], proj_ref[:, :proj_cols])
        out = out + dot(block[:, HALF:], proj_other_ref[:, :proj_cols]) + bias_ref[...]
        cosine, sine = cos_ref[at], sin_ref[at]
        for h in range(query_cols // HEAD_SIZE + 1):
            head = out[:, h * HEAD_SIZE : (h + 1) * HEAD_SIZE]
            turned = (head * cosine + turn(head) * sine).astype(BF16)
            if h * HEAD_SIZE < query_cols:
                query_ref[at, h * HEAD_SIZE : (h + 1) * HEAD_SIZE] = turned
            else:
                kv_ref[at, :HEAD_SIZE] = turned
        kv_ref[at, HEAD_SIZE:] = out[:, query_cols + HEAD_SIZE :].astype(BF16)
        kv_copy(j).start()

    gather.run_each(0, each)
    gather.run_each(1, each)
    gather.step(2)
    gather.run_each(2, each)
    swap_landed(7)
    swap_copy(9).start()
    gather.step(3)
    gather.run_each(3, each)
    for i in range(1, PIECES):
        piece_copy(i, 0).start()
    swap_landed(6)
    cot_gather = Gather(me, cot_ref, c_sends, c_recv)
    cot_gather.step(0)
    swap_landed(9)
    swap_copy(11).start()
    relay_x(0)
    for j in range(LINE):
        kv_copy(j).wait_recv()
    attend_local(query_ref, kv_ref, kv_other_ref, attended_ref, probs_ref, r)
    swap_landed(11)

    def block_of(j):
        block = attended_ref[block_rows(j)]
        return jnp.concatenate(
            [
                dot(block, proj_ref[:, proj_cols:], PAIR_COLS),
                dot(block, proj_other_ref[:, proj_cols:], PAIR_COLS),
            ],
            1,
        )

    scatter = Scatter(me, block_of, landing, s_sends, s_recv)
    scatter.step(3)
    for store in stores[:11]:
        store.start()
    relay_x(1)
    scatter.step(2)
    relay_x(2)
    scatter.step(1)
    relay_y(0)
    relay_x(3)
    scatter.finish(mid_ref)
    mid = mid_ref[...] + x_ref[...].astype(F32)
    mid_ref[...] = mid
    normed_two_ref[block_rows(me)] = (mid * norm_scale(mid) * gains_ref[1:2]).astype(BF16)

    def turn_block(j):
        turned_ref[:, block_rows(j)] = normed_two_ref[block_rows(j)].T

    second = Gather(me, normed_two_ref, n_sends, n_recv)
    second.step(0)
    stores[11].start()
    second.run_each(0, turn_block)
    relay_y(1)
    relay_x(4)
    second.step(1)
    second.run_each(1, turn_block)
    relay_y(2)
    relay_x(5)
    second.step(2)
    second.run_each(2, turn_block)
    relay_y(3)
    second.step(3)
    second.run_each(3, turn_block)
    relay_y(4)
    stores[12].start()
    stores[13].start()
    cot_gather.step(1, forward=False)
    stores[14].start()
    relay_y(5)
    for i in range(PIECES):
        for way in (2, 3):
            of_y = y if way == 2 else 1 - y
            landed(weights_other_hbm.at[i // 2, piece(i, of_y), its_rows], piece_recv.at[way, i])
        for way in range(4):
            piece_copy(i, way).wait_send()
    for i in range(len(swaps)):
        swap_copy(i).wait_send()
    for j in range(LINE):
        kv_copy(j).wait_send()
    for store in stores:
        store.wait()
    gather.drain()
    cot_gather.drain(0, 1)
    second.drain()
    scatter.drain()


def front_call(proj_cols, query_cols, hidden, *args):
    heads = query_cols // HEAD_SIZE
    gains = shape(2, MODEL_WIDTH, F32)
    outs = [
        shape(BLOCK, MODEL_WIDTH),
        shape(LOCAL, MODEL_WIDTH),
        shape(LOCAL, query_cols),
        shape(LOCAL, 2 * HEAD_SIZE),
        shape(LOCAL, 2 * HEAD_SIZE),
        shape(LOCAL, HEAD_SIZE, F32),
        shape(LOCAL, HEAD_SIZE, F32),
        gains,
        shape(LOCAL, query_cols),
        jax.ShapeDtypeStruct((2 * heads, 2 * BLOCK, 4 * BLOCK), BF16),
        shape(BLOCK, MODEL_WIDTH, F32),
        shape(LOCAL, MODEL_WIDTH),
        shape(MODEL_WIDTH, LOCAL),
        shape(LOCAL, MODEL_WIDTH),
        shape(HALF, proj_cols + query_cols),
        shape(HALF, proj_cols + query_cols),
        jax.ShapeDtypeStruct((3, hidden, HALF), BF16),
    ]
    return pl.pallas_call(
        front_body,
        out_shape=outs,
        in_specs=[VMEM_SPEC] * 7 + [ANY_SPEC] * 3,
        out_specs=[VMEM_SPEC if out is gains else ANY_SPEC for out in outs],
        scratch_shapes=[pltpu.VMEM(out.shape, out.dtype) for out in outs[:-1] if out is not gains]
        + [
            pltpu.VMEM((2, BLOCK, HALF), BF16),
            pltpu.VMEM((2 * BLOCK, HEAD_SIZE), F32),
            pltpu.VMEM((1, proj_cols), F32),
            pltpu.VMEM((2, LINE, BLOCK, MODEL_WIDTH), BF16),
            DMA((15,)),
            DMA((12,)),
            DMA((12,)),
            DMA((4, PIECES)),
            DMA((4, PIECES)),
            DMA((LINE,)),
            DMA((LINE,)),
        ]
        + gather_sems() * 3
        + scatter_sems(),
        compiler_params=pltpu.CompilerParams(
            collective_id=1, has_side_effects=True, vmem_limit_bytes=67_043_328
        ),
        cost_estimate=pl.CostEstimate(
            flops=4 * 10**9, bytes_accessed=40_000_000, transcendentals=0
        ),
        name="front",
    )(*args)


DOWN, GATE, UPPER, CHAIN = 0, 1, 2, 3
UNITS = ((1, 1), (1, 0), (0, 1), (0, 0))
TILE = 256


def add_into(total_ref, term_ref, cols):
    @pl.loop(0, total_ref.shape[0] // 32)
    def _(i):
        at = aligned(i * 32, 32, 32)
        total_ref[at, cols] = (
            total_ref[at, cols].astype(F32) + term_ref[at, cols].astype(F32)
        ).astype(BF16)


def rear_body(
    mid_ref, gains_ref,
    normed_two_hbm, turned_hbm, cot_hbm, gate_hbm, upper_hbm, down_hbm, other_hbm, proj_hbm, proj_other_hbm, query_hbm, kv_hbm,
    kv_other_hbm, attended_hbm, probs_hbm, cos_hbm, sin_hbm, x_hbm, normed_one_hbm,
    out_ref, in_ref, small_ref, query_w_ref, output_w_ref, kv_all_ref, kept_hbm, land2_hbm, land3_hbm,
    cot_ref, activated_ref, gate_grad_ref, upper_grad_ref, out_part_ref, back_part_ref, turned_ref,
    kv_got_ref, got_ref, out_landing, landing, sums, gives, gots,
    chain_gots, chain_land2, chain_land3, kv_line, small_line, small_swap, small_give,
    small_group,
    load_sems, w_sems, c_sends, c_recv, o_sends, o_recv, r_sends, r_recv, a_sends, a_recv,
    give_sends, give_recv, two_sends, two_recv, three_sends, three_recv, stage_sem, kept_sems,
    swap_sends, swap_recv, kv_sends, kv_recv, kvd_sends, kvd_recv, line_sends, line_recv,
    small_sends, small_recv, credit,
):
    me, r, d = lax.axis_index("col"), lax.axis_index("row"), lax.axis_index("dp")
    y, core = d // 2, lax.rem(d, 2)
    x_to, y_to, core_to = 1 - r, 2 * (1 - y) + core, 2 * y + 1 - core
    diagonal_to = 2 * (1 - y) + 1 - core
    hidden = activated_ref.shape[1]
    query_cols = query_w_ref.shape[1]
    proj_cols = query_cols + 2 * HEAD_SIZE
    chain_cols = proj_cols + query_cols
    owns = (gate_hbm, upper_hbm, down_hbm)

    def cot_loads(act):
        for i in range(3):
            j = me - 1 + i

            @pl.when((j >= 0) & (j < LINE))
            def _():
                rows = block_rows(j)
                act(pltpu.make_async_copy(cot_hbm.at[rows], cot_ref.at[rows], load_sems.at[i]))

    turned_load = pltpu.make_async_copy(turned_hbm, turned_ref.at[1], load_sems.at[14])
    turned_load.start()
    cot_loads(lambda copy: copy.start())

    halves = {m: (hidden // 2 // BLOCK + 2) * BLOCK for m in (DOWN, GATE, UPPER)}
    halves[CHAIN] = chain_cols // 2

    def columns(m, axis):
        width = chain_cols if m == CHAIN else hidden
        return pl.ds(0, halves[m]) if axis == "row" else pl.ds(halves[m], width - halves[m])

    def unit_rows(h, rel):
        of_y = 1 - y if rel else y
        return aligned(h * HALF + of_y * 2 * UNIT, 2 * UNIT)

    def split(res, keep_ref, give_ref, at):
        low, high = res[:UNIT], res[UNIT:]
        keep_ref[:, at] = jnp.where(core == 0, low, high).astype(BF16)
        give_ref[:, at] = jnp.where(core == 0, high, low).astype(BF16)

    order = [
        (DOWN, 0), (DOWN, 1), (DOWN, 2), (UPPER, 0), (UPPER, 1), (UPPER, 2), (DOWN, 3),
        (GATE, 0), (GATE, 1), (GATE, 2), (UPPER, 3), (GATE, 3),
    ]
    columns_of = {DOWN: activated_ref, GATE: gate_grad_ref, UPPER: upper_grad_ref}
    ring = 3

    def total_of(m, h, rel):
        return sums.at[m * 4 + h * 2 + rel]

    def give_copy(u):
        return send(
            gives.at[u % 2], gots.at[u % ring], give_sends.at[u], give_recv.at[u], "dp", core_to
        )

    def compute(u):
        m, i = order[u]
        h, rel = UNITS[i]
        if u >= 2:
            give_copy(u - 2).wait_send()
        left = 0 if m == DOWN else 1
        rows = unit_rows(h, rel)
        tile = 512

        def run(at):
            res = dot(turned_ref[left, rows], columns_of[m][:, at])
            split(res, total_of(m, h, rel), gives.at[u % 2], at)

        @pl.loop(0, hidden // tile)
        def _(i):
            run(aligned(i * tile, tile))

        if hidden % tile:
            run(pl.ds(hidden // tile * tile, hidden % tile))
        if u >= ring:
            pl.semaphore_wait(credit, 1)
        give_copy(u).start()

    def two_copy(m, k, chain_sums=None):
        h, rel = ((1, 0), (1, 1), (0, 1), (1, 1))[k]
        axis, to = (("row", x_to), ("dp", y_to))[k // 2]
        at = columns(m, axis)
        if m == CHAIN:
            src, dst = chain_sums.at[h * 2 + rel, :, at], chain_land2.at[k % 2, :, at]
        else:
            src, dst = total_of(m, h, rel).at[:, at], land2_hbm.at[m * 2 + k % 2, :, at]
        return send(src, dst, two_sends.at[m, k], two_recv.at[m, k], axis, to)

    def combine(u):
        m, i = order[u]
        h, rel = UNITS[i]
        give_copy(u).wait_recv()
        add_into(total_of(m, h, rel), gots.at[u % ring], pl.ds(0, hidden))
        if u < len(order) - ring:
            pl.semaphore_signal(credit, 1, device_id={"dp": core_to}, device_id_type=MESH_ID)
        for k in {(1, 1): (1, 3), (1, 0): (0,), (0, 1): (2,), (0, 0): ()}[h, rel]:
            two_copy(m, k).start()

    def three_copy(m, k, chain_sums=None):
        h, rel = ((0, 1), (1, 0))[k]
        axis, to = (("dp", y_to), ("row", x_to))[k]
        at = columns(m, ("row", "dp")[k])
        if m == CHAIN:
            src, dst = chain_sums.at[h * 2 + rel, :, at], chain_land3.at[:, at]
        else:
            src, dst = total_of(m, h, rel).at[:, at], land3_hbm.at[m, :, at]
        return send(src, dst, three_sends.at[m, k], three_recv.at[m, k], axis, to)

    def kept_copy(m):
        return pltpu.make_async_copy(total_of(m, 0, 0), kept_hbm.at[m], kept_sems.at[m])

    def stage(m, i):
        return pltpu.make_async_copy(land2_hbm.at[m * 2 + i], gots.at[i], stage_sem.at[m, i])

    def second_stage(m, now=(0, 1)):
        for k in range(4):
            two_copy(m, k).wait_recv()
        for i in (1, 0):
            stage(m, i).start()
        stage(m, 1).wait()
        add_into(total_of(m, 0, 1), gots.at[1], columns(m, "row"))
        if 0 in now:
            three_copy(m, 0).start()
        add_into(total_of(m, 1, 0), gots.at[1], columns(m, "dp"))
        if 1 in now:
            three_copy(m, 1).start()
        stage(m, 0).wait()
        add_into(total_of(m, 0, 0), gots.at[0], pl.ds(0, hidden))
        kept_copy(m).start()

    barrier = pltpu.get_barrier_semaphore()
    group_size = 8
    own = r * 4 + d

    def member(i):
        index = lax.rem(own + i, group_size)
        return {"row": index // 4, "dp": lax.rem(index, 4)}

    for i in range(1, group_size):
        pl.semaphore_signal(barrier, 1, device_id=member(i), device_id_type=MESH_ID)
    for s in range(1, LINE):
        pl.semaphore_signal(
            barrier, 1, device_id={"col": lax.rem(me + s, LINE)}, device_id_type=MESH_ID
        )

    cot_gather = Gather(me, cot_ref, c_sends, c_recv)
    out_scatter = Scatter(
        me, lambda j: out_part_ref[block_rows(j)].astype(F32), out_landing, o_sends, o_recv
    )

    def feed(weights, gates, total, normed_two_ref):
        tiles = hidden // TILE
        rest = hidden % TILE

        def loads(t, slot, size):
            rows = aligned(t * TILE, size, TILE)
            for m in range(3):
                for i, src in enumerate((owns[m].at[rows], other_hbm.at[m, rows])):
                    yield pltpu.make_async_copy(
                        src,
                        weights.at[slot, m, pl.ds(0, size), pl.ds(i * HALF, HALF)],
                        w_sems.at[slot, m, i],
                    )

        def start(t, slot, size):
            for copy in loads(t, slot, size):
                copy.start()

        def ready(t, slot, size):
            for copy in loads(t, slot, size):
                copy.wait()

        def sweep(body, first_slot, hooks, again):
            @pl.loop(0, tiles)
            def _(t):
                slot = lax.rem(t + first_slot, 2)
                ready(t, slot, TILE)

                @pl.when(t < tiles - 1)
                def _():
                    start(t + 1, 1 - slot, TILE)

                @pl.when(t == tiles - 1)
                def _():
                    start(tiles, 1 - slot, rest)

                body(aligned(t * TILE, TILE), slot, TILE)
                for at, hook in hooks:
                    pl.when(t == at)(hook)

            slot = (tiles + first_slot) % 2
            ready(tiles, slot, rest)
            if again:
                start(0, 1 - slot, TILE)
            body(pl.ds(tiles * TILE, rest), slot, rest)

        def add_products(slot, size, factors, cols):
            width = 512

            @pl.loop(0, MODEL_WIDTH // width)
            def _(i):
                at = aligned(i * width, width)
                term = sum(
                    dot(factor[:, cols], weights[slot, m, pl.ds(0, size), at])
                    for factor, m in factors
                )
                total[:, at] += term

        def forward(cols, slot, size):
            here = pl.ds(0, size)
            gate = dot(normed_two_ref[...], weights[slot, 0, here], PAIR_COLS)
            upper = dot(normed_two_ref[...], weights[slot, 1, here], PAIR_COLS)
            activated = (gate * jax.nn.sigmoid(gate) * upper).astype(BF16)
            gates[0, :, cols] = gate.astype(BF16)
            gates[1, :, cols] = upper.astype(BF16)
            activated_ref[:, cols] = activated
            total[...] += dot(activated, weights[slot, 2, here])

        def backward(cols, slot, size):
            here = pl.ds(0, size)
            act_grad = dot(cot_ref[...], weights[slot, 2, here], PAIR_COLS)
            gate, upper = gates[0, :, cols].astype(F32), gates[1, :, cols].astype(F32)
            sig = jax.nn.sigmoid(gate)
            gate_grad = (act_grad * upper * sig * (1.0 + gate * (1.0 - sig))).astype(BF16)
            upper_grad = (act_grad * gate * sig).astype(BF16)
            gate_grad_ref[:, cols] = gate_grad
            upper_grad_ref[:, cols] = upper_grad
            add_products(slot, size, ((gate_grad_ref, 0), (upper_grad_ref, 1)), cols)

        load = pltpu.make_async_copy(normed_two_hbm, normed_two_ref, load_sems.at[15])
        load.start()
        start(0, 0, TILE)
        total[...] = jnp.zeros_like(total)
        pl.semaphore_wait(barrier, group_size - 1 + LINE - 1)
        cot_loads(lambda copy: copy.wait())
        cot_gather.step(1, wait=False)
        load.wait()
        turned_load.wait()
        sweep(forward, 0, [(4, lambda: cot_gather.step(2))], True)
        out_part_ref[...] = total[...].astype(BF16)
        out_scatter.step(3)
        cot_gather.step(3)
        turned_ref[0] = cot_ref[...].T
        total[...] = jnp.zeros_like(total)
        compute(0)
        compute(1)
        hooks = [
            (0, lambda: combine(0)), (1, lambda: combine(1)), (4, lambda: out_scatter.step(2)),
        ]
        sweep(backward, (tiles + 1) % 2, hooks, False)
        back_part_ref[...] = total[...].astype(BF16)
        cot_gather.drain(1, LINE - 1)

    pl.run_scoped(
        feed,
        pltpu.VMEM((2, 3, TILE, MODEL_WIDTH), BF16),
        pltpu.VMEM((2, LOCAL, hidden), BF16),
        pltpu.VMEM((LOCAL, MODEL_WIDTH), F32),
        pltpu.VMEM((LOCAL, MODEL_WIDTH), BF16),
    )

    def rest(
        proj_ref, proj_other_ref, query_ref, kv_ref, kv_other_ref, attended_ref, probs_ref, cos_ref,
        sin_ref, x_ref, normed_one_ref, mid_grad_ref, own_ref, att_grad_ref,
        kv_grad_ref, kv_give_ref, proj_grad_ref, chain_sums, back_give,
    ):
        pairs = (
            (proj_hbm, proj_ref), (proj_other_hbm, proj_other_ref), (query_hbm, query_ref),
            (kv_hbm, kv_ref), (kv_other_hbm, kv_other_ref), (attended_hbm, attended_ref),
            (probs_hbm, probs_ref), (cos_hbm, cos_ref), (sin_hbm, sin_ref), (x_hbm, x_ref),
            (normed_one_hbm, normed_one_ref),
        )
        reads = [
            pltpu.make_async_copy(src, dst, load_sems.at[3 + i])
            for i, (src, dst) in enumerate(pairs)
        ]

        mid_half_ref = cot_ref

        scatter = Scatter(
            me, lambda j: back_part_ref[block_rows(j)].astype(F32), landing, r_sends, r_recv
        )
        scatter.step(3)
        for read in reads:
            read.start()
        compute(2)
        for u in (3, 4, 5):
            compute(u)
            combine(u - 1)
        scatter.step(2)
        for u in (6, 7):
            compute(u)
            combine(u - 1)
        scatter.step(1)
        for u in (8, 9):
            compute(u)
            combine(u - 1)
        scatter.finish(mid_grad_ref)
        mid, grad = mid_ref[...], mid_grad_ref[...]
        rinv = norm_scale(mid)
        small_line[me, :, MODEL_WIDTH : 2 * MODEL_WIDTH] = jnp.sum(grad * mid * rinv, 0, keepdims=True)
        scaled = grad * gains_ref[1:2]
        inner = jnp.sum(scaled * mid, -1, keepdims=True)
        mid_grad = (
            cot_ref[block_rows(me)].astype(F32)
            + rinv * scaled
            - mid * rinv**3 * inner / MODEL_WIDTH
        )
        mid_grad_ref[...] = mid_grad
        mid_half_ref[block_rows(me)] = mid_grad.astype(BF16)

        gather = Gather(me, mid_half_ref, a_sends, a_recv)
        gather.step(0)
        scatter.drain()
        for read in reads:
            read.wait()

        def each(j):
            block = mid_half_ref[block_rows(j)]
            att_grad_ref[block_rows(j)] = (
                dot(block[:, :HALF], proj_ref[:, proj_cols:])
                + dot(block[:, HALF:], proj_other_ref[:, proj_cols:])
            ).astype(BF16)

        gather.run_each(0, each)
        for u in (10, 11):
            compute(u)
            combine(u - 1)
        combine(11)
        gather.step(1)
        gather.run_each(1, each)
        second_stage(DOWN)
        gather.step(2)
        gather.run_each(2, each)
        second_stage(UPPER, (0,))
        gather.step(3)
        gather.run_each(3, each)
        out_scatter.step(1)
        attend_back_body(
            query_ref, kv_ref, kv_other_ref, attended_ref, probs_ref, att_grad_ref, cos_ref,
            sin_ref, proj_grad_ref, kv_grad_ref, kv_give_ref,
        )

        def swap_copy(i):
            src, dst = (
                (kv_give_ref, kv_got_ref),
                (back_give.at[0], got_ref.at[0]),
                (back_give.at[1], got_ref.at[1]),
            )[i]
            return send(src, dst, swap_sends.at[i], swap_recv.at[i], "row", x_to)

        swap_copy(0).start()
        swap_copy(0).wait_recv()
        kv = kv_grad_ref[...] + kv_got_ref[...].astype(F32)
        key = kv[:, :HEAD_SIZE]
        proj_grad_ref[:, query_cols : query_cols + HEAD_SIZE] = (
            key * cos_ref[...] - turn(key) * sin_ref[...]
        ).astype(BF16)
        proj_grad_ref[:, query_cols + HEAD_SIZE :] = kv[:, HEAD_SIZE:].astype(BF16)

        def block_of(j):
            block = proj_grad_ref[block_rows(j)]
            return jnp.concatenate(
                [
                    dot(block, proj_ref[:, :proj_cols], PAIR_COLS),
                    dot(block, proj_other_ref[:, :proj_cols], PAIR_COLS),
                ],
                1,
            )

        def chain_from(i):
            return gives.at[i // 2, :, pl.ds(i % 2 * chain_cols, chain_cols)]

        def chain_give(i):
            return send(
                chain_from(i), chain_gots.at[i], give_sends.at[12 + i], give_recv.at[12 + i],
                "dp", core_to,
            )

        def chain_compute(i):
            h, rel = UNITS[i]
            rows = unit_rows(h, rel)
            keep = chain_sums.at[h * 2 + rel]
            res = dot(normed_one_ref[:, rows], proj_grad_ref[...], PAIR_ROWS)
            split(res, keep, chain_from(i), pl.ds(0, proj_cols))
            res = dot(mid_half_ref[:, rows], attended_ref[...], PAIR_ROWS)
            split(res, keep, chain_from(i), pl.ds(proj_cols, query_cols))
            chain_give(i).start()

        def chain_combine(i):
            h, rel = UNITS[i]
            chain_give(i).wait_recv()
            add_into(chain_sums.at[h * 2 + rel], chain_gots.at[i], pl.ds(0, chain_cols))
            for k in {(1, 1): (1, 3), (1, 0): (0,), (0, 1): (2,), (0, 0): ()}[h, rel]:
                two_copy(CHAIN, k, chain_sums).start()

        second = Scatter(me, block_of, landing, r_sends, r_recv)
        second.step(3)
        for u in (len(order) - 2, len(order) - 1):
            give_copy(u).wait_send()
        for i in range(4):
            chain_compute(i)
        for i in range(4):
            chain_combine(i)
        three_copy(UPPER, 1).start()
        small_line[me, :, 2 * MODEL_WIDTH :] = jnp.sum(
            proj_grad_ref[...].astype(F32), 0, keepdims=True
        )
        second.step(2)
        second_stage(GATE, (0,))
        out_scatter.finish(own_ref)
        out = own_ref[...] + mid_ref[...]
        out_ref[:, block_rows(r)] = out[:, :HALF].T
        back_give[1] = out[:, HALF:].astype(BF16)
        second.step(1)
        for k in range(4):
            two_copy(CHAIN, k, chain_sums).wait_recv()
        add_into(chain_sums.at[1], chain_land2.at[1], columns(CHAIN, "row"))
        three_copy(CHAIN, 0, chain_sums).start()
        add_into(chain_sums.at[2], chain_land2.at[1], columns(CHAIN, "dp"))
        three_copy(CHAIN, 1, chain_sums).start()
        add_into(chain_sums.at[0], chain_land2.at[0], pl.ds(0, chain_cols))
        three_copy(GATE, 1).start()
        swap_copy(2).start()
        for k in range(2):
            three_copy(CHAIN, k, chain_sums).wait_recv()
        total = chain_sums[0].astype(F32) + chain_land3[...].astype(F32)
        query_w_ref[...] = total[:, :query_cols]
        output_w_ref[...] = total[:, proj_cols:]
        kv_line[me] = total[:, query_cols:proj_cols].astype(BF16)

        def kv_line_copy(s):
            to = lax.rem(me + s, LINE)
            return send(kv_line.at[me], kv_line.at[me], kv_sends.at[s], kv_recv.at[me], "col", to)

        for s in range(1, LINE):
            kv_line_copy(s).start()
        second.finish(own_ref)
        x, grad = x_ref[...].astype(F32), own_ref[...]
        rinv = norm_scale(x)
        scaled = grad * gains_ref[0:1]
        inner = jnp.sum(scaled * x, -1, keepdims=True)
        input_grad = mid_grad_ref[...] + rinv * scaled - x * rinv**3 * inner / MODEL_WIDTH
        back_give[0] = input_grad[:, HALF:].astype(BF16)
        swap_copy(1).start()
        small_line[me, :, :MODEL_WIDTH] = jnp.sum(grad * x * rinv, 0, keepdims=True)

        def small_line_copy(s):
            to = lax.rem(me + s, LINE)
            return send(
                small_line.at[me], small_line.at[me], line_sends.at[s], line_recv.at[me], "col", to
            )

        for s in range(1, LINE):
            small_line_copy(s).start()
        in_ref[:, block_rows(r)] = input_grad[:, :HALF].T

        group = LINE // KEYVALUE_HEADS
        for s in range(1, LINE):
            landed(kv_line.at[me], kv_recv.at[lax.rem(me + s, LINE)])
        dp_rows = aligned(d * UNIT, UNIT, UNIT)
        for h in range(KEYVALUE_HEADS):
            pair = kv_line[h * group].astype(F32)
            for i in range(1, group):
                pair = pair + kv_line[h * group + i].astype(F32)
            for i in range(2):
                at = (i * KEYVALUE_HEADS + h) * HEAD_SIZE
                kv_all_ref[dp_rows, at : at + HEAD_SIZE] = pair[
                    :, i * HEAD_SIZE : (i + 1) * HEAD_SIZE
                ].astype(BF16)

        def kv_rows(of):
            return kv_all_ref.at[aligned(of * UNIT, UNIT, UNIT)]

        def kv_dp_copy(i):
            rows = kv_rows(y_to if i == 2 else d)
            to = y_to if i == 1 else core_to
            return send(rows, rows, kvd_sends.at[i], kvd_recv.at[i], "dp", to)

        kv_dp_copy(1).start()
        kv_dp_copy(0).start()

        for s in range(1, LINE):
            landed(small_line.at[me], line_recv.at[lax.rem(me + s, LINE)])
        lines = [small_line[j] for j in range(LINE)]
        total_line = lines[0] + lines[1] + lines[2] + lines[3]
        small_swap[...] = jnp.zeros_like(small_swap)
        small_swap[0:1] = total_line[:, :MODEL_WIDTH]
        small_swap[1:2] = total_line[:, MODEL_WIDTH : 2 * MODEL_WIDTH]
        bias_at = 2 * MODEL_WIDTH
        small_swap[2:3, :query_cols] = small_line[me, :, bias_at : bias_at + query_cols]
        for i in range(2):
            for h in range(KEYVALUE_HEADS):
                at = bias_at + query_cols + i * HEAD_SIZE
                part = lines[h * group][:, at : at + HEAD_SIZE]
                for j in range(1, group):
                    part = part + lines[h * group + j][:, at : at + HEAD_SIZE]
                at = (i * KEYVALUE_HEADS + h) * HEAD_SIZE
                small_swap[3:4, at : at + HEAD_SIZE] = part

        small_give[0] = small_swap[:, :HALF]
        small_give[1, :2] = small_swap[:2, HALF:]
        small_give[1, 2:] = small_swap[2:, :HALF]
        small_group[own] = small_give[0]

        def small_copy(i):
            to = member(i)
            kind = jnp.where(to["row"] == r, 0, 1)
            return pltpu.make_async_remote_copy(
                small_give.at[kind], small_group.at[own], small_sends.at[i], small_recv.at[own],
                device_id=to, device_id_type=MESH_ID,
            )

        for i in range(1, group_size):
            small_copy(i).start()
        landed(kv_rows(y_to), kvd_recv.at[1])
        kv_dp_copy(2).start()
        for i in (2, 1):
            swap_copy(i).wait_recv()
            to_ref = (in_ref, out_ref)[i - 1]
            to_ref[:, block_rows(1 - r)] = got_ref[i - 1].astype(F32).T
        for i in range(1, group_size):
            source = lax.rem(own + i, group_size)
            landed(small_group.at[source], small_recv.at[source])
        small_ref[...] = sum(small_group[i] for i in range(group_size))

        landed(kv_rows(core_to), kvd_recv.at[0])
        landed(kv_rows(diagonal_to), kvd_recv.at[2])
        for m in (DOWN, GATE, UPPER):
            for k in range(2):
                three_copy(m, k).wait_recv()
                three_copy(m, k).wait_send()
            kept_copy(m).wait()
            for k in range(4):
                two_copy(m, k).wait_send()
        for i in range(4):
            chain_give(i).wait_send()
            two_copy(CHAIN, i, chain_sums).wait_send()
        for k in range(2):
            three_copy(CHAIN, k, chain_sums).wait_send()
        for i in range(3):
            swap_copy(i).wait_send()
            kv_dp_copy(i).wait_send()
            kv_line_copy(1 + i).wait_send()
            small_line_copy(1 + i).wait_send()
        for i in range(1, group_size):
            small_copy(i).wait_send()
        gather.drain()
        out_scatter.drain()
        second.drain()

    wide = (HALF, chain_cols)
    pl.run_scoped(
        rest,
        pltpu.VMEM(wide, BF16),
        pltpu.VMEM(wide, BF16),
        pltpu.VMEM((LOCAL, query_cols), BF16),
        pltpu.VMEM((LOCAL, 2 * HEAD_SIZE), BF16),
        pltpu.VMEM((LOCAL, 2 * HEAD_SIZE), BF16),
        pltpu.VMEM((LOCAL, query_cols), BF16),
        pltpu.VMEM(probs_hbm.shape, BF16),
        pltpu.VMEM((LOCAL, HEAD_SIZE), F32),
        pltpu.VMEM((LOCAL, HEAD_SIZE), F32),
        pltpu.VMEM((BLOCK, MODEL_WIDTH), BF16),
        pltpu.VMEM((LOCAL, MODEL_WIDTH), BF16),
        pltpu.VMEM((BLOCK, MODEL_WIDTH), F32),
        pltpu.VMEM((BLOCK, MODEL_WIDTH), F32),
        pltpu.VMEM((LOCAL, query_cols), BF16),
        pltpu.VMEM((LOCAL, 2 * HEAD_SIZE), F32),
        pltpu.VMEM((LOCAL, 2 * HEAD_SIZE), BF16),
        pltpu.VMEM((LOCAL, proj_cols), BF16),
        pltpu.VMEM((4, UNIT, chain_cols), BF16),
        pltpu.VMEM((2, BLOCK, HALF), BF16),
    )


def rear_call(hidden, proj_cols, query_cols, *args):
    chain_cols = proj_cols + query_cols
    outs = [
        shape(HALF, 2 * BLOCK, F32),
        shape(HALF, 2 * BLOCK, F32),
        shape(8, HALF, F32),
        shape(UNIT, query_cols, F32),
        shape(UNIT, query_cols, F32),
        shape(4 * UNIT, 2 * KEYVALUE_HEADS * HEAD_SIZE),
        jax.ShapeDtypeStruct((3, UNIT, hidden), BF16),
        jax.ShapeDtypeStruct((6, UNIT, hidden), BF16),
        jax.ShapeDtypeStruct((3, UNIT, hidden), BF16),
    ]
    local = (LOCAL, MODEL_WIDTH)
    line = (2, LINE, BLOCK, MODEL_WIDTH)
    return pl.pallas_call(
        rear_body,
        out_shape=outs,
        in_specs=[VMEM_SPEC] * 2 + [ANY_SPEC] * (len(args) - 2),
        out_specs=[VMEM_SPEC] * 6 + [ANY_SPEC] * 3,
        scratch_shapes=[
            pltpu.VMEM(local, BF16),
            pltpu.VMEM((LOCAL, hidden), BF16),
            pltpu.VMEM((LOCAL, hidden), BF16),
            pltpu.VMEM((LOCAL, hidden), BF16),
            pltpu.VMEM(local, BF16),
            pltpu.VMEM(local, BF16),
            pltpu.VMEM((2, MODEL_WIDTH, LOCAL), BF16),
            pltpu.VMEM((LOCAL, 2 * HEAD_SIZE), BF16),
            pltpu.VMEM((2, BLOCK, HALF), BF16),
            pltpu.VMEM(line, BF16),
            pltpu.VMEM(line, BF16),
            pltpu.VMEM((12, UNIT, hidden), BF16),
            pltpu.VMEM((2, UNIT, hidden), BF16),
            pltpu.VMEM((3, UNIT, hidden), BF16),
            pltpu.VMEM((4, UNIT, chain_cols), BF16),
            pltpu.VMEM((2, UNIT, chain_cols), BF16),
            pltpu.VMEM((UNIT, chain_cols), BF16),
            pltpu.VMEM((LINE, UNIT, 2 * HEAD_SIZE), BF16),
            pltpu.VMEM((LINE, 1, 2 * MODEL_WIDTH + proj_cols), F32),
            pltpu.VMEM((8, MODEL_WIDTH), F32),
            pltpu.VMEM((2, 8, HALF), F32),
            pltpu.VMEM((8, 8, HALF), F32),
            DMA((16,)),
            DMA((2, 3, 2)),
        ]
        + gather_sems()
        + scatter_sems()
        + scatter_sems()
        + gather_sems()
        + [
            DMA((16,)), DMA((16,)),
            DMA((4, 4)), DMA((4, 4)),
            DMA((4, 2)), DMA((4, 2)),
            DMA((3, 2)), DMA((3,)),
            DMA((3,)), DMA((3,)),
            DMA((LINE,)), DMA((LINE,)),
            DMA((3,)), DMA((3,)),
            DMA((LINE,)), DMA((LINE,)),
            DMA((8,)), DMA((8,)),
            pltpu.SemaphoreType.REGULAR,
        ],
        compiler_params=pltpu.CompilerParams(
            collective_id=2, has_side_effects=True, vmem_limit_bytes=67_043_328
        ),
        cost_estimate=pl.CostEstimate(
            flops=4 * 10**10, bytes_accessed=80_000_000, transcendentals=0
        ),
        name="rear",
    )(*args)


def fast_device(
    block_input,
    position_ids,
    attention_gain,
    query_weight,
    query_bias,
    key_value_weight,
    key_value_bias,
    output_weight,
    feedforward_gain,
    gate_weight,
    upper_weight,
    down_weight,
    out_cotangent,
):
    query_cols = query_weight.shape[1]
    hidden = gate_weight.shape[1]
    proj_cols = query_cols + 2 * HEAD_SIZE
    frequencies = THETA ** (-(jnp.arange(HEAD_SIZE // 2, dtype=F32) * 2.0 / HEAD_SIZE))
    angles = position_ids.astype(F32)[:, None] * frequencies[None, :]
    table = jnp.concatenate([jnp.cos(angles), jnp.sin(angles)], -1)
    small = jnp.concatenate([attention_gain, feedforward_gain, query_bias, key_value_bias])[None]
    gate_t, upper_t, down_t = gate_weight.T, upper_weight.T, down_weight.T
    (
        x_own, normed_one, query_rot, kv_own, kv_other, cosine, sine, gains, attended, probs,
        mid, normed_two, normed_turned, cot_part, own_proj, other_proj, other_weights,
    ) = front_call(
        proj_cols, query_cols, hidden,
        block_input, out_cotangent, table, small, query_weight, key_value_weight, output_weight,
        gate_t, upper_t, down_t,
    )
    out, input_grad, sums, query_sum, output_sum, kv_all, kept, _, landing = rear_call(
        hidden, proj_cols, query_cols,
        mid, gains,
        normed_two, normed_turned, cot_part, gate_t, upper_t, down_t, other_weights, own_proj, other_proj, query_rot, kv_own,
        kv_other, attended, probs, cosine, sine, x_own, normed_one,
    )
    down_sum, gate_sum, upper_sum = (
        kept[m].astype(F32) + landing[m].astype(F32) for m in range(3)
    )
    bias_rows = query_cols // lax.axis_size("dp")
    query_bias_grad = lax.dynamic_slice_in_dim(
        sums[2], lax.axis_index("dp") * bias_rows, bias_rows, 0
    )
    return (
        out,
        input_grad,
        sums[0],
        query_sum,
        query_bias_grad,
        kv_all.astype(F32),
        sums[3, : 2 * KEYVALUE_HEADS * HEAD_SIZE],
        output_sum,
        sums[1],
        gate_sum,
        upper_sum,
        down_sum,
    )


def per_device(*arrays):
    sizes = tuple(lax.axis_size(axis) for axis in ("dp", "row", "col"))
    if sizes == (4, 2, LINE) and arrays[0].shape == (HALF, 2 * BLOCK):
        return fast_device(*arrays)
    return general_device(*arrays)


def solution(mesh):
    placed = (
        P("row", ("dp", "col")),
        P(("dp", "row")),
        P("row"),
        P("row", "col"),
        P("col"),
        P("row", None),
        P(),
        P("row", "col"),
        P("row"),
        P("row", "col"),
        P("row", "col"),
        P("row", "col"),
        P("row", ("dp", "col")),
    )
    return jax.shard_map(
        per_device,
        mesh=mesh,
        in_specs=placed,
        out_specs=(
            P("row", ("dp", "col")),
            P("row", ("dp", "col")),
            P("row"),
            P(("row", "dp"), "col"),
            P(("col", "dp")),
            P("row", None),
            P(),
            P(("row", "dp"), "col"),
            P("row"),
            P(("row", "dp"), "col"),
            P(("row", "dp"), "col"),
            P(("row", "dp"), "col"),
        ),
        check_vma=False,
    )
```

```python
import jax
import jax.numpy as jnp
from jax import lax
from jax.experimental import pallas as pl
from jax.experimental.pallas import tpu as pltpu
from jax.sharding import PartitionSpec as P

MODEL_WIDTH = 1536
KEYVALUE_HEADS = 2
HEAD_SIZE = 128


EPS = 1e-06
THETA = 1000000.0
NEG = -1e30


def rope_tables(position_ids):
    half_dim = HEAD_SIZE // 2
    frequencies = THETA ** (-(jnp.arange(half_dim, dtype=jnp.float32) * 2.0 / HEAD_SIZE))
    angles = position_ids.astype(jnp.float32)[:, None] * frequencies[None, :]
    cosine_values = jnp.cos(angles)
    sine_lookup = jnp.sin(angles)
    return (
        jnp.concatenate([cosine_values, cosine_values], -1),
        jnp.concatenate([sine_lookup, sine_lookup], -1),
    )


def apply_rotation(values, cosine_values, sine_lookup):
    half_dim = HEAD_SIZE // 2
    turned = jnp.concatenate([-values[..., half_dim:], values[..., :half_dim]], -1)
    return values * cosine_values[:, None, :] + turned * sine_lookup[:, None, :]


def unrotate(gradient, cosine_values, sine_lookup):
    half_dim = HEAD_SIZE // 2
    scaled = gradient * sine_lookup[:, None, :]
    turned = jnp.concatenate([scaled[..., half_dim:], -scaled[..., :half_dim]], -1)
    return gradient * cosine_values[:, None, :] + turned


def row_total(partial_value):
    return lax.psum(partial_value, "row")


def norm_forward(x_float, gain):
    squares = jnp.sum(x_float * x_float, -1)
    rinv = lax.rsqrt(row_total(squares) / MODEL_WIDTH + EPS)[:, None]
    return ((x_float * rinv * gain).astype(jnp.bfloat16), rinv)


def norm_backward(normed_grad, x_float, rinv, gain):
    scaled = normed_grad * gain
    inner = row_total(jnp.sum(scaled * x_float, -1))[:, None]
    input_part = rinv * scaled - x_float * rinv**3 * inner / MODEL_WIDTH
    gain_part = jnp.sum(normed_grad * x_float * rinv, 0)
    return (input_part, gain_part)


def column_gather(values):
    return lax.all_gather(values, "col", axis=0, tiled=True)


def column_sum(partial_value):
    return lax.psum_scatter(
        partial_value.astype(jnp.bfloat16), "col", scatter_dimension=0, tiled=True
    ).astype(jnp.float32)


def row_product(gathered, weight):
    return (
        lax.psum_scatter(
            jnp.dot(gathered, weight, preferred_element_type=jnp.float32).astype(jnp.bfloat16),
            "row",
            scatter_dimension=0,
            tiled=True,
        ).astype(jnp.float32),
        gathered,
    )


def row_project(local_part, weight):
    return lax.dot_general(
        lax.all_gather(local_part, "row", axis=0, tiled=True),
        weight,
        (((1,), (1,)), ((), ())),
        preferred_element_type=jnp.float32,
    )


def row_fold(local_part, partner, weight):
    pair_dims = (((0,), (0,)), ((), ()))

    def accumulate(block_rows):
        grad_sum = lax.dot_general(
            partner, block_rows, pair_dims, preferred_element_type=jnp.float32
        )
        if weight is None:
            return (grad_sum,)
        back_proj = lax.dot_general(
            block_rows, weight, (((1,), (1,)), ((), ())), preferred_element_type=jnp.float32
        )
        column_totals = jnp.sum(block_rows, 0, dtype=jnp.float32)
        return (grad_sum, back_proj, column_totals)

    return accumulate(lax.all_gather(local_part, "row", axis=0, tiled=True))


def causal_scores(query_rot, rotated_keys):
    scores = jnp.einsum(
        "ihd,jd->hij", query_rot, rotated_keys, preferred_element_type=jnp.float32
    ) * HEAD_SIZE ** (-0.5)
    length = query_rot.shape[0]
    allowed = jnp.arange(length)[:, None] >= jnp.arange(length)[None, :]
    return jnp.where(allowed[None], scores, NEG)


def attend(query_rot, rotated_keys, value_second_part):
    scores = causal_scores(query_rot, rotated_keys)
    row_max = jnp.max(scores, -1, keepdims=True)
    log_total = row_max + jnp.log(jnp.sum(jnp.exp(scores - row_max), -1, keepdims=True))
    probs_half = jnp.exp(scores - log_total).astype(jnp.bfloat16)
    attended = jnp.einsum(
        "hij,jd->ihd", probs_half, value_second_part, preferred_element_type=jnp.float32
    ).astype(jnp.bfloat16)
    return (attended, log_total)


def attend_back(query_rot, rotated_keys, value_second_part, attended, att_grad, log_total):
    scale = HEAD_SIZE ** (-0.5)
    softmax_probs = jnp.exp(causal_scores(query_rot, rotated_keys) - log_total)
    probs_half = softmax_probs.astype(jnp.bfloat16)
    prob_grad = jnp.einsum(
        "ihd,jd->hij", att_grad, value_second_part, preferred_element_type=jnp.float32
    )
    row_delta = jnp.einsum("ihd,ihd->hi", att_grad, attended, preferred_element_type=jnp.float32)
    score_half = (softmax_probs * (prob_grad - row_delta[:, :, None])).astype(jnp.bfloat16)
    query_grad = (
        jnp.einsum("hij,jd->ihd", score_half, rotated_keys, preferred_element_type=jnp.float32)
        * scale
    )
    key_grad = (
        jnp.einsum("hij,ihd->jd", score_half, query_rot, preferred_element_type=jnp.float32) * scale
    )
    value_grad = jnp.einsum("hij,ihd->jd", probs_half, att_grad, preferred_element_type=jnp.float32)
    return (query_grad, key_grad, value_grad)


def general_device(
    block_input,
    position_ids,
    attention_gain,
    query_weight,
    query_bias,
    key_value_weight,
    key_value_bias,
    output_weight,
    feedforward_gain,
    gate_weight,
    upper_weight,
    down_weight,
    out_cotangent,
):
    single_float_type = jnp.float32
    brain_float_type = jnp.bfloat16
    column_number = lax.axis_size("col")
    seq_len = position_ids.shape[0]
    heads_here = query_weight.shape[1] // HEAD_SIZE
    query_cols = query_weight.shape[1]
    hidden_cols = gate_weight.shape[1]
    key_value_head = lax.axis_index("col") // (column_number // KEYVALUE_HEADS)
    key_start = key_value_head * HEAD_SIZE
    value_offset = KEYVALUE_HEADS * HEAD_SIZE + key_value_head * HEAD_SIZE
    keyval_local = jnp.concatenate(
        [
            lax.dynamic_slice_in_dim(key_value_weight, key_start, HEAD_SIZE, 1),
            lax.dynamic_slice_in_dim(key_value_weight, value_offset, HEAD_SIZE, 1),
        ],
        1,
    )
    bias_local = jnp.concatenate(
        [
            lax.dynamic_slice_in_dim(key_value_bias, key_start, HEAD_SIZE, 0),
            lax.dynamic_slice_in_dim(key_value_bias, value_offset, HEAD_SIZE, 0),
        ],
        0,
    )
    proj_weight = jnp.concatenate([query_weight, keyval_local], 1)
    proj_bias = jnp.concatenate([query_bias, bias_local], 0)
    pair_weight = jnp.concatenate([gate_weight, upper_weight], 1)
    cosine_values, sine_lookup = rope_tables(position_ids)
    x_float = block_input.T.astype(single_float_type)
    cot_local = out_cotangent.T
    normed_one, rinv_one = norm_forward(x_float, attention_gain)
    normed_one_all = column_gather(normed_one)
    proj_out = row_product(normed_one_all, proj_weight)[0] + proj_bias
    query_rot = apply_rotation(
        proj_out[:, :query_cols].reshape(seq_len, heads_here, HEAD_SIZE), cosine_values, sine_lookup
    ).astype(brain_float_type)
    rotated_keys = apply_rotation(
        proj_out[:, query_cols : query_cols + HEAD_SIZE][:, None, :], cosine_values, sine_lookup
    )[:, 0].astype(brain_float_type)
    value_second_part = proj_out[:, query_cols + HEAD_SIZE :].astype(brain_float_type)
    attended, log_total = attend(query_rot, rotated_keys, value_second_part)
    attended_flat = attended.reshape(seq_len, query_cols)
    hidden_res = x_float + column_sum(row_project(attended_flat, output_weight))
    normed_two, rinv_two = norm_forward(hidden_res, feedforward_gain)
    normed_two_all = column_gather(normed_two)
    gate_upper, normed_two_seq = row_product(normed_two_all, pair_weight)
    gate_lin = gate_upper[:, :hidden_cols]
    upper_lin = gate_upper[:, hidden_cols:]
    sigmoid_gate = jax.nn.sigmoid(gate_lin)
    activated = (gate_lin * sigmoid_gate * upper_lin).astype(brain_float_type)
    block_output = hidden_res + column_sum(row_project(activated, down_weight))
    cotangent_all = column_gather(cot_local)
    act_grad = row_product(cotangent_all, down_weight)[0]
    down_grad = row_fold(activated, cotangent_all, None)[0]
    gate_grad = act_grad * upper_lin * sigmoid_gate * (1.0 + gate_lin * (1.0 - sigmoid_gate))
    upper_grad = act_grad * gate_lin * sigmoid_gate
    pair_grad_half = jnp.concatenate([gate_grad, upper_grad], 1).astype(brain_float_type)
    folded_two = row_fold(pair_grad_half, normed_two_all, pair_weight)
    pair_weight_grad = folded_two[0]
    spread_two = folded_two[1]
    normed_two_grad = column_sum(spread_two)
    hidden_part, ffn_gain_part = norm_backward(
        normed_two_grad, hidden_res, rinv_two, feedforward_gain
    )
    hidden_grad = cot_local.astype(single_float_type) + hidden_part
    hidden_half = hidden_grad.astype(brain_float_type)
    hidden_all = column_gather(hidden_half)
    att_grad = (
        row_product(hidden_all, output_weight)[0]
        .astype(brain_float_type)
        .reshape(seq_len, heads_here, HEAD_SIZE)
    )
    output_grad = row_fold(attended_flat, hidden_all, None)[0]
    query_grad, key_grad, value_grad = attend_back(
        query_rot, rotated_keys, value_second_part, attended, att_grad, log_total
    )
    query_half = (
        unrotate(query_grad, cosine_values, sine_lookup)
        .astype(brain_float_type)
        .reshape(seq_len, query_cols)
    )
    key_half = unrotate(key_grad[:, None, :], cosine_values, sine_lookup)[:, 0].astype(
        brain_float_type
    )
    value_grad_half = value_grad.astype(brain_float_type)
    proj_grad_half = jnp.concatenate([query_half, key_half, value_grad_half], 1)
    folded_one = row_fold(proj_grad_half, normed_one_all, proj_weight)
    projection_weight_gradient = folded_one[0]
    normed_one_grad = column_sum(folded_one[1])
    proj_bias_grad = folded_one[2]
    input_part, attn_gain_part = norm_backward(normed_one_grad, x_float, rinv_one, attention_gain)
    input_grad = hidden_grad + input_part
    key_value_gradient = jnp.zeros(
        (projection_weight_gradient.shape[0], 2 * KEYVALUE_HEADS * HEAD_SIZE), single_float_type
    )
    key_value_gradient = lax.dynamic_update_slice_in_dim(
        key_value_gradient,
        projection_weight_gradient[:, query_cols : query_cols + HEAD_SIZE],
        key_start,
        1,
    )
    key_value_gradient = lax.dynamic_update_slice_in_dim(
        key_value_gradient, projection_weight_gradient[:, query_cols + HEAD_SIZE :], value_offset, 1
    )
    key_value_bias_gradient = jnp.zeros((2 * KEYVALUE_HEADS * HEAD_SIZE,), single_float_type)
    key_value_bias_gradient = lax.dynamic_update_slice_in_dim(
        key_value_bias_gradient, proj_bias_grad[query_cols : query_cols + HEAD_SIZE], key_start, 0
    )
    key_value_bias_gradient = lax.dynamic_update_slice_in_dim(
        key_value_bias_gradient, proj_bias_grad[query_cols + HEAD_SIZE :], value_offset, 0
    )
    shared = (
        lax.psum(key_value_gradient.astype(jnp.bfloat16), ("dp", "col")).astype(jnp.float32),
        lax.psum(key_value_bias_gradient.astype(jnp.bfloat16), ("dp", "col")).astype(jnp.float32),
        lax.psum(attn_gain_part.astype(jnp.bfloat16), ("dp", "col")).astype(jnp.float32),
        lax.psum(ffn_gain_part.astype(jnp.bfloat16), ("dp", "col")).astype(jnp.float32),
    )
    summed = (
        lax.psum_scatter(
            projection_weight_gradient[:, :query_cols].astype(jnp.bfloat16),
            "dp",
            scatter_dimension=0,
            tiled=True,
        ).astype(jnp.float32),
        lax.psum_scatter(
            proj_bias_grad[:query_cols].astype(jnp.bfloat16), "dp", scatter_dimension=0, tiled=True
        ).astype(jnp.float32),
        lax.psum_scatter(
            output_grad.astype(jnp.bfloat16), "dp", scatter_dimension=0, tiled=True
        ).astype(jnp.float32),
        lax.psum_scatter(
            pair_weight_grad[:, :hidden_cols].astype(jnp.bfloat16),
            "dp",
            scatter_dimension=0,
            tiled=True,
        ).astype(jnp.float32),
        lax.psum_scatter(
            pair_weight_grad[:, hidden_cols:].astype(jnp.bfloat16),
            "dp",
            scatter_dimension=0,
            tiled=True,
        ).astype(jnp.float32),
        lax.psum_scatter(
            down_grad.astype(jnp.bfloat16), "dp", scatter_dimension=0, tiled=True
        ).astype(jnp.float32),
    )
    return (
        block_output.T,
        input_grad.T,
        shared[2],
        summed[0],
        summed[1],
        shared[0],
        shared[1],
        summed[2],
        shared[3],
        summed[3],
        summed[4],
        summed[5],
    )


MESH_ID = pl.DeviceIdType.MESH
F32 = jnp.float32
BF16 = jnp.bfloat16
LINE = 4
BLOCK = 128
SUB = 2
PART = BLOCK // SUB
LOCAL = LINE * BLOCK
HALF = MODEL_WIDTH // 2
UNIT = MODEL_WIDTH // 8
VMEM_SPEC = pl.BlockSpec(memory_space=pltpu.VMEM)
ANY_SPEC = pl.BlockSpec(memory_space=pl.ANY)
PAIR_ROWS = (((0,), (0,)), ((), ()))
PAIR_COLS = (((1,), (1,)), ((), ()))
SCALE = HEAD_SIZE ** (-0.5)
DMA = pltpu.SemaphoreType.DMA


def greet(me, others):
    barrier = pltpu.get_barrier_semaphore()
    for axis, index in others:
        pl.semaphore_signal(barrier, 1, device_id={axis: index}, device_id_type=MESH_ID)

    @pl.when(me > 0)
    def _():
        pl.semaphore_signal(barrier, 1, device_id={"col": me - 1}, device_id_type=MESH_ID)

    @pl.when(me < LINE - 1)
    def _():
        pl.semaphore_signal(barrier, 1, device_id={"col": me + 1}, device_id_type=MESH_ID)

    @pl.when((me > 0) & (me < LINE - 1))
    def _():
        pl.semaphore_wait(barrier, 2 + len(others))

    @pl.when((me == 0) | (me == LINE - 1))
    def _():
        pl.semaphore_wait(barrier, 1 + len(others))


def aligned(start, size, to=BLOCK):
    return pl.ds(pl.multiple_of(start, to), size)


def block_rows(index):
    return aligned(index * BLOCK, BLOCK)


def send(src, dst, send_sem, recv_sem, axis, to):
    return pltpu.make_async_remote_copy(
        src, dst, send_sem, recv_sem, device_id={axis: to}, device_id_type=MESH_ID
    )


def landed(ref, sem):
    pltpu.make_async_copy(ref, ref, sem).wait()


class Gather:
    def __init__(self, me, all_ref, sends, recv):
        self.me, self.all_ref, self.sends, self.recv = me, all_ref, sends, recv

    def rows(self, j, p):
        return self.all_ref.at[aligned(j * BLOCK + p * PART, PART, PART)]

    def copy(self, j, p, s, side):
        rows = self.rows(j, p)
        return send(
            rows, rows, self.sends.at[side, s, p], self.recv.at[j, p], "col",
            self.me + 1 - 2 * side,
        )

    def has_next(self, side):
        to = self.me + 1 - 2 * side
        return (to >= 0) & (to < LINE)

    def step(self, s, wait=True, forward=True):
        @pl.loop(0, 2 * SUB)
        def _(i):
            side, p = lax.rem(i, 2), i // 2
            j = self.me - (1 - 2 * side) * s

            @pl.when((j >= 0) & (j < LINE))
            def _():
                if s and wait:
                    landed(self.rows(j, p), self.recv.at[j, p])

                if forward and s < LINE - 1:

                    @pl.when(self.has_next(side))
                    def _():
                        self.copy(j, p, s, side).start()

    def run_each(self, s, each):
        if s == 0:
            each(self.me)
            return

        @pl.loop(0, 2)
        def _(side):
            j = self.me - (1 - 2 * side) * s

            @pl.when((j >= 0) & (j < LINE))
            def _():
                each(j)

    def drain(self, first=0, last=LINE - 1):
        for s in range(first, last):

            @pl.loop(0, 2)
            def _(side):
                j = self.me - (1 - 2 * side) * s

                @pl.when((j >= 0) & (j < LINE) & self.has_next(side))
                def _():
                    for p in range(SUB):
                        self.copy(self.me, p, s, side).wait_send()


class Scatter:
    def __init__(self, me, block_of, landing, sends, recv):
        self.me, self.block_of, self.landing = me, block_of, landing
        self.sends, self.recv = sends, recv

    def rows(self, side, j, p):
        return self.landing.at[side, j, pl.ds(p * PART, PART)]

    def copy(self, side, j, p):
        rows = self.rows(side, j, p)
        return send(
            rows, rows, self.sends.at[side, j, p], self.recv.at[side, j, p], "col",
            self.me + 1 - 2 * side,
        )

    def has_last(self, side):
        came = self.me - 1 + 2 * side
        return (came >= 0) & (came < LINE)

    def step(self, s):
        far = jnp.where(self.me < LINE // 2, 1, 0)

        @pl.loop(0, 2)
        def _(i):
            side = lax.rem(i + far, 2)
            j = self.me + (1 - 2 * side) * s

            @pl.when((j >= 0) & (j < LINE))
            def _():
                mine = self.block_of(j)
                for p in range(SUB):
                    term = mine[p * PART : (p + 1) * PART]
                    rows = self.rows(side, j, p)

                    @pl.when(self.has_last(side))
                    def _():
                        landed(rows, self.recv.at[side, j, p])
                        rows[...] = (term + rows[...].astype(F32)).astype(BF16)

                    @pl.when(jnp.logical_not(self.has_last(side)))
                    def _():
                        rows[...] = term.astype(BF16)

                    self.copy(side, j, p).start()

    def finish(self, out_ref):
        me = self.me
        out_ref[...] = self.block_of(me)

        @pl.loop(0, 2)
        def _(side):
            @pl.when(self.has_last(side))
            def _():
                for p in range(SUB):
                    rows = self.rows(side, me, p)
                    landed(rows, self.recv.at[side, me, p])
                    out_ref[p * PART : (p + 1) * PART] += rows[...].astype(F32)

    def drain(self):
        for s in range(1, LINE):

            @pl.loop(0, 2)
            def _(side):
                j = self.me + (1 - 2 * side) * s

                @pl.when((j >= 0) & (j < LINE))
                def _():
                    for p in range(SUB):
                        self.copy(side, j, p).wait_send()


def gather_sems():
    return [DMA((2, LINE, SUB)), DMA((LINE, SUB))]


def scatter_sems():
    return [DMA((2, LINE, SUB)), DMA((2, LINE, SUB))]


def dot(a, b, dims=(((1,), (0,)), ((), ()))):
    return lax.dot_general(a, b, dims, preferred_element_type=F32)


def turn(values):
    return pltpu.roll(values, HEAD_SIZE // 2, 1)


def norm_scale(values):
    return lax.rsqrt(jnp.sum(values * values, -1, keepdims=True) / MODEL_WIDTH + EPS)


def shape(rows, cols, dtype=BF16):
    return jax.ShapeDtypeStruct((rows, cols), dtype)


def attend_local(query_ref, own_ref, other_ref, attended_ref, probs_ref, r):
    rows = 2 * BLOCK
    shape = (rows, rows)
    at_row = lax.broadcasted_iota(jnp.int32, shape, 0)
    at_col = lax.broadcasted_iota(jnp.int32, shape, 1)
    own_mask = at_row >= at_col
    other_mask = at_col // BLOCK < at_row // BLOCK + r
    heads = query_ref.shape[1] // HEAD_SIZE
    for s in range(2):
        part = slice(s * rows, (s + 1) * rows)
        for h in range(heads):
            cols = slice(h * HEAD_SIZE, (h + 1) * HEAD_SIZE)
            query = query_ref[part, cols]
            own = jnp.where(own_mask, dot(query, own_ref[part, :HEAD_SIZE], PAIR_COLS) * SCALE, NEG)
            other = jnp.where(
                other_mask, dot(query, other_ref[part, :HEAD_SIZE], PAIR_COLS) * SCALE, NEG
            )
            top = jnp.maximum(
                jnp.max(own, -1, keepdims=True), jnp.max(other, -1, keepdims=True)
            )
            total = jnp.sum(jnp.exp(own - top), -1, keepdims=True) + jnp.sum(
                jnp.exp(other - top), -1, keepdims=True
            )
            log_total = top + jnp.log(total)
            own = jnp.exp(own - log_total).astype(BF16)
            other = jnp.exp(other - log_total).astype(BF16)
            attended_ref[part, cols] = (
                dot(own, own_ref[part, HEAD_SIZE:]) + dot(other, other_ref[part, HEAD_SIZE:])
            ).astype(BF16)
            probs_ref[s * heads + h, :, :rows] = own
            probs_ref[s * heads + h, :, rows:] = other


def attend_back_body(
    query_ref, own_ref, other_ref, attended_ref, probs_ref, grad_ref, cos_ref, sin_ref,
    query_grad_ref, own_grad_ref, other_grad_ref,
):
    rows = 2 * BLOCK
    heads = query_ref.shape[1] // HEAD_SIZE
    for s in range(2):
        part = slice(s * rows, (s + 1) * rows)
        own_key, other_key = own_ref[part, :HEAD_SIZE], other_ref[part, :HEAD_SIZE]
        own_value, other_value = own_ref[part, HEAD_SIZE:], other_ref[part, HEAD_SIZE:]
        sums = [jnp.zeros((rows, HEAD_SIZE), F32) for _ in range(4)]
        for h in range(heads):
            cols = slice(h * HEAD_SIZE, (h + 1) * HEAD_SIZE)
            query, grad = query_ref[part, cols], grad_ref[part, cols]
            own_p = probs_ref[s * heads + h, :, :rows]
            other_p = probs_ref[s * heads + h, :, rows:]
            delta = jnp.sum(
                grad.astype(F32) * attended_ref[part, cols].astype(F32), -1, keepdims=True
            )
            own_s = (own_p.astype(F32) * (dot(grad, own_value, PAIR_COLS) - delta)).astype(BF16)
            other_s = (other_p.astype(F32) * (dot(grad, other_value, PAIR_COLS) - delta)).astype(BF16)
            query_grad = (dot(own_s, own_key) + dot(other_s, other_key)) * SCALE
            query_grad_ref[part, cols] = (
                query_grad * cos_ref[part] - turn(query_grad) * sin_ref[part]
            ).astype(BF16)
            for i, (weights, partner) in enumerate(
                ((own_s, query), (own_p, grad), (other_s, query), (other_p, grad))
            ):
                sums[i] = sums[i] + dot(weights, partner, PAIR_ROWS)
        own_grad_ref[part, :HEAD_SIZE] = sums[0] * SCALE
        own_grad_ref[part, HEAD_SIZE:] = sums[1]
        other_grad_ref[part, :HEAD_SIZE] = (sums[2] * SCALE).astype(BF16)
        other_grad_ref[part, HEAD_SIZE:] = sums[3].astype(BF16)


PIECES = 6


def front_body(
    input_ref, cot_in_ref, table_ref, attention_gain_ref, feedforward_gain_ref, query_bias_ref,
    kv_bias_ref, query_w_ref, kv_w_ref, output_w_ref,
    gate_hbm, upper_hbm, down_hbm,
    x_hbm, normed_hbm, query_hbm, kv_hbm, kv_other_hbm, cos_hbm, sin_hbm, gains_ref,
    attended_hbm, probs_hbm, mid_hbm, normed_two_hbm, turned_hbm, cot_hbm, proj_hbm, proj_other_hbm,
    weights_other_hbm,
    x_ref, normed_ref, query_ref, kv_ref, kv_other_ref, cos_ref, sin_ref,
    attended_ref, probs_ref, mid_ref, normed_two_ref, turned_ref, cot_ref, proj_ref, proj_other_ref,
    passing, tables, bias_ref, small_ref, landing, store_sems,
    swap_sends, swap_recv, piece_sends, piece_recv, kv_sends, kv_recv,
    g_sends, g_recv, c_sends, c_recv, n_sends, n_recv, s_sends, s_recv,
):
    me, r, d = lax.axis_index("col"), lax.axis_index("row"), lax.axis_index("dp")
    y, core = d // 2, lax.rem(d, 2)
    x_to, y_to, core_to = 1 - r, 2 * (1 - y) + core, 2 * y + 1 - core
    query_cols = query_ref.shape[1]
    proj_cols = query_cols + 2 * HEAD_SIZE
    quarter = HALF // 2
    my_rows = aligned(core * quarter, quarter, quarter)
    its_rows = aligned((1 - core) * quarter, quarter, quarter)
    eighth = quarter // 2
    to_y = aligned(core * quarter + y * eighth, eighth, eighth)
    in_cols, out_cols = pl.ds(0, proj_cols), pl.ds(proj_cols, query_cols)
    kv_width = KEYVALUE_HEADS * HEAD_SIZE
    kv_at = me // (LINE // KEYVALUE_HEADS) * HEAD_SIZE

    stores = [
        pltpu.make_async_copy(src, dst, store_sems.at[i])
        for i, (src, dst) in enumerate(
            (
                (x_ref, x_hbm), (cos_ref, cos_hbm), (sin_ref, sin_hbm), (proj_ref, proj_hbm),
                (normed_ref, normed_hbm), (query_ref, query_hbm), (kv_ref, kv_hbm),
                (kv_other_ref, kv_other_hbm), (probs_ref, probs_hbm), (attended_ref, attended_hbm),
                (proj_other_ref, proj_other_hbm), (mid_ref, mid_hbm),
                (normed_two_ref, normed_two_hbm), (turned_ref, turned_hbm), (cot_ref, cot_hbm),
            )
        )
    ]

    low = 0
    for vector_ref in (attention_gain_ref, feedforward_gain_ref, query_bias_ref, kv_bias_ref):
        size = vector_ref.shape[0]
        small_ref[0, low : low + size] = vector_ref[...]
        low += size

    passing[0] = input_ref[:, block_rows(1 - r)].T
    x_ref[:, :HALF] = input_ref[:, block_rows(r)].T
    proj_ref[:, :query_cols] = query_w_ref[...]
    for i in range(2):
        proj_ref[:, query_cols + i * HEAD_SIZE : query_cols + (i + 1) * HEAD_SIZE] = kv_w_ref[
            :, aligned(i * kv_width + kv_at, HEAD_SIZE)
        ]
    greet(me, [("row", x_to), ("dp", y_to), ("dp", core_to)])

    swaps = [
        (passing.at[0], x_ref.at[:, HALF:], "row", x_to),
        (small_ref.at[:, :HALF], gains_ref.at[pl.ds(0, 1), HALF:], "row", x_to),
        (small_ref.at[:, HALF : 2 * HALF], gains_ref.at[pl.ds(1, 1), HALF:], "row", x_to),
        (proj_ref.at[to_y, in_cols], proj_other_ref.at[to_y, in_cols], "row", x_to),
        (table_ref.at[block_rows(1 - r)], tables.at[pl.ds(0, BLOCK)], "row", x_to),
        (table_ref.at[block_rows(3 - r)], tables.at[pl.ds(BLOCK, BLOCK)], "row", x_to),
        (passing.at[1], cot_ref.at[block_rows(me), HALF:], "row", x_to),
        (proj_ref.at[to_y, out_cols], proj_other_ref.at[to_y, out_cols], "row", x_to),
        (proj_other_ref.at[to_y, in_cols], proj_other_ref.at[to_y, in_cols], "dp", y_to),
        (proj_other_ref.at[to_y, out_cols], proj_other_ref.at[to_y, out_cols], "dp", y_to),
        (proj_other_ref.at[my_rows, in_cols], proj_other_ref.at[my_rows, in_cols], "dp", core_to),
        (proj_other_ref.at[my_rows, out_cols], proj_other_ref.at[my_rows, out_cols], "dp", core_to),
    ]

    def swap_copy(i):
        src, dst, axis, to = swaps[i]
        return send(src, dst, swap_sends.at[i], swap_recv.at[i], axis, to)

    def swap_landed(i):
        swap_copy(i).wait_recv()

    rows = gate_hbm.shape[0] // 4
    owns = (gate_hbm, upper_hbm, down_hbm)

    def piece(i, of_y):
        return aligned((of_y * 2 + i % 2) * rows, rows, rows)

    def piece_copy(i, way):
        m = i // 2
        of_y = 1 - y if way == 3 else y
        at = weights_other_hbm.at[m, piece(i, of_y), my_rows]
        src = owns[m].at[piece(i, of_y), my_rows] if way == 0 else at
        axis, to = (("row", x_to), ("dp", y_to), ("dp", core_to), ("dp", core_to))[way]
        return send(src, at, piece_sends.at[way, i], piece_recv.at[way, i], axis, to)

    def relay_x(i):
        piece_copy(i, 0).wait_recv()
        piece_copy(i, 1).start()
        piece_copy(i, 2).start()

    def relay_y(i):
        piece_copy(i, 1).wait_recv()
        piece_copy(i, 3).start()

    for i in range(6):
        swap_copy(i).start()
    passing[1] = cot_in_ref[:, block_rows(1 - r)].T
    proj_ref[:, proj_cols:] = output_w_ref[...]
    swap_copy(6).start()
    swap_copy(7).start()
    piece_copy(0, 0).start()
    cot_ref[block_rows(me), :HALF] = cot_in_ref[:, block_rows(r)].T
    gains_ref[0:1, :HALF] = small_ref[:, :HALF]
    gains_ref[1:2, :HALF] = small_ref[:, HALF : 2 * HALF]
    bias_ref[:, :query_cols] = small_ref[:, 2 * HALF : 2 * HALF + query_cols]
    for i in range(2):
        bias_ref[:, query_cols + i * HEAD_SIZE : query_cols + (i + 1) * HEAD_SIZE] = small_ref[
            :, aligned(2 * HALF + query_cols + i * kv_width + kv_at, HEAD_SIZE)
        ]
    swap_landed(0)
    swap_landed(1)
    swap_landed(2)
    x = x_ref[...].astype(F32)
    normed_ref[block_rows(me)] = (x * norm_scale(x) * gains_ref[0:1]).astype(BF16)
    gather = Gather(me, normed_ref, g_sends, g_recv)
    gather.step(0)

    lane = lax.broadcasted_iota(jnp.int32, (BLOCK, HEAD_SIZE), 1)
    first = lane < HEAD_SIZE // 2
    swap_landed(3)
    swap_copy(8).start()
    gather.step(1)
    swap_landed(8)
    swap_copy(10).start()
    swap_landed(4)
    swap_landed(5)
    for i in range(4):
        if i < 2:
            table = table_ref[block_rows(r + 2 * i)]
        else:
            table = tables[(i - 2) * BLOCK : (i - 1) * BLOCK]
        turned = turn(table)
        at = block_rows((r if i < 2 else 1 - r) * 2 + i % 2)
        cos_ref[at] = jnp.where(first, table, turned)
        sin_ref[at] = jnp.where(first, -turned, table)
    swap_landed(10)

    def kv_copy(j):
        at = block_rows(j)
        return send(
            kv_ref.at[at], kv_other_ref.at[at], kv_sends.at[j], kv_recv.at[j], "row", x_to
        )

    def each(j):
        at = block_rows(j)
        block = normed_ref[at]
        out = dot(block[:, :HALF], proj_ref[:, :proj_cols])
        out = out + dot(block[:, HALF:], proj_other_ref[:, :proj_cols]) + bias_ref[...]
        cosine, sine = cos_ref[at], sin_ref[at]
        for h in range(query_cols // HEAD_SIZE + 1):
            head = out[:, h * HEAD_SIZE : (h + 1) * HEAD_SIZE]
            turned = (head * cosine + turn(head) * sine).astype(BF16)
            if h * HEAD_SIZE < query_cols:
                query_ref[at, h * HEAD_SIZE : (h + 1) * HEAD_SIZE] = turned
            else:
                kv_ref[at, :HEAD_SIZE] = turned
        kv_ref[at, HEAD_SIZE:] = out[:, query_cols + HEAD_SIZE :].astype(BF16)
        kv_copy(j).start()

    gather.run_each(0, each)
    gather.run_each(1, each)
    gather.step(2)
    gather.run_each(2, each)
    swap_landed(7)
    swap_copy(9).start()
    gather.step(3)
    gather.run_each(3, each)
    for i in range(1, PIECES):
        piece_copy(i, 0).start()
    swap_landed(6)
    cot_gather = Gather(me, cot_ref, c_sends, c_recv)
    cot_gather.step(0)
    swap_landed(9)
    swap_copy(11).start()
    relay_x(0)
    for j in range(LINE):
        kv_copy(j).wait_recv()
    attend_local(query_ref, kv_ref, kv_other_ref, attended_ref, probs_ref, r)
    swap_landed(11)

    def block_of(j):
        block = attended_ref[block_rows(j)]
        return jnp.concatenate(
            [
                dot(block, proj_ref[:, proj_cols:], PAIR_COLS),
                dot(block, proj_other_ref[:, proj_cols:], PAIR_COLS),
            ],
            1,
        )

    scatter = Scatter(me, block_of, landing, s_sends, s_recv)
    scatter.step(3)
    for store in stores[:11]:
        store.start()
    relay_x(1)
    scatter.step(2)
    relay_x(2)
    scatter.step(1)
    relay_y(0)
    relay_x(3)
    scatter.finish(mid_ref)
    mid = mid_ref[...] + x_ref[...].astype(F32)
    mid_ref[...] = mid
    normed_two_ref[block_rows(me)] = (mid * norm_scale(mid) * gains_ref[1:2]).astype(BF16)

    def turn_block(j):
        turned_ref[:, block_rows(j)] = normed_two_ref[block_rows(j)].T

    second = Gather(me, normed_two_ref, n_sends, n_recv)
    second.step(0)
    stores[11].start()
    second.run_each(0, turn_block)
    relay_y(1)
    relay_x(4)
    second.step(1)
    second.run_each(1, turn_block)
    relay_y(2)
    relay_x(5)
    second.step(2)
    second.run_each(2, turn_block)
    relay_y(3)
    second.step(3)
    second.run_each(3, turn_block)
    relay_y(4)
    stores[12].start()
    stores[13].start()
    cot_gather.step(1, forward=False)
    stores[14].start()
    relay_y(5)
    for i in range(PIECES):
        for way in (2, 3):
            of_y = y if way == 2 else 1 - y
            landed(weights_other_hbm.at[i // 2, piece(i, of_y), its_rows], piece_recv.at[way, i])
        for way in range(4):
            piece_copy(i, way).wait_send()
    for i in range(len(swaps)):
        swap_copy(i).wait_send()
    for j in range(LINE):
        kv_copy(j).wait_send()
    for store in stores:
        store.wait()
    gather.drain()
    cot_gather.drain(0, 1)
    second.drain()
    scatter.drain()


def front_call(proj_cols, query_cols, hidden, *args):
    heads = query_cols // HEAD_SIZE
    gains = shape(2, MODEL_WIDTH, F32)
    outs = [
        shape(BLOCK, MODEL_WIDTH),
        shape(LOCAL, MODEL_WIDTH),
        shape(LOCAL, query_cols),
        shape(LOCAL, 2 * HEAD_SIZE),
        shape(LOCAL, 2 * HEAD_SIZE),
        shape(LOCAL, HEAD_SIZE, F32),
        shape(LOCAL, HEAD_SIZE, F32),
        gains,
        shape(LOCAL, query_cols),
        jax.ShapeDtypeStruct((2 * heads, 2 * BLOCK, 4 * BLOCK), BF16),
        shape(BLOCK, MODEL_WIDTH, F32),
        shape(LOCAL, MODEL_WIDTH),
        shape(MODEL_WIDTH, LOCAL),
        shape(LOCAL, MODEL_WIDTH),
        shape(HALF, proj_cols + query_cols),
        shape(HALF, proj_cols + query_cols),
        jax.ShapeDtypeStruct((3, hidden, HALF), BF16),
    ]
    return pl.pallas_call(
        front_body,
        out_shape=outs,
        in_specs=[VMEM_SPEC] * 10 + [ANY_SPEC] * 3,
        out_specs=[VMEM_SPEC if out is gains else ANY_SPEC for out in outs],
        scratch_shapes=[pltpu.VMEM(out.shape, out.dtype) for out in outs[:-1] if out is not gains]
        + [
            pltpu.VMEM((2, BLOCK, HALF), BF16),
            pltpu.VMEM((2 * BLOCK, HEAD_SIZE), F32),
            pltpu.VMEM((1, proj_cols), F32),
            pltpu.VMEM((1, 2 * HALF + query_cols + 2 * KEYVALUE_HEADS * HEAD_SIZE), F32),
            pltpu.VMEM((2, LINE, BLOCK, MODEL_WIDTH), BF16),
            DMA((15,)),
            DMA((12,)),
            DMA((12,)),
            DMA((4, PIECES)),
            DMA((4, PIECES)),
            DMA((LINE,)),
            DMA((LINE,)),
        ]
        + gather_sems() * 3
        + scatter_sems(),
        compiler_params=pltpu.CompilerParams(
            collective_id=1, has_side_effects=True, vmem_limit_bytes=67_043_328
        ),
        cost_estimate=pl.CostEstimate(
            flops=4 * 10**9, bytes_accessed=40_000_000, transcendentals=0
        ),
        name="front",
    )(*args)


DOWN, GATE, UPPER, CHAIN = 0, 1, 2, 3
UNITS = ((1, 1), (1, 0), (0, 1), (0, 0))
TILE = 256


def add_into(total_ref, term_ref, cols):
    @pl.loop(0, total_ref.shape[0] // 32)
    def _(i):
        at = aligned(i * 32, 32, 32)
        total_ref[at, cols] = (
            total_ref[at, cols].astype(F32) + term_ref[at, cols].astype(F32)
        ).astype(BF16)


def rear_body(
    mid_ref, gains_ref,
    normed_two_hbm, turned_hbm, cot_hbm, gate_hbm, upper_hbm, down_hbm, other_hbm, proj_hbm, proj_other_hbm, query_hbm, kv_hbm,
    kv_other_hbm, attended_hbm, probs_hbm, cos_hbm, sin_hbm, x_hbm, normed_one_hbm,
    out_ref, in_ref, small_ref, query_w_ref, output_w_ref, kv_all_ref, kept_hbm, land2_hbm, land3_hbm,
    cot_ref, activated_ref, gate_grad_ref, upper_grad_ref, out_part_ref, back_part_ref, turned_ref,
    kv_got_ref, got_ref, out_landing, landing, sums, gives, gots,
    chain_gots, chain_land2, chain_land3, kv_line, small_line, small_swap, small_give,
    small_group,
    load_sems, w_sems, c_sends, c_recv, o_sends, o_recv, r_sends, r_recv, a_sends, a_recv,
    give_sends, give_recv, two_sends, two_recv, three_sends, three_recv, stage_sem, kept_sems,
    swap_sends, swap_recv, kv_sends, kv_recv, kvd_sends, kvd_recv, line_sends, line_recv,
    small_sends, small_recv, credit,
):
    me, r, d = lax.axis_index("col"), lax.axis_index("row"), lax.axis_index("dp")
    y, core = d // 2, lax.rem(d, 2)
    x_to, y_to, core_to = 1 - r, 2 * (1 - y) + core, 2 * y + 1 - core
    diagonal_to = 2 * (1 - y) + 1 - core
    hidden = activated_ref.shape[1]
    query_cols = query_w_ref.shape[1]
    proj_cols = query_cols + 2 * HEAD_SIZE
    chain_cols = proj_cols + query_cols
    owns = (gate_hbm, upper_hbm, down_hbm)

    def cot_loads(act):
        for i in range(3):
            j = me - 1 + i

            @pl.when((j >= 0) & (j < LINE))
            def _():
                rows = block_rows(j)
                act(pltpu.make_async_copy(cot_hbm.at[rows], cot_ref.at[rows], load_sems.at[i]))

    turned_load = pltpu.make_async_copy(turned_hbm, turned_ref.at[1], load_sems.at[14])
    turned_load.start()
    cot_loads(lambda copy: copy.start())

    halves = {m: (hidden // 2 // BLOCK + 2) * BLOCK for m in (DOWN, GATE, UPPER)}
    halves[CHAIN] = chain_cols // 2

    def columns(m, axis):
        width = chain_cols if m == CHAIN else hidden
        return pl.ds(0, halves[m]) if axis == "row" else pl.ds(halves[m], width - halves[m])

    def unit_rows(h, rel):
        of_y = 1 - y if rel else y
        return aligned(h * HALF + of_y * 2 * UNIT, 2 * UNIT)

    def split(res, keep_ref, give_ref, at):
        low, high = res[:UNIT], res[UNIT:]
        keep_ref[:, at] = jnp.where(core == 0, low, high).astype(BF16)
        give_ref[:, at] = jnp.where(core == 0, high, low).astype(BF16)

    order = [
        (DOWN, 0), (DOWN, 1), (DOWN, 2), (UPPER, 0), (UPPER, 1), (UPPER, 2), (DOWN, 3),
        (GATE, 0), (GATE, 1), (GATE, 2), (UPPER, 3), (GATE, 3),
    ]
    columns_of = {DOWN: activated_ref, GATE: gate_grad_ref, UPPER: upper_grad_ref}
    ring = 3

    def total_of(m, h, rel):
        return sums.at[m * 4 + h * 2 + rel]

    def give_copy(u):
        return send(
            gives.at[u % 2], gots.at[u % ring], give_sends.at[u], give_recv.at[u], "dp", core_to
        )

    def compute(u):
        m, i = order[u]
        h, rel = UNITS[i]
        if u >= 2:
            give_copy(u - 2).wait_send()
        left = 0 if m == DOWN else 1
        rows = unit_rows(h, rel)
        tile = 512

        def run(at):
            res = dot(turned_ref[left, rows], columns_of[m][:, at])
            split(res, total_of(m, h, rel), gives.at[u % 2], at)

        @pl.loop(0, hidden // tile)
        def _(i):
            run(aligned(i * tile, tile))

        if hidden % tile:
            run(pl.ds(hidden // tile * tile, hidden % tile))
        if u >= ring:
            pl.semaphore_wait(credit, 1)
        give_copy(u).start()

    def two_copy(m, k, chain_sums=None):
        h, rel = ((1, 0), (1, 1), (0, 1), (1, 1))[k]
        axis, to = (("row", x_to), ("dp", y_to))[k // 2]
        at = columns(m, axis)
        if m == CHAIN:
            src, dst = chain_sums.at[h * 2 + rel, :, at], chain_land2.at[k % 2, :, at]
        else:
            src, dst = total_of(m, h, rel).at[:, at], land2_hbm.at[m * 2 + k % 2, :, at]
        return send(src, dst, two_sends.at[m, k], two_recv.at[m, k], axis, to)

    def combine(u):
        m, i = order[u]
        h, rel = UNITS[i]
        give_copy(u).wait_recv()
        add_into(total_of(m, h, rel), gots.at[u % ring], pl.ds(0, hidden))
        if u < len(order) - ring:
            pl.semaphore_signal(credit, 1, device_id={"dp": core_to}, device_id_type=MESH_ID)
        for k in {(1, 1): (1, 3), (1, 0): (0,), (0, 1): (2,), (0, 0): ()}[h, rel]:
            two_copy(m, k).start()

    def three_copy(m, k, chain_sums=None):
        h, rel = ((0, 1), (1, 0))[k]
        axis, to = (("dp", y_to), ("row", x_to))[k]
        at = columns(m, ("row", "dp")[k])
        if m == CHAIN:
            src, dst = chain_sums.at[h * 2 + rel, :, at], chain_land3.at[:, at]
        else:
            src, dst = total_of(m, h, rel).at[:, at], land3_hbm.at[m, :, at]
        return send(src, dst, three_sends.at[m, k], three_recv.at[m, k], axis, to)

    def kept_copy(m):
        return pltpu.make_async_copy(total_of(m, 0, 0), kept_hbm.at[m], kept_sems.at[m])

    def stage(m, i):
        return pltpu.make_async_copy(land2_hbm.at[m * 2 + i], gots.at[i], stage_sem.at[m, i])

    def second_stage(m, now=(0, 1)):
        for k in range(4):
            two_copy(m, k).wait_recv()
        for i in (1, 0):
            stage(m, i).start()
        stage(m, 1).wait()
        add_into(total_of(m, 0, 1), gots.at[1], columns(m, "row"))
        if 0 in now:
            three_copy(m, 0).start()
        add_into(total_of(m, 1, 0), gots.at[1], columns(m, "dp"))
        if 1 in now:
            three_copy(m, 1).start()
        stage(m, 0).wait()
        add_into(total_of(m, 0, 0), gots.at[0], pl.ds(0, hidden))
        kept_copy(m).start()

    barrier = pltpu.get_barrier_semaphore()
    group_size = 8
    own = r * 4 + d

    def member(i):
        index = lax.rem(own + i, group_size)
        return {"row": index // 4, "dp": lax.rem(index, 4)}

    for i in range(1, group_size):
        pl.semaphore_signal(barrier, 1, device_id=member(i), device_id_type=MESH_ID)
    for s in range(1, LINE):
        pl.semaphore_signal(
            barrier, 1, device_id={"col": lax.rem(me + s, LINE)}, device_id_type=MESH_ID
        )

    cot_gather = Gather(me, cot_ref, c_sends, c_recv)
    out_scatter = Scatter(
        me, lambda j: out_part_ref[block_rows(j)].astype(F32), out_landing, o_sends, o_recv
    )

    def feed(weights, gates, total, normed_two_ref):
        tiles = hidden // TILE
        rest = hidden % TILE

        def loads(t, slot, size):
            rows = aligned(t * TILE, size, TILE)
            for m in range(3):
                for i, src in enumerate((owns[m].at[rows], other_hbm.at[m, rows])):
                    yield pltpu.make_async_copy(
                        src,
                        weights.at[slot, m, pl.ds(0, size), pl.ds(i * HALF, HALF)],
                        w_sems.at[slot, m, i],
                    )

        def start(t, slot, size):
            for copy in loads(t, slot, size):
                copy.start()

        def ready(t, slot, size):
            for copy in loads(t, slot, size):
                copy.wait()

        def sweep(body, first_slot, hooks, again):
            @pl.loop(0, tiles)
            def _(t):
                slot = lax.rem(t + first_slot, 2)
                ready(t, slot, TILE)

                @pl.when(t < tiles - 1)
                def _():
                    start(t + 1, 1 - slot, TILE)

                @pl.when(t == tiles - 1)
                def _():
                    start(tiles, 1 - slot, rest)

                body(aligned(t * TILE, TILE), slot, TILE)
                for at, hook in hooks:
                    pl.when(t == at)(hook)

            slot = (tiles + first_slot) % 2
            ready(tiles, slot, rest)
            if again:
                start(0, 1 - slot, TILE)
            body(pl.ds(tiles * TILE, rest), slot, rest)

        def add_products(slot, size, factors, cols):
            width = 768

            @pl.loop(0, MODEL_WIDTH // width)
            def _(i):
                at = aligned(i * width, width)
                left = jnp.concatenate([factor[:, cols] for factor, _ in factors], 1)
                right = jnp.concatenate(
                    [weights[slot, m, pl.ds(0, size), at] for _, m in factors], 0
                )
                total[:, at] += dot(left, right)

        def forward(cols, slot, size):
            here = pl.ds(0, size)
            gate = dot(normed_two_ref[...], weights[slot, 0, here], PAIR_COLS)
            upper = dot(normed_two_ref[...], weights[slot, 1, here], PAIR_COLS)
            activated = (gate * jax.nn.sigmoid(gate) * upper).astype(BF16)
            gates[0, :, cols] = gate.astype(BF16)
            gates[1, :, cols] = upper.astype(BF16)
            activated_ref[:, cols] = activated
            total[...] += dot(activated, weights[slot, 2, here])

        def backward(cols, slot, size):
            here = pl.ds(0, size)
            act_grad = dot(cot_ref[...], weights[slot, 2, here], PAIR_COLS)
            gate, upper = gates[0, :, cols].astype(F32), gates[1, :, cols].astype(F32)
            sig = jax.nn.sigmoid(gate)
            gate_grad = (act_grad * upper * sig * (1.0 + gate * (1.0 - sig))).astype(BF16)
            upper_grad = (act_grad * gate * sig).astype(BF16)
            gate_grad_ref[:, cols] = gate_grad
            upper_grad_ref[:, cols] = upper_grad
            add_products(slot, size, ((gate_grad_ref, 0), (upper_grad_ref, 1)), cols)

        load = pltpu.make_async_copy(normed_two_hbm, normed_two_ref, load_sems.at[15])
        load.start()
        start(0, 0, TILE)
        total[...] = jnp.zeros_like(total)
        pl.semaphore_wait(barrier, group_size - 1 + LINE - 1)
        cot_loads(lambda copy: copy.wait())
        cot_gather.step(1, wait=False)
        load.wait()
        turned_load.wait()
        sweep(forward, 0, [(4, lambda: cot_gather.step(2))], True)
        out_part_ref[...] = total[...].astype(BF16)
        out_scatter.step(3)
        cot_gather.step(3)
        turned_ref[0] = cot_ref[...].T
        total[...] = jnp.zeros_like(total)
        compute(0)
        compute(1)
        hooks = [
            (0, lambda: combine(0)), (1, lambda: combine(1)), (4, lambda: out_scatter.step(2)),
        ]
        sweep(backward, (tiles + 1) % 2, hooks, False)
        back_part_ref[...] = total[...].astype(BF16)
        cot_gather.drain(1, LINE - 1)

    pl.run_scoped(
        feed,
        pltpu.VMEM((2, 3, TILE, MODEL_WIDTH), BF16),
        pltpu.VMEM((2, LOCAL, hidden), BF16),
        pltpu.VMEM((LOCAL, MODEL_WIDTH), F32),
        pltpu.VMEM((LOCAL, MODEL_WIDTH), BF16),
    )

    def rest(
        proj_ref, proj_other_ref, query_ref, kv_ref, kv_other_ref, attended_ref, probs_ref, cos_ref,
        sin_ref, x_ref, normed_one_ref, mid_grad_ref, own_ref, att_grad_ref,
        kv_grad_ref, kv_give_ref, proj_grad_ref, chain_sums, back_give,
    ):
        pairs = (
            (proj_hbm, proj_ref), (proj_other_hbm, proj_other_ref), (query_hbm, query_ref),
            (kv_hbm, kv_ref), (kv_other_hbm, kv_other_ref), (attended_hbm, attended_ref),
            (probs_hbm, probs_ref), (cos_hbm, cos_ref), (sin_hbm, sin_ref), (x_hbm, x_ref),
            (normed_one_hbm, normed_one_ref),
        )
        reads = [
            pltpu.make_async_copy(src, dst, load_sems.at[3 + i])
            for i, (src, dst) in enumerate(pairs)
        ]

        mid_half_ref = cot_ref

        scatter = Scatter(
            me, lambda j: back_part_ref[block_rows(j)].astype(F32), landing, r_sends, r_recv
        )
        scatter.step(3)
        for read in reads:
            read.start()
        compute(2)
        for u in (3, 4, 5):
            compute(u)
            combine(u - 1)
        scatter.step(2)
        for u in (6, 7):
            compute(u)
            combine(u - 1)
        scatter.step(1)
        for u in (8, 9):
            compute(u)
            combine(u - 1)
        scatter.finish(mid_grad_ref)
        mid, grad = mid_ref[...], mid_grad_ref[...]
        rinv = norm_scale(mid)
        small_line[me, :, MODEL_WIDTH : 2 * MODEL_WIDTH] = jnp.sum(grad * mid * rinv, 0, keepdims=True)
        scaled = grad * gains_ref[1:2]
        inner = jnp.sum(scaled * mid, -1, keepdims=True)
        mid_grad = (
            cot_ref[block_rows(me)].astype(F32)
            + rinv * scaled
            - mid * rinv**3 * inner / MODEL_WIDTH
        )
        mid_grad_ref[...] = mid_grad
        mid_half_ref[block_rows(me)] = mid_grad.astype(BF16)

        gather = Gather(me, mid_half_ref, a_sends, a_recv)
        gather.step(0)
        scatter.drain()
        for read in reads:
            read.wait()

        def each(j):
            block = mid_half_ref[block_rows(j)]
            att_grad_ref[block_rows(j)] = (
                dot(block[:, :HALF], proj_ref[:, proj_cols:])
                + dot(block[:, HALF:], proj_other_ref[:, proj_cols:])
            ).astype(BF16)

        gather.run_each(0, each)
        for u in (10, 11):
            compute(u)
            combine(u - 1)
        combine(11)
        gather.step(1)
        gather.run_each(1, each)
        second_stage(DOWN)
        gather.step(2)
        gather.run_each(2, each)
        second_stage(UPPER, (0,))
        gather.step(3)
        gather.run_each(3, each)
        out_scatter.step(1)
        attend_back_body(
            query_ref, kv_ref, kv_other_ref, attended_ref, probs_ref, att_grad_ref, cos_ref,
            sin_ref, proj_grad_ref, kv_grad_ref, kv_give_ref,
        )

        def swap_copy(i):
            src, dst = (
                (kv_give_ref, kv_got_ref),
                (back_give.at[0], got_ref.at[0]),
                (back_give.at[1], got_ref.at[1]),
            )[i]
            return send(src, dst, swap_sends.at[i], swap_recv.at[i], "row", x_to)

        swap_copy(0).start()
        swap_copy(0).wait_recv()
        kv = kv_grad_ref[...] + kv_got_ref[...].astype(F32)
        key = kv[:, :HEAD_SIZE]
        proj_grad_ref[:, query_cols : query_cols + HEAD_SIZE] = (
            key * cos_ref[...] - turn(key) * sin_ref[...]
        ).astype(BF16)
        proj_grad_ref[:, query_cols + HEAD_SIZE :] = kv[:, HEAD_SIZE:].astype(BF16)

        def block_of(j):
            block = proj_grad_ref[block_rows(j)]
            return jnp.concatenate(
                [
                    dot(block, proj_ref[:, :proj_cols], PAIR_COLS),
                    dot(block, proj_other_ref[:, :proj_cols], PAIR_COLS),
                ],
                1,
            )

        def chain_from(i):
            return gives.at[i // 2, :, pl.ds(i % 2 * chain_cols, chain_cols)]

        def chain_give(i):
            return send(
                chain_from(i), chain_gots.at[i], give_sends.at[12 + i], give_recv.at[12 + i],
                "dp", core_to,
            )

        def chain_compute(i):
            h, rel = UNITS[i]
            rows = unit_rows(h, rel)
            keep = chain_sums.at[h * 2 + rel]
            res = dot(normed_one_ref[:, rows], proj_grad_ref[...], PAIR_ROWS)
            split(res, keep, chain_from(i), pl.ds(0, proj_cols))
            res = dot(mid_half_ref[:, rows], attended_ref[...], PAIR_ROWS)
            split(res, keep, chain_from(i), pl.ds(proj_cols, query_cols))
            chain_give(i).start()

        def chain_combine(i):
            h, rel = UNITS[i]
            chain_give(i).wait_recv()
            add_into(chain_sums.at[h * 2 + rel], chain_gots.at[i], pl.ds(0, chain_cols))
            for k in {(1, 1): (1, 3), (1, 0): (0,), (0, 1): (2,), (0, 0): ()}[h, rel]:
                two_copy(CHAIN, k, chain_sums).start()

        second = Scatter(me, block_of, landing, r_sends, r_recv)
        second.step(3)
        for u in (len(order) - 2, len(order) - 1):
            give_copy(u).wait_send()
        for i in range(4):
            chain_compute(i)
        for i in range(4):
            chain_combine(i)
        three_copy(UPPER, 1).start()
        small_line[me, :, 2 * MODEL_WIDTH :] = jnp.sum(
            proj_grad_ref[...].astype(F32), 0, keepdims=True
        )
        second.step(2)
        second_stage(GATE, (0,))
        out_scatter.finish(own_ref)
        out = own_ref[...] + mid_ref[...]
        out_ref[:, block_rows(r)] = out[:, :HALF].T
        back_give[1] = out[:, HALF:].astype(BF16)
        second.step(1)
        for k in range(4):
            two_copy(CHAIN, k, chain_sums).wait_recv()
        add_into(chain_sums.at[1], chain_land2.at[1], columns(CHAIN, "row"))
        three_copy(CHAIN, 0, chain_sums).start()
        add_into(chain_sums.at[2], chain_land2.at[1], columns(CHAIN, "dp"))
        three_copy(CHAIN, 1, chain_sums).start()
        add_into(chain_sums.at[0], chain_land2.at[0], pl.ds(0, chain_cols))
        three_copy(GATE, 1).start()
        swap_copy(2).start()
        for k in range(2):
            three_copy(CHAIN, k, chain_sums).wait_recv()
        total = chain_sums[0].astype(F32) + chain_land3[...].astype(F32)
        query_w_ref[...] = total[:, :query_cols]
        output_w_ref[...] = total[:, proj_cols:]
        kv_line[me] = total[:, query_cols:proj_cols].astype(BF16)

        def kv_line_copy(s):
            to = lax.rem(me + s, LINE)
            return send(kv_line.at[me], kv_line.at[me], kv_sends.at[s], kv_recv.at[me], "col", to)

        for s in range(1, LINE):
            kv_line_copy(s).start()
        second.finish(own_ref)
        x, grad = x_ref[...].astype(F32), own_ref[...]
        rinv = norm_scale(x)
        scaled = grad * gains_ref[0:1]
        inner = jnp.sum(scaled * x, -1, keepdims=True)
        input_grad = mid_grad_ref[...] + rinv * scaled - x * rinv**3 * inner / MODEL_WIDTH
        back_give[0] = input_grad[:, HALF:].astype(BF16)
        swap_copy(1).start()
        small_line[me, :, :MODEL_WIDTH] = jnp.sum(grad * x * rinv, 0, keepdims=True)

        def small_line_copy(s):
            to = lax.rem(me + s, LINE)
            return send(
                small_line.at[me], small_line.at[me], line_sends.at[s], line_recv.at[me], "col", to
            )

        for s in range(1, LINE):
            small_line_copy(s).start()
        in_ref[:, block_rows(r)] = input_grad[:, :HALF].T

        group = LINE // KEYVALUE_HEADS
        for s in range(1, LINE):
            landed(kv_line.at[me], kv_recv.at[lax.rem(me + s, LINE)])
        dp_rows = aligned(d * UNIT, UNIT, UNIT)
        for h in range(KEYVALUE_HEADS):
            pair = kv_line[h * group].astype(F32)
            for i in range(1, group):
                pair = pair + kv_line[h * group + i].astype(F32)
            for i in range(2):
                at = (i * KEYVALUE_HEADS + h) * HEAD_SIZE
                kv_all_ref[dp_rows, at : at + HEAD_SIZE] = pair[
                    :, i * HEAD_SIZE : (i + 1) * HEAD_SIZE
                ].astype(BF16)

        def kv_rows(of):
            return kv_all_ref.at[aligned(of * UNIT, UNIT, UNIT)]

        def kv_dp_copy(i):
            rows = kv_rows(y_to if i == 2 else d)
            to = y_to if i == 1 else core_to
            return send(rows, rows, kvd_sends.at[i], kvd_recv.at[i], "dp", to)

        kv_dp_copy(1).start()
        kv_dp_copy(0).start()

        for s in range(1, LINE):
            landed(small_line.at[me], line_recv.at[lax.rem(me + s, LINE)])
        lines = [small_line[j] for j in range(LINE)]
        total_line = lines[0] + lines[1] + lines[2] + lines[3]
        small_swap[...] = jnp.zeros_like(small_swap)
        small_swap[0:1] = total_line[:, :MODEL_WIDTH]
        small_swap[1:2] = total_line[:, MODEL_WIDTH : 2 * MODEL_WIDTH]
        bias_at = 2 * MODEL_WIDTH
        small_swap[2:3, :query_cols] = small_line[me, :, bias_at : bias_at + query_cols]
        for i in range(2):
            for h in range(KEYVALUE_HEADS):
                at = bias_at + query_cols + i * HEAD_SIZE
                part = lines[h * group][:, at : at + HEAD_SIZE]
                for j in range(1, group):
                    part = part + lines[h * group + j][:, at : at + HEAD_SIZE]
                at = (i * KEYVALUE_HEADS + h) * HEAD_SIZE
                small_swap[3:4, at : at + HEAD_SIZE] = part

        small_give[0] = small_swap[:, :HALF]
        small_give[1, :2] = small_swap[:2, HALF:]
        small_give[1, 2:] = small_swap[2:, :HALF]
        small_group[own] = small_give[0]

        def small_copy(i):
            to = member(i)
            kind = jnp.where(to["row"] == r, 0, 1)
            return pltpu.make_async_remote_copy(
                small_give.at[kind], small_group.at[own], small_sends.at[i], small_recv.at[own],
                device_id=to, device_id_type=MESH_ID,
            )

        for i in range(1, group_size):
            small_copy(i).start()
        landed(kv_rows(y_to), kvd_recv.at[1])
        kv_dp_copy(2).start()
        for i in (2, 1):
            swap_copy(i).wait_recv()
            to_ref = (in_ref, out_ref)[i - 1]
            to_ref[:, block_rows(1 - r)] = got_ref[i - 1].astype(F32).T
        for i in range(1, group_size):
            source = lax.rem(own + i, group_size)
            landed(small_group.at[source], small_recv.at[source])
        small_ref[...] = sum(small_group[i] for i in range(group_size))

        landed(kv_rows(core_to), kvd_recv.at[0])
        landed(kv_rows(diagonal_to), kvd_recv.at[2])
        for m in (DOWN, GATE, UPPER):
            for k in range(2):
                three_copy(m, k).wait_recv()
                three_copy(m, k).wait_send()
            kept_copy(m).wait()
            for k in range(4):
                two_copy(m, k).wait_send()
        for i in range(4):
            chain_give(i).wait_send()
            two_copy(CHAIN, i, chain_sums).wait_send()
        for k in range(2):
            three_copy(CHAIN, k, chain_sums).wait_send()
        for i in range(3):
            swap_copy(i).wait_send()
            kv_dp_copy(i).wait_send()
            kv_line_copy(1 + i).wait_send()
            small_line_copy(1 + i).wait_send()
        for i in range(1, group_size):
            small_copy(i).wait_send()
        gather.drain()
        out_scatter.drain()
        second.drain()

    wide = (HALF, chain_cols)
    pl.run_scoped(
        rest,
        pltpu.VMEM(wide, BF16),
        pltpu.VMEM(wide, BF16),
        pltpu.VMEM((LOCAL, query_cols), BF16),
        pltpu.VMEM((LOCAL, 2 * HEAD_SIZE), BF16),
        pltpu.VMEM((LOCAL, 2 * HEAD_SIZE), BF16),
        pltpu.VMEM((LOCAL, query_cols), BF16),
        pltpu.VMEM(probs_hbm.shape, BF16),
        pltpu.VMEM((LOCAL, HEAD_SIZE), F32),
        pltpu.VMEM((LOCAL, HEAD_SIZE), F32),
        pltpu.VMEM((BLOCK, MODEL_WIDTH), BF16),
        pltpu.VMEM((LOCAL, MODEL_WIDTH), BF16),
        pltpu.VMEM((BLOCK, MODEL_WIDTH), F32),
        pltpu.VMEM((BLOCK, MODEL_WIDTH), F32),
        pltpu.VMEM((LOCAL, query_cols), BF16),
        pltpu.VMEM((LOCAL, 2 * HEAD_SIZE), F32),
        pltpu.VMEM((LOCAL, 2 * HEAD_SIZE), BF16),
        pltpu.VMEM((LOCAL, proj_cols), BF16),
        pltpu.VMEM((4, UNIT, chain_cols), BF16),
        pltpu.VMEM((2, BLOCK, HALF), BF16),
    )


def rear_call(hidden, proj_cols, query_cols, *args):
    chain_cols = proj_cols + query_cols
    outs = [
        shape(HALF, 2 * BLOCK, F32),
        shape(HALF, 2 * BLOCK, F32),
        shape(8, HALF, F32),
        shape(UNIT, query_cols, F32),
        shape(UNIT, query_cols, F32),
        shape(4 * UNIT, 2 * KEYVALUE_HEADS * HEAD_SIZE),
        jax.ShapeDtypeStruct((3, UNIT, hidden), BF16),
        jax.ShapeDtypeStruct((6, UNIT, hidden), BF16),
        jax.ShapeDtypeStruct((3, UNIT, hidden), BF16),
    ]
    local = (LOCAL, MODEL_WIDTH)
    line = (2, LINE, BLOCK, MODEL_WIDTH)
    return pl.pallas_call(
        rear_body,
        out_shape=outs,
        in_specs=[VMEM_SPEC] * 2 + [ANY_SPEC] * (len(args) - 2),
        out_specs=[VMEM_SPEC] * 6 + [ANY_SPEC] * 3,
        scratch_shapes=[
            pltpu.VMEM(local, BF16),
            pltpu.VMEM((LOCAL, hidden), BF16),
            pltpu.VMEM((LOCAL, hidden), BF16),
            pltpu.VMEM((LOCAL, hidden), BF16),
            pltpu.VMEM(local, BF16),
            pltpu.VMEM(local, BF16),
            pltpu.VMEM((2, MODEL_WIDTH, LOCAL), BF16),
            pltpu.VMEM((LOCAL, 2 * HEAD_SIZE), BF16),
            pltpu.VMEM((2, BLOCK, HALF), BF16),
            pltpu.VMEM(line, BF16),
            pltpu.VMEM(line, BF16),
            pltpu.VMEM((12, UNIT, hidden), BF16),
            pltpu.VMEM((2, UNIT, hidden), BF16),
            pltpu.VMEM((3, UNIT, hidden), BF16),
            pltpu.VMEM((4, UNIT, chain_cols), BF16),
            pltpu.VMEM((2, UNIT, chain_cols), BF16),
            pltpu.VMEM((UNIT, chain_cols), BF16),
            pltpu.VMEM((LINE, UNIT, 2 * HEAD_SIZE), BF16),
            pltpu.VMEM((LINE, 1, 2 * MODEL_WIDTH + proj_cols), F32),
            pltpu.VMEM((8, MODEL_WIDTH), F32),
            pltpu.VMEM((2, 8, HALF), F32),
            pltpu.VMEM((8, 8, HALF), F32),
            DMA((16,)),
            DMA((2, 3, 2)),
        ]
        + gather_sems()
        + scatter_sems()
        + scatter_sems()
        + gather_sems()
        + [
            DMA((16,)), DMA((16,)),
            DMA((4, 4)), DMA((4, 4)),
            DMA((4, 2)), DMA((4, 2)),
            DMA((3, 2)), DMA((3,)),
            DMA((3,)), DMA((3,)),
            DMA((LINE,)), DMA((LINE,)),
            DMA((3,)), DMA((3,)),
            DMA((LINE,)), DMA((LINE,)),
            DMA((8,)), DMA((8,)),
            pltpu.SemaphoreType.REGULAR,
        ],
        compiler_params=pltpu.CompilerParams(
            collective_id=2, has_side_effects=True, vmem_limit_bytes=67_043_328
        ),
        cost_estimate=pl.CostEstimate(
            flops=4 * 10**10, bytes_accessed=80_000_000, transcendentals=0
        ),
        name="rear",
    )(*args)


def finish_body(
    out_hbm, in_hbm, query_hbm, output_hbm, kv_hbm, kept_hbm, landing_hbm, small_ref,
    out_to, in_to, query_to, output_to, kv_to, down_to, gate_to, upper_to,
    attention_gain_to, feedforward_gain_to, query_bias_to, kv_bias_to,
    out_ref, in_ref, query_ref, output_ref, kv_ref, kv_wide, kept, landing, wide, load_sems, store_sems,
):
    passed = (
        (out_hbm, out_ref, out_to), (in_hbm, in_ref, in_to), (query_hbm, query_ref, query_to),
        (output_hbm, output_ref, output_to),
    )
    sums = (down_to, gate_to, upper_to)
    loads = []
    for m in range(3):
        loads.append(pltpu.make_async_copy(kept_hbm.at[m], kept.at[m], load_sems.at[2 * m]))
        loads.append(pltpu.make_async_copy(landing_hbm.at[m], landing.at[m], load_sems.at[2 * m + 1]))
    loads.append(pltpu.make_async_copy(kv_hbm, kv_ref, load_sems.at[6]))
    for i, (src, here, _) in enumerate(passed):
        loads.append(pltpu.make_async_copy(src, here, load_sems.at[7 + i]))
    stores = [pltpu.make_async_copy(wide.at[m], sums[m], store_sems.at[m]) for m in range(3)]
    stores.append(pltpu.make_async_copy(kv_wide, kv_to, store_sems.at[3]))
    for i, (_, here, to) in enumerate(passed):
        stores.append(pltpu.make_async_copy(here, to, store_sems.at[4 + i]))
    for load in loads:
        load.start()
    for m in range(3):
        loads[2 * m].wait()
        loads[2 * m + 1].wait()

        @pl.loop(0, UNIT // 32)
        def _(i):
            at = aligned(i * 32, 32, 32)
            wide[m, at] = kept[m, at].astype(F32) + landing[m, at].astype(F32)

        stores[m].start()
    loads[6].wait()
    kv_wide[...] = kv_ref[...].astype(F32)
    stores[3].start()
    for i in range(4):
        loads[7 + i].wait()
        stores[4 + i].start()
    attention_gain_to[...] = small_ref[0]
    feedforward_gain_to[...] = small_ref[1]
    query_bias_to[...] = small_ref[2, : query_bias_to.shape[0]]
    kv_bias_to[...] = small_ref[3, : kv_bias_to.shape[0]]
    for store in stores:
        store.wait()


def finish_call(out, input_grad, query_sum, output_sum, kv_all, kept, landing, sums):
    like = lambda v, dtype: jax.ShapeDtypeStruct(v.shape, dtype)
    unit = jax.ShapeDtypeStruct(kept.shape[1:], F32)
    vector = lambda n: jax.ShapeDtypeStruct((n,), F32)
    passed = [like(v, F32) for v in (out, input_grad, query_sum, output_sum)]
    outs = passed + [like(kv_all, F32)] + [unit] * 3
    small = [vector(HALF), vector(HALF), vector(query_sum.shape[1]), vector(kv_all.shape[1])]
    return pl.pallas_call(
        finish_body,
        out_shape=outs + small,
        in_specs=[ANY_SPEC] * 7 + [VMEM_SPEC],
        out_specs=[ANY_SPEC] * 8 + [VMEM_SPEC] * 4,
        scratch_shapes=[pltpu.VMEM(v.shape, F32) for v in passed]
        + [
            pltpu.VMEM(kv_all.shape, BF16),
            pltpu.VMEM(kv_all.shape, F32),
            pltpu.VMEM(kept.shape, BF16),
            pltpu.VMEM(kept.shape, BF16),
            pltpu.VMEM(kept.shape, F32),
            DMA((11,)),
            DMA((8,)),
        ],
        compiler_params=pltpu.CompilerParams(vmem_limit_bytes=67_043_328),
        name="finish",
    )(out, input_grad, query_sum, output_sum, kv_all, kept, landing, sums)


def fast_device(
    block_input,
    position_ids,
    attention_gain,
    query_weight,
    query_bias,
    key_value_weight,
    key_value_bias,
    output_weight,
    feedforward_gain,
    gate_weight,
    upper_weight,
    down_weight,
    out_cotangent,
):
    query_cols = query_weight.shape[1]
    hidden = gate_weight.shape[1]
    proj_cols = query_cols + 2 * HEAD_SIZE
    frequencies = THETA ** (-(jnp.arange(HEAD_SIZE // 2, dtype=F32) * 2.0 / HEAD_SIZE))
    angles = position_ids.astype(F32)[:, None] * frequencies[None, :]
    table = jnp.concatenate([jnp.cos(angles), jnp.sin(angles)], -1)
    gate_t, upper_t, down_t = gate_weight.T, upper_weight.T, down_weight.T
    (
        x_own, normed_one, query_rot, kv_own, kv_other, cosine, sine, gains, attended, probs,
        mid, normed_two, normed_turned, cot_part, own_proj, other_proj, other_weights,
    ) = front_call(
        proj_cols, query_cols, hidden,
        block_input, out_cotangent, table, attention_gain, feedforward_gain, query_bias,
        key_value_bias, query_weight, key_value_weight, output_weight,
        gate_t, upper_t, down_t,
    )
    out, input_grad, sums, query_sum, output_sum, kv_all, kept, _, landing = rear_call(
        hidden, proj_cols, query_cols,
        mid, gains,
        normed_two, normed_turned, cot_part, gate_t, upper_t, down_t, other_weights, own_proj, other_proj, query_rot, kv_own,
        kv_other, attended, probs, cosine, sine, x_own, normed_one,
    )
    (
        out, input_grad, query_sum, output_sum, kv_sum, down_sum, gate_sum, upper_sum,
        attention_gain_sum, feedforward_gain_sum, query_bias_sum, kv_bias_sum,
    ) = finish_call(out, input_grad, query_sum, output_sum, kv_all, kept, landing, sums)
    bias_rows = query_cols // lax.axis_size("dp")
    query_bias_grad = lax.dynamic_slice_in_dim(
        query_bias_sum, lax.axis_index("dp") * bias_rows, bias_rows, 0
    )
    return (
        out,
        input_grad,
        attention_gain_sum,
        query_sum,
        query_bias_grad,
        kv_sum,
        kv_bias_sum,
        output_sum,
        feedforward_gain_sum,
        gate_sum,
        upper_sum,
        down_sum,
    )


def per_device(*arrays):
    sizes = tuple(lax.axis_size(axis) for axis in ("dp", "row", "col"))
    if sizes == (4, 2, LINE) and arrays[0].shape == (HALF, 2 * BLOCK):
        return fast_device(*arrays)
    return general_device(*arrays)


def solution(mesh):
    placed = (
        P("row", ("dp", "col")),
        P(("dp", "row")),
        P("row"),
        P("row", "col"),
        P("col"),
        P("row", None),
        P(),
        P("row", "col"),
        P("row"),
        P("row", "col"),
        P("row", "col"),
        P("row", "col"),
        P("row", ("dp", "col")),
    )
    return jax.shard_map(
        per_device,
        mesh=mesh,
        in_specs=placed,
        out_specs=(
            P("row", ("dp", "col")),
            P("row", ("dp", "col")),
            P("row"),
            P(("row", "dp"), "col"),
            P(("col", "dp")),
            P("row", None),
            P(),
            P(("row", "dp"), "col"),
            P("row"),
            P(("row", "dp"), "col"),
            P(("row", "dp"), "col"),
            P(("row", "dp"), "col"),
        ),
        check_vma=False,
    )
```

```python
import jax
import jax.numpy as jnp
from jax import lax
from jax.experimental import pallas as pl
from jax.experimental.pallas import tpu as pltpu
from jax.sharding import PartitionSpec as P

MODEL_WIDTH = 1536
KEYVALUE_HEADS = 2
HEAD_SIZE = 128


EPS = 1e-06
THETA = 1000000.0
NEG = -1e30


def rope_tables(position_ids):
    half_dim = HEAD_SIZE // 2
    frequencies = THETA ** (-(jnp.arange(half_dim, dtype=jnp.float32) * 2.0 / HEAD_SIZE))
    angles = position_ids.astype(jnp.float32)[:, None] * frequencies[None, :]
    cosine_values = jnp.cos(angles)
    sine_lookup = jnp.sin(angles)
    return (
        jnp.concatenate([cosine_values, cosine_values], -1),
        jnp.concatenate([sine_lookup, sine_lookup], -1),
    )


def apply_rotation(values, cosine_values, sine_lookup):
    half_dim = HEAD_SIZE // 2
    turned = jnp.concatenate([-values[..., half_dim:], values[..., :half_dim]], -1)
    return values * cosine_values[:, None, :] + turned * sine_lookup[:, None, :]


def unrotate(gradient, cosine_values, sine_lookup):
    half_dim = HEAD_SIZE // 2
    scaled = gradient * sine_lookup[:, None, :]
    turned = jnp.concatenate([scaled[..., half_dim:], -scaled[..., :half_dim]], -1)
    return gradient * cosine_values[:, None, :] + turned


def row_total(partial_value):
    return lax.psum(partial_value, "row")


def norm_forward(x_float, gain):
    squares = jnp.sum(x_float * x_float, -1)
    rinv = lax.rsqrt(row_total(squares) / MODEL_WIDTH + EPS)[:, None]
    return ((x_float * rinv * gain).astype(jnp.bfloat16), rinv)


def norm_backward(normed_grad, x_float, rinv, gain):
    scaled = normed_grad * gain
    inner = row_total(jnp.sum(scaled * x_float, -1))[:, None]
    input_part = rinv * scaled - x_float * rinv**3 * inner / MODEL_WIDTH
    gain_part = jnp.sum(normed_grad * x_float * rinv, 0)
    return (input_part, gain_part)


def column_gather(values):
    return lax.all_gather(values, "col", axis=0, tiled=True)


def column_sum(partial_value):
    return lax.psum_scatter(
        partial_value.astype(jnp.bfloat16), "col", scatter_dimension=0, tiled=True
    ).astype(jnp.float32)


def row_product(gathered, weight):
    return (
        lax.psum_scatter(
            jnp.dot(gathered, weight, preferred_element_type=jnp.float32).astype(jnp.bfloat16),
            "row",
            scatter_dimension=0,
            tiled=True,
        ).astype(jnp.float32),
        gathered,
    )


def row_project(local_part, weight):
    return lax.dot_general(
        lax.all_gather(local_part, "row", axis=0, tiled=True),
        weight,
        (((1,), (1,)), ((), ())),
        preferred_element_type=jnp.float32,
    )


def row_fold(local_part, partner, weight):
    pair_dims = (((0,), (0,)), ((), ()))

    def accumulate(block_rows):
        grad_sum = lax.dot_general(
            partner, block_rows, pair_dims, preferred_element_type=jnp.float32
        )
        if weight is None:
            return (grad_sum,)
        back_proj = lax.dot_general(
            block_rows, weight, (((1,), (1,)), ((), ())), preferred_element_type=jnp.float32
        )
        column_totals = jnp.sum(block_rows, 0, dtype=jnp.float32)
        return (grad_sum, back_proj, column_totals)

    return accumulate(lax.all_gather(local_part, "row", axis=0, tiled=True))


def causal_scores(query_rot, rotated_keys):
    scores = jnp.einsum(
        "ihd,jd->hij", query_rot, rotated_keys, preferred_element_type=jnp.float32
    ) * HEAD_SIZE ** (-0.5)
    length = query_rot.shape[0]
    allowed = jnp.arange(length)[:, None] >= jnp.arange(length)[None, :]
    return jnp.where(allowed[None], scores, NEG)


def attend(query_rot, rotated_keys, value_second_part):
    scores = causal_scores(query_rot, rotated_keys)
    row_max = jnp.max(scores, -1, keepdims=True)
    log_total = row_max + jnp.log(jnp.sum(jnp.exp(scores - row_max), -1, keepdims=True))
    probs_half = jnp.exp(scores - log_total).astype(jnp.bfloat16)
    attended = jnp.einsum(
        "hij,jd->ihd", probs_half, value_second_part, preferred_element_type=jnp.float32
    ).astype(jnp.bfloat16)
    return (attended, log_total)


def attend_back(query_rot, rotated_keys, value_second_part, attended, att_grad, log_total):
    scale = HEAD_SIZE ** (-0.5)
    softmax_probs = jnp.exp(causal_scores(query_rot, rotated_keys) - log_total)
    probs_half = softmax_probs.astype(jnp.bfloat16)
    prob_grad = jnp.einsum(
        "ihd,jd->hij", att_grad, value_second_part, preferred_element_type=jnp.float32
    )
    row_delta = jnp.einsum("ihd,ihd->hi", att_grad, attended, preferred_element_type=jnp.float32)
    score_half = (softmax_probs * (prob_grad - row_delta[:, :, None])).astype(jnp.bfloat16)
    query_grad = (
        jnp.einsum("hij,jd->ihd", score_half, rotated_keys, preferred_element_type=jnp.float32)
        * scale
    )
    key_grad = (
        jnp.einsum("hij,ihd->jd", score_half, query_rot, preferred_element_type=jnp.float32) * scale
    )
    value_grad = jnp.einsum("hij,ihd->jd", probs_half, att_grad, preferred_element_type=jnp.float32)
    return (query_grad, key_grad, value_grad)


def general_device(
    block_input,
    position_ids,
    attention_gain,
    query_weight,
    query_bias,
    key_value_weight,
    key_value_bias,
    output_weight,
    feedforward_gain,
    gate_weight,
    upper_weight,
    down_weight,
    out_cotangent,
):
    single_float_type = jnp.float32
    brain_float_type = jnp.bfloat16
    column_number = lax.axis_size("col")
    seq_len = position_ids.shape[0]
    heads_here = query_weight.shape[1] // HEAD_SIZE
    query_cols = query_weight.shape[1]
    hidden_cols = gate_weight.shape[1]
    key_value_head = lax.axis_index("col") // (column_number // KEYVALUE_HEADS)
    key_start = key_value_head * HEAD_SIZE
    value_offset = KEYVALUE_HEADS * HEAD_SIZE + key_value_head * HEAD_SIZE
    keyval_local = jnp.concatenate(
        [
            lax.dynamic_slice_in_dim(key_value_weight, key_start, HEAD_SIZE, 1),
            lax.dynamic_slice_in_dim(key_value_weight, value_offset, HEAD_SIZE, 1),
        ],
        1,
    )
    bias_local = jnp.concatenate(
        [
            lax.dynamic_slice_in_dim(key_value_bias, key_start, HEAD_SIZE, 0),
            lax.dynamic_slice_in_dim(key_value_bias, value_offset, HEAD_SIZE, 0),
        ],
        0,
    )
    proj_weight = jnp.concatenate([query_weight, keyval_local], 1)
    proj_bias = jnp.concatenate([query_bias, bias_local], 0)
    pair_weight = jnp.concatenate([gate_weight, upper_weight], 1)
    cosine_values, sine_lookup = rope_tables(position_ids)
    x_float = block_input.T.astype(single_float_type)
    cot_local = out_cotangent.T
    normed_one, rinv_one = norm_forward(x_float, attention_gain)
    normed_one_all = column_gather(normed_one)
    proj_out = row_product(normed_one_all, proj_weight)[0] + proj_bias
    query_rot = apply_rotation(
        proj_out[:, :query_cols].reshape(seq_len, heads_here, HEAD_SIZE), cosine_values, sine_lookup
    ).astype(brain_float_type)
    rotated_keys = apply_rotation(
        proj_out[:, query_cols : query_cols + HEAD_SIZE][:, None, :], cosine_values, sine_lookup
    )[:, 0].astype(brain_float_type)
    value_second_part = proj_out[:, query_cols + HEAD_SIZE :].astype(brain_float_type)
    attended, log_total = attend(query_rot, rotated_keys, value_second_part)
    attended_flat = attended.reshape(seq_len, query_cols)
    hidden_res = x_float + column_sum(row_project(attended_flat, output_weight))
    normed_two, rinv_two = norm_forward(hidden_res, feedforward_gain)
    normed_two_all = column_gather(normed_two)
    gate_upper, normed_two_seq = row_product(normed_two_all, pair_weight)
    gate_lin = gate_upper[:, :hidden_cols]
    upper_lin = gate_upper[:, hidden_cols:]
    sigmoid_gate = jax.nn.sigmoid(gate_lin)
    activated = (gate_lin * sigmoid_gate * upper_lin).astype(brain_float_type)
    block_output = hidden_res + column_sum(row_project(activated, down_weight))
    cotangent_all = column_gather(cot_local)
    act_grad = row_product(cotangent_all, down_weight)[0]
    down_grad = row_fold(activated, cotangent_all, None)[0]
    gate_grad = act_grad * upper_lin * sigmoid_gate * (1.0 + gate_lin * (1.0 - sigmoid_gate))
    upper_grad = act_grad * gate_lin * sigmoid_gate
    pair_grad_half = jnp.concatenate([gate_grad, upper_grad], 1).astype(brain_float_type)
    folded_two = row_fold(pair_grad_half, normed_two_all, pair_weight)
    pair_weight_grad = folded_two[0]
    spread_two = folded_two[1]
    normed_two_grad = column_sum(spread_two)
    hidden_part, ffn_gain_part = norm_backward(
        normed_two_grad, hidden_res, rinv_two, feedforward_gain
    )
    hidden_grad = cot_local.astype(single_float_type) + hidden_part
    hidden_half = hidden_grad.astype(brain_float_type)
    hidden_all = column_gather(hidden_half)
    att_grad = (
        row_product(hidden_all, output_weight)[0]
        .astype(brain_float_type)
        .reshape(seq_len, heads_here, HEAD_SIZE)
    )
    output_grad = row_fold(attended_flat, hidden_all, None)[0]
    query_grad, key_grad, value_grad = attend_back(
        query_rot, rotated_keys, value_second_part, attended, att_grad, log_total
    )
    query_half = (
        unrotate(query_grad, cosine_values, sine_lookup)
        .astype(brain_float_type)
        .reshape(seq_len, query_cols)
    )
    key_half = unrotate(key_grad[:, None, :], cosine_values, sine_lookup)[:, 0].astype(
        brain_float_type
    )
    value_grad_half = value_grad.astype(brain_float_type)
    proj_grad_half = jnp.concatenate([query_half, key_half, value_grad_half], 1)
    folded_one = row_fold(proj_grad_half, normed_one_all, proj_weight)
    projection_weight_gradient = folded_one[0]
    normed_one_grad = column_sum(folded_one[1])
    proj_bias_grad = folded_one[2]
    input_part, attn_gain_part = norm_backward(normed_one_grad, x_float, rinv_one, attention_gain)
    input_grad = hidden_grad + input_part
    key_value_gradient = jnp.zeros(
        (projection_weight_gradient.shape[0], 2 * KEYVALUE_HEADS * HEAD_SIZE), single_float_type
    )
    key_value_gradient = lax.dynamic_update_slice_in_dim(
        key_value_gradient,
        projection_weight_gradient[:, query_cols : query_cols + HEAD_SIZE],
        key_start,
        1,
    )
    key_value_gradient = lax.dynamic_update_slice_in_dim(
        key_value_gradient, projection_weight_gradient[:, query_cols + HEAD_SIZE :], value_offset, 1
    )
    key_value_bias_gradient = jnp.zeros((2 * KEYVALUE_HEADS * HEAD_SIZE,), single_float_type)
    key_value_bias_gradient = lax.dynamic_update_slice_in_dim(
        key_value_bias_gradient, proj_bias_grad[query_cols : query_cols + HEAD_SIZE], key_start, 0
    )
    key_value_bias_gradient = lax.dynamic_update_slice_in_dim(
        key_value_bias_gradient, proj_bias_grad[query_cols + HEAD_SIZE :], value_offset, 0
    )
    shared = (
        lax.psum(key_value_gradient.astype(jnp.bfloat16), ("dp", "col")).astype(jnp.float32),
        lax.psum(key_value_bias_gradient.astype(jnp.bfloat16), ("dp", "col")).astype(jnp.float32),
        lax.psum(attn_gain_part.astype(jnp.bfloat16), ("dp", "col")).astype(jnp.float32),
        lax.psum(ffn_gain_part.astype(jnp.bfloat16), ("dp", "col")).astype(jnp.float32),
    )
    summed = (
        lax.psum_scatter(
            projection_weight_gradient[:, :query_cols].astype(jnp.bfloat16),
            "dp",
            scatter_dimension=0,
            tiled=True,
        ).astype(jnp.float32),
        lax.psum_scatter(
            proj_bias_grad[:query_cols].astype(jnp.bfloat16), "dp", scatter_dimension=0, tiled=True
        ).astype(jnp.float32),
        lax.psum_scatter(
            output_grad.astype(jnp.bfloat16), "dp", scatter_dimension=0, tiled=True
        ).astype(jnp.float32),
        lax.psum_scatter(
            pair_weight_grad[:, :hidden_cols].astype(jnp.bfloat16),
            "dp",
            scatter_dimension=0,
            tiled=True,
        ).astype(jnp.float32),
        lax.psum_scatter(
            pair_weight_grad[:, hidden_cols:].astype(jnp.bfloat16),
            "dp",
            scatter_dimension=0,
            tiled=True,
        ).astype(jnp.float32),
        lax.psum_scatter(
            down_grad.astype(jnp.bfloat16), "dp", scatter_dimension=0, tiled=True
        ).astype(jnp.float32),
    )
    return (
        block_output.T,
        input_grad.T,
        shared[2],
        summed[0],
        summed[1],
        shared[0],
        shared[1],
        summed[2],
        shared[3],
        summed[3],
        summed[4],
        summed[5],
    )


MESH_ID = pl.DeviceIdType.MESH
F32 = jnp.float32
BF16 = jnp.bfloat16
LINE = 4
BLOCK = 128
SUB = 2
PART = BLOCK // SUB
LOCAL = LINE * BLOCK
HALF = MODEL_WIDTH // 2
UNIT = MODEL_WIDTH // 8
VMEM_SPEC = pl.BlockSpec(memory_space=pltpu.VMEM)
ANY_SPEC = pl.BlockSpec(memory_space=pl.ANY)
PAIR_ROWS = (((0,), (0,)), ((), ()))
PAIR_COLS = (((1,), (1,)), ((), ()))
SCALE = HEAD_SIZE ** (-0.5)
DMA = pltpu.SemaphoreType.DMA


def greet(me, others):
    barrier = pltpu.get_barrier_semaphore()
    for axis, index in others:
        pl.semaphore_signal(barrier, 1, device_id={axis: index}, device_id_type=MESH_ID)

    @pl.when(me > 0)
    def _():
        pl.semaphore_signal(barrier, 1, device_id={"col": me - 1}, device_id_type=MESH_ID)

    @pl.when(me < LINE - 1)
    def _():
        pl.semaphore_signal(barrier, 1, device_id={"col": me + 1}, device_id_type=MESH_ID)

    @pl.when((me > 0) & (me < LINE - 1))
    def _():
        pl.semaphore_wait(barrier, 2 + len(others))

    @pl.when((me == 0) | (me == LINE - 1))
    def _():
        pl.semaphore_wait(barrier, 1 + len(others))


def aligned(start, size, to=BLOCK):
    return pl.ds(pl.multiple_of(start, to), size)


def block_rows(index):
    return aligned(index * BLOCK, BLOCK)


def send(src, dst, send_sem, recv_sem, axis, to):
    return pltpu.make_async_remote_copy(
        src, dst, send_sem, recv_sem, device_id={axis: to}, device_id_type=MESH_ID
    )


def landed(ref, sem):
    pltpu.make_async_copy(ref, ref, sem).wait()


class Gather:
    def __init__(self, me, all_ref, sends, recv):
        self.me, self.all_ref, self.sends, self.recv = me, all_ref, sends, recv

    def rows(self, j, p):
        return self.all_ref.at[aligned(j * BLOCK + p * PART, PART, PART)]

    def copy(self, j, p, s, side):
        rows = self.rows(j, p)
        return send(
            rows, rows, self.sends.at[side, s, p], self.recv.at[j, p], "col",
            self.me + 1 - 2 * side,
        )

    def has_next(self, side):
        to = self.me + 1 - 2 * side
        return (to >= 0) & (to < LINE)

    def step(self, s, wait=True, forward=True):
        @pl.loop(0, 2 * SUB)
        def _(i):
            side, p = lax.rem(i, 2), i // 2
            j = self.me - (1 - 2 * side) * s

            @pl.when((j >= 0) & (j < LINE))
            def _():
                if s and wait:
                    landed(self.rows(j, p), self.recv.at[j, p])

                if forward and s < LINE - 1:

                    @pl.when(self.has_next(side))
                    def _():
                        self.copy(j, p, s, side).start()

    def run_each(self, s, each):
        if s == 0:
            each(self.me)
            return

        @pl.loop(0, 2)
        def _(side):
            j = self.me - (1 - 2 * side) * s

            @pl.when((j >= 0) & (j < LINE))
            def _():
                each(j)

    def drain(self, first=0, last=LINE - 1):
        for s in range(first, last):

            @pl.loop(0, 2)
            def _(side):
                j = self.me - (1 - 2 * side) * s

                @pl.when((j >= 0) & (j < LINE) & self.has_next(side))
                def _():
                    for p in range(SUB):
                        self.copy(self.me, p, s, side).wait_send()


class Scatter:
    def __init__(self, me, block_of, landing, sends, recv):
        self.me, self.block_of, self.landing = me, block_of, landing
        self.sends, self.recv = sends, recv

    def rows(self, side, j, p):
        return self.landing.at[side, j, pl.ds(p * PART, PART)]

    def copy(self, side, j, p):
        rows = self.rows(side, j, p)
        return send(
            rows, rows, self.sends.at[side, j, p], self.recv.at[side, j, p], "col",
            self.me + 1 - 2 * side,
        )

    def has_last(self, side):
        came = self.me - 1 + 2 * side
        return (came >= 0) & (came < LINE)

    def step(self, s):
        far = jnp.where(self.me < LINE // 2, 1, 0)

        @pl.loop(0, 2)
        def _(i):
            side = lax.rem(i + far, 2)
            j = self.me + (1 - 2 * side) * s

            @pl.when((j >= 0) & (j < LINE))
            def _():
                mine = self.block_of(j)
                for p in range(SUB):
                    term = mine[p * PART : (p + 1) * PART]
                    rows = self.rows(side, j, p)

                    @pl.when(self.has_last(side))
                    def _():
                        landed(rows, self.recv.at[side, j, p])
                        rows[...] = (term + rows[...].astype(F32)).astype(BF16)

                    @pl.when(jnp.logical_not(self.has_last(side)))
                    def _():
                        rows[...] = term.astype(BF16)

                    self.copy(side, j, p).start()

    def finish(self, out_ref):
        me = self.me
        out_ref[...] = self.block_of(me)

        @pl.loop(0, 2)
        def _(side):
            @pl.when(self.has_last(side))
            def _():
                for p in range(SUB):
                    rows = self.rows(side, me, p)
                    landed(rows, self.recv.at[side, me, p])
                    out_ref[p * PART : (p + 1) * PART] += rows[...].astype(F32)

    def drain(self):
        for s in range(1, LINE):

            @pl.loop(0, 2)
            def _(side):
                j = self.me + (1 - 2 * side) * s

                @pl.when((j >= 0) & (j < LINE))
                def _():
                    for p in range(SUB):
                        self.copy(side, j, p).wait_send()


def gather_sems():
    return [DMA((2, LINE, SUB)), DMA((LINE, SUB))]


def scatter_sems():
    return [DMA((2, LINE, SUB)), DMA((2, LINE, SUB))]


def dot(a, b, dims=(((1,), (0,)), ((), ()))):
    return lax.dot_general(a, b, dims, preferred_element_type=F32)


def turn(values):
    return pltpu.roll(values, HEAD_SIZE // 2, 1)


def norm_scale(values):
    return lax.rsqrt(jnp.sum(values * values, -1, keepdims=True) / MODEL_WIDTH + EPS)


def shape(rows, cols, dtype=BF16):
    return jax.ShapeDtypeStruct((rows, cols), dtype)


def attend_local(query_ref, own_ref, other_ref, attended_ref, probs_ref, r):
    rows = 2 * BLOCK
    shape = (rows, rows)
    at_row = lax.broadcasted_iota(jnp.int32, shape, 0)
    at_col = lax.broadcasted_iota(jnp.int32, shape, 1)
    own_mask = at_row >= at_col
    other_mask = at_col // BLOCK < at_row // BLOCK + r
    heads = query_ref.shape[1] // HEAD_SIZE
    for s in range(2):
        part = slice(s * rows, (s + 1) * rows)
        for h in range(heads):
            cols = slice(h * HEAD_SIZE, (h + 1) * HEAD_SIZE)
            query = query_ref[part, cols]
            own = jnp.where(own_mask, dot(query, own_ref[part, :HEAD_SIZE], PAIR_COLS) * SCALE, NEG)
            other = jnp.where(
                other_mask, dot(query, other_ref[part, :HEAD_SIZE], PAIR_COLS) * SCALE, NEG
            )
            top = jnp.maximum(
                jnp.max(own, -1, keepdims=True), jnp.max(other, -1, keepdims=True)
            )
            total = jnp.sum(jnp.exp(own - top), -1, keepdims=True) + jnp.sum(
                jnp.exp(other - top), -1, keepdims=True
            )
            log_total = top + jnp.log(total)
            own = jnp.exp(own - log_total).astype(BF16)
            other = jnp.exp(other - log_total).astype(BF16)
            attended_ref[part, cols] = (
                dot(own, own_ref[part, HEAD_SIZE:]) + dot(other, other_ref[part, HEAD_SIZE:])
            ).astype(BF16)
            probs_ref[s * heads + h, :, :rows] = own
            probs_ref[s * heads + h, :, rows:] = other


def attend_back_body(
    query_ref, own_ref, other_ref, attended_ref, probs_ref, grad_ref, cos_ref, sin_ref,
    query_grad_ref, own_grad_ref, other_grad_ref,
):
    rows = 2 * BLOCK
    heads = query_ref.shape[1] // HEAD_SIZE
    for s in range(2):
        part = slice(s * rows, (s + 1) * rows)
        own_key, other_key = own_ref[part, :HEAD_SIZE], other_ref[part, :HEAD_SIZE]
        own_value, other_value = own_ref[part, HEAD_SIZE:], other_ref[part, HEAD_SIZE:]
        sums = [jnp.zeros((rows, HEAD_SIZE), F32) for _ in range(4)]
        for h in range(heads):
            cols = slice(h * HEAD_SIZE, (h + 1) * HEAD_SIZE)
            query, grad = query_ref[part, cols], grad_ref[part, cols]
            own_p = probs_ref[s * heads + h, :, :rows]
            other_p = probs_ref[s * heads + h, :, rows:]
            delta = jnp.sum(
                grad.astype(F32) * attended_ref[part, cols].astype(F32), -1, keepdims=True
            )
            own_s = (own_p.astype(F32) * (dot(grad, own_value, PAIR_COLS) - delta)).astype(BF16)
            other_s = (other_p.astype(F32) * (dot(grad, other_value, PAIR_COLS) - delta)).astype(BF16)
            query_grad = (dot(own_s, own_key) + dot(other_s, other_key)) * SCALE
            query_grad_ref[part, cols] = (
                query_grad * cos_ref[part] - turn(query_grad) * sin_ref[part]
            ).astype(BF16)
            for i, (weights, partner) in enumerate(
                ((own_s, query), (own_p, grad), (other_s, query), (other_p, grad))
            ):
                sums[i] = sums[i] + dot(weights, partner, PAIR_ROWS)
        own_grad_ref[part, :HEAD_SIZE] = sums[0] * SCALE
        own_grad_ref[part, HEAD_SIZE:] = sums[1]
        other_grad_ref[part, :HEAD_SIZE] = (sums[2] * SCALE).astype(BF16)
        other_grad_ref[part, HEAD_SIZE:] = sums[3].astype(BF16)


PIECES = 6


def front_body(
    input_ref, cot_in_ref, table_ref, attention_gain_ref, feedforward_gain_ref, query_bias_ref,
    kv_bias_ref, query_w_ref, kv_w_ref, output_w_ref,
    gate_hbm, upper_hbm, down_hbm,
    x_hbm, normed_hbm, query_hbm, kv_hbm, kv_other_hbm, cos_hbm, sin_hbm, gains_ref,
    attended_hbm, probs_hbm, mid_hbm, normed_two_hbm, turned_hbm, cot_hbm, proj_hbm, proj_other_hbm,
    weights_other_hbm,
    x_ref, normed_ref, query_ref, kv_ref, kv_other_ref, cos_ref, sin_ref,
    attended_ref, probs_ref, mid_ref, normed_two_ref, turned_ref, cot_ref, proj_ref, proj_other_ref,
    passing, tables, bias_ref, small_ref, landing, store_sems,
    swap_sends, swap_recv, piece_sends, piece_recv, kv_sends, kv_recv,
    g_sends, g_recv, c_sends, c_recv, n_sends, n_recv, s_sends, s_recv,
):
    me, r, d = lax.axis_index("col"), lax.axis_index("row"), lax.axis_index("dp")
    y, core = d // 2, lax.rem(d, 2)
    x_to, y_to, core_to = 1 - r, 2 * (1 - y) + core, 2 * y + 1 - core
    query_cols = query_ref.shape[1]
    proj_cols = query_cols + 2 * HEAD_SIZE
    quarter = HALF // 2
    my_rows = aligned(core * quarter, quarter, quarter)
    its_rows = aligned((1 - core) * quarter, quarter, quarter)
    eighth = quarter // 2
    to_y = aligned(core * quarter + y * eighth, eighth, eighth)
    in_cols, out_cols = pl.ds(0, proj_cols), pl.ds(proj_cols, query_cols)
    kv_width = KEYVALUE_HEADS * HEAD_SIZE
    kv_at = me // (LINE // KEYVALUE_HEADS) * HEAD_SIZE

    stores = [
        pltpu.make_async_copy(src, dst, store_sems.at[i])
        for i, (src, dst) in enumerate(
            (
                (x_ref, x_hbm), (cos_ref, cos_hbm), (sin_ref, sin_hbm), (proj_ref, proj_hbm),
                (normed_ref, normed_hbm), (query_ref, query_hbm), (kv_ref, kv_hbm),
                (kv_other_ref, kv_other_hbm), (probs_ref, probs_hbm), (attended_ref, attended_hbm),
                (proj_other_ref, proj_other_hbm), (mid_ref, mid_hbm),
                (normed_two_ref, normed_two_hbm), (turned_ref, turned_hbm), (cot_ref, cot_hbm),
            )
        )
    ]

    low = 0
    for vector_ref in (attention_gain_ref, feedforward_gain_ref, query_bias_ref, kv_bias_ref):
        size = vector_ref.shape[0]
        small_ref[0, low : low + size] = vector_ref[...]
        low += size

    passing[0] = input_ref[:, block_rows(1 - r)].T
    x_ref[:, :HALF] = input_ref[:, block_rows(r)].T
    proj_ref[:, :query_cols] = query_w_ref[...]
    for i in range(2):
        proj_ref[:, query_cols + i * HEAD_SIZE : query_cols + (i + 1) * HEAD_SIZE] = kv_w_ref[
            :, aligned(i * kv_width + kv_at, HEAD_SIZE)
        ]
    greet(me, [("row", x_to), ("dp", y_to), ("dp", core_to)])

    swaps = [
        (passing.at[0], x_ref.at[:, HALF:], "row", x_to),
        (small_ref.at[:, :HALF], gains_ref.at[pl.ds(0, 1), HALF:], "row", x_to),
        (small_ref.at[:, HALF : 2 * HALF], gains_ref.at[pl.ds(1, 1), HALF:], "row", x_to),
        (proj_ref.at[to_y, in_cols], proj_other_ref.at[to_y, in_cols], "row", x_to),
        (table_ref.at[block_rows(1 - r)], tables.at[pl.ds(0, BLOCK)], "row", x_to),
        (table_ref.at[block_rows(3 - r)], tables.at[pl.ds(BLOCK, BLOCK)], "row", x_to),
        (passing.at[1], cot_ref.at[block_rows(me), HALF:], "row", x_to),
        (proj_ref.at[to_y, out_cols], proj_other_ref.at[to_y, out_cols], "row", x_to),
        (proj_other_ref.at[to_y, in_cols], proj_other_ref.at[to_y, in_cols], "dp", y_to),
        (proj_other_ref.at[to_y, out_cols], proj_other_ref.at[to_y, out_cols], "dp", y_to),
        (proj_other_ref.at[my_rows, in_cols], proj_other_ref.at[my_rows, in_cols], "dp", core_to),
        (proj_other_ref.at[my_rows, out_cols], proj_other_ref.at[my_rows, out_cols], "dp", core_to),
    ]

    def swap_copy(i):
        src, dst, axis, to = swaps[i]
        return send(src, dst, swap_sends.at[i], swap_recv.at[i], axis, to)

    def swap_landed(i):
        swap_copy(i).wait_recv()

    rows = gate_hbm.shape[0] // 4
    owns = (gate_hbm, upper_hbm, down_hbm)

    def piece(i, of_y):
        return aligned((of_y * 2 + i % 2) * rows, rows, rows)

    def piece_copy(i, way):
        m = i // 2
        of_y = 1 - y if way == 3 else y
        at = weights_other_hbm.at[m, piece(i, of_y), my_rows]
        src = owns[m].at[piece(i, of_y), my_rows] if way == 0 else at
        axis, to = (("row", x_to), ("dp", y_to), ("dp", core_to), ("dp", core_to))[way]
        return send(src, at, piece_sends.at[way, i], piece_recv.at[way, i], axis, to)

    def relay_x(i):
        piece_copy(i, 0).wait_recv()
        piece_copy(i, 1).start()
        piece_copy(i, 2).start()

    def relay_y(i):
        piece_copy(i, 1).wait_recv()
        piece_copy(i, 3).start()

    for i in range(6):
        swap_copy(i).start()
    passing[1] = cot_in_ref[:, block_rows(1 - r)].T
    proj_ref[:, proj_cols:] = output_w_ref[...]
    swap_copy(6).start()
    swap_copy(7).start()
    piece_copy(0, 0).start()
    cot_ref[block_rows(me), :HALF] = cot_in_ref[:, block_rows(r)].T
    gains_ref[0:1, :HALF] = small_ref[:, :HALF]
    gains_ref[1:2, :HALF] = small_ref[:, HALF : 2 * HALF]
    bias_ref[:, :query_cols] = small_ref[:, 2 * HALF : 2 * HALF + query_cols]
    for i in range(2):
        bias_ref[:, query_cols + i * HEAD_SIZE : query_cols + (i + 1) * HEAD_SIZE] = small_ref[
            :, aligned(2 * HALF + query_cols + i * kv_width + kv_at, HEAD_SIZE)
        ]
    swap_landed(0)
    swap_landed(1)
    swap_landed(2)
    x = x_ref[...].astype(F32)
    normed_ref[block_rows(me)] = (x * norm_scale(x) * gains_ref[0:1]).astype(BF16)
    gather = Gather(me, normed_ref, g_sends, g_recv)
    gather.step(0)

    lane = lax.broadcasted_iota(jnp.int32, (BLOCK, HEAD_SIZE), 1)
    first = lane < HEAD_SIZE // 2
    swap_landed(3)
    swap_copy(8).start()
    gather.step(1)
    swap_landed(8)
    swap_copy(10).start()
    swap_landed(4)
    swap_landed(5)
    for i in range(4):
        if i < 2:
            table = table_ref[block_rows(r + 2 * i)]
        else:
            table = tables[(i - 2) * BLOCK : (i - 1) * BLOCK]
        turned = turn(table)
        at = block_rows((r if i < 2 else 1 - r) * 2 + i % 2)
        cos_ref[at] = jnp.where(first, table, turned)
        sin_ref[at] = jnp.where(first, -turned, table)
    swap_landed(10)

    def kv_copy(j):
        at = block_rows(j)
        return send(
            kv_ref.at[at], kv_other_ref.at[at], kv_sends.at[j], kv_recv.at[j], "row", x_to
        )

    def each(j):
        at = block_rows(j)
        block = normed_ref[at]
        out = dot(block[:, :HALF], proj_ref[:, :proj_cols])
        out = out + dot(block[:, HALF:], proj_other_ref[:, :proj_cols]) + bias_ref[...]
        cosine, sine = cos_ref[at], sin_ref[at]
        for h in range(query_cols // HEAD_SIZE + 1):
            head = out[:, h * HEAD_SIZE : (h + 1) * HEAD_SIZE]
            turned = (head * cosine + turn(head) * sine).astype(BF16)
            if h * HEAD_SIZE < query_cols:
                query_ref[at, h * HEAD_SIZE : (h + 1) * HEAD_SIZE] = turned
            else:
                kv_ref[at, :HEAD_SIZE] = turned
        kv_ref[at, HEAD_SIZE:] = out[:, query_cols + HEAD_SIZE :].astype(BF16)
        kv_copy(j).start()

    gather.run_each(0, each)
    gather.run_each(1, each)
    gather.step(2)
    gather.run_each(2, each)
    swap_landed(7)
    swap_copy(9).start()
    gather.step(3)
    gather.run_each(3, each)
    for i in range(1, PIECES):
        piece_copy(i, 0).start()
    swap_landed(6)
    cot_gather = Gather(me, cot_ref, c_sends, c_recv)
    cot_gather.step(0)
    swap_landed(9)
    swap_copy(11).start()
    relay_x(0)
    for j in range(LINE):
        kv_copy(j).wait_recv()
    attend_local(query_ref, kv_ref, kv_other_ref, attended_ref, probs_ref, r)
    swap_landed(11)

    def block_of(j):
        block = attended_ref[block_rows(j)]
        return jnp.concatenate(
            [
                dot(block, proj_ref[:, proj_cols:], PAIR_COLS),
                dot(block, proj_other_ref[:, proj_cols:], PAIR_COLS),
            ],
            1,
        )

    scatter = Scatter(me, block_of, landing, s_sends, s_recv)
    scatter.step(3)
    for store in stores[:11]:
        store.start()
    relay_x(1)
    scatter.step(2)
    relay_x(2)
    scatter.step(1)
    relay_y(0)
    relay_x(3)
    scatter.finish(mid_ref)
    mid = mid_ref[...] + x_ref[...].astype(F32)
    mid_ref[...] = mid
    normed_two_ref[block_rows(me)] = (mid * norm_scale(mid) * gains_ref[1:2]).astype(BF16)

    def turn_block(j):
        turned_ref[:, block_rows(j)] = normed_two_ref[block_rows(j)].T

    second = Gather(me, normed_two_ref, n_sends, n_recv)
    second.step(0)
    stores[11].start()
    second.run_each(0, turn_block)
    relay_y(1)
    relay_x(4)
    second.step(1)
    second.run_each(1, turn_block)
    relay_y(2)
    relay_x(5)
    second.step(2)
    second.run_each(2, turn_block)
    relay_y(3)
    second.step(3)
    second.run_each(3, turn_block)
    relay_y(4)
    stores[12].start()
    stores[13].start()
    cot_gather.step(1, forward=False)
    stores[14].start()
    relay_y(5)
    for i in range(PIECES):
        for way in (2, 3):
            of_y = y if way == 2 else 1 - y
            landed(weights_other_hbm.at[i // 2, piece(i, of_y), its_rows], piece_recv.at[way, i])
        for way in range(4):
            piece_copy(i, way).wait_send()
    for i in range(len(swaps)):
        swap_copy(i).wait_send()
    for j in range(LINE):
        kv_copy(j).wait_send()
    for store in stores:
        store.wait()
    gather.drain()
    cot_gather.drain(0, 1)
    second.drain()
    scatter.drain()


def front_call(proj_cols, query_cols, hidden, *args):
    heads = query_cols // HEAD_SIZE
    gains = shape(2, MODEL_WIDTH, F32)
    outs = [
        shape(BLOCK, MODEL_WIDTH),
        shape(LOCAL, MODEL_WIDTH),
        shape(LOCAL, query_cols),
        shape(LOCAL, 2 * HEAD_SIZE),
        shape(LOCAL, 2 * HEAD_SIZE),
        shape(LOCAL, HEAD_SIZE, F32),
        shape(LOCAL, HEAD_SIZE, F32),
        gains,
        shape(LOCAL, query_cols),
        jax.ShapeDtypeStruct((2 * heads, 2 * BLOCK, 4 * BLOCK), BF16),
        shape(BLOCK, MODEL_WIDTH, F32),
        shape(LOCAL, MODEL_WIDTH),
        shape(MODEL_WIDTH, LOCAL),
        shape(LOCAL, MODEL_WIDTH),
        shape(HALF, proj_cols + query_cols),
        shape(HALF, proj_cols + query_cols),
        jax.ShapeDtypeStruct((3, hidden, HALF), BF16),
    ]
    return pl.pallas_call(
        front_body,
        out_shape=outs,
        in_specs=[VMEM_SPEC] * 10 + [ANY_SPEC] * 3,
        out_specs=[VMEM_SPEC if out is gains else ANY_SPEC for out in outs],
        scratch_shapes=[pltpu.VMEM(out.shape, out.dtype) for out in outs[:-1] if out is not gains]
        + [
            pltpu.VMEM((2, BLOCK, HALF), BF16),
            pltpu.VMEM((2 * BLOCK, HEAD_SIZE), F32),
            pltpu.VMEM((1, proj_cols), F32),
            pltpu.VMEM((1, 2 * HALF + query_cols + 2 * KEYVALUE_HEADS * HEAD_SIZE), F32),
            pltpu.VMEM((2, LINE, BLOCK, MODEL_WIDTH), BF16),
            DMA((15,)),
            DMA((12,)),
            DMA((12,)),
            DMA((4, PIECES)),
            DMA((4, PIECES)),
            DMA((LINE,)),
            DMA((LINE,)),
        ]
        + gather_sems() * 3
        + scatter_sems(),
        compiler_params=pltpu.CompilerParams(
            collective_id=1, has_side_effects=True, vmem_limit_bytes=67_043_328
        ),
        cost_estimate=pl.CostEstimate(
            flops=4 * 10**9, bytes_accessed=40_000_000, transcendentals=0
        ),
        name="front",
    )(*args)


DOWN, GATE, UPPER, CHAIN = 0, 1, 2, 3
UNITS = ((1, 1), (1, 0), (0, 1), (0, 0))
TILE = 256


def add_into(total_ref, term_ref, cols):
    @pl.loop(0, total_ref.shape[0] // 32)
    def _(i):
        at = aligned(i * 32, 32, 32)
        total_ref[at, cols] = (
            total_ref[at, cols].astype(F32) + term_ref[at, cols].astype(F32)
        ).astype(BF16)


def rear_body(
    mid_ref, gains_ref,
    normed_two_hbm, turned_hbm, cot_hbm, gate_hbm, upper_hbm, down_hbm, other_hbm, proj_hbm, proj_other_hbm, query_hbm, kv_hbm,
    kv_other_hbm, attended_hbm, probs_hbm, cos_hbm, sin_hbm, x_hbm, normed_one_hbm,
    out_ref, in_ref, small_ref, query_w_ref, output_w_ref, kv_all_ref, kept_hbm, land2_hbm, land3_hbm,
    cot_ref, activated_ref, gate_grad_ref, upper_grad_ref, out_part_ref, back_part_ref, turned_ref,
    kv_got_ref, got_ref, out_landing, landing, sums, gives, gots,
    chain_gots, chain_land2, chain_land3, kv_line, small_line, small_swap, small_give,
    small_group,
    load_sems, w_sems, c_sends, c_recv, o_sends, o_recv, r_sends, r_recv, a_sends, a_recv,
    give_sends, give_recv, two_sends, two_recv, three_sends, three_recv, stage_sem, kept_sems,
    swap_sends, swap_recv, kv_sends, kv_recv, kvd_sends, kvd_recv, line_sends, line_recv,
    small_sends, small_recv, credit,
):
    me, r, d = lax.axis_index("col"), lax.axis_index("row"), lax.axis_index("dp")
    y, core = d // 2, lax.rem(d, 2)
    x_to, y_to, core_to = 1 - r, 2 * (1 - y) + core, 2 * y + 1 - core
    diagonal_to = 2 * (1 - y) + 1 - core
    hidden = activated_ref.shape[1]
    query_cols = query_w_ref.shape[1]
    proj_cols = query_cols + 2 * HEAD_SIZE
    chain_cols = proj_cols + query_cols
    owns = (gate_hbm, upper_hbm, down_hbm)

    def cot_loads(act):
        for i in range(3):
            j = me - 1 + i

            @pl.when((j >= 0) & (j < LINE))
            def _():
                rows = block_rows(j)
                act(pltpu.make_async_copy(cot_hbm.at[rows], cot_ref.at[rows], load_sems.at[i]))

    turned_load = pltpu.make_async_copy(turned_hbm, turned_ref.at[1], load_sems.at[14])
    turned_load.start()
    cot_loads(lambda copy: copy.start())

    halves = {m: (hidden // 2 // BLOCK + 2) * BLOCK for m in (DOWN, GATE, UPPER)}
    halves[CHAIN] = chain_cols // 2

    def columns(m, axis):
        width = chain_cols if m == CHAIN else hidden
        return pl.ds(0, halves[m]) if axis == "row" else pl.ds(halves[m], width - halves[m])

    def unit_rows(h, rel):
        of_y = 1 - y if rel else y
        return aligned(h * HALF + of_y * 2 * UNIT, 2 * UNIT)

    def split(res, keep_ref, give_ref, at):
        low, high = res[:UNIT], res[UNIT:]
        keep_ref[:, at] = jnp.where(core == 0, low, high).astype(BF16)
        give_ref[:, at] = jnp.where(core == 0, high, low).astype(BF16)

    order = [
        (DOWN, 0), (DOWN, 1), (DOWN, 2), (UPPER, 0), (UPPER, 1), (UPPER, 2), (DOWN, 3),
        (GATE, 0), (GATE, 1), (GATE, 2), (UPPER, 3), (GATE, 3),
    ]
    columns_of = {DOWN: activated_ref, GATE: gate_grad_ref, UPPER: upper_grad_ref}
    ring = 3

    def total_of(m, h, rel):
        return sums.at[m * 4 + h * 2 + rel]

    def give_copy(u):
        return send(
            gives.at[u % 2], gots.at[u % ring], give_sends.at[u], give_recv.at[u], "dp", core_to
        )

    def compute(u):
        m, i = order[u]
        h, rel = UNITS[i]
        if u >= 2:
            give_copy(u - 2).wait_send()
        left = 0 if m == DOWN else 1
        rows = unit_rows(h, rel)
        tile = 512

        def run(at):
            res = dot(turned_ref[left, rows], columns_of[m][:, at])
            split(res, total_of(m, h, rel), gives.at[u % 2], at)

        @pl.loop(0, hidden // tile)
        def _(i):
            run(aligned(i * tile, tile))

        if hidden % tile:
            run(pl.ds(hidden // tile * tile, hidden % tile))
        if u >= ring:
            pl.semaphore_wait(credit, 1)
        give_copy(u).start()

    def two_copy(m, k, chain_sums=None):
        h, rel = ((1, 0), (1, 1), (0, 1), (1, 1))[k]
        axis, to = (("row", x_to), ("dp", y_to))[k // 2]
        at = columns(m, axis)
        if m == CHAIN:
            src, dst = chain_sums.at[h * 2 + rel, :, at], chain_land2.at[k % 2, :, at]
        else:
            src, dst = total_of(m, h, rel).at[:, at], land2_hbm.at[m * 2 + k % 2, :, at]
        return send(src, dst, two_sends.at[m, k], two_recv.at[m, k], axis, to)

    def combine(u):
        m, i = order[u]
        h, rel = UNITS[i]
        give_copy(u).wait_recv()
        add_into(total_of(m, h, rel), gots.at[u % ring], pl.ds(0, hidden))
        if u < len(order) - ring:
            pl.semaphore_signal(credit, 1, device_id={"dp": core_to}, device_id_type=MESH_ID)
        for k in {(1, 1): (1, 3), (1, 0): (0,), (0, 1): (2,), (0, 0): ()}[h, rel]:
            two_copy(m, k).start()

    def three_copy(m, k, chain_sums=None):
        h, rel = ((0, 1), (1, 0))[k]
        axis, to = (("dp", y_to), ("row", x_to))[k]
        at = columns(m, ("row", "dp")[k])
        if m == CHAIN:
            src, dst = chain_sums.at[h * 2 + rel, :, at], chain_land3.at[:, at]
        else:
            src, dst = total_of(m, h, rel).at[:, at], land3_hbm.at[m, :, at]
        return send(src, dst, three_sends.at[m, k], three_recv.at[m, k], axis, to)

    def kept_copy(m):
        return pltpu.make_async_copy(total_of(m, 0, 0), kept_hbm.at[m], kept_sems.at[m])

    def stage(m, i):
        return pltpu.make_async_copy(land2_hbm.at[m * 2 + i], gots.at[i], stage_sem.at[m, i])

    def second_stage(m, now=(0, 1)):
        for k in range(4):
            two_copy(m, k).wait_recv()
        for i in (1, 0):
            stage(m, i).start()
        stage(m, 1).wait()
        add_into(total_of(m, 0, 1), gots.at[1], columns(m, "row"))
        if 0 in now:
            three_copy(m, 0).start()
        add_into(total_of(m, 1, 0), gots.at[1], columns(m, "dp"))
        if 1 in now:
            three_copy(m, 1).start()
        stage(m, 0).wait()
        add_into(total_of(m, 0, 0), gots.at[0], pl.ds(0, hidden))
        kept_copy(m).start()

    barrier = pltpu.get_barrier_semaphore()
    group_size = 8
    own = r * 4 + d

    def member(i):
        index = lax.rem(own + i, group_size)
        return {"row": index // 4, "dp": lax.rem(index, 4)}

    for i in range(1, group_size):
        pl.semaphore_signal(barrier, 1, device_id=member(i), device_id_type=MESH_ID)
    for s in range(1, LINE):
        pl.semaphore_signal(
            barrier, 1, device_id={"col": lax.rem(me + s, LINE)}, device_id_type=MESH_ID
        )

    cot_gather = Gather(me, cot_ref, c_sends, c_recv)
    out_scatter = Scatter(
        me, lambda j: out_part_ref[block_rows(j)].astype(F32), out_landing, o_sends, o_recv
    )

    def feed(weights, gates, total, normed_two_ref):
        tiles = hidden // TILE
        rest = hidden % TILE

        def loads(t, slot, size):
            rows = aligned(t * TILE, size, TILE)
            for m in range(3):
                for i, src in enumerate((owns[m].at[rows], other_hbm.at[m, rows])):
                    yield pltpu.make_async_copy(
                        src,
                        weights.at[slot, m, pl.ds(0, size), pl.ds(i * HALF, HALF)],
                        w_sems.at[slot, m, i],
                    )

        def start(t, slot, size):
            for copy in loads(t, slot, size):
                copy.start()

        def ready(t, slot, size):
            for copy in loads(t, slot, size):
                copy.wait()

        def sweep(body, first_slot, hooks, again):
            @pl.loop(0, tiles)
            def _(t):
                slot = lax.rem(t + first_slot, 2)
                ready(t, slot, TILE)

                @pl.when(t < tiles - 1)
                def _():
                    start(t + 1, 1 - slot, TILE)

                @pl.when(t == tiles - 1)
                def _():
                    start(tiles, 1 - slot, rest)

                body(aligned(t * TILE, TILE), slot, TILE)
                for at, hook in hooks:
                    pl.when(t == at)(hook)

            slot = (tiles + first_slot) % 2
            ready(tiles, slot, rest)
            if again:
                start(0, 1 - slot, TILE)
            body(pl.ds(tiles * TILE, rest), slot, rest)

        def add_products(slot, size, factors, cols):
            width = 768

            @pl.loop(0, MODEL_WIDTH // width)
            def _(i):
                at = aligned(i * width, width)
                left = jnp.concatenate([factor[:, cols] for factor, _ in factors], 1)
                right = jnp.concatenate(
                    [weights[slot, m, pl.ds(0, size), at] for _, m in factors], 0
                )
                total[:, at] += dot(left, right)

        def forward(cols, slot, size):
            here = pl.ds(0, size)
            gate = dot(normed_two_ref[...], weights[slot, 0, here], PAIR_COLS)
            upper = dot(normed_two_ref[...], weights[slot, 1, here], PAIR_COLS)
            activated = (gate * jax.nn.sigmoid(gate) * upper).astype(BF16)
            gates[0, :, cols] = gate.astype(BF16)
            gates[1, :, cols] = upper.astype(BF16)
            activated_ref[:, cols] = activated
            total[...] += dot(activated, weights[slot, 2, here])

        def backward(cols, slot, size):
            here = pl.ds(0, size)
            act_grad = dot(cot_ref[...], weights[slot, 2, here], PAIR_COLS)
            gate, upper = gates[0, :, cols].astype(F32), gates[1, :, cols].astype(F32)
            sig = jax.nn.sigmoid(gate)
            gate_grad = (act_grad * upper * sig * (1.0 + gate * (1.0 - sig))).astype(BF16)
            upper_grad = (act_grad * gate * sig).astype(BF16)
            gate_grad_ref[:, cols] = gate_grad
            upper_grad_ref[:, cols] = upper_grad
            add_products(slot, size, ((gate_grad_ref, 0), (upper_grad_ref, 1)), cols)

        load = pltpu.make_async_copy(normed_two_hbm, normed_two_ref, load_sems.at[15])
        load.start()
        start(0, 0, TILE)
        total[...] = jnp.zeros_like(total)
        pl.semaphore_wait(barrier, group_size - 1 + LINE - 1)
        cot_loads(lambda copy: copy.wait())
        cot_gather.step(1, wait=False)
        load.wait()
        turned_load.wait()
        sweep(forward, 0, [(4, lambda: cot_gather.step(2))], True)
        out_part_ref[...] = total[...].astype(BF16)
        out_scatter.step(3)
        cot_gather.step(3)
        turned_ref[0] = cot_ref[...].T
        total[...] = jnp.zeros_like(total)
        compute(0)
        compute(1)
        hooks = [
            (0, lambda: combine(0)), (1, lambda: combine(1)), (4, lambda: out_scatter.step(2)),
        ]
        sweep(backward, (tiles + 1) % 2, hooks, False)
        back_part_ref[...] = total[...].astype(BF16)
        cot_gather.drain(1, LINE - 1)

    pl.run_scoped(
        feed,
        pltpu.VMEM((2, 3, TILE, MODEL_WIDTH), BF16),
        pltpu.VMEM((2, LOCAL, hidden), BF16),
        pltpu.VMEM((LOCAL, MODEL_WIDTH), F32),
        pltpu.VMEM((LOCAL, MODEL_WIDTH), BF16),
    )

    def rest(
        proj_ref, proj_other_ref, query_ref, kv_ref, kv_other_ref, attended_ref, probs_ref, cos_ref,
        sin_ref, x_ref, normed_one_ref, mid_grad_ref, own_ref, att_grad_ref,
        kv_grad_ref, kv_give_ref, proj_grad_ref, chain_sums, back_give,
    ):
        pairs = (
            (proj_hbm, proj_ref), (proj_other_hbm, proj_other_ref), (query_hbm, query_ref),
            (kv_hbm, kv_ref), (kv_other_hbm, kv_other_ref), (attended_hbm, attended_ref),
            (probs_hbm, probs_ref), (cos_hbm, cos_ref), (sin_hbm, sin_ref), (x_hbm, x_ref),
            (normed_one_hbm, normed_one_ref),
        )
        reads = [
            pltpu.make_async_copy(src, dst, load_sems.at[3 + i])
            for i, (src, dst) in enumerate(pairs)
        ]

        mid_half_ref = cot_ref

        scatter = Scatter(
            me, lambda j: back_part_ref[block_rows(j)].astype(F32), landing, r_sends, r_recv
        )
        scatter.step(3)
        for read in reads:
            read.start()
        compute(2)
        for u in (3, 4, 5):
            compute(u)
            combine(u - 1)
        scatter.step(2)
        for u in (6, 7):
            compute(u)
            combine(u - 1)
        scatter.step(1)
        for u in (8, 9):
            compute(u)
            combine(u - 1)
        scatter.finish(mid_grad_ref)
        mid, grad = mid_ref[...], mid_grad_ref[...]
        rinv = norm_scale(mid)
        small_line[me, :, MODEL_WIDTH : 2 * MODEL_WIDTH] = jnp.sum(grad * mid * rinv, 0, keepdims=True)
        scaled = grad * gains_ref[1:2]
        inner = jnp.sum(scaled * mid, -1, keepdims=True)
        mid_grad = (
            cot_ref[block_rows(me)].astype(F32)
            + rinv * scaled
            - mid * rinv**3 * inner / MODEL_WIDTH
        )
        mid_grad_ref[...] = mid_grad
        mid_half_ref[block_rows(me)] = mid_grad.astype(BF16)

        gather = Gather(me, mid_half_ref, a_sends, a_recv)
        gather.step(0)
        scatter.drain()
        for read in reads:
            read.wait()

        def each(j):
            block = mid_half_ref[block_rows(j)]
            att_grad_ref[block_rows(j)] = (
                dot(block[:, :HALF], proj_ref[:, proj_cols:])
                + dot(block[:, HALF:], proj_other_ref[:, proj_cols:])
            ).astype(BF16)

        gather.run_each(0, each)
        for u in (10, 11):
            compute(u)
            combine(u - 1)
        combine(11)
        gather.step(1)
        gather.run_each(1, each)
        second_stage(DOWN)
        gather.step(2)
        gather.run_each(2, each)
        second_stage(UPPER, (0,))
        gather.step(3)
        gather.run_each(3, each)
        out_scatter.step(1)
        attend_back_body(
            query_ref, kv_ref, kv_other_ref, attended_ref, probs_ref, att_grad_ref, cos_ref,
            sin_ref, proj_grad_ref, kv_grad_ref, kv_give_ref,
        )

        def swap_copy(i):
            src, dst = (
                (kv_give_ref, kv_got_ref),
                (back_give.at[0], got_ref.at[0]),
                (back_give.at[1], got_ref.at[1]),
            )[i]
            return send(src, dst, swap_sends.at[i], swap_recv.at[i], "row", x_to)

        swap_copy(0).start()
        swap_copy(0).wait_recv()
        kv = kv_grad_ref[...] + kv_got_ref[...].astype(F32)
        key = kv[:, :HEAD_SIZE]
        proj_grad_ref[:, query_cols : query_cols + HEAD_SIZE] = (
            key * cos_ref[...] - turn(key) * sin_ref[...]
        ).astype(BF16)
        proj_grad_ref[:, query_cols + HEAD_SIZE :] = kv[:, HEAD_SIZE:].astype(BF16)

        def block_of(j):
            block = proj_grad_ref[block_rows(j)]
            return jnp.concatenate(
                [
                    dot(block, proj_ref[:, :proj_cols], PAIR_COLS),
                    dot(block, proj_other_ref[:, :proj_cols], PAIR_COLS),
                ],
                1,
            )

        def chain_from(i):
            return gives.at[i // 2, :, pl.ds(i % 2 * chain_cols, chain_cols)]

        def chain_give(i):
            return send(
                chain_from(i), chain_gots.at[i], give_sends.at[12 + i], give_recv.at[12 + i],
                "dp", core_to,
            )

        def chain_compute(i):
            h, rel = UNITS[i]
            rows = unit_rows(h, rel)
            keep = chain_sums.at[h * 2 + rel]
            res = dot(normed_one_ref[:, rows], proj_grad_ref[...], PAIR_ROWS)
            split(res, keep, chain_from(i), pl.ds(0, proj_cols))
            res = dot(mid_half_ref[:, rows], attended_ref[...], PAIR_ROWS)
            split(res, keep, chain_from(i), pl.ds(proj_cols, query_cols))
            chain_give(i).start()

        def chain_combine(i):
            h, rel = UNITS[i]
            chain_give(i).wait_recv()
            add_into(chain_sums.at[h * 2 + rel], chain_gots.at[i], pl.ds(0, chain_cols))
            for k in {(1, 1): (1, 3), (1, 0): (0,), (0, 1): (2,), (0, 0): ()}[h, rel]:
                two_copy(CHAIN, k, chain_sums).start()

        second = Scatter(me, block_of, landing, r_sends, r_recv)
        second.step(3)
        for u in (len(order) - 2, len(order) - 1):
            give_copy(u).wait_send()
        for i in range(4):
            chain_compute(i)
        for i in range(4):
            chain_combine(i)
        three_copy(UPPER, 1).start()
        small_line[me, :, 2 * MODEL_WIDTH :] = jnp.sum(
            proj_grad_ref[...].astype(F32), 0, keepdims=True
        )
        second.step(2)
        second_stage(GATE, (0,))
        out_scatter.finish(own_ref)
        out = own_ref[...] + mid_ref[...]
        out_ref[:, block_rows(r)] = out[:, :HALF].T
        back_give[1] = out[:, HALF:].astype(BF16)
        second.step(1)
        for k in range(4):
            two_copy(CHAIN, k, chain_sums).wait_recv()
        add_into(chain_sums.at[1], chain_land2.at[1], columns(CHAIN, "row"))
        three_copy(CHAIN, 0, chain_sums).start()
        add_into(chain_sums.at[2], chain_land2.at[1], columns(CHAIN, "dp"))
        three_copy(CHAIN, 1, chain_sums).start()
        add_into(chain_sums.at[0], chain_land2.at[0], pl.ds(0, chain_cols))
        three_copy(GATE, 1).start()
        swap_copy(2).start()
        for k in range(2):
            three_copy(CHAIN, k, chain_sums).wait_recv()
        total = chain_sums[0].astype(F32) + chain_land3[...].astype(F32)
        query_w_ref[...] = total[:, :query_cols]
        output_w_ref[...] = total[:, proj_cols:]
        kv_line[me] = total[:, query_cols:proj_cols].astype(BF16)

        def kv_line_copy(s):
            to = lax.rem(me + s, LINE)
            return send(kv_line.at[me], kv_line.at[me], kv_sends.at[s], kv_recv.at[me], "col", to)

        for s in range(1, LINE):
            kv_line_copy(s).start()
        second.finish(own_ref)
        x, grad = x_ref[...].astype(F32), own_ref[...]
        rinv = norm_scale(x)
        scaled = grad * gains_ref[0:1]
        inner = jnp.sum(scaled * x, -1, keepdims=True)
        input_grad = mid_grad_ref[...] + rinv * scaled - x * rinv**3 * inner / MODEL_WIDTH
        back_give[0] = input_grad[:, HALF:].astype(BF16)
        swap_copy(1).start()
        small_line[me, :, :MODEL_WIDTH] = jnp.sum(grad * x * rinv, 0, keepdims=True)

        def small_line_copy(s):
            to = lax.rem(me + s, LINE)
            return send(
                small_line.at[me], small_line.at[me], line_sends.at[s], line_recv.at[me], "col", to
            )

        for s in range(1, LINE):
            small_line_copy(s).start()
        in_ref[:, block_rows(r)] = input_grad[:, :HALF].T

        group = LINE // KEYVALUE_HEADS
        for s in range(1, LINE):
            landed(kv_line.at[me], kv_recv.at[lax.rem(me + s, LINE)])
        dp_rows = aligned(d * UNIT, UNIT, UNIT)
        for h in range(KEYVALUE_HEADS):
            pair = kv_line[h * group].astype(F32)
            for i in range(1, group):
                pair = pair + kv_line[h * group + i].astype(F32)
            for i in range(2):
                at = (i * KEYVALUE_HEADS + h) * HEAD_SIZE
                kv_all_ref[dp_rows, at : at + HEAD_SIZE] = pair[
                    :, i * HEAD_SIZE : (i + 1) * HEAD_SIZE
                ].astype(BF16)

        def kv_rows(of):
            return kv_all_ref.at[aligned(of * UNIT, UNIT, UNIT)]

        def kv_dp_copy(i):
            rows = kv_rows(y_to if i == 2 else d)
            to = y_to if i == 1 else core_to
            return send(rows, rows, kvd_sends.at[i], kvd_recv.at[i], "dp", to)

        kv_dp_copy(1).start()
        kv_dp_copy(0).start()

        for s in range(1, LINE):
            landed(small_line.at[me], line_recv.at[lax.rem(me + s, LINE)])
        lines = [small_line[j] for j in range(LINE)]
        total_line = lines[0] + lines[1] + lines[2] + lines[3]
        small_swap[...] = jnp.zeros_like(small_swap)
        small_swap[0:1] = total_line[:, :MODEL_WIDTH]
        small_swap[1:2] = total_line[:, MODEL_WIDTH : 2 * MODEL_WIDTH]
        bias_at = 2 * MODEL_WIDTH
        small_swap[2:3, :query_cols] = small_line[me, :, bias_at : bias_at + query_cols]
        for i in range(2):
            for h in range(KEYVALUE_HEADS):
                at = bias_at + query_cols + i * HEAD_SIZE
                part = lines[h * group][:, at : at + HEAD_SIZE]
                for j in range(1, group):
                    part = part + lines[h * group + j][:, at : at + HEAD_SIZE]
                at = (i * KEYVALUE_HEADS + h) * HEAD_SIZE
                small_swap[3:4, at : at + HEAD_SIZE] = part

        small_give[0] = small_swap[:, :HALF]
        small_give[1, :2] = small_swap[:2, HALF:]
        small_give[1, 2:] = small_swap[2:, :HALF]
        small_group[own] = small_give[0]

        def small_copy(i):
            to = member(i)
            kind = jnp.where(to["row"] == r, 0, 1)
            return pltpu.make_async_remote_copy(
                small_give.at[kind], small_group.at[own], small_sends.at[i], small_recv.at[own],
                device_id=to, device_id_type=MESH_ID,
            )

        for i in range(1, group_size):
            small_copy(i).start()
        landed(kv_rows(y_to), kvd_recv.at[1])
        kv_dp_copy(2).start()
        for i in (2, 1):
            swap_copy(i).wait_recv()
            to_ref = (in_ref, out_ref)[i - 1]
            to_ref[:, block_rows(1 - r)] = got_ref[i - 1].astype(F32).T
        for i in range(1, group_size):
            source = lax.rem(own + i, group_size)
            landed(small_group.at[source], small_recv.at[source])
        small_ref[...] = sum(small_group[i] for i in range(group_size))

        landed(kv_rows(core_to), kvd_recv.at[0])
        landed(kv_rows(diagonal_to), kvd_recv.at[2])
        for m in (DOWN, GATE, UPPER):
            for k in range(2):
                three_copy(m, k).wait_recv()
                three_copy(m, k).wait_send()
            kept_copy(m).wait()
            for k in range(4):
                two_copy(m, k).wait_send()
        for i in range(4):
            chain_give(i).wait_send()
            two_copy(CHAIN, i, chain_sums).wait_send()
        for k in range(2):
            three_copy(CHAIN, k, chain_sums).wait_send()
        for i in range(3):
            swap_copy(i).wait_send()
            kv_dp_copy(i).wait_send()
            kv_line_copy(1 + i).wait_send()
            small_line_copy(1 + i).wait_send()
        for i in range(1, group_size):
            small_copy(i).wait_send()
        gather.drain()
        out_scatter.drain()
        second.drain()

    wide = (HALF, chain_cols)
    pl.run_scoped(
        rest,
        pltpu.VMEM(wide, BF16),
        pltpu.VMEM(wide, BF16),
        pltpu.VMEM((LOCAL, query_cols), BF16),
        pltpu.VMEM((LOCAL, 2 * HEAD_SIZE), BF16),
        pltpu.VMEM((LOCAL, 2 * HEAD_SIZE), BF16),
        pltpu.VMEM((LOCAL, query_cols), BF16),
        pltpu.VMEM(probs_hbm.shape, BF16),
        pltpu.VMEM((LOCAL, HEAD_SIZE), F32),
        pltpu.VMEM((LOCAL, HEAD_SIZE), F32),
        pltpu.VMEM((BLOCK, MODEL_WIDTH), BF16),
        pltpu.VMEM((LOCAL, MODEL_WIDTH), BF16),
        pltpu.VMEM((BLOCK, MODEL_WIDTH), F32),
        pltpu.VMEM((BLOCK, MODEL_WIDTH), F32),
        pltpu.VMEM((LOCAL, query_cols), BF16),
        pltpu.VMEM((LOCAL, 2 * HEAD_SIZE), F32),
        pltpu.VMEM((LOCAL, 2 * HEAD_SIZE), BF16),
        pltpu.VMEM((LOCAL, proj_cols), BF16),
        pltpu.VMEM((4, UNIT, chain_cols), BF16),
        pltpu.VMEM((2, BLOCK, HALF), BF16),
    )


def rear_call(hidden, proj_cols, query_cols, *args):
    chain_cols = proj_cols + query_cols
    outs = [
        shape(HALF, 2 * BLOCK, F32),
        shape(HALF, 2 * BLOCK, F32),
        shape(8, HALF, F32),
        shape(UNIT, query_cols, F32),
        shape(UNIT, query_cols, F32),
        shape(4 * UNIT, 2 * KEYVALUE_HEADS * HEAD_SIZE),
        jax.ShapeDtypeStruct((3, UNIT, hidden), BF16),
        jax.ShapeDtypeStruct((6, UNIT, hidden), BF16),
        jax.ShapeDtypeStruct((3, UNIT, hidden), BF16),
    ]
    local = (LOCAL, MODEL_WIDTH)
    line = (2, LINE, BLOCK, MODEL_WIDTH)
    return pl.pallas_call(
        rear_body,
        out_shape=outs,
        in_specs=[VMEM_SPEC] * 2 + [ANY_SPEC] * (len(args) - 2),
        out_specs=[VMEM_SPEC] * 6 + [ANY_SPEC] * 3,
        scratch_shapes=[
            pltpu.VMEM(local, BF16),
            pltpu.VMEM((LOCAL, hidden), BF16),
            pltpu.VMEM((LOCAL, hidden), BF16),
            pltpu.VMEM((LOCAL, hidden), BF16),
            pltpu.VMEM(local, BF16),
            pltpu.VMEM(local, BF16),
            pltpu.VMEM((2, MODEL_WIDTH, LOCAL), BF16),
            pltpu.VMEM((LOCAL, 2 * HEAD_SIZE), BF16),
            pltpu.VMEM((2, BLOCK, HALF), BF16),
            pltpu.VMEM(line, BF16),
            pltpu.VMEM(line, BF16),
            pltpu.VMEM((12, UNIT, hidden), BF16),
            pltpu.VMEM((2, UNIT, hidden), BF16),
            pltpu.VMEM((3, UNIT, hidden), BF16),
            pltpu.VMEM((4, UNIT, chain_cols), BF16),
            pltpu.VMEM((2, UNIT, chain_cols), BF16),
            pltpu.VMEM((UNIT, chain_cols), BF16),
            pltpu.VMEM((LINE, UNIT, 2 * HEAD_SIZE), BF16),
            pltpu.VMEM((LINE, 1, 2 * MODEL_WIDTH + proj_cols), F32),
            pltpu.VMEM((8, MODEL_WIDTH), F32),
            pltpu.VMEM((2, 8, HALF), F32),
            pltpu.VMEM((8, 8, HALF), F32),
            DMA((16,)),
            DMA((2, 3, 2)),
        ]
        + gather_sems()
        + scatter_sems()
        + scatter_sems()
        + gather_sems()
        + [
            DMA((16,)), DMA((16,)),
            DMA((4, 4)), DMA((4, 4)),
            DMA((4, 2)), DMA((4, 2)),
            DMA((3, 2)), DMA((3,)),
            DMA((3,)), DMA((3,)),
            DMA((LINE,)), DMA((LINE,)),
            DMA((3,)), DMA((3,)),
            DMA((LINE,)), DMA((LINE,)),
            DMA((8,)), DMA((8,)),
            pltpu.SemaphoreType.REGULAR,
        ],
        compiler_params=pltpu.CompilerParams(
            collective_id=2, has_side_effects=True, vmem_limit_bytes=67_043_328
        ),
        cost_estimate=pl.CostEstimate(
            flops=4 * 10**10, bytes_accessed=80_000_000, transcendentals=0
        ),
        name="rear",
    )(*args)


def finish_body(
    out_hbm, in_hbm, query_hbm, output_hbm, kv_hbm, kept_hbm, landing_hbm, small_ref,
    out_to, in_to, query_to, output_to, kv_to, down_to, gate_to, upper_to,
    attention_gain_to, feedforward_gain_to, query_bias_to, kv_bias_to,
    out_ref, in_ref, query_ref, output_ref, kv_ref, kv_wide, kept, landing, wide, load_sems, store_sems,
):
    passed = (
        (out_hbm, out_ref, out_to), (in_hbm, in_ref, in_to), (query_hbm, query_ref, query_to),
        (output_hbm, output_ref, output_to),
    )
    sums = (down_to, gate_to, upper_to)
    loads = []
    for m in range(3):
        loads.append(pltpu.make_async_copy(kept_hbm.at[m], kept.at[m], load_sems.at[2 * m]))
        loads.append(pltpu.make_async_copy(landing_hbm.at[m], landing.at[m], load_sems.at[2 * m + 1]))
    loads.append(pltpu.make_async_copy(kv_hbm, kv_ref, load_sems.at[6]))
    for i, (src, here, _) in enumerate(passed):
        loads.append(pltpu.make_async_copy(src, here, load_sems.at[7 + i]))
    stores = [pltpu.make_async_copy(wide.at[m], sums[m], store_sems.at[m]) for m in range(3)]
    stores.append(pltpu.make_async_copy(kv_wide, kv_to, store_sems.at[3]))
    for i, (_, here, to) in enumerate(passed):
        stores.append(pltpu.make_async_copy(here, to, store_sems.at[4 + i]))
    for load in loads:
        load.start()
    for m in range(3):
        loads[2 * m].wait()
        loads[2 * m + 1].wait()

        @pl.loop(0, UNIT // 32)
        def _(i):
            at = aligned(i * 32, 32, 32)
            wide[m, at] = kept[m, at].astype(F32) + landing[m, at].astype(F32)

        stores[m].start()
    loads[6].wait()
    kv_wide[...] = kv_ref[...].astype(F32)
    stores[3].start()
    for i in range(4):
        loads[7 + i].wait()
        stores[4 + i].start()
    attention_gain_to[...] = small_ref[0]
    feedforward_gain_to[...] = small_ref[1]
    rows = query_bias_to.shape[0]
    for i in range(4):

        @pl.when(lax.axis_index("dp") == i)
        def _():
            query_bias_to[...] = small_ref[2, i * rows : (i + 1) * rows]

    kv_bias_to[...] = small_ref[3, : kv_bias_to.shape[0]]
    for store in stores:
        store.wait()


def finish_call(out, input_grad, query_sum, output_sum, kv_all, kept, landing, sums):
    like = lambda v, dtype: jax.ShapeDtypeStruct(v.shape, dtype)
    unit = jax.ShapeDtypeStruct(kept.shape[1:], F32)
    vector = lambda n: jax.ShapeDtypeStruct((n,), F32)
    passed = [like(v, F32) for v in (out, input_grad, query_sum, output_sum)]
    outs = passed + [like(kv_all, F32)] + [unit] * 3
    small = [vector(HALF), vector(HALF), vector(query_sum.shape[1] // 4), vector(kv_all.shape[1])]
    return pl.pallas_call(
        finish_body,
        out_shape=outs + small,
        in_specs=[ANY_SPEC] * 7 + [VMEM_SPEC],
        out_specs=[ANY_SPEC] * 8 + [VMEM_SPEC] * 4,
        scratch_shapes=[pltpu.VMEM(v.shape, F32) for v in passed]
        + [
            pltpu.VMEM(kv_all.shape, BF16),
            pltpu.VMEM(kv_all.shape, F32),
            pltpu.VMEM(kept.shape, BF16),
            pltpu.VMEM(kept.shape, BF16),
            pltpu.VMEM(kept.shape, F32),
            DMA((11,)),
            DMA((8,)),
        ],
        compiler_params=pltpu.CompilerParams(vmem_limit_bytes=67_043_328),
        name="finish",
    )(out, input_grad, query_sum, output_sum, kv_all, kept, landing, sums)


def fast_device(
    block_input,
    position_ids,
    attention_gain,
    query_weight,
    query_bias,
    key_value_weight,
    key_value_bias,
    output_weight,
    feedforward_gain,
    gate_weight,
    upper_weight,
    down_weight,
    out_cotangent,
):
    query_cols = query_weight.shape[1]
    hidden = gate_weight.shape[1]
    proj_cols = query_cols + 2 * HEAD_SIZE
    frequencies = THETA ** (-(jnp.arange(HEAD_SIZE // 2, dtype=F32) * 2.0 / HEAD_SIZE))
    angles = position_ids.astype(F32)[:, None] * frequencies[None, :]
    table = jnp.concatenate([jnp.cos(angles), jnp.sin(angles)], -1)
    gate_t, upper_t, down_t = gate_weight.T, upper_weight.T, down_weight.T
    (
        x_own, normed_one, query_rot, kv_own, kv_other, cosine, sine, gains, attended, probs,
        mid, normed_two, normed_turned, cot_part, own_proj, other_proj, other_weights,
    ) = front_call(
        proj_cols, query_cols, hidden,
        block_input, out_cotangent, table, attention_gain, feedforward_gain, query_bias,
        key_value_bias, query_weight, key_value_weight, output_weight,
        gate_t, upper_t, down_t,
    )
    out, input_grad, sums, query_sum, output_sum, kv_all, kept, _, landing = rear_call(
        hidden, proj_cols, query_cols,
        mid, gains,
        normed_two, normed_turned, cot_part, gate_t, upper_t, down_t, other_weights, own_proj, other_proj, query_rot, kv_own,
        kv_other, attended, probs, cosine, sine, x_own, normed_one,
    )
    (
        out, input_grad, query_sum, output_sum, kv_sum, down_sum, gate_sum, upper_sum,
        attention_gain_sum, feedforward_gain_sum, query_bias_sum, kv_bias_sum,
    ) = finish_call(out, input_grad, query_sum, output_sum, kv_all, kept, landing, sums)
    return (
        out,
        input_grad,
        attention_gain_sum,
        query_sum,
        query_bias_sum,
        kv_sum,
        kv_bias_sum,
        output_sum,
        feedforward_gain_sum,
        gate_sum,
        upper_sum,
        down_sum,
    )


def per_device(*arrays):
    sizes = tuple(lax.axis_size(axis) for axis in ("dp", "row", "col"))
    if sizes == (4, 2, LINE) and arrays[0].shape == (HALF, 2 * BLOCK):
        return fast_device(*arrays)
    return general_device(*arrays)


def solution(mesh):
    placed = (
        P("row", ("dp", "col")),
        P(("dp", "row")),
        P("row"),
        P("row", "col"),
        P("col"),
        P("row", None),
        P(),
        P("row", "col"),
        P("row"),
        P("row", "col"),
        P("row", "col"),
        P("row", "col"),
        P("row", ("dp", "col")),
    )
    return jax.shard_map(
        per_device,
        mesh=mesh,
        in_specs=placed,
        out_specs=(
            P("row", ("dp", "col")),
            P("row", ("dp", "col")),
            P("row"),
            P(("row", "dp"), "col"),
            P(("col", "dp")),
            P("row", None),
            P(),
            P(("row", "dp"), "col"),
            P("row"),
            P(("row", "dp"), "col"),
            P(("row", "dp"), "col"),
            P(("row", "dp"), "col"),
        ),
        check_vma=False,
    )
```
